32 devices in a mesh: shard: 4 (over y, core), ctx: 2 (over x), tp: 4 (over z).
Axes of the slice: x: 2, y: 2, z: 4, core: 2. Of those that a mesh axis runs over, the one named last changes fastest.
Arguments:
- block_input: bfloat16 [1024, 2048], P(('shard', 'ctx')), may hold values from -6 to 6
- norm1_gain: bfloat16 [2048], P('shard'), may hold values from 0.5 to 1.5
- q_weight: bfloat16 [2048, 3072], P('shard', 'tp'), may hold values from -0.15467961 to 0.15467961
- kva_weight: bfloat16 [2048, 576], P('shard'), may hold values from -0.15467961 to 0.15467961
- kv_norm_gain: bfloat16 [512], P('shard'), may hold values from 0.5 to 1.5
- kvb_weight: bfloat16 [512, 4096], P('shard', 'tp'), may hold values from -0.30935922 to 0.30935922
- out_weight: bfloat16 [2048, 2048], P('tp', 'shard'), may hold values from -0.75 to 0.75
- norm2_gain: bfloat16 [2048], P('shard'), may hold values from 0.5 to 1.5
- router_weight: bfloat16 [2048, 16], P('shard'), may hold values from -0.92807765 to 0.92807765
- shared_gate: bfloat16 [2048, 2816], P('shard', 'tp'), may hold values from -0.125 to 0.125
- shared_up: bfloat16 [2048, 2816], P('shard', 'tp'), may hold values from -0.125 to 0.125
- shared_down: bfloat16 [2816, 2048], P('tp', 'shard'), may hold values from -0.109375 to 0.109375
- expert_gate: bfloat16 [16, 2048, 1408], P(('shard', 'ctx'), None, 'tp'), may hold values from -0.125 to 0.125
- expert_up: bfloat16 [16, 2048, 1408], P(('shard', 'ctx'), None, 'tp'), may hold values from -0.125 to 0.125
- expert_down: bfloat16 [16, 1408, 2048], P(('shard', 'ctx'), 'tp'), may hold values from -0.15625 to 0.15625
- routes: int32 [1024, 6], P(('shard', 'ctx')), may hold values from 0 to 15, all different within a row; in each aligned block of 128 rows (0 to 127, 128 to 255, ...) at most 96 rows name the same one
- cotangent: float32 [1024, 2048], P(('shard', 'ctx')), may hold values from -6 to 6
Outputs:
- block_output: float32 [1024, 2048], P(('shard', 'ctx'))
- input_grad: float32 [1024, 2048], P(('shard', 'ctx'))
- grad_norm1: float32 [2048], P('shard')
- grad_query_w: float32 [2048, 3072], P('shard', 'tp')
- grad_latent_w: float32 [2048, 576], P('shard')
- grad_kv_norm: float32 [512], P('shard')
- grad_expand_w: float32 [512, 4096], P('shard', 'tp')
- grad_out_w: float32 [2048, 2048], P('tp', 'shard')
- grad_norm2: float32 [2048], P('shard')
- grad_router: float32 [2048, 16], P('shard')
- grad_shared_gate: float32 [2048, 2816], P('shard', 'tp')
- grad_shared_up: float32 [2048, 2816], P('shard', 'tp')
- grad_shared_down: float32 [2816, 2048], P('tp', 'shard')
- grad_expert_gate: float32 [16, 2048, 1408], P(('shard', 'ctx'), None, 'tp')
- grad_expert_up: float32 [16, 2048, 1408], P(('shard', 'ctx'), None, 'tp')
- grad_expert_down: float32 [16, 1408, 2048], P(('shard', 'ctx'), 'tp')
The draws below stay inside these ranges and needn't reach their ends.
Inputs may be any that keep to these rules, and one draw needn't show every extreme that they name: `routes`: in the rows of one device (aligned blocks of 128 rows) each row names 6 different experts, and no expert is named by more than 96 rows of a block; some expert is named by exactly 96 rows.
All inputs are finite; a program needn't handle non-finite values.
Results may differ from the reference program's by a relative error of at most 0.04.
Values may be sent and summed in bfloat16 or wider, within the bound.
A program may use at most 256 MiB of HBM per device.

```python
import math
import jax
import jax.numpy as jnp
import numpy as np
from jax import lax

D = 2048
H = 16
DN = 128
DR = 64
DV = 128
KVR = 512
FE = 1408
FS = 2816
TOPK = 6
BLK = 128
E = 16
L = 256
TOKENS = 1024
CAP = 96
N_CTX = 2


TARGET_SCORE = 320.0


PLANT_ROWS = 8


def common_signs(key, salt, length):
    coin_flips = jax.random.randint(jax.random.fold_in(key, salt), (length,), 0, 2)
    return coin_flips.astype(jnp.float32) * 2.0 - 1.0


def plant_factor():
    product = TARGET_SCORE * math.sqrt(DN + DR) / (DN * math.sqrt(D) * math.sqrt(KVR))
    return math.sqrt(min(product, 0.16))


def draw_block_input(key, part):
    signs = common_signs(key, 7001, D)
    noise_key = jax.random.fold_in(key, 7101)
    noise = jnp.clip(jax.random.normal(noise_key, (TOKENS, D), jnp.float32), -6.0, 6.0)
    lead_drop = 0.35
    token_index = jnp.arange(TOKENS, dtype=jnp.int32)
    position = token_index % L
    sequence = token_index // L
    spacing = max(L // PLANT_ROWS, 1)
    plant_slot = jnp.minimum(position // spacing, PLANT_ROWS - 1)
    offsets = jax.random.randint(jax.random.fold_in(key, 7103), (TOKENS // L, PLANT_ROWS), 0, spacing)
    chosen = (position % spacing == offsets[sequence, plant_slot]) & (position // spacing < PLANT_ROWS)
    lead = 1.0 - lead_drop * (sequence % 4).astype(jnp.float32) / 3.0
    along = lead * (1.0 - 0.006 * plant_slot.astype(jnp.float32))
    across = jnp.sqrt(1.0 - along * along)
    planted = along[:, None] * signs[None, :] + across[:, None] * noise
    result = jnp.where(chosen[:, None], planted, noise)
    return jnp.clip(result, -6.0, 6.0).astype(jnp.bfloat16)


def draw_q_weight(key, part):
    signs = common_signs(key, 7001, D)
    head_width = DN + DR
    column = jnp.arange(H * head_width, dtype=jnp.int32) % head_width
    keyed = (column < DN).astype(jnp.float32)
    noise = jnp.clip(jax.random.normal(jax.random.fold_in(key, 7201), (D, H * head_width), jnp.float32), -6.0, 6.0)
    return ((noise + plant_factor() * signs[:, None] * keyed[None, :]) * D ** (-0.5)).astype(jnp.bfloat16)


def draw_kva_weight(key, part):
    signs = common_signs(key, 7001, D)
    latent_signs = common_signs(key, 7002, KVR)
    pattern = jnp.concatenate([latent_signs, jnp.zeros((DR,), jnp.float32)])
    noise = jnp.clip(jax.random.normal(jax.random.fold_in(key, 7202), (D, KVR + DR), jnp.float32), -6.0, 6.0)
    return ((noise + plant_factor() * signs[:, None] * pattern[None, :]) * D ** (-0.5)).astype(jnp.bfloat16)


def draw_kvb_weight(key, part):
    latent_signs = common_signs(key, 7002, KVR)
    head_width = DN + DV
    column = jnp.arange(H * head_width, dtype=jnp.int32) % head_width
    keyed = (column < DN).astype(jnp.float32)
    noise = jnp.clip(jax.random.normal(jax.random.fold_in(key, 7203), (KVR, H * head_width), jnp.float32), -6.0, 6.0)
    return ((noise + plant_factor() * latent_signs[:, None] * keyed[None, :]) * KVR ** (-0.5)).astype(jnp.bfloat16)


def draw_router_weight(key, part):
    noise_key = jax.random.fold_in(key, 7301)
    noise = jnp.clip(jax.random.normal(noise_key, (D, E), jnp.float32), -6.0, 6.0)
    result = noise * D ** (-0.5)
    return result.astype(jnp.bfloat16)


def levels(key, shape, shards, smallest, top_value):
    def one(axis_at, blocks):
        steps = jax.random.uniform(jax.random.fold_in(jax.random.fold_in(key, 6), axis_at), (blocks,), jnp.float32, smallest / len(shards), top_value / len(shards))
        return jnp.repeat(jnp.exp(steps), shape[axis_at] // blocks).reshape((-1,) + (1,) * (len(shape) - axis_at - 1))

    level = one(*shards[0])
    for cut in shards[1:]:
        level = level * one(*cut)
    return level


def assign_block(rng, own, number, rows, count, top, most, lean):
    order = jax.random.permutation(rng, count)
    crowded, usual = portions_of(count, rows * top, most, lean, True), portions_of(count, rows * top, most, lean, False)
    places = jnp.arange(count)

    def named(tallies, turn):
        used = int((tallies > 0).sum())
        fixed = max(1, used // 4)
        passed = fixed + (places - fixed + turn * (used - fixed)) % max(1, count - fixed)
        return jnp.zeros((count,), jnp.int32).at[order[jnp.where(places < fixed, places, passed)]].set(jnp.asarray(tallies, jnp.int32))

    tallies = jnp.where(number % 4 == 0, named(crowded, number // 4), named(usual, number - number // 4 - 1))
    mixed = jax.random.permutation(jax.random.fold_in(own, 3), count)
    source_of, receiver = mixed[0:count // 2 * 2:2], mixed[1:count // 2 * 2:2]
    margin = jnp.minimum(tallies[source_of] - 1, most - tallies[receiver]) // 2
    margin = jnp.where((source_of == order[0]) | (receiver == order[0]) | (tallies[receiver] == 0), 0, jnp.maximum(margin, 0))
    passed = jax.random.randint(jax.random.fold_in(own, 4), (count // 2,), 0, 1 << 20) % (margin + 1)
    tallies = tallies.at[source_of].add(-passed).at[receiver].add(passed)
    items = jnp.searchsorted(jnp.cumsum(tallies), jnp.arange(rows * top), side="right").astype(jnp.int32)
    table = items.reshape(top, rows).T
    table = table[jax.random.permutation(jax.random.fold_in(own, 1), rows)]
    turn = jax.random.randint(jax.random.fold_in(own, 2), (rows, 1), 0, top)
    return jnp.take_along_axis(table, (jnp.arange(top)[None, :] + turn) % top, axis=1)


def portions_of(number_of, total, most, slope, full):
    weights = [(1 << 20) // math.isqrt(grade ** slope) + 1 for grade in range(1, number_of + 1)]
    largest = most if full else min(most, max(-(-total // number_of), total * weights[0] // sum(weights)))
    least = 1 if total - largest >= number_of - 1 else 0
    given, spare = [largest] + [least] * (number_of - 1), total - largest - least * (number_of - 1)
    while spare > 0:
        movable = [i for i in range(1, number_of) if given[i] < largest] or [i for i in range(1, number_of) if given[i] < most]
        whole, budget = sum([weights[i] for i in movable]), spare
        for i in movable:
            more = min(most - given[i], max(1, budget * weights[i] // whole), spare)
            given[i] = given[i] + more
            spare = spare - more
    return np.array(given)


def bell_draw(stream_key, shape, width, limit, pieces=(), kind=jnp.bfloat16):
    drawn = jax.random.normal(stream_key, shape, jnp.float32) * width
    if len(pieces) > 0:
        drawn = levels(stream_key, shape, pieces, -0.22, 0.18) * drawn
    return jnp.clip(drawn, min=-limit, max=limit).astype(kind)


def setup_inputs(seed: int = 0) -> dict:
    splits = jax.random.split(jax.random.key(seed), 18)
    block_input = draw_block_input(jax.random.fold_in(splits[17], 71), 0)
    norm1_gain = jnp.clip(1.0 + 0.1 * jax.random.normal(splits[1], (D,), jnp.float32), 0.5, 1.5).astype(jnp.bfloat16)
    q_weight = draw_q_weight(jax.random.fold_in(splits[17], 71), 0)
    kva_weight = draw_kva_weight(jax.random.fold_in(splits[17], 71), 0)
    kv_norm_gain = jnp.clip(1.0 + 0.1 * jax.random.normal(splits[4], (KVR,), jnp.float32), 0.5, 1.5).astype(jnp.bfloat16)
    kvb_weight = draw_kvb_weight(jax.random.fold_in(splits[17], 71), 0)
    out_weight = bell_draw(splits[6], (H * DV, D), (max(1, H * DV * 8 // L)) ** -0.5, 0.75, ((0, 4), (1, 4)))
    norm2_gain = jnp.clip(1.0 + 0.1 * jax.random.normal(splits[7], (D,), jnp.float32), 0.5, 1.5).astype(jnp.bfloat16)
    router_weight = draw_router_weight(jax.random.fold_in(splits[17], 71), 0)
    shared_gate = bell_draw(splits[9], (D, FS), D ** -0.5, 0.125, ((0, 4), (1, 4)))
    shared_up = bell_draw(splits[10], (D, FS), D ** -0.5, 0.125, ((0, 4), (1, 4)))
    shared_down = bell_draw(splits[11], (FS, D), FS ** -0.5, 0.109375, ((0, 4), (1, 4)))
    expert_gate = bell_draw(splits[12], (E, D, FE), D ** -0.5, 0.125, ((0, 8), (2, 4)))
    expert_up = bell_draw(splits[13], (E, D, FE), D ** -0.5, 0.125, ((0, 8), (2, 4)))
    expert_down = bell_draw(splits[14], (E, FE, D), FE ** -0.5, 0.15625, ((0, 8), (1, 4)))
    routes_keys = jax.random.split(jax.random.fold_in(splits[15], 1), TOKENS // BLK)
    routes_turns = jax.random.permutation(jax.random.fold_in(splits[15], 3), TOKENS // BLK)
    routes = jax.vmap(lambda own, number: assign_block(jax.random.fold_in(splits[15], 2), own, number, BLK, E, TOPK, CAP, 2))(routes_keys, routes_turns).reshape((TOKENS, TOPK))
    cotangent = bell_draw(splits[16], (TOKENS, D), 1.0, 6.0, ((0, 8),), jnp.float32)
    return dict(block_input=block_input, norm1_gain=norm1_gain, q_weight=q_weight, kva_weight=kva_weight, kv_norm_gain=kv_norm_gain, kvb_weight=kvb_weight, out_weight=out_weight, norm2_gain=norm2_gain, router_weight=router_weight, shared_gate=shared_gate, shared_up=shared_up, shared_down=shared_down, expert_gate=expert_gate, expert_up=expert_up, expert_down=expert_down, routes=routes, cotangent=cotangent)


EPS = 1e-06
NEG = -1e+30

def norm_rows(value, gain):
    factor = lax.rsqrt(lax.optimization_barrier(jnp.mean(value * value, axis=-1, keepdims=True)) + EPS)
    return value * factor * gain.astype(jnp.float32)

def rope_tables(count, offset):
    half_size = DR // 2
    position = jnp.arange(count, dtype=jnp.float32) + offset
    freqs = 10000.0 ** (-(jnp.arange(half_size, dtype=jnp.float32) * 2.0 / DR))
    angle = position[:, None] * freqs[None, :]
    return (jnp.cos(angle), jnp.sin(angle))

def rotate(value, cosine, sine_table):
    half_size = DR // 2
    first = value[..., :half_size]
    second = value[..., half_size:]
    return jnp.concatenate([first * cosine - second * sine_table, first * sine_table + second * cosine], axis=-1)

def rotate_back(grad, cosine, sine_table):
    half_size = DR // 2
    first = grad[..., :half_size]
    second = grad[..., half_size:]
    return jnp.concatenate([first * cosine + second * sine_table, second * cosine - first * sine_table], axis=-1)

def silu_slope(value):
    sigmoid = jax.nn.sigmoid(value)
    return sigmoid * (1.0 + value * (1.0 - sigmoid))

def mdot(left, right):
    return jnp.dot(left, right, preferred_element_type=jnp.float32)

def reference(block_input, norm1_gain, q_weight, kva_weight, kv_norm_gain, kvb_weight, out_weight, norm2_gain, router_weight, shared_gate, shared_up, shared_down, expert_gate, expert_up, expert_down, routes, cotangent):
    seq_count = TOKENS // L
    score_scale = (DN + DR) ** (-0.5)
    x_float = block_input.astype(jnp.float32)
    normed_one = norm_rows(x_float, norm1_gain).astype(jnp.bfloat16)
    cosine, sine_table = rope_tables(L, 0.0)
    query = mdot(normed_one, q_weight).reshape(seq_count, L, H, DN + DR)
    query_rot = rotate(query[..., DN:], cosine[None, :, None, :], sine_table[None, :, None, :])
    query = jnp.concatenate([query[..., :DN], query_rot], axis=-1).astype(jnp.bfloat16)
    latent = mdot(normed_one, kva_weight)
    compressed = latent[:, :KVR]
    latent_n = norm_rows(compressed, kv_norm_gain).astype(jnp.bfloat16)
    rope_key = rotate(latent[:, KVR:].reshape(seq_count, L, DR), cosine[None], sine_table[None]).astype(jnp.bfloat16)
    key_value = mdot(latent_n, kvb_weight).astype(jnp.bfloat16).reshape(seq_count, L, H, DN + DV)
    query_nope = query[..., :DN].astype(jnp.float32)
    query_rope = query[..., DN:].astype(jnp.float32)
    positions = jnp.arange(L, dtype=jnp.int32)

    def scores_at(block_id):
        blk_start = block_id * BLK
        kv_block = lax.dynamic_slice_in_dim(key_value, blk_start, BLK, 1).astype(jnp.float32)
        rope_block = lax.dynamic_slice_in_dim(rope_key, blk_start, BLK, 1).astype(jnp.float32)
        score = jnp.einsum('sqhd,skhd->shqk', query_nope, kv_block[..., :DN])
        score = score + jnp.einsum('sqhd,skd->shqk', query_rope, rope_block)
        score = score * score_scale
        key_pos = blk_start + jnp.arange(BLK, dtype=jnp.int32)
        score = jnp.where(key_pos[None, None, None, :] <= positions[None, None, :, None], score, NEG)
        return (score, kv_block, rope_block)

    def forward_block(carry, block_id):
        run_max, run_sum, weighted = carry
        score, kv_block, rope_block = scores_at(block_id)
        new_max = jnp.maximum(run_max, lax.optimization_barrier(jnp.max(score, axis=-1)))
        factor = jnp.exp(run_max - new_max)
        expo = jnp.exp(score - new_max[..., None])
        run_sum = factor * run_sum + lax.optimization_barrier(jnp.sum(expo, axis=-1))
        weighted = factor[..., None] * weighted + jnp.einsum('shqk,skhd->shqd', expo.astype(jnp.bfloat16).astype(jnp.float32), kv_block[..., DN:])
        return ((new_max, run_sum, weighted), None)
    start_state = (jnp.full((seq_count, H, L), NEG, jnp.float32), jnp.zeros((seq_count, H, L), jnp.float32), jnp.zeros((seq_count, H, L, DV), jnp.float32))
    (run_max, run_sum, weighted), _ = lax.scan(forward_block, start_state, jnp.arange(N_CTX, dtype=jnp.int32))
    lse = run_max + jnp.log(run_sum)
    attn = (weighted / run_sum[..., None]).astype(jnp.bfloat16)
    attn_flat = attn.transpose(0, 2, 1, 3).reshape(TOKENS, H * DV)
    mid = x_float + mdot(attn_flat, out_weight)
    normed_two = norm_rows(mid, norm2_gain).astype(jnp.bfloat16)
    probs = jax.nn.softmax(mdot(normed_two, router_weight), axis=-1)
    picks = (routes[:, :, None] == jnp.arange(E, dtype=jnp.int32)[None, None, :]).astype(jnp.float32)
    route_w = lax.optimization_barrier(jnp.sum(picks * probs[:, None, :], axis=-1))
    shared_a = mdot(normed_two, shared_gate)
    shared_b = mdot(normed_two, shared_up)
    shared_h = (jax.nn.silu(shared_a) * shared_b).astype(jnp.bfloat16)
    shared_y = mdot(shared_h, shared_down)
    entry_count = TOKENS * TOPK
    groups = TOKENS // BLK
    flat_routes = routes.reshape(-1)
    onehot = (flat_routes.reshape(groups, BLK * TOPK)[:, :, None] == jnp.arange(E, dtype=jnp.int32)[None, None, :]).astype(jnp.int32)
    rank = lax.optimization_barrier(jnp.sum((jnp.cumsum(onehot, axis=1) - 1) * onehot, axis=2)).reshape(-1)
    group_of = jnp.arange(entry_count, dtype=jnp.int32) // (BLK * TOPK)
    table = jnp.full((E, groups * CAP), entry_count, jnp.int32)
    table = table.at[flat_routes, group_of * CAP + rank].set(jnp.arange(entry_count, dtype=jnp.int32))
    flat_w = route_w.reshape(-1)

    def expert_step(carry, inputs):
        mixed, back_rows, weight_grad = carry
        gate_w, up_w, down_w, entries = inputs
        valid = entries < entry_count
        safe_idx = jnp.minimum(entries, entry_count - 1)
        token_idx = safe_idx // TOPK
        rows_in = jnp.where(valid[:, None], normed_two[token_idx], jnp.zeros((), jnp.bfloat16))
        weight = jnp.where(valid, flat_w[safe_idx], 0.0)
        grad_rows = jnp.where(valid[:, None], cotangent[token_idx], 0.0)
        gate_act = mdot(rows_in, gate_w)
        up_act = mdot(rows_in, up_w)
        hidden = (jax.nn.silu(gate_act) * up_act).astype(jnp.bfloat16)
        out_rows = mdot(hidden, down_w)
        mixed = mixed.at[token_idx].add(weight[:, None] * out_rows)
        weight_grad = weight_grad.at[entries].add(lax.optimization_barrier(jnp.sum(grad_rows * out_rows, axis=-1)), mode='drop')
        routed_grad = (weight[:, None] * grad_rows).astype(jnp.bfloat16)
        hidden_grad = mdot(routed_grad, down_w.T)
        gate_grad = (hidden_grad * up_act * silu_slope(gate_act)).astype(jnp.bfloat16)
        up_grad = (hidden_grad * jax.nn.silu(gate_act)).astype(jnp.bfloat16)
        grad_down = mdot(hidden.T, routed_grad)
        grad_gate = mdot(rows_in.T, gate_grad)
        grad_up = mdot(rows_in.T, up_grad)
        row_grad = mdot(gate_grad, gate_w.T) + mdot(up_grad, up_w.T)
        back_rows = back_rows.at[token_idx].add(row_grad)
        return ((mixed, back_rows, weight_grad), (grad_gate, grad_up, grad_down))
    expert_init = (jnp.zeros((TOKENS, D), jnp.float32), jnp.zeros((TOKENS, D), jnp.float32), jnp.zeros((entry_count,), jnp.float32))
    (mixed, routed_back, weight_grad), (grad_expert_gate, grad_expert_up, grad_expert_down) = lax.scan(expert_step, expert_init, (expert_gate, expert_up, expert_down, table))
    block_output = mid + (shared_y + mixed)
    route_grad = weight_grad.reshape(TOKENS, TOPK)
    cot_b = cotangent.astype(jnp.bfloat16)
    shared_grad = mdot(cot_b, shared_down.T)
    sgate_grad = (shared_grad * shared_b * silu_slope(shared_a)).astype(jnp.bfloat16)
    sup_grad = (shared_grad * jax.nn.silu(shared_a)).astype(jnp.bfloat16)
    grad_shared_down = mdot(shared_h.T, cot_b)
    grad_shared_gate = mdot(normed_two.T, sgate_grad)
    grad_shared_up = mdot(normed_two.T, sup_grad)
    prob_grad = lax.optimization_barrier(jnp.sum(picks * route_grad[:, :, None], axis=1))
    logit_grad = (probs * (prob_grad - lax.optimization_barrier(jnp.sum(probs * prob_grad, axis=-1, keepdims=True)))).astype(jnp.bfloat16)
    grad_router = mdot(normed_two.T, logit_grad)
    two_grad = routed_back + mdot(sgate_grad, shared_gate.T) + mdot(sup_grad, shared_up.T) + mdot(logit_grad, router_weight.T)
    _, norm_two_back = jax.vjp(norm_rows, mid, norm2_gain.astype(jnp.float32))
    mid_norm_grad, grad_norm2 = norm_two_back(two_grad)
    mid_grad = cotangent + mid_norm_grad
    mid_b = mid_grad.astype(jnp.bfloat16)
    grad_out_w = mdot(attn_flat.T, mid_b)
    out_grad = mdot(mid_b, out_weight.T).reshape(seq_count, L, H, DV).transpose(0, 2, 1, 3)
    out_grad_b = out_grad.astype(jnp.bfloat16).astype(jnp.float32)
    delta = lax.optimization_barrier(jnp.sum(out_grad * attn.astype(jnp.float32), axis=-1))

    def back_block(carry, block_id):
        nope_grad, rope_qgrad = carry
        score, kv_block, rope_block = scores_at(block_id)
        probs_blk = jnp.exp(score - lse[..., None])
        prob_b = probs_blk.astype(jnp.bfloat16).astype(jnp.float32)
        dprob = jnp.einsum('shqd,skhd->shqk', out_grad_b, kv_block[..., DN:])
        dscore = (probs_blk * (dprob - delta[..., None])).astype(jnp.bfloat16).astype(jnp.float32)
        nope_grad = nope_grad + jnp.einsum('shqk,skhd->sqhd', dscore, kv_block[..., :DN]) * score_scale
        rope_qgrad = rope_qgrad + jnp.einsum('shqk,skd->sqhd', dscore, rope_block) * score_scale
        key_nope_grad = jnp.einsum('shqk,sqhd->skhd', dscore, query_nope) * score_scale
        key_rope_grad = jnp.einsum('shqk,sqhd->skd', dscore, query_rope) * score_scale
        value_grad = jnp.einsum('shqk,shqd->skhd', prob_b, out_grad_b)
        return ((nope_grad, rope_qgrad), (jnp.concatenate([key_nope_grad, value_grad], axis=-1), key_rope_grad))
    back_init = (jnp.zeros((seq_count, L, H, DN), jnp.float32), jnp.zeros((seq_count, L, H, DR), jnp.float32))
    (nope_grad, rope_qgrad), (kv_blocks, rope_blocks) = lax.scan(back_block, back_init, jnp.arange(N_CTX, dtype=jnp.int32))
    kv_grad = kv_blocks.transpose(1, 0, 2, 3, 4).reshape(TOKENS, H * (DN + DV)).astype(jnp.bfloat16)
    rope_sum = rope_blocks.transpose(1, 0, 2, 3).reshape(seq_count, L, DR)
    rope_grad = rotate_back(rope_sum, cosine[None], sine_table[None]).reshape(TOKENS, DR)
    grad_expand_w = mdot(latent_n.T, kv_grad)
    latent_part = mdot(kv_grad, kvb_weight.T)
    _, kv_back = jax.vjp(norm_rows, compressed, kv_norm_gain.astype(jnp.float32))
    compressed_grad, grad_kv_norm = kv_back(latent_part)
    latent_grad = jnp.concatenate([compressed_grad, rope_grad], axis=-1).astype(jnp.bfloat16)
    rope_qback = rotate_back(rope_qgrad, cosine[None, :, None, :], sine_table[None, :, None, :])
    query_grad = jnp.concatenate([nope_grad, rope_qback], axis=-1).astype(jnp.bfloat16).reshape(TOKENS, H * (DN + DR))
    grad_query_w = mdot(normed_one.T, query_grad)
    grad_latent_w = mdot(normed_one.T, latent_grad)
    one_grad = mdot(query_grad, q_weight.T) + mdot(latent_grad, kva_weight.T)
    _, one_back = jax.vjp(norm_rows, x_float, norm1_gain.astype(jnp.float32))
    input_norm_grad, grad_norm1 = one_back(one_grad)
    input_grad = mid_grad + input_norm_grad
    return (block_output, input_grad, grad_norm1, grad_query_w, grad_latent_w, grad_kv_norm, grad_expand_w, grad_out_w, grad_norm2, grad_router, grad_shared_gate, grad_shared_up, grad_shared_down, grad_expert_gate, grad_expert_up, grad_expert_down)
```

```python
import functools

import jax
import jax.numpy as jnp
from jax import lax
from jax.experimental import pallas as pl
from jax.experimental.pallas import tpu as pltpu
from jax.sharding import PartitionSpec as P

DN = 128
DR = 64
DV = 128
KVR = 512
LANES = 128
SHARD, CTX, TP = "shard", "ctx", "tp"

EPS = 1e-06
NEG = -1e30

BF = jnp.bfloat16
F32 = jnp.float32
MESH = pl.DeviceIdType.MESH
ANY = pl.ANY
VMEM = pltpu.VMEM


def norm_rows(value, gain):
    factor = lax.rsqrt(jnp.mean(value * value, axis=-1, keepdims=True) + EPS)
    return value * factor * gain.astype(F32)


def norm_back(value, gain, grad):
    factor = lax.rsqrt(jnp.mean(value * value, axis=-1, keepdims=True) + EPS)
    scaled = grad * gain.astype(F32)
    inner = jnp.mean(scaled * value, axis=-1, keepdims=True)
    return factor * (scaled - value * (factor * factor * inner)), grad * value * factor


def rope_tables(count, offset):
    half_size = DR // 2
    position = jnp.arange(count, dtype=F32) + offset
    freqs = 10000.0 ** (-(jnp.arange(half_size, dtype=F32) * 2.0 / DR))
    angle = position[:, None] * freqs[None, :]
    return (jnp.cos(angle), jnp.sin(angle))


def rotate(value, cosine, sine_table):
    half_size = DR // 2
    first = value[..., :half_size]
    second = value[..., half_size:]
    return jnp.concatenate(
        [first * cosine - second * sine_table, first * sine_table + second * cosine], axis=-1
    )


def rotate_back(grad, cosine, sine_table):
    half_size = DR // 2
    first = grad[..., :half_size]
    second = grad[..., half_size:]
    return jnp.concatenate(
        [first * cosine + second * sine_table, second * cosine - first * sine_table], axis=-1
    )


def silu_slope(value):
    sigmoid = jax.nn.sigmoid(value)
    return sigmoid * (1.0 + value * (1.0 - sigmoid))


def mdot(left, right):
    return jnp.dot(left, right, preferred_element_type=F32)


def dot_nt(left, right):
    return lax.dot_general(left, right, (((1,), (1,)), ((), ())), preferred_element_type=F32)


def dot_tn(left, right):
    return lax.dot_general(left, right, (((0,), (0,)), ((), ())), preferred_element_type=F32)


class Place:
    def __init__(self, n_tp):
        self.s = lax.axis_index(SHARD)
        self.c = lax.axis_index(CTX)
        self.t = lax.axis_index(TP)
        self.core = lax.rem(self.s, 2)
        self.y = self.s // 2
        self.n_tp = n_tp

    def at(self, s, c, t):
        return {SHARD: s, CTX: c, TP: t}

    @property
    def over_x(self):
        return self.at(self.s, 1 - self.c, self.t)

    @property
    def over_y(self):
        return self.at(lax.rem(self.s + 2, 4), self.c, self.t)

    @property
    def over_core(self):
        return self.at(self.s + 1 - 2 * self.core, self.c, self.t)

    def along(self, step):
        return self.at(self.s, self.c, lax.rem(self.t + step + self.n_tp, self.n_tp))

    def flip(self, dy, dcore, dx):
        y = self.y + dy * (1 - 2 * self.y)
        core = self.core + dcore * (1 - 2 * self.core)
        x = self.c + dx * (1 - 2 * self.c)
        return self.at(2 * y + core, x, self.t)


def slot(s, c):
    return 2 * s + c


class Net:
    def __init__(self, send, recv, local):
        self.send, self.recv, self.local = send, recv, local
        self.puts, self.locals = [], []
        self.n_local = 0

    def put(self, src, dst, to):
        i = len(self.puts)
        copy = pltpu.make_async_remote_copy(
            src_ref=src,
            dst_ref=dst,
            send_sem=self.send.at[i],
            recv_sem=self.recv.at[i],
            device_id=to,
            device_id_type=MESH,
        )
        copy.start()
        self.puts.append(copy)
        return copy

    def move(self, src, dst):
        copy = pltpu.make_async_copy(src, dst, self.local.at[self.n_local])
        self.n_local += 1
        copy.start()
        return copy

    def finish(self):
        for copy in self.puts:
            copy.wait_send()


def greet(peers):
    barrier = pltpu.get_barrier_semaphore()
    for peer in peers:
        pl.semaphore_signal(barrier, inc=1, device_id=peer, device_id_type=MESH)
    pl.semaphore_wait(barrier, len(peers))


def comm_call(body, ins, outs, scratch, n_put, n_local, collective_id, name, in_space, out_space):
    return pl.pallas_call(
        body,
        out_shape=tuple(jax.ShapeDtypeStruct(shape, dtype) for shape, dtype in outs),
        in_specs=[pl.BlockSpec(memory_space=space) for space in in_space],
        out_specs=tuple(pl.BlockSpec(memory_space=space) for space in out_space),
        scratch_shapes=[
            *scratch,
            pltpu.SemaphoreType.DMA((n_put,)),
            pltpu.SemaphoreType.DMA((n_put,)),
            pltpu.SemaphoreType.DMA((max(n_local, 1),)),
        ],
        compiler_params=pltpu.CompilerParams(
            collective_id=collective_id, has_side_effects=True, vmem_limit_bytes=60 * 2**20
        ),
        name=name,
    )(*ins)


def start_gather(weights, small, block, n_tp):
    shapes = [w.shape for w in weights]

    def body(*refs):
        n = len(shapes)
        w_in, (small_in, x_in) = refs[:n], refs[n : n + 2]
        w_out, (small_out, x_out) = refs[n + 2 : 2 * n + 2], refs[2 * n + 2 : 2 * n + 4]
        bounce = refs[2 * n + 4 : 3 * n + 6]
        send, recv, local = refs[3 * n + 6 :]
        me = Place(n_tp)
        net = Net(send, recv, local)
        greet([me.over_x, me.over_y, me.over_core])

        def half(ref, index, which, rows):
            return ref.at[index, pl.ds(which * (rows // 2), rows // 2)]

        other = lax.rem(me.s + 2, 4)
        loads = [net.move(src, b) for src, b in zip((*w_in, small_in, x_in), bounce)]
        from_y, own = [], []
        for ref, out, shape in zip(w_in, w_out, shapes):
            rows = shape[0]
            from_y.append(
                net.put(ref.at[pl.ds(me.c * (rows // 2), rows // 2)], half(out, me.s, me.c, rows), me.over_y)
            )
            if ref is w_in[0]:
                wait_x = net.put(x_in, x_out.at[me.c], me.over_x)
        for ref, out in zip(w_in, w_out):
            own.append(net.put(ref, out.at[me.s], me.over_core))
        small_y = net.put(small_in, small_out.at[me.s], me.over_y)
        small_c = net.put(small_in, small_out.at[me.s], me.over_core)
        stores = []
        outs = [o.at[me.s] for o in (*w_out, small_out)] + [x_out.at[me.c]]
        for load, b, out in zip(loads, bounce, outs):
            load.wait()
            stores.append(net.move(b, out))
        from_x, relays = [], []
        for got, out, shape in zip(from_y, w_out, shapes):
            rows = shape[0]
            got.wait_recv()
            piece = half(out, other, me.c, rows)
            from_x.append(net.put(piece, piece, me.over_x))
            relays.append(net.put(piece, piece, me.over_core))
        small_y.wait_recv()
        relays.append(net.put(small_out.at[other], small_out.at[other], me.over_core))
        for got, out, shape in zip(from_x, w_out, shapes):
            rows = shape[0]
            got.wait_recv()
            piece = half(out, other, 1 - me.c, rows)
            relays.append(net.put(piece, piece, me.over_core))
        wait_x.wait_recv()
        small_c.wait_recv()
        for got in own + relays:
            got.wait_recv()
        for store in stores:
            store.wait()
        net.finish()

    n = len(weights)
    outs = [((4, *w.shape), BF) for w in weights] + [((4, *small.shape), small.dtype), ((2, *block.shape), BF)]
    return comm_call(
        body,
        (*weights, small, block),
        outs,
        [VMEM(w.shape, w.dtype) for w in (*weights, small, block)],
        5 * n + 4,
        2 * n + 4,
        0,
        "start_gather",
        [ANY] * (n + 2),
        [ANY] * (n + 2),
    )


def tp_reduce_scatter(part, n_tp, collective_id, name):
    rows, width = part.shape
    piece = rows // n_tp

    def body(in_ref, out_ref, got, send, recv, local):
        me = Place(n_tp)
        net = Net(send, recv, local)
        greet([me.along(k) for k in range(1, n_tp)])
        waits = []
        for k in range(1, n_tp):
            to = lax.rem(me.t + k, n_tp)
            waits.append(
                net.put(in_ref.at[pl.ds(to * piece, piece)], got.at[k - 1], me.along(k))
            )
        for wait in waits:
            wait.wait_recv()
        total = in_ref[pl.ds(pl.multiple_of(me.t * piece, piece), piece), :].astype(F32)
        for k in range(1, n_tp):
            total = total + got[k - 1].astype(F32)
        out_ref[...] = total
        net.finish()

    return comm_call(
        body,
        (part,),
        [((piece, width), F32)],
        [VMEM((n_tp - 1, piece, width), BF)],
        n_tp - 1,
        0,
        collective_id,
        name,
        [VMEM],
        [VMEM],
    )[0]


def tp_ring(net, me, own, out, base):
    piece = own.shape[0]
    half = piece // 2

    def rows(p, which=None):
        start = base + p * piece
        if which is None:
            return out.at[pl.ds(start, piece)]
        return out.at[pl.ds(start + which * half, half)]

    right, left = me.along(1), me.along(-1)
    p_left, p_right = lax.rem(me.t + 3, 4), lax.rem(me.t + 1, 4)
    far = lax.rem(me.t + 2, 4)
    to_right = net.put(own, rows(me.t), right)
    to_left = net.put(own, rows(me.t), left)
    to_right.wait_recv()
    hop_right = net.put(rows(p_left, 0), rows(p_left, 0), right)
    yield p_left
    to_left.wait_recv()
    hop_left = net.put(rows(p_right, 1), rows(p_right, 1), left)
    yield p_right
    hop_right.wait_recv()
    hop_left.wait_recv()
    yield far


def tp_all_gather(pieces, n_tp, collective_id, name):
    def body(*refs):
        n = len(pieces)
        ins, outs, (send, recv, local) = refs[:n], refs[n : 2 * n], refs[2 * n :]
        me = Place(n_tp)
        net = Net(send, recv, local)
        greet([me.along(1), me.along(-1)])
        rings = []
        for src, dst in zip(ins, outs):
            size = src.shape[0]
            rings.append(tp_ring(net, me, src, dst, 0))
        for _ in range(3):
            for ring in rings:
                next(ring)
        for src, dst in zip(ins, outs):
            size = src.shape[0]
            dst[pl.ds(pl.multiple_of(me.t * size, size), size), :] = src[...]
        net.finish()

    return comm_call(
        body,
        pieces,
        [((n_tp * p.shape[0], p.shape[1]), p.dtype) for p in pieces],
        [],
        4 * len(pieces),
        0,
        collective_id,
        name,
        [VMEM] * len(pieces),
        [VMEM] * len(pieces),
    )


def relay_chunks(net, me, out, chunks):
    g_x, g_y = slot(me.s, 1 - me.c), slot(lax.rem(me.s + 2, 4), me.c)
    g_d = slot(lax.rem(me.s + 2, 4), 1 - me.c)
    first = 1 - me.core
    relay_slot = first * g_x + me.core * g_y
    relay_to = me.flip(first, 0, me.core)
    diags, waits = [], []
    for from_x, from_y, (start, size) in chunks:
        from_x.wait_recv()
        from_y.wait_recv()
        src = out.at[relay_slot, pl.ds(start, size)]
        diags.append(net.put(src, src, relay_to))
        for g in (g_x, g_y):
            piece = out.at[g, pl.ds(start, size)]
            waits.append(net.put(piece, piece, me.over_core))
    for diag, (_, _, (start, size)) in zip(diags, chunks):
        diag.wait_recv()
        piece = out.at[g_d, pl.ds(start, size)]
        waits.append(net.put(piece, piece, me.over_core))
    return waits


def gather_everywhere(own, n_tp, collective_id, name):
    piece, width = own.shape

    def body(in_ref, out_ref, bounce, send, recv, local):
        me = Place(n_tp)
        net = Net(send, recv, local)
        greet([me.over_x, me.over_y, me.over_core, me.along(1), me.along(-1)])
        load = net.move(in_ref, bounce)
        g_me = slot(me.s, me.c)
        chunks, cores = [], []

        def spread(src, p):
            dst = out_ref.at[g_me, pl.ds(p * piece, piece)]
            from_x = net.put(src, dst, me.over_x)
            from_y = net.put(src, dst, me.over_y)
            cores.append(net.put(src, dst, me.over_core))
            chunks.append((from_x, from_y, (p * piece, piece)))

        spread(in_ref, me.t)
        ring = tp_ring(net, me, in_ref, out_ref.at[g_me], 0)
        load.wait()
        store = net.move(bounce, out_ref.at[g_me, pl.ds(me.t * piece, piece)])
        for p in ring:
            spread(out_ref.at[g_me, pl.ds(p * piece, piece)], p)
        waits = cores + relay_chunks(net, me, out_ref, chunks)
        for wait in waits:
            wait.wait_recv()
        store.wait()
        net.finish()

    return comm_call(
        body,
        (own,),
        [((8, n_tp * piece, width), own.dtype)],
        [VMEM(own.shape, own.dtype)],
        4 * 7 + 4,
        2,
        collective_id,
        name,
        [ANY],
        [ANY],
    )[0]


def plane_exchange(gathers, columns, rows88, n_tp, collective_id, name, n_chunk=4):
    ng, nc, nr = len(gathers), len(columns), len(rows88)
    ins = (*gathers, *columns, *rows88)

    def body(*refs):
        n = ng + nc + nr
        src, dst, bounce = refs[:n], refs[n : 2 * n], refs[2 * n : 3 * n]
        send, recv, local = refs[3 * n :]
        me = Place(n_tp)
        net = Net(send, recv, local)
        flips = [(dy, dk, dx) for dy in (0, 1) for dk in (0, 1) for dx in (0, 1)][1:]
        if nc or nr:
            greet([me.flip(*f) for f in flips])
        else:
            greet([me.over_x, me.over_y, me.over_core])
        g_me = slot(me.s, me.c)
        loads, waits, work = [], [], []
        for i in range(n):
            s, d, b = src[i], dst[i], bounce[i]
            if i < ng:
                rows = s.shape[0]
                size = rows // n_chunk
                chunks = []
                for j in range(n_chunk):
                    part = s.at[pl.ds(j * size, size)]
                    to = d.at[g_me, pl.ds(j * size, size)]
                    chunks.append((net.put(part, to, me.over_x), net.put(part, to, me.over_y), (j * size, size)))
                    waits.append(net.put(part, to, me.over_core))
                work.append((d, chunks))
                loads.append((net.move(s, b), b, d.at[g_me]))
            elif i < ng + nc:
                w = s.shape[1] // 4
                for f in flips:
                    peer = me.flip(*f)
                    part = s.at[:, pl.ds(pl.multiple_of(peer[SHARD] * w, LANES), w)]
                    waits.append(net.put(part, d.at[g_me], peer))
                part = s.at[:, pl.ds(pl.multiple_of(me.s * w, LANES), w)]
                loads.append((net.move(part, b), b, d.at[g_me]))
            else:
                h, w = s.shape[0] // 8, s.shape[1]
                to = d.at[:, pl.ds(pl.multiple_of(me.s * w, LANES), w)]
                for f in ((0, 1, 0), (1, 0, 0), (1, 1, 0)):
                    peer = me.flip(*f)
                    row = pl.multiple_of(slot(peer[SHARD], peer[CTX]) * h, 8)
                    waits.append(net.put(s.at[pl.ds(row, h)], to, peer))
                row = pl.multiple_of(g_me * h, 8)
                loads.append((net.move(s.at[pl.ds(row, h)], b), b, to))
        stores = []
        for load, b, to in loads:
            load.wait()
            stores.append(net.move(b, to))
        for d, chunks in work:
            waits += relay_chunks(net, me, d, chunks)
        for wait in waits:
            wait.wait_recv()
        for store in stores:
            store.wait()
        net.finish()

    outs, scratch = [], []
    for a in gathers:
        outs.append(((8, *a.shape), a.dtype))
        scratch.append(VMEM(a.shape, a.dtype))
    for a in columns:
        outs.append(((8, a.shape[0], a.shape[1] // 4), a.dtype))
        scratch.append(VMEM((a.shape[0], a.shape[1] // 4), a.dtype))
    for a in rows88:
        outs.append(((a.shape[0] // 8, a.shape[1] * 4), a.dtype))
        scratch.append(VMEM((a.shape[0] // 8, a.shape[1]), a.dtype))
    return comm_call(
        body,
        ins,
        outs,
        scratch,
        ng * 7 * n_chunk + nc * 7 + nr * 3,
        2 * len(ins),
        collective_id,
        name,
        [ANY] * len(ins),
        [ANY] * len(ins),
    )


def ctx_swap(block, collective_id, name):
    def body(in_ref, out_ref, send, recv, local):
        me = Place(1)
        net = Net(send, recv, local)
        greet([me.over_x])
        net.put(in_ref, out_ref, me.over_x).wait_recv()
        net.finish()

    return comm_call(
        body, (block,), [(block.shape, block.dtype)], [], 1, 0, collective_id, name, [ANY], [ANY]
    )[0]


def reduce_everywhere(part, n_tp, collective_id, name):
    _, rows, width = part.shape
    half = width // 2
    piece = rows // n_tp
    step = 16

    def body(in_ref, out_ref, mine, rc, rx, ry, q0, q1, r0, r1, last, got, send, recv, local):
        me = Place(n_tp)
        net = Net(send, recv, local)
        greet([me.over_x, me.over_y, me.over_core] + [me.along(k) for k in range(1, n_tp)])
        a, b = pl.ds(0, half), pl.ds(half, half)
        order = [(1, 1), (0, 1), (1, 0), (0, 0)]
        pairs = []
        for dy, dx in order:
            y, x = me.y + dy * (1 - 2 * me.y), me.c + dx * (1 - 2 * me.c)
            pairs.append((2 * y + x, slot(2 * y + me.core, x), slot(2 * y + 1 - me.core, x)))
        loads, cores = [], []
        for i, g_mine, g_other in pairs:
            cores.append(net.put(in_ref.at[g_other], rc.at[i], me.over_core))
            loads.append(net.move(in_ref.at[g_mine], mine.at[i]))

        def add(target, cols, left, right):
            def one(r, carry):
                at = pl.ds(pl.multiple_of(r * step, step), step)
                total = left(at).astype(F32) + right(at).astype(F32)
                target[at, cols] = total.astype(target.dtype)
                return carry

            lax.fori_loop(0, rows // step, one, 0)

        def sum_cores(k):
            i = pairs[k][0]
            loads[k].wait()
            cores[k].wait_recv()
            add(mine.at[i], pl.ds(0, width), lambda at: mine[i, at, :], lambda at: rc[i, at, :])
            return i

        i_yx = sum_cores(0)
        ax0 = net.put(mine.at[i_yx, :, a], rx.at[1 - me.y], me.over_x)
        by0 = net.put(mine.at[i_yx, :, b], ry.at[1 - me.c], me.over_y)
        i_x = sum_cores(1)
        ax1 = net.put(mine.at[i_x, :, a], rx.at[me.y], me.over_x)
        i_y = sum_cores(2)
        by1 = net.put(mine.at[i_y, :, b], ry.at[me.c], me.over_y)
        i_me = sum_cores(3)
        every = pl.ds(0, half)
        ax0.wait_recv()
        add(q0, every, lambda at: mine[i_y, at, a], lambda at: rx[1 - me.y, at, :])
        y0 = net.put(q0, r0, me.over_y)
        by0.wait_recv()
        add(q1, every, lambda at: mine[i_x, at, b], lambda at: ry[1 - me.c, at, :])
        x1 = net.put(q1, r1, me.over_x)
        ax1.wait_recv()
        by1.wait_recv()
        y0.wait_recv()
        x1.wait_recv()

        def final(r, carry):
            at = pl.ds(pl.multiple_of(r * step, step), step)
            left = mine[i_me, at, a].astype(F32) + rx[me.y, at, :].astype(F32) + r0[at, :].astype(F32)
            right = mine[i_me, at, b].astype(F32) + ry[me.c, at, :].astype(F32) + r1[at, :].astype(F32)
            last[at, a] = left.astype(BF)
            last[at, b] = right.astype(BF)
            return carry

        lax.fori_loop(0, rows // step, final, 0)
        waits = []
        for k in range(1, n_tp):
            to = lax.rem(me.t + k, n_tp)
            waits.append(net.put(last.at[pl.ds(to * piece, piece)], got.at[k - 1], me.along(k)))
        for wait in waits:
            wait.wait_recv()
        for r in range(piece // step):
            at = pl.ds(pl.multiple_of(me.t * piece + r * step, step), step)
            total = last[at, :].astype(F32)
            for k in range(n_tp - 1):
                total = total + got[k, r * step : (r + 1) * step, :].astype(F32)
            out_ref[r * step : (r + 1) * step, :] = total
        net.finish()

    block = (rows, width)
    return comm_call(
        body,
        (part,),
        [((piece, width), F32)],
        [
            VMEM((4, *block), BF),
            VMEM((4, *block), BF),
            VMEM((2, rows, half), BF),
            VMEM((2, rows, half), BF),
            VMEM((rows, half), BF),
            VMEM((rows, half), BF),
            VMEM((rows, half), BF),
            VMEM((rows, half), BF),
            VMEM(block, BF),
            VMEM((n_tp - 1, piece, width), BF),
        ],
        10 + n_tp - 1,
        4,
        collective_id,
        name,
        [ANY],
        [VMEM],
    )[0]


def sum_everywhere(part, n_tp, collective_id, name):
    def body(in_ref, out_ref, from_tp, mid, from_plane, send, recv, local):
        me = Place(n_tp)
        net = Net(send, recv, local)
        flips = [(dy, dk, dx) for dy in (0, 1) for dk in (0, 1) for dx in (0, 1)][1:]
        greet([me.along(k) for k in range(1, n_tp)] + [me.flip(*f) for f in flips])
        waits = [net.put(in_ref, from_tp.at[k - 1], me.along(k)) for k in range(1, n_tp)]
        for wait in waits:
            wait.wait_recv()
        total = in_ref[...]
        for k in range(n_tp - 1):
            total = total + from_tp[k]
        mid[...] = total
        waits = [net.put(mid, from_plane.at[i], me.flip(*f)) for i, f in enumerate(flips)]
        for wait in waits:
            wait.wait_recv()
        for i in range(7):
            total = total + from_plane[i]
        out_ref[...] = total
        net.finish()

    return comm_call(
        body,
        (part,),
        [(part.shape, F32)],
        [VMEM((n_tp - 1, *part.shape), F32), VMEM(part.shape, F32), VMEM((7, *part.shape), F32)],
        n_tp - 1 + 7,
        0,
        collective_id,
        name,
        [VMEM],
        [VMEM],
    )[0]


def per_device(
    block_input,
    norm1_gain,
    q_weight,
    kva_weight,
    kv_norm_gain,
    kvb_weight,
    out_weight,
    norm2_gain,
    router_weight,
    shared_gate,
    shared_up,
    shared_down,
    expert_gate,
    expert_up,
    expert_down,
    routes,
    cotangent,
):
    n_tp = lax.axis_size(TP)
    rows, width = block_input.shape
    topk = routes.shape[1]
    experts = router_weight.shape[1]
    local_experts = expert_gate.shape[0]
    heads = q_weight.shape[1] // (DN + DR)
    scale = (DN + DR) ** (-0.5)
    piece = rows // n_tp
    s_id, c_id, t_id = lax.axis_index(SHARD), lax.axis_index(CTX), lax.axis_index(TP)
    shard_w = width // 4
    kv_w = KVR // 4

    small = jnp.concatenate(
        [
            norm1_gain.reshape(-1, LANES),
            norm2_gain.reshape(-1, LANES),
            kv_norm_gain.reshape(-1, LANES),
            jnp.zeros((7, LANES), BF),
            jnp.pad(router_weight, ((0, 0), (0, LANES - experts))),
        ]
    )
    w_query, w_latent, w_expand, w_output, small_all, x_pair = start_gather(
        (q_weight, kva_weight, kvb_weight, out_weight), small, block_input, n_tp
    )
    w_query = w_query.reshape(width, -1)
    w_latent = w_latent.reshape(width, -1)
    w_expand = w_expand.reshape(KVR, -1)
    w_output = w_output.transpose(1, 0, 2).reshape(-1, width)
    gain_one = small_all[:, 0:4].reshape(-1)
    gain_two = small_all[:, 4:8].reshape(-1)
    gain_kv = small_all[:, 8:9].reshape(-1)
    w_router = small_all[:, 16:, :experts].reshape(width, experts)

    cot_b = cotangent.astype(BF)
    cot_pack = jnp.concatenate(
        [cot_b, jnp.pad(routes.astype(BF), ((0, 0), (0, LANES - topk)))], axis=1
    )
    cot_all, sg_t, su_t, sd = plane_exchange(
        (cot_pack,), (), (shared_gate.T, shared_up.T, shared_down), n_tp, 1, "early_exchange"
    )
    cot_all = cot_all.reshape(-1, width + LANES)
    routes_all = cot_all[:, width : width + topk].astype(jnp.int32)
    cot_all = cot_all[:, :width]

    x_float = block_input.astype(F32)
    cosine, sine = rope_tables(rows, (c_id * rows).astype(F32))
    cos_all, sin_all = rope_tables(2 * rows, jnp.float32(0))
    normed_pair = norm_rows(x_pair.reshape(2 * rows, width).astype(F32), gain_one).astype(BF)
    normed_one = norm_rows(x_float, gain_one).astype(BF)
    query = mdot(normed_one, w_query).reshape(rows, heads, DN + DR)
    query_nope = query[..., :DN].astype(BF)
    query_rope = rotate(query[..., DN:], cosine[:, None, :], sine[:, None, :]).astype(BF)
    latent = mdot(normed_pair, w_latent)
    latent_pair = norm_rows(latent[:, :KVR], gain_kv).astype(BF)
    rope_pair = rotate(latent[:, KVR:], cos_all, sin_all).astype(BF)
    kv_pair = mdot(latent_pair, w_expand).astype(BF).reshape(2 * rows, heads, DN + DV)
    key_pair, value_pair = kv_pair[..., :DN], kv_pair[..., DN:]
    score = jnp.einsum("qhd,khd->hqk", query_nope, key_pair, preferred_element_type=F32)
    score = score + jnp.einsum("qhd,kd->hqk", query_rope, rope_pair, preferred_element_type=F32)
    q_pos = c_id * rows + jnp.arange(rows, dtype=jnp.int32)
    k_pos = jnp.arange(2 * rows, dtype=jnp.int32)
    score = jnp.where(k_pos[None, None, :] <= q_pos[None, :, None], score * scale, NEG)
    top = jnp.max(score, axis=-1, keepdims=True)
    expo = jnp.exp(score - top)
    total = jnp.sum(expo, axis=-1, keepdims=True)
    attn = jnp.einsum("hqk,khd->hqd", expo.astype(BF), value_pair, preferred_element_type=F32)
    attn_rows = (attn / total).astype(BF).transpose(1, 0, 2)
    lse = top + jnp.log(total)
    attn_flat = attn_rows.reshape(rows, heads * DV)

    def own(a):
        return lax.dynamic_slice_in_dim(a, t_id * piece, piece, 0)

    attn_full = tp_reduce_scatter(mdot(attn_flat, w_output).astype(BF), n_tp, 2, "attn_scatter")
    mid = own(x_float) + attn_full
    two_own = norm_rows(mid, gain_two).astype(BF)
    normed_two = gather_everywhere(two_own, n_tp, 3, "normed_two_gather").reshape(-1, width)

    probs = jax.nn.softmax(mdot(normed_two, w_router), axis=-1)
    first = slot(s_id, c_id) * local_experts
    hots = []
    for j in range(local_experts):
        chosen = jnp.any(routes_all == first + j, axis=1, keepdims=True)
        prob = jnp.sum(
            jnp.where(jnp.arange(experts, dtype=jnp.int32)[None, :] == first + j, probs, 0.0),
            axis=1,
            keepdims=True,
        )
        hots.append((chosen, jnp.where(chosen, prob, 0.0)))
    moe_part = None
    two_part = None
    pg_cols = []
    lanes = jnp.arange(LANES, dtype=jnp.int32)[None, :]
    grads_gate, grads_up, grads_down = [], [], []
    for j in range(local_experts + 1):
        shared = j == local_experts
        if shared:
            gate_act, up_act = dot_nt(normed_two, sg_t), dot_nt(normed_two, su_t)
            back = dot_nt(cot_all, sd)
        else:
            gate_act = mdot(normed_two, expert_gate[j])
            up_act = mdot(normed_two, expert_up[j])
            back = dot_nt(cot_all, expert_down[j])
        silu = jax.nn.silu(gate_act)
        hidden = silu * up_act
        if not shared:
            chosen, weight = hots[j]
            hidden_grad = back * weight
            route_grad = jnp.where(chosen, jnp.sum(hidden * back, axis=1, keepdims=True), 0.0)
            hidden = hidden * weight
            high = route_grad.astype(BF)
            low = (route_grad - high.astype(F32)).astype(BF)
            pg_cols.append(
                jnp.where(lanes == first + j, high, jnp.where(lanes == first + j + 64, low, jnp.zeros((), BF)))
            )
        else:
            hidden_grad = back
        hidden = hidden.astype(BF)
        gate_grad = (hidden_grad * up_act * silu_slope(gate_act)).astype(BF)
        up_grad = (hidden_grad * silu).astype(BF)
        if shared:
            y = mdot(hidden, sd)
            dn = mdot(gate_grad, sg_t) + mdot(up_grad, su_t)
            grads = [dot_tn(gate_grad, normed_two), dot_tn(up_grad, normed_two), dot_tn(hidden, cot_all)]
            shared_grads = [g.astype(BF) for g in grads]
        else:
            y = mdot(hidden, expert_down[j])
            dn = dot_nt(gate_grad, expert_gate[j]) + dot_nt(up_grad, expert_up[j])
            grads_gate.append(dot_tn(normed_two, gate_grad))
            grads_up.append(dot_tn(normed_two, up_grad))
            grads_down.append(dot_tn(hidden, cot_all))
        moe_part = y if moe_part is None else moe_part + y
        two_part = dn if two_part is None else two_part + dn
    pg_part = functools.reduce(jnp.add, pg_cols)
    part = jnp.concatenate(
        [moe_part.astype(BF), two_part.astype(BF), pg_part, jnp.zeros_like(pg_part)], axis=1
    ).reshape(8, rows, -1)
    summed = reduce_everywhere(part, n_tp, 4, "feed_forward_scatter")
    moe_out, two_grad = summed[:, :width], summed[:, width : 2 * width]
    prob_grad = summed[:, 2 * width : 2 * width + experts]
    prob_grad = prob_grad + summed[:, 2 * width + 64 : 2 * width + 64 + experts]
    out_own = mid + moe_out
    grad_expert_gate, grad_expert_up, grad_expert_down = (
        jnp.stack(g) for g in (grads_gate, grads_up, grads_down)
    )

    probs_own = jax.nn.softmax(mdot(two_own, w_router), axis=-1)
    logit_grad = (
        probs_own * (prob_grad - jnp.sum(probs_own * prob_grad, axis=-1, keepdims=True))
    ).astype(BF)
    two_grad = two_grad + dot_nt(logit_grad, w_router)
    mid_norm_grad, gain_two_terms = norm_back(mid, gain_two, two_grad)
    mid_grad = own(cotangent) + mid_norm_grad
    mid_pack = jnp.concatenate(
        [mid_grad.astype(BF), jnp.pad(logit_grad, ((0, 0), (0, LANES - experts)))], axis=1
    )
    (mid_pack,) = tp_all_gather((mid_pack,), n_tp, 5, "mid_grad_gather")
    mid_b = mid_pack[:, :width]

    out_grad = dot_nt(mid_b, w_output).reshape(rows, heads, DV)
    out_grad_b = out_grad.astype(BF)
    delta = jnp.sum(out_grad * attn_rows.astype(F32), axis=-1).T[..., None]
    prob = jnp.exp(score - lse)
    dprob = jnp.einsum("qhd,khd->hqk", out_grad_b, value_pair, preferred_element_type=F32)
    dscore = (prob * (dprob - delta)).astype(BF)
    nope_grad = jnp.einsum("hqk,khd->qhd", dscore, key_pair, preferred_element_type=F32) * scale
    rope_qgrad = jnp.einsum("hqk,kd->qhd", dscore, rope_pair, preferred_element_type=F32) * scale
    key_grad = jnp.einsum("hqk,qhd->khd", dscore, query_nope, preferred_element_type=F32) * scale
    value_grad = jnp.einsum(
        "hqk,qhd->khd", prob.astype(BF), out_grad_b, preferred_element_type=F32
    )
    rope_kgrad = jnp.einsum("hqk,qhd->kd", dscore, query_rope, preferred_element_type=F32) * scale
    kv_terms = jnp.concatenate(
        [
            jnp.concatenate([key_grad, value_grad], axis=-1).reshape(2 * rows, -1),
            jnp.pad(rope_kgrad, ((0, 0), (0, LANES - DR))),
        ],
        axis=1,
    )
    mine = lax.dynamic_slice_in_dim(kv_terms, c_id * rows, rows, 0)
    other = lax.dynamic_slice_in_dim(kv_terms, (1 - c_id) * rows, rows, 0).astype(BF)
    kv_sum = mine + ctx_swap(other, 6, "kv_grad_swap").astype(F32)
    kv_grad = kv_sum[:, : heads * (DN + DV)].astype(BF)
    rope_part = rotate_back(kv_sum[:, heads * (DN + DV) :][:, :DR], cosine, sine)
    rope_qback = rotate_back(rope_qgrad, cosine[:, None, :], sine[:, None, :])
    query_grad = jnp.concatenate([nope_grad, rope_qback], axis=-1).astype(BF).reshape(rows, -1)
    latent_part = dot_nt(kv_grad, w_expand)
    one_part = dot_nt(query_grad, w_query)
    back_part = jnp.concatenate(
        [one_part, latent_part, jnp.pad(rope_part, ((0, 0), (0, LANES - DR)))], axis=1
    ).astype(BF)
    back = tp_reduce_scatter(back_part, n_tp, 7, "attn_back_scatter")

    compressed = own(lax.dynamic_slice_in_dim(latent, c_id * rows, rows, 0))[:, :KVR]
    compressed_grad, gain_kv_terms = norm_back(compressed, gain_kv, back[:, width : width + KVR])
    latent_grad = jnp.concatenate(
        [compressed_grad, back[:, width + KVR : width + KVR + DR]], axis=1
    ).astype(BF)
    one_grad = back[:, :width] + dot_nt(latent_grad, w_latent)
    input_norm_grad, gain_one_terms = norm_back(own(x_float), gain_one, one_grad)
    input_own = mid_grad + input_norm_grad

    block_output, input_grad = tp_all_gather((out_own, input_own), n_tp, 8, "output_gather")
    lat_pack = jnp.pad(latent_grad, ((0, 0), (0, 5 * LANES - KVR - DR)))
    (latent_rows,) = tp_all_gather((lat_pack,), n_tp, 9, "latent_gather")
    latent_own = lax.dynamic_slice_in_dim(latent_pair, c_id * rows, rows, 0)
    head_pack = jnp.concatenate(
        [query_grad, kv_grad, attn_flat, latent_rows, mid_pack[:, width:]], axis=1
    )
    head_all, one_cols, lat_cols, mid_cols, sg_cols, su_cols, sd_cols = plane_exchange(
        (head_pack,), (normed_one, latent_own, mid_b, *shared_grads), (), n_tp, 10, "late_exchange"
    )
    head_all = head_all.reshape(8 * rows, -1)
    edges = [0, heads * (DN + DR), heads * (DN + DV), heads * DV, 5 * LANES, LANES]
    edges = [sum(edges[: i + 1]) for i in range(len(edges))]
    dq_all, dkv_all, attn_all, lat_all, logit_all = (
        head_all[:, a:b] for a, b in zip(edges[:-1], edges[1:])
    )
    one_cols = one_cols.reshape(8 * rows, -1)
    lat_cols = lat_cols.reshape(8 * rows, -1)
    mid_cols = mid_cols.reshape(8 * rows, -1)
    grad_query = dot_tn(one_cols, dq_all)
    grad_latent = dot_tn(one_cols, lat_all[:, : KVR + DR])
    grad_expand = dot_tn(lat_cols, dkv_all)
    grad_out_w = dot_tn(attn_all, mid_cols)
    two_cols = lax.dynamic_slice_in_dim(normed_two, s_id * shard_w, shard_w, 1)
    grad_router = dot_tn(two_cols, logit_all[:, :experts])
    grad_sgate = sg_cols.reshape(-1, shard_w).T.astype(F32)
    grad_sup = su_cols.reshape(-1, shard_w).T.astype(F32)
    grad_sdown = sd_cols.reshape(-1, shard_w).astype(F32)

    gains = jnp.concatenate(
        [
            jnp.sum(gain_one_terms, axis=0),
            jnp.sum(gain_two_terms, axis=0),
            jnp.sum(gain_kv_terms, axis=0),
            jnp.zeros((512,), F32),
        ]
    ).reshape(8, -1)
    gains = sum_everywhere(gains, n_tp, 11, "gain_sum").reshape(-1)
    grad_one = lax.dynamic_slice_in_dim(gains, s_id * shard_w, shard_w, 0)
    grad_two = lax.dynamic_slice_in_dim(gains, width + s_id * shard_w, shard_w, 0)
    grad_kv = lax.dynamic_slice_in_dim(gains, 2 * width + s_id * kv_w, kv_w, 0)
    return (
        block_output,
        input_grad,
        grad_one,
        grad_query,
        grad_latent,
        grad_kv,
        grad_expand,
        grad_out_w,
        grad_two,
        grad_router,
        grad_sgate,
        grad_sup,
        grad_sdown,
        grad_expert_gate,
        grad_expert_up,
        grad_expert_down,
    )


def send_rows(buffer):
    return lax.all_to_all(buffer, (SHARD, CTX), split_axis=0, concat_axis=0, tiled=True)


def return_rows(partial_value, slots):
    back_rows = lax.all_to_all(
        partial_value, (SHARD, CTX), split_axis=0, concat_axis=0, tiled=True
    )
    flat_back = back_rows.reshape(-1, back_rows.shape[-1])
    return flat_back[slots]


def per_device_general(
    block_input,
    norm1_gain,
    q_weight,
    kva_weight,
    kv_norm_gain,
    kvb_weight,
    out_weight,
    norm2_gain,
    router_weight,
    shared_gate,
    shared_up,
    shared_down,
    expert_gate,
    expert_up,
    expert_down,
    routes,
    cotangent,
):
    tok_rows = block_input.shape[0]
    head_count = q_weight.shape[1] // (DN + DR)
    score_scale = (DN + DR) ** (-0.5)
    (
        gain_one,
        w_query,
        w_latent,
        gain_kv,
        w_expand,
        w_output,
        gain_two,
        w_router,
        w_sgate,
        w_sup,
        w_sdown,
    ) = (
        lax.all_gather(norm1_gain, SHARD, axis=0, tiled=True),
        lax.all_gather(q_weight, SHARD, axis=0, tiled=True),
        lax.all_gather(kva_weight, SHARD, axis=0, tiled=True),
        lax.all_gather(kv_norm_gain, SHARD, axis=0, tiled=True),
        lax.all_gather(kvb_weight, SHARD, axis=0, tiled=True),
        lax.all_gather(out_weight, SHARD, axis=1, tiled=True),
        lax.all_gather(norm2_gain, SHARD, axis=0, tiled=True),
        lax.all_gather(router_weight, SHARD, axis=0, tiled=True),
        lax.all_gather(shared_gate, SHARD, axis=0, tiled=True),
        lax.all_gather(shared_up, SHARD, axis=0, tiled=True),
        lax.all_gather(shared_down, SHARD, axis=1, tiled=True),
    )
    block_index = lax.axis_index(CTX)
    cosine, sine_table = rope_tables(tok_rows, (block_index * tok_rows).astype(jnp.float32))
    x_float = block_input.astype(jnp.float32)
    normed_one = norm_rows(x_float, gain_one).astype(jnp.bfloat16)
    query = mdot(normed_one, w_query).reshape(tok_rows, head_count, DN + DR)
    query_rot = rotate(query[..., DN:], cosine[:, None, :], sine_table[:, None, :])
    query = jnp.concatenate([query[..., :DN], query_rot], axis=-1).astype(jnp.bfloat16)
    query_nope = query[..., :DN]
    query_rope = query[..., DN:]
    latent = mdot(normed_one, w_latent)
    compressed = latent[:, :KVR]
    latent_n = norm_rows(compressed, gain_kv).astype(jnp.bfloat16)
    rope_key = rotate(latent[:, KVR:], cosine, sine_table).astype(jnp.bfloat16)
    first_piece = mdot(latent_n, w_expand).astype(jnp.bfloat16)
    gathered, rope_all = (
        lax.all_gather(first_piece, CTX, axis=0, tiled=True),
        lax.all_gather(rope_key, CTX, axis=0, tiled=True),
    )
    query_pos = block_index * tok_rows + jnp.arange(tok_rows, dtype=jnp.int32)

    def scores_at(block_id):
        blk_start = block_id * tok_rows
        kv_block = lax.dynamic_slice_in_dim(gathered, blk_start, tok_rows, 0).reshape(
            tok_rows, head_count, DN + DV
        )
        rope_block = lax.dynamic_slice_in_dim(rope_all, blk_start, tok_rows, 0)
        score = jnp.einsum(
            "qhd,khd->hqk", query_nope, kv_block[..., :DN], preferred_element_type=jnp.float32
        )
        score = score + jnp.einsum(
            "qhd,kd->hqk", query_rope, rope_block, preferred_element_type=jnp.float32
        )
        score = score * score_scale
        key_pos = blk_start + jnp.arange(tok_rows, dtype=jnp.int32)
        score = jnp.where(key_pos[None, None, :] <= query_pos[None, :, None], score, NEG)
        return (score, kv_block, rope_block)

    def forward_block(block_id, carry):
        run_max, run_sum, weighted = carry
        score, kv_block, rope_block = scores_at(block_id)
        new_max = jnp.maximum(run_max, jnp.max(score, axis=-1))
        factor = jnp.exp(run_max - new_max)
        expo = jnp.exp(score - new_max[..., None])
        run_sum = factor * run_sum + jnp.sum(expo, axis=-1)
        weighted = factor[..., None] * weighted + jnp.einsum(
            "hqk,khd->hqd",
            expo.astype(jnp.bfloat16),
            kv_block[..., DN:],
            preferred_element_type=jnp.float32,
        )
        return (new_max, run_sum, weighted)

    start_state = (
        jnp.full((head_count, tok_rows), NEG, jnp.float32),
        jnp.zeros((head_count, tok_rows), jnp.float32),
        jnp.zeros((head_count, tok_rows, DV), jnp.float32),
    )
    run_max, run_sum, weighted = lax.fori_loop(0, block_index + 1, forward_block, start_state)
    lse = run_max + jnp.log(run_sum)
    attn_rows = (weighted / run_sum[..., None]).astype(jnp.bfloat16).transpose(1, 0, 2)
    attn_flat = attn_rows.reshape(tok_rows, head_count * DV)
    attn_full = lax.psum(mdot(attn_flat, w_output), TP)
    mid = x_float + attn_full
    normed_two = norm_rows(mid, gain_two).astype(jnp.bfloat16)
    probs = jax.nn.softmax(mdot(normed_two, w_router), axis=-1)
    experts = probs.shape[1]
    topk = routes.shape[1]
    picks = (routes[:, :, None] == jnp.arange(experts, dtype=jnp.int32)[None, None, :]).astype(
        jnp.float32
    )
    route_w = jnp.sum(picks * probs[:, None, :], axis=-1)
    shared_a = mdot(normed_two, w_sgate)
    shared_b = mdot(normed_two, w_sup)
    shared_h = (jax.nn.silu(shared_a) * shared_b).astype(jnp.bfloat16)
    shared_y = mdot(shared_h, w_sdown)
    capacity = 2 * tok_rows * topk // experts
    owners = lax.axis_size((SHARD, CTX))
    local_experts = expert_gate.shape[0]
    width = normed_two.shape[1]
    flat_routes = routes.reshape(-1)
    onehot = (flat_routes[:, None] == jnp.arange(experts, dtype=jnp.int32)[None, :]).astype(
        jnp.int32
    )
    rank = jnp.sum((jnp.cumsum(onehot, axis=0) - 1) * onehot, axis=1)
    slots = flat_routes * capacity + rank
    source_row = jnp.arange(tok_rows * topk, dtype=jnp.int32) // topk
    send_buffer = (
        jnp.zeros((experts * capacity, width), jnp.bfloat16).at[slots].set(normed_two[source_row])
    )
    received = send_rows(send_buffer.reshape(owners, local_experts * capacity, width)).reshape(
        owners, local_experts, capacity, width
    )
    gate_act = jnp.einsum(
        "gecd,edf->gecf", received, expert_gate, preferred_element_type=jnp.float32
    )
    up_act = jnp.einsum("gecd,edf->gecf", received, expert_up, preferred_element_type=jnp.float32)
    hidden = (jax.nn.silu(gate_act) * up_act).astype(jnp.bfloat16)
    expert_y = jnp.einsum("gecf,efd->gecd", hidden, expert_down, preferred_element_type=jnp.float32)
    routed_out = return_rows(
        expert_y.reshape(owners, local_experts * capacity, width), slots
    ).reshape(tok_rows, topk, width)
    routed_part = jnp.sum(route_w[:, :, None] * routed_out, axis=1) + shared_y
    weight_part = jnp.sum(routed_out * cotangent[:, None, :], axis=-1)
    moe_out, route_grad = lax.psum((routed_part, weight_part), TP)
    block_output = mid + moe_out
    cot_b = cotangent.astype(jnp.bfloat16)
    routed_grad = (
        (route_w[:, :, None] * cotangent[:, None, :])
        .astype(jnp.bfloat16)
        .reshape(tok_rows * topk, width)
    )
    grad_buffer = jnp.zeros((experts * capacity, width), jnp.bfloat16).at[slots].set(routed_grad)
    grad_recv = send_rows(grad_buffer.reshape(owners, local_experts * capacity, width)).reshape(
        owners, local_experts, capacity, width
    )
    hidden_grad = jnp.einsum(
        "gecd,efd->gecf", grad_recv, expert_down, preferred_element_type=jnp.float32
    )
    gate_grad = (hidden_grad * up_act * silu_slope(gate_act)).astype(jnp.bfloat16)
    up_grad = (hidden_grad * jax.nn.silu(gate_act)).astype(jnp.bfloat16)
    grad_expert_down = jnp.einsum(
        "gecf,gecd->efd", hidden, grad_recv, preferred_element_type=jnp.float32
    )
    grad_expert_gate = jnp.einsum(
        "gecd,gecf->edf", received, gate_grad, preferred_element_type=jnp.float32
    )
    grad_expert_up = jnp.einsum(
        "gecd,gecf->edf", received, up_grad, preferred_element_type=jnp.float32
    )
    row_grad = jnp.einsum(
        "gecf,edf->gecd", gate_grad, expert_gate, preferred_element_type=jnp.float32
    )
    row_grad = row_grad + jnp.einsum(
        "gecf,edf->gecd", up_grad, expert_up, preferred_element_type=jnp.float32
    )
    routed_back = return_rows(
        row_grad.reshape(owners, local_experts * capacity, width), slots
    ).reshape(tok_rows, topk, width)
    shared_grad = jnp.einsum("td,fd->tf", cot_b, w_sdown, preferred_element_type=jnp.float32)
    sgate_grad = (shared_grad * shared_b * silu_slope(shared_a)).astype(jnp.bfloat16)
    sup_grad = (shared_grad * jax.nn.silu(shared_a)).astype(jnp.bfloat16)
    grad_sdown = jnp.einsum("tf,td->fd", shared_h, cot_b, preferred_element_type=jnp.float32)
    grad_sgate = jnp.einsum("td,tf->df", normed_two, sgate_grad, preferred_element_type=jnp.float32)
    grad_sup = jnp.einsum("td,tf->df", normed_two, sup_grad, preferred_element_type=jnp.float32)
    two_part = jnp.sum(routed_back, axis=1)
    two_part = two_part + jnp.einsum(
        "tf,df->td", sgate_grad, w_sgate, preferred_element_type=jnp.float32
    )
    two_part = two_part + jnp.einsum(
        "tf,df->td", sup_grad, w_sup, preferred_element_type=jnp.float32
    )
    two_grad = lax.psum(two_part, TP)
    prob_grad = jnp.sum(picks * route_grad[:, :, None], axis=1)
    logit_grad = (probs * (prob_grad - jnp.sum(probs * prob_grad, axis=-1, keepdims=True))).astype(
        jnp.bfloat16
    )
    grad_router = jnp.einsum(
        "td,te->de", normed_two, logit_grad, preferred_element_type=jnp.float32
    )
    two_grad = two_grad + jnp.einsum(
        "te,de->td", logit_grad, w_router, preferred_element_type=jnp.float32
    )
    _, norm_two_back = jax.vjp(norm_rows, mid, gain_two.astype(jnp.float32))
    mid_norm_grad, grad_gain_two = norm_two_back(two_grad)
    mid_grad = cotangent + mid_norm_grad
    mid_b = mid_grad.astype(jnp.bfloat16)
    grad_out_w = jnp.einsum("tj,td->jd", attn_flat, mid_b, preferred_element_type=jnp.float32)
    out_grad = jnp.einsum("td,jd->tj", mid_b, w_output, preferred_element_type=jnp.float32).reshape(
        tok_rows, head_count, DV
    )
    out_grad_b = out_grad.astype(jnp.bfloat16)
    delta = jnp.sum(out_grad * attn_rows.astype(jnp.float32), axis=-1).T
    key_count = gathered.shape[0]
    term_width = head_count * (DN + DV + DR)

    def back_block(block_id, carry):
        nope_grad, rope_qgrad, terms = carry
        score, kv_block, rope_block = scores_at(block_id)
        probs_blk = jnp.exp(score - lse[..., None])
        prob_b = probs_blk.astype(jnp.bfloat16)
        dprob = jnp.einsum(
            "qhd,khd->hqk", out_grad_b, kv_block[..., DN:], preferred_element_type=jnp.float32
        )
        dscore = (probs_blk * (dprob - delta[..., None])).astype(jnp.bfloat16)
        nope_grad = (
            nope_grad
            + jnp.einsum(
                "hqk,khd->qhd", dscore, kv_block[..., :DN], preferred_element_type=jnp.float32
            )
            * score_scale
        )
        rope_qgrad = (
            rope_qgrad
            + jnp.einsum("hqk,kd->qhd", dscore, rope_block, preferred_element_type=jnp.float32)
            * score_scale
        )
        key_nope_grad = (
            jnp.einsum("hqk,qhd->khd", dscore, query_nope, preferred_element_type=jnp.float32)
            * score_scale
        )
        key_rope_grad = (
            jnp.einsum("hqk,qhd->khd", dscore, query_rope, preferred_element_type=jnp.float32)
            * score_scale
        )
        value_grad = jnp.einsum(
            "hqk,qhd->khd", prob_b, out_grad_b, preferred_element_type=jnp.float32
        )
        block_terms = jnp.concatenate([key_nope_grad, value_grad, key_rope_grad], axis=-1).reshape(
            tok_rows, term_width
        )
        terms = lax.dynamic_update_slice_in_dim(terms, block_terms, block_id * tok_rows, 0)
        return (nope_grad, rope_qgrad, terms)

    back_init = (
        jnp.zeros((tok_rows, head_count, DN), jnp.float32),
        jnp.zeros((tok_rows, head_count, DR), jnp.float32),
        jnp.zeros((key_count, term_width), jnp.float32),
    )
    nope_grad, rope_qgrad, terms = lax.fori_loop(0, block_index + 1, back_block, back_init)
    key_terms = lax.psum_scatter(terms, CTX, scatter_dimension=0, tiled=True).reshape(
        tok_rows, head_count, DN + DV + DR
    )
    kv_grad = (
        key_terms[..., : DN + DV].reshape(tok_rows, head_count * (DN + DV)).astype(jnp.bfloat16)
    )
    rope_grad = rotate_back(jnp.sum(key_terms[..., DN + DV :], axis=1), cosine, sine_table)
    grad_expand = jnp.einsum("ti,tj->ij", latent_n, kv_grad, preferred_element_type=jnp.float32)
    latent_part = jnp.einsum("tj,ij->ti", kv_grad, w_expand, preferred_element_type=jnp.float32)
    rope_qback = rotate_back(rope_qgrad, cosine[:, None, :], sine_table[:, None, :])
    query_grad = (
        jnp.concatenate([nope_grad, rope_qback], axis=-1)
        .astype(jnp.bfloat16)
        .reshape(tok_rows, head_count * (DN + DR))
    )
    grad_query = jnp.einsum("td,tj->dj", normed_one, query_grad, preferred_element_type=jnp.float32)
    normed_part = jnp.einsum("tj,dj->td", query_grad, w_query, preferred_element_type=jnp.float32)
    latent_sum, normed_sum = lax.psum(
        (jnp.concatenate([latent_part, rope_grad], axis=-1), normed_part), TP
    )
    _, kv_back = jax.vjp(norm_rows, compressed, gain_kv.astype(jnp.float32))
    compressed_grad, grad_gain_kv = kv_back(latent_sum[:, :KVR])
    latent_grad = jnp.concatenate([compressed_grad, latent_sum[:, KVR:]], axis=-1).astype(
        jnp.bfloat16
    )
    grad_latent = jnp.einsum(
        "td,tl->dl", normed_one, latent_grad, preferred_element_type=jnp.float32
    )
    one_grad = normed_sum + jnp.einsum(
        "tl,dl->td", latent_grad, w_latent, preferred_element_type=jnp.float32
    )
    _, one_back = jax.vjp(norm_rows, x_float, gain_one.astype(jnp.float32))
    input_norm_grad, grad_gain_one = one_back(one_grad)
    input_grad = mid_grad + input_norm_grad
    (
        red_one,
        red_query,
        red_latent,
        red_kv,
        red_expand,
        red_output,
        red_two,
        red_router,
        red_sgate,
        red_sup,
        red_sdown,
    ) = (
        lax.psum_scatter(grad_gain_one, SHARD, scatter_dimension=0, tiled=True),
        lax.psum_scatter(grad_query, SHARD, scatter_dimension=0, tiled=True),
        lax.psum_scatter(grad_latent, SHARD, scatter_dimension=0, tiled=True),
        lax.psum_scatter(grad_gain_kv, SHARD, scatter_dimension=0, tiled=True),
        lax.psum_scatter(grad_expand, SHARD, scatter_dimension=0, tiled=True),
        lax.psum_scatter(grad_out_w, SHARD, scatter_dimension=1, tiled=True),
        lax.psum_scatter(grad_gain_two, SHARD, scatter_dimension=0, tiled=True),
        lax.psum_scatter(grad_router, SHARD, scatter_dimension=0, tiled=True),
        lax.psum_scatter(grad_sgate, SHARD, scatter_dimension=0, tiled=True),
        lax.psum_scatter(grad_sup, SHARD, scatter_dimension=0, tiled=True),
        lax.psum_scatter(grad_sdown, SHARD, scatter_dimension=1, tiled=True),
    )
    (
        sum_one,
        sum_query,
        sum_latent,
        sum_kv,
        sum_expand,
        sum_output,
        sum_two,
        sum_router,
        sum_sgate,
        sum_sup,
        sum_sdown,
    ) = lax.psum(
        (
            red_one,
            red_query,
            red_latent,
            red_kv,
            red_expand,
            red_output,
            red_two,
            red_router,
            red_sgate,
            red_sup,
            red_sdown,
        ),
        CTX,
    )
    return (
        block_output,
        input_grad,
        sum_one,
        sum_query,
        sum_latent,
        sum_kv,
        sum_expand,
        sum_output,
        sum_two,
        sum_router,
        sum_sgate,
        sum_sup,
        sum_sdown,
        grad_expert_gate,
        grad_expert_up,
        grad_expert_down,
    )


def solution(mesh):
    in_specs = (
        P((SHARD, CTX), None),
        P(SHARD),
        P(SHARD, TP),
        P(SHARD, None),
        P(SHARD),
        P(SHARD, TP),
        P(TP, SHARD),
        P(SHARD),
        P(SHARD, None),
        P(SHARD, TP),
        P(SHARD, TP),
        P(TP, SHARD),
        P((SHARD, CTX), None, TP),
        P((SHARD, CTX), None, TP),
        P((SHARD, CTX), TP, None),
        P((SHARD, CTX), None),
        P((SHARD, CTX), None),
    )
    out_specs = (
        P((SHARD, CTX), None),
        P((SHARD, CTX), None),
        P(SHARD),
        P(SHARD, TP),
        P(SHARD, None),
        P(SHARD),
        P(SHARD, TP),
        P(TP, SHARD),
        P(SHARD),
        P(SHARD, None),
        P(SHARD, TP),
        P(SHARD, TP),
        P(TP, SHARD),
        P((SHARD, CTX), None, TP),
        P((SHARD, CTX), None, TP),
        P((SHARD, CTX), TP, None),
    )
    routed = mesh.shape[SHARD] == 4 and mesh.shape[CTX] == 2 and mesh.shape[TP] == 4
    return jax.shard_map(
        per_device if routed else per_device_general, mesh=mesh, in_specs=in_specs, out_specs=out_specs, check_vma=False
    )
```

```python
import functools

import jax
import jax.numpy as jnp
from jax import lax
from jax.experimental import pallas as pl
from jax.experimental.pallas import tpu as pltpu
from jax.sharding import PartitionSpec as P

DN = 128
DR = 64
DV = 128
KVR = 512
LANES = 128
SHARD, CTX, TP = "shard", "ctx", "tp"

EPS = 1e-06
NEG = -1e30

BF = jnp.bfloat16
F32 = jnp.float32
MESH = pl.DeviceIdType.MESH
ANY = pl.ANY
VMEM = pltpu.VMEM


def norm_rows(value, gain):
    factor = lax.rsqrt(jnp.mean(value * value, axis=-1, keepdims=True) + EPS)
    return value * factor * gain.astype(F32)


def norm_back(value, gain, grad):
    factor = lax.rsqrt(jnp.mean(value * value, axis=-1, keepdims=True) + EPS)
    scaled = grad * gain.astype(F32)
    inner = jnp.mean(scaled * value, axis=-1, keepdims=True)
    return factor * (scaled - value * (factor * factor * inner)), grad * value * factor


def rope_tables(count, offset):
    half_size = DR // 2
    position = jnp.arange(count, dtype=F32) + offset
    freqs = 10000.0 ** (-(jnp.arange(half_size, dtype=F32) * 2.0 / DR))
    angle = position[:, None] * freqs[None, :]
    return (jnp.cos(angle), jnp.sin(angle))


def rotate(value, cosine, sine_table):
    half_size = DR // 2
    first = value[..., :half_size]
    second = value[..., half_size:]
    return jnp.concatenate(
        [first * cosine - second * sine_table, first * sine_table + second * cosine], axis=-1
    )


def rotate_back(grad, cosine, sine_table):
    half_size = DR // 2
    first = grad[..., :half_size]
    second = grad[..., half_size:]
    return jnp.concatenate(
        [first * cosine + second * sine_table, second * cosine - first * sine_table], axis=-1
    )


def silu_slope(value):
    sigmoid = jax.nn.sigmoid(value)
    return sigmoid * (1.0 + value * (1.0 - sigmoid))


def mdot(left, right):
    return jnp.dot(left, right, preferred_element_type=F32)


def dot_nt(left, right):
    return lax.dot_general(left, right, (((1,), (1,)), ((), ())), preferred_element_type=F32)


def dot_tn(left, right):
    return lax.dot_general(left, right, (((0,), (0,)), ((), ())), preferred_element_type=F32)


class Place:
    def __init__(self, n_tp):
        self.s = lax.axis_index(SHARD)
        self.c = lax.axis_index(CTX)
        self.t = lax.axis_index(TP)
        self.core = lax.rem(self.s, 2)
        self.y = self.s // 2
        self.n_tp = n_tp

    def at(self, s, c, t):
        return {SHARD: s, CTX: c, TP: t}

    @property
    def over_x(self):
        return self.at(self.s, 1 - self.c, self.t)

    @property
    def over_y(self):
        return self.at(lax.rem(self.s + 2, 4), self.c, self.t)

    @property
    def over_core(self):
        return self.at(self.s + 1 - 2 * self.core, self.c, self.t)

    def along(self, step):
        return self.at(self.s, self.c, lax.rem(self.t + step + self.n_tp, self.n_tp))

    def flip(self, dy, dcore, dx):
        y = self.y + dy * (1 - 2 * self.y)
        core = self.core + dcore * (1 - 2 * self.core)
        x = self.c + dx * (1 - 2 * self.c)
        return self.at(2 * y + core, x, self.t)


def slot(s, c):
    return 2 * s + c


class Net:
    def __init__(self, send, recv, local):
        self.send, self.recv, self.local = send, recv, local
        self.puts, self.locals = [], []
        self.n_local = 0

    def put(self, src, dst, to):
        i = len(self.puts)
        copy = pltpu.make_async_remote_copy(
            src_ref=src,
            dst_ref=dst,
            send_sem=self.send.at[i],
            recv_sem=self.recv.at[i],
            device_id=to,
            device_id_type=MESH,
        )
        copy.start()
        self.puts.append(copy)
        return copy

    def move(self, src, dst):
        copy = pltpu.make_async_copy(src, dst, self.local.at[self.n_local])
        self.n_local += 1
        copy.start()
        return copy

    def finish(self):
        for copy in self.puts:
            copy.wait_send()


def greet(peers):
    barrier = pltpu.get_barrier_semaphore()
    for peer in peers:
        pl.semaphore_signal(barrier, inc=1, device_id=peer, device_id_type=MESH)
    pl.semaphore_wait(barrier, len(peers))


def comm_call(body, ins, outs, scratch, n_put, n_local, collective_id, name, in_space, out_space):
    return pl.pallas_call(
        body,
        out_shape=tuple(jax.ShapeDtypeStruct(shape, dtype) for shape, dtype in outs),
        in_specs=[pl.BlockSpec(memory_space=space) for space in in_space],
        out_specs=tuple(pl.BlockSpec(memory_space=space) for space in out_space),
        scratch_shapes=[
            *scratch,
            pltpu.SemaphoreType.DMA((n_put,)),
            pltpu.SemaphoreType.DMA((n_put,)),
            pltpu.SemaphoreType.DMA((max(n_local, 1),)),
        ],
        compiler_params=pltpu.CompilerParams(
            collective_id=collective_id, has_side_effects=True, vmem_limit_bytes=60 * 2**20
        ),
        name=name,
    )(*ins)


def start_gather(weights, small, block, n_tp):
    shapes = [w.shape for w in weights]

    def body(*refs):
        n = len(shapes)
        w_in, (small_in, x_in) = refs[:n], refs[n : n + 2]
        w_out, (small_out, x_out) = refs[n + 2 : 2 * n + 2], refs[2 * n + 2 : 2 * n + 4]
        bounce = refs[2 * n + 4 : 3 * n + 6]
        send, recv, local = refs[3 * n + 6 :]
        me = Place(n_tp)
        net = Net(send, recv, local)
        greet([me.over_x, me.over_y, me.over_core])

        def half(ref, index, which, rows):
            return ref.at[index, pl.ds(which * (rows // 2), rows // 2)]

        other = lax.rem(me.s + 2, 4)
        loads = [net.move(src, b) for src, b in zip((*w_in, small_in, x_in), bounce)]
        from_y, own = [], []
        for ref, out, shape in zip(w_in, w_out, shapes):
            rows = shape[0]
            from_y.append(
                net.put(ref.at[pl.ds(me.c * (rows // 2), rows // 2)], half(out, me.s, me.c, rows), me.over_y)
            )
            if ref is w_in[0]:
                wait_x = net.put(x_in, x_out.at[me.c], me.over_x)
        for ref, out in zip(w_in, w_out):
            own.append(net.put(ref, out.at[me.s], me.over_core))
        small_y = net.put(small_in, small_out.at[me.s], me.over_y)
        small_c = net.put(small_in, small_out.at[me.s], me.over_core)
        stores = []
        outs = [o.at[me.s] for o in (*w_out, small_out)] + [x_out.at[me.c]]
        for load, b, out in zip(loads, bounce, outs):
            load.wait()
            stores.append(net.move(b, out))
        from_x, relays = [], []
        for got, out, shape in zip(from_y, w_out, shapes):
            rows = shape[0]
            got.wait_recv()
            piece = half(out, other, me.c, rows)
            from_x.append(net.put(piece, piece, me.over_x))
            relays.append(net.put(piece, piece, me.over_core))
        small_y.wait_recv()
        relays.append(net.put(small_out.at[other], small_out.at[other], me.over_core))
        for got, out, shape in zip(from_x, w_out, shapes):
            rows = shape[0]
            got.wait_recv()
            piece = half(out, other, 1 - me.c, rows)
            relays.append(net.put(piece, piece, me.over_core))
        wait_x.wait_recv()
        small_c.wait_recv()
        for got in own + relays:
            got.wait_recv()
        for store in stores:
            store.wait()
        net.finish()

    n = len(weights)
    outs = [((4, *w.shape), BF) for w in weights] + [((4, *small.shape), small.dtype), ((2, *block.shape), BF)]
    return comm_call(
        body,
        (*weights, small, block),
        outs,
        [VMEM(w.shape, w.dtype) for w in (*weights, small, block)],
        5 * n + 4,
        2 * n + 4,
        0,
        "start_gather",
        [ANY] * (n + 2),
        [ANY] * (n + 2),
    )


def tp_reduce_scatter(part, n_tp, collective_id, name):
    rows, width = part.shape
    piece = rows // n_tp

    def body(in_ref, out_ref, got, send, recv, local):
        me = Place(n_tp)
        net = Net(send, recv, local)
        greet([me.along(k) for k in range(1, n_tp)])
        waits = []
        for k in range(1, n_tp):
            to = lax.rem(me.t + k, n_tp)
            waits.append(
                net.put(in_ref.at[pl.ds(to * piece, piece)], got.at[k - 1], me.along(k))
            )
        for wait in waits:
            wait.wait_recv()
        total = in_ref[pl.ds(pl.multiple_of(me.t * piece, piece), piece), :].astype(F32)
        for k in range(1, n_tp):
            total = total + got[k - 1].astype(F32)
        out_ref[...] = total
        net.finish()

    return comm_call(
        body,
        (part,),
        [((piece, width), F32)],
        [VMEM((n_tp - 1, piece, width), BF)],
        n_tp - 1,
        0,
        collective_id,
        name,
        [VMEM],
        [VMEM],
    )[0]


def tp_ring(net, me, own, out, base):
    piece = own.shape[0]
    half = piece // 2

    def rows(p, which=None):
        start = base + p * piece
        if which is None:
            return out.at[pl.ds(start, piece)]
        return out.at[pl.ds(start + which * half, half)]

    right, left = me.along(1), me.along(-1)
    p_left, p_right = lax.rem(me.t + 3, 4), lax.rem(me.t + 1, 4)
    far = lax.rem(me.t + 2, 4)
    to_right = net.put(own, rows(me.t), right)
    to_left = net.put(own, rows(me.t), left)
    to_right.wait_recv()
    hop_right = net.put(rows(p_left, 0), rows(p_left, 0), right)
    yield p_left
    to_left.wait_recv()
    hop_left = net.put(rows(p_right, 1), rows(p_right, 1), left)
    yield p_right
    hop_right.wait_recv()
    hop_left.wait_recv()
    yield far


def tp_all_gather(pieces, n_tp, collective_id, name):
    def body(*refs):
        n = len(pieces)
        ins, outs, (send, recv, local) = refs[:n], refs[n : 2 * n], refs[2 * n :]
        me = Place(n_tp)
        net = Net(send, recv, local)
        greet([me.along(1), me.along(-1)])
        rings = []
        for src, dst in zip(ins, outs):
            size = src.shape[0]
            rings.append(tp_ring(net, me, src, dst, 0))
        for _ in range(3):
            for ring in rings:
                next(ring)
        for src, dst in zip(ins, outs):
            size = src.shape[0]
            dst[pl.ds(pl.multiple_of(me.t * size, size), size), :] = src[...]
        net.finish()

    return comm_call(
        body,
        pieces,
        [((n_tp * p.shape[0], p.shape[1]), p.dtype) for p in pieces],
        [],
        4 * len(pieces),
        0,
        collective_id,
        name,
        [VMEM] * len(pieces),
        [VMEM] * len(pieces),
    )


def relay_chunks(net, me, out, chunks):
    g_x, g_y = slot(me.s, 1 - me.c), slot(lax.rem(me.s + 2, 4), me.c)
    g_d = slot(lax.rem(me.s + 2, 4), 1 - me.c)
    first = 1 - me.core
    relay_slot = first * g_x + me.core * g_y
    relay_to = me.flip(first, 0, me.core)
    diags, waits = [], []
    for from_x, from_y, (start, size) in chunks:
        from_x.wait_recv()
        from_y.wait_recv()
        src = out.at[relay_slot, pl.ds(start, size)]
        diags.append(net.put(src, src, relay_to))
        for g in (g_x, g_y):
            piece = out.at[g, pl.ds(start, size)]
            waits.append(net.put(piece, piece, me.over_core))
    for diag, (_, _, (start, size)) in zip(diags, chunks):
        diag.wait_recv()
        piece = out.at[g_d, pl.ds(start, size)]
        waits.append(net.put(piece, piece, me.over_core))
    return waits


def gather_everywhere(own, n_tp, collective_id, name):
    piece, width = own.shape

    def body(in_ref, out_ref, bounce, send, recv, local):
        me = Place(n_tp)
        net = Net(send, recv, local)
        greet([me.over_x, me.over_y, me.over_core, me.along(1), me.along(-1)])
        load = net.move(in_ref, bounce)
        g_me = slot(me.s, me.c)
        chunks, cores = [], []

        def spread(src, p):
            dst = out_ref.at[g_me, pl.ds(p * piece, piece)]
            from_x = net.put(src, dst, me.over_x)
            from_y = net.put(src, dst, me.over_y)
            cores.append(net.put(src, dst, me.over_core))
            chunks.append((from_x, from_y, (p * piece, piece)))

        spread(in_ref, me.t)
        ring = tp_ring(net, me, in_ref, out_ref.at[g_me], 0)
        load.wait()
        store = net.move(bounce, out_ref.at[g_me, pl.ds(me.t * piece, piece)])
        for p in ring:
            spread(out_ref.at[g_me, pl.ds(p * piece, piece)], p)
        waits = cores + relay_chunks(net, me, out_ref, chunks)
        for wait in waits:
            wait.wait_recv()
        store.wait()
        net.finish()

    return comm_call(
        body,
        (own,),
        [((8, n_tp * piece, width), own.dtype)],
        [VMEM(own.shape, own.dtype)],
        4 * 7 + 4,
        2,
        collective_id,
        name,
        [ANY],
        [ANY],
    )[0]


def plane_exchange(gathers, columns, rows88, n_tp, collective_id, name, n_chunk=4):
    ng, nc, nr = len(gathers), len(columns), len(rows88)
    ins = (*gathers, *columns, *rows88)

    def body(*refs):
        n = ng + nc + nr
        src, dst, bounce = refs[:n], refs[n : 2 * n], refs[2 * n : 3 * n]
        send, recv, local = refs[3 * n :]
        me = Place(n_tp)
        net = Net(send, recv, local)
        flips = [(dy, dk, dx) for dy in (0, 1) for dk in (0, 1) for dx in (0, 1)][1:]
        if nc or nr:
            greet([me.flip(*f) for f in flips])
        else:
            greet([me.over_x, me.over_y, me.over_core])
        g_me = slot(me.s, me.c)
        loads, waits, work = [], [], []
        for i in range(n):
            s, d, b = src[i], dst[i], bounce[i]
            if i < ng:
                rows = s.shape[0]
                size = rows // n_chunk
                chunks = []
                for j in range(n_chunk):
                    part = s.at[pl.ds(j * size, size)]
                    to = d.at[g_me, pl.ds(j * size, size)]
                    chunks.append((net.put(part, to, me.over_x), net.put(part, to, me.over_y), (j * size, size)))
                    waits.append(net.put(part, to, me.over_core))
                work.append((d, chunks))
                loads.append((net.move(s, b), b, d.at[g_me]))
            elif i < ng + nc:
                w = s.shape[1] // 4
                for f in flips:
                    peer = me.flip(*f)
                    part = s.at[:, pl.ds(pl.multiple_of(peer[SHARD] * w, LANES), w)]
                    waits.append(net.put(part, d.at[g_me], peer))
                part = s.at[:, pl.ds(pl.multiple_of(me.s * w, LANES), w)]
                loads.append((net.move(part, b), b, d.at[g_me]))
            else:
                h, w = s.shape[0] // 8, s.shape[1]
                to = d.at[:, pl.ds(pl.multiple_of(me.s * w, LANES), w)]
                for f in ((0, 1, 0), (1, 0, 0), (1, 1, 0)):
                    peer = me.flip(*f)
                    row = pl.multiple_of(slot(peer[SHARD], peer[CTX]) * h, 8)
                    waits.append(net.put(s.at[pl.ds(row, h)], to, peer))
                row = pl.multiple_of(g_me * h, 8)
                loads.append((net.move(s.at[pl.ds(row, h)], b), b, to))
        stores = []
        for load, b, to in loads:
            load.wait()
            stores.append(net.move(b, to))
        for d, chunks in work:
            waits += relay_chunks(net, me, d, chunks)
        for wait in waits:
            wait.wait_recv()
        for store in stores:
            store.wait()
        net.finish()

    outs, scratch = [], []
    for a in gathers:
        outs.append(((8, *a.shape), a.dtype))
        scratch.append(VMEM(a.shape, a.dtype))
    for a in columns:
        outs.append(((8, a.shape[0], a.shape[1] // 4), a.dtype))
        scratch.append(VMEM((a.shape[0], a.shape[1] // 4), a.dtype))
    for a in rows88:
        outs.append(((a.shape[0] // 8, a.shape[1] * 4), a.dtype))
        scratch.append(VMEM((a.shape[0] // 8, a.shape[1]), a.dtype))
    return comm_call(
        body,
        ins,
        outs,
        scratch,
        ng * 7 * n_chunk + nc * 7 + nr * 3,
        2 * len(ins),
        collective_id,
        name,
        [ANY] * len(ins),
        [ANY] * len(ins),
    )


def ctx_swap(block, collective_id, name):
    def body(in_ref, out_ref, send, recv, local):
        me = Place(1)
        net = Net(send, recv, local)
        greet([me.over_x])
        net.put(in_ref, out_ref, me.over_x).wait_recv()
        net.finish()

    return comm_call(
        body, (block,), [(block.shape, block.dtype)], [], 1, 0, collective_id, name, [ANY], [ANY]
    )[0]


def reduce_everywhere(part, n_tp, collective_id, name):
    _, rows, width = part.shape
    half = width // 2
    piece = rows // n_tp
    step = 16

    def body(in_ref, out_ref, mine, rc, rx, ry, q0, q1, r0, r1, last, got, send, recv, local):
        me = Place(n_tp)
        net = Net(send, recv, local)
        greet([me.over_x, me.over_y, me.over_core] + [me.along(k) for k in range(1, n_tp)])
        a, b = pl.ds(0, half), pl.ds(half, half)
        order = [(1, 1), (0, 1), (1, 0), (0, 0)]
        pairs = []
        for dy, dx in order:
            y, x = me.y + dy * (1 - 2 * me.y), me.c + dx * (1 - 2 * me.c)
            pairs.append((2 * y + x, slot(2 * y + me.core, x), slot(2 * y + 1 - me.core, x)))
        loads, cores = [], []
        for i, g_mine, g_other in pairs:
            cores.append(net.put(in_ref.at[g_other], rc.at[i], me.over_core))
            loads.append(net.move(in_ref.at[g_mine], mine.at[i]))

        def add(target, cols, left, right):
            def one(r, carry):
                at = pl.ds(pl.multiple_of(r * step, step), step)
                total = left(at).astype(F32) + right(at).astype(F32)
                target[at, cols] = total.astype(target.dtype)
                return carry

            lax.fori_loop(0, rows // step, one, 0)

        def sum_cores(k):
            i = pairs[k][0]
            loads[k].wait()
            cores[k].wait_recv()
            add(mine.at[i], pl.ds(0, width), lambda at: mine[i, at, :], lambda at: rc[i, at, :])
            return i

        i_yx = sum_cores(0)
        ax0 = net.put(mine.at[i_yx, :, a], rx.at[1 - me.y], me.over_x)
        by0 = net.put(mine.at[i_yx, :, b], ry.at[1 - me.c], me.over_y)
        i_x = sum_cores(1)
        ax1 = net.put(mine.at[i_x, :, a], rx.at[me.y], me.over_x)
        i_y = sum_cores(2)
        by1 = net.put(mine.at[i_y, :, b], ry.at[me.c], me.over_y)
        i_me = sum_cores(3)
        every = pl.ds(0, half)
        ax0.wait_recv()
        add(q0, every, lambda at: mine[i_y, at, a], lambda at: rx[1 - me.y, at, :])
        y0 = net.put(q0, r0, me.over_y)
        by0.wait_recv()
        add(q1, every, lambda at: mine[i_x, at, b], lambda at: ry[1 - me.c, at, :])
        x1 = net.put(q1, r1, me.over_x)
        ax1.wait_recv()
        by1.wait_recv()
        y0.wait_recv()
        x1.wait_recv()

        def final(r, carry):
            at = pl.ds(pl.multiple_of(r * step, step), step)
            left = mine[i_me, at, a].astype(F32) + rx[me.y, at, :].astype(F32) + r0[at, :].astype(F32)
            right = mine[i_me, at, b].astype(F32) + ry[me.c, at, :].astype(F32) + r1[at, :].astype(F32)
            last[at, a] = left.astype(BF)
            last[at, b] = right.astype(BF)
            return carry

        lax.fori_loop(0, rows // step, final, 0)
        waits = []
        for k in range(1, n_tp):
            to = lax.rem(me.t + k, n_tp)
            waits.append(net.put(last.at[pl.ds(to * piece, piece)], got.at[k - 1], me.along(k)))
        for wait in waits:
            wait.wait_recv()
        for r in range(piece // step):
            at = pl.ds(pl.multiple_of(me.t * piece + r * step, step), step)
            total = last[at, :].astype(F32)
            for k in range(n_tp - 1):
                total = total + got[k, r * step : (r + 1) * step, :].astype(F32)
            out_ref[r * step : (r + 1) * step, :] = total
        net.finish()

    block = (rows, width)
    return comm_call(
        body,
        (part,),
        [((piece, width), F32)],
        [
            VMEM((4, *block), BF),
            VMEM((4, *block), BF),
            VMEM((2, rows, half), BF),
            VMEM((2, rows, half), BF),
            VMEM((rows, half), BF),
            VMEM((rows, half), BF),
            VMEM((rows, half), BF),
            VMEM((rows, half), BF),
            VMEM(block, BF),
            VMEM((n_tp - 1, piece, width), BF),
        ],
        10 + n_tp - 1,
        4,
        collective_id,
        name,
        [ANY],
        [VMEM],
    )[0]


def sum_everywhere(part, n_tp, collective_id, name):
    def body(in_ref, out_ref, from_tp, mid, from_plane, send, recv, local):
        me = Place(n_tp)
        net = Net(send, recv, local)
        flips = [(dy, dk, dx) for dy in (0, 1) for dk in (0, 1) for dx in (0, 1)][1:]
        greet([me.along(k) for k in range(1, n_tp)] + [me.flip(*f) for f in flips])
        waits = [net.put(in_ref, from_tp.at[k - 1], me.along(k)) for k in range(1, n_tp)]
        for wait in waits:
            wait.wait_recv()
        total = in_ref[...]
        for k in range(n_tp - 1):
            total = total + from_tp[k]
        mid[...] = total
        waits = [net.put(mid, from_plane.at[i], me.flip(*f)) for i, f in enumerate(flips)]
        for wait in waits:
            wait.wait_recv()
        for i in range(7):
            total = total + from_plane[i]
        out_ref[...] = total
        net.finish()

    return comm_call(
        body,
        (part,),
        [(part.shape, F32)],
        [VMEM((n_tp - 1, *part.shape), F32), VMEM(part.shape, F32), VMEM((7, *part.shape), F32)],
        n_tp - 1 + 7,
        0,
        collective_id,
        name,
        [VMEM],
        [VMEM],
    )[0]


class Wire:
    def __init__(self, net, build):
        self.net, self.build, self.i = net, build, net.wires
        net.wires += 1

    def copy(self):
        src, dst, to = self.build()
        return pltpu.make_async_remote_copy(
            src_ref=src,
            dst_ref=dst,
            send_sem=self.net.send.at[self.i],
            recv_sem=self.net.recv.at[self.i],
            device_id=to,
            device_id_type=MESH,
        )

    def start(self):
        self.copy().start()

    def landed(self):
        self.copy().wait_recv()

    def sent(self):
        self.copy().wait_send()


class Wires:
    def __init__(self, send, recv):
        self.send, self.recv, self.wires, self.all = send, recv, 0, []

    def wire(self, build):
        made = Wire(self, build)
        self.all.append(made)
        return made


def feed_forward(two_own, cot_all, gate, up, down, sg_t, su_t, sd, w_router, experts, topk, n_tp):
    piece, width = two_own.shape
    rows = piece * n_tp
    tokens = 8 * rows
    pack = cot_all.shape[-1]
    hid, hid_s = gate.shape[2], sg_t.shape[0]
    edge = width // 2
    part_w = width + LANES
    group = 2 * rows
    shard_w = width // 4
    n_wires = 4 + 12 + 16 + 4 + 6 + (n_tp - 1)

    def body(*refs):
        (two_ref, cot_ref, gate_ref, up_ref, down_ref, sg_ref, su_ref, sd_ref, wr_ref) = refs[:9]
        (two_out, y_out, dg_out, du_out, dd_out, ds_out, n2_out) = refs[9:16]
        (nb, cb, wg, wu, wd, ws, wr, hwe, gge, uue, hws, ggs, uus, dnb, yb) = refs[16:31]
        (rc, rxa, ryb, q0, q1, r0, r1, last, got, dgs, dds, dss) = refs[31:43]
        send, recv, load, store = refs[43:]
        me = Place(n_tp)
        net = Wires(send, recv)

        def chip(dy, dx):
            return 2 * (me.y + dy * (1 - 2 * me.y)) + me.c + dx * (1 - 2 * me.c)

        def block(ch, core, p=None):
            start = ch * group + core * rows
            if p is None:
                return pl.ds(pl.multiple_of(start, rows), rows)
            return pl.ds(pl.multiple_of(start + p * piece, piece), piece)

        here = chip(0, 0)
        pieces = [me.t, lax.rem(me.t + 3, 4), lax.rem(me.t + 1, 4), lax.rem(me.t + 2, 4)]
        half = piece // 2

        def halves(p, which):
            start = here * group + me.core * rows + p * piece + which * half
            return nb.at[pl.ds(pl.multiple_of(start, half), half)]

        def mine(p):
            return nb.at[block(here, me.core, p)]

        right, left = me.along(1), me.along(-1)
        z_r = net.wire(lambda: (two_ref, mine(me.t), right))
        z_l = net.wire(lambda: (two_ref, mine(me.t), left))
        hop_r = net.wire(lambda: (halves(pieces[1], 0), halves(pieces[1], 0), right))
        hop_l = net.wire(lambda: (halves(pieces[2], 1), halves(pieces[2], 1), left))
        to_x, to_y, to_c = [], [], []
        for j in range(4):
            src = (lambda: two_ref) if j == 0 else (lambda j=j: mine(pieces[j]))
            to_x.append(net.wire(lambda j=j, src=src: (src(), mine(pieces[j]), me.over_x)))
            to_y.append(net.wire(lambda j=j, src=src: (src(), mine(pieces[j]), me.over_y)))
            to_c.append(net.wire(lambda j=j, src=src: (src(), mine(pieces[j]), me.over_core)))
        chip_x, chip_y, chip_d = chip(0, 1), chip(1, 0), chip(1, 1)
        first = 1 - me.core
        relay_chip = first * chip_x + me.core * chip_y
        relay_to = me.flip(first, 0, me.core)
        relay, fwd_x, fwd_y, fwd_d = [], [], [], []
        for j in range(4):
            same = lambda ch, j=j: nb.at[block(ch, me.core, pieces[j])]
            relay.append(net.wire(lambda same=same: (same(relay_chip), same(relay_chip), relay_to)))
            fwd_x.append(net.wire(lambda same=same: (same(chip_x), same(chip_x), me.over_core)))
            fwd_y.append(net.wire(lambda same=same: (same(chip_y), same(chip_y), me.over_core)))
            fwd_d.append(net.wire(lambda same=same: (same(chip_d), same(chip_d), me.over_core)))

        a, b = pl.ds(0, edge), pl.ds(edge, part_w - edge)
        flips = [(0, 0), (0, 1), (1, 0), (1, 1)]
        core_w = [
            net.wire(
                lambda k=k: (dnb.at[block(chip(*flips[k]), 1 - me.core)], rc.at[k], me.over_core)
            )
            for k in range(4)
        ]
        ax0 = net.wire(lambda: (dnb.at[block(chip_d, me.core), a], rxa.at[0], me.over_x))
        by0 = net.wire(lambda: (dnb.at[block(chip_d, me.core), b], ryb.at[0], me.over_y))
        ax1 = net.wire(lambda: (dnb.at[block(chip_x, me.core), a], rxa.at[1], me.over_x))
        by1 = net.wire(lambda: (dnb.at[block(chip_y, me.core), b], ryb.at[1], me.over_y))
        y0 = net.wire(lambda: (q0, r0, me.over_y))
        x1 = net.wire(lambda: (q1, r1, me.over_x))
        z_w = []
        for k in range(1, n_tp):
            to = lax.rem(me.t + k, n_tp)
            z_w.append(
                net.wire(
                    lambda k=k, to=to: (
                        last.at[pl.ds(pl.multiple_of(to * piece, piece), piece)],
                        got.at[k - 1],
                        me.along(k),
                    )
                )
            )

        loads = [
            pltpu.make_async_copy(src, dst, load.at[i])
            for i, (src, dst) in enumerate(
                [(down_ref, wd), (gate_ref, wg), (up_ref, wu), (wr_ref, wr)]
                + [(ref, ws.at[i]) for i, ref in enumerate((sg_ref, su_ref, sd_ref))]
                + [
                    (cot_ref.at[g], cb.at[pl.ds((2 * (g // 4) + g % 2) * group + (g % 4) // 2 * rows, rows)])
                    for g in range(8)
                ]
            )
        ]
        for copy in loads:
            copy.start()
        greet([me.over_x, me.over_y, me.over_core] + [me.along(k) for k in range(1, n_tp)])
        for wire in (z_r, z_l, to_x[0], to_y[0], to_c[0]):
            wire.start()
        nb[block(here, me.core, me.t), :] = two_ref[...]
        z_r.landed()
        hop_r.start()
        for wires in (to_x, to_y, to_c):
            wires[1].start()
        z_l.landed()
        hop_l.start()
        for wires in (to_x, to_y, to_c):
            wires[2].start()
        for copy in loads:
            copy.wait()
        hop_r.landed()
        hop_l.landed()
        for wires in (to_x, to_y, to_c):
            wires[3].start()
        for wire in to_c:
            wire.landed()

        lane = lax.broadcasted_iota(jnp.int32, (group, LANES), 1)
        e_first = slot(me.s, me.c) * 2
        lane_row = lax.broadcasted_iota(jnp.int32, (1, LANES), 1)

        def flip_chip(k):
            return chip(k // 2, lax.rem(k, 2))

        def hidden(k, carry):
            at = pl.ds(pl.multiple_of(flip_chip(k) * group, group), group)

            @pl.when(k == 1)
            def _():
                for j in range(4):
                    to_x[j].landed()
                    to_y[j].landed()
                    relay[j].start()
                    fwd_x[j].start()
                    fwd_y[j].start()
                for j in range(4):
                    fwd_x[j].landed()

            @pl.when(k == 2)
            def _():
                for j in range(4):
                    fwd_y[j].landed()

            @pl.when(k == 3)
            def _():
                for j in range(4):
                    relay[j].landed()
                    fwd_d[j].start()
                for j in range(4):
                    fwd_d[j].landed()

            logits = jnp.where(lane < experts, mdot(nb[at, :], wr[...]), NEG)
            e = jnp.exp(logits - jnp.max(logits, axis=1, keepdims=True))
            probs = e / jnp.sum(e, axis=1, keepdims=True)
            routed = cb[at, width : width + LANES].astype(F32)
            pg = jnp.zeros((group, LANES), F32)
            for j in range(3):
                shared = j == 2
                if shared:
                    g = dot_nt(nb[at, :], ws[0])
                    u = dot_nt(nb[at, :], ws[1])
                    back = dot_nt(cb[at, 0:width], ws[2])
                else:
                    g = mdot(nb[at, :], wg[j])
                    u = mdot(nb[at, :], wu[j])
                    back = dot_nt(cb[at, 0:width], wd[j])
                sig = 1.0 / (1.0 + jnp.exp(-g))
                silu = g * sig
                h = silu * u
                if not shared:
                    expert = e_first + j
                    hit = jnp.where(
                        (lane < topk) & (routed == expert.astype(F32)), 1.0, 0.0
                    )
                    chosen = jnp.max(hit, axis=1, keepdims=True)
                    weight = chosen * jnp.sum(
                        jnp.where(lane == expert, probs, 0.0), axis=1, keepdims=True
                    )
                    grad = chosen * jnp.sum(h * back, axis=1, keepdims=True)
                    high = grad.astype(BF).astype(F32)
                    pg = jnp.where(lane == expert, high, pg)
                    pg = jnp.where(lane == expert + LANES // 2, grad - high, pg)
                    h = h * weight
                    back = back * weight
                gate_grad = (back * u * (sig * (1.0 + g * (1.0 - sig)))).astype(BF)
                up_grad = (back * silu).astype(BF)
                if shared:
                    hws[at, :] = h.astype(BF)
                    ggs[at, :] = gate_grad
                    uus[at, :] = up_grad
                else:
                    hwe[j, at, :] = h.astype(BF)
                    gge[j, at, :] = gate_grad
                    uue[j, at, :] = up_grad
            dnb[at, width:part_w] = pg.astype(BF)
            return carry

        lax.fori_loop(0, 4, hidden, 0)

        n2_copies = []
        cols_s = pl.ds(pl.multiple_of(me.s * shard_w, shard_w), shard_w)
        for g in range(8):
            row = (2 * (g // 4) + g % 2) * group + (g % 4) // 2 * rows
            n2_copies.append(
                pltpu.make_async_copy(nb.at[pl.ds(row, rows), cols_s], n2_out.at[g], store.at[g])
            )
            n2_copies[-1].start()

        step = 16

        def add(target, t_at, cols, left, right, count):
            def one(r, carry):
                at = pl.ds(pl.multiple_of(r * step, step), step)
                total = left(r).astype(F32) + right(r).astype(F32)
                target[pl.ds(pl.multiple_of(t_at + r * step, step), step), cols] = total.astype(
                    target.dtype
                )
                return carry

            lax.fori_loop(0, count // step, one, 0)

        def row_at(base, r):
            return pl.ds(pl.multiple_of(base + r * step, step), step)

        every = pl.ds(0, part_w)

        def sum_cores(k):
            base = chip(*flips[k]) * group + me.core * rows
            core_w[k].landed()
            add(
                dnb,
                base,
                every,
                lambda r: dnb[row_at(base, r), every],
                lambda r: rc[k, row_at(0, r), :],
                rows,
            )

        n_col = 4
        col_w = width // n_col

        def normed_grad(i, carry):
            k = 3 - i
            at = pl.ds(pl.multiple_of(flip_chip(k) * group, group), group)

            def columns(n, carry):
                cols = pl.ds(pl.multiple_of(n * col_w, col_w), col_w)
                total = mdot(ggs[at, :], ws[0, :, cols]) + mdot(uus[at, :], ws[1, :, cols])
                for j in range(2):
                    total = total + dot_nt(gge[j, at, :], wg[j, cols, :])
                    total = total + dot_nt(uue[j, at, :], wu[j, cols, :])
                dnb[at, cols] = total.astype(BF)
                return carry

            lax.fori_loop(0, n_col, columns, 0)
            for kk in range(4):

                @pl.when(k == kk)
                def _():
                    core_w[kk].start()
                    if kk < 3:
                        sum_cores(kk + 1)
                    if kk == 2:
                        ax0.start()
                        by0.start()
                    if kk == 1:
                        by1.start()
                    if kk == 0:
                        ax1.start()

            return carry

        lax.fori_loop(0, 4, normed_grad, 0)

        def stage_two():
            base_y, base_x = chip_y * group + me.core * rows, chip_x * group + me.core * rows
            ax0.landed()
            add(q0, 0, pl.ds(0, edge), lambda r: dnb[row_at(base_y, r), a], lambda r: rxa[0, row_at(0, r), :], rows)
            y0.start()
            by0.landed()
            add(
                q1,
                0,
                pl.ds(0, part_w - edge),
                lambda r: dnb[row_at(base_x, r), b],
                lambda r: ryb[0, row_at(0, r), :],
                rows,
            )
            x1.start()

        def output(k, carry):
            at = pl.ds(pl.multiple_of(k * group, group), group)

            @pl.when(k == 1)
            def _():
                sum_cores(0)

            @pl.when(k == 3)
            def _():
                stage_two()

            def columns(n, carry):
                cols = pl.ds(pl.multiple_of(n * col_w, col_w), col_w)
                total = mdot(hws[at, :], ws[2, :, cols])
                for j in range(2):
                    total = total + mdot(hwe[j, at, :], wd[j, :, cols])
                yb[at, cols] = total.astype(BF)
                return carry

            lax.fori_loop(0, n_col, columns, 0)
            return carry

        lax.fori_loop(0, 4, output, 0)
        y_copy = pltpu.make_async_copy(yb, y_out, store.at[8])
        y_copy.start()

        def finish_plane():
            base = here * group + me.core * rows
            for wire in (ax1, by1, y0, x1):
                wire.landed()

            def final(r, carry):
                at, big = row_at(0, r), row_at(base, r)
                one = dnb[big, a].astype(F32) + rxa[1, at, :].astype(F32) + r0[at, :].astype(F32)
                two = dnb[big, b].astype(F32) + ryb[1, at, :].astype(F32) + r1[at, :].astype(F32)
                last[at, a] = one.astype(BF)
                last[at, b] = two.astype(BF)
                return carry

            lax.fori_loop(0, rows // step, final, 0)
            for wire in z_w:
                wire.start()

        m_w = 256

        def stores(m, buf):
            rows_m = pl.ds(pl.multiple_of(m * m_w, m_w), m_w)
            made = []
            for j in range(2):
                for i, out in enumerate((dg_out, du_out)):
                    made.append(
                        pltpu.make_async_copy(
                            dgs.at[buf, 2 * j + i], out.at[j, rows_m], store.at[9 + 4 * buf + 2 * j + i]
                        )
                    )
            return made

        def gate_up(m, carry):
            buf = lax.rem(m, 2)
            cols = pl.ds(pl.multiple_of(m * m_w, m_w), m_w)

            @pl.when(m >= 2)
            def _():
                for bb in range(2):

                    @pl.when(buf == bb)
                    def _():
                        for copy in stores(m - 2, bb):
                            copy.wait()

            @pl.when(m == 4)
            def _():
                finish_plane()

            left = nb[:, cols]
            for j in range(2):
                dgs[buf, 2 * j] = dot_tn(left, gge[j])
                dgs[buf, 2 * j + 1] = dot_tn(left, uue[j])
            dss[0, :, cols] = dot_tn(ggs[...], left).astype(BF)
            dss[1, :, cols] = dot_tn(uus[...], left).astype(BF)
            for bb in range(2):

                @pl.when(buf == bb)
                def _():
                    for copy in stores(m, bb):
                        copy.start()

            return carry

        n_m = width // m_w
        lax.fori_loop(0, n_m, gate_up, 0)
        for m in (n_m - 2, n_m - 1):
            for copy in stores(m, m % 2):
                copy.wait()

        def down_stores(m, buf):
            cols = pl.ds(pl.multiple_of(m * m_w, m_w), m_w)
            return [
                pltpu.make_async_copy(dds.at[buf, j], dd_out.at[j, :, cols], store.at[17 + 2 * buf + j])
                for j in range(2)
            ]

        def down_grad(m, carry):
            buf = lax.rem(m, 2)
            cols = pl.ds(pl.multiple_of(m * m_w, m_w), m_w)

            @pl.when(m >= 2)
            def _():
                for bb in range(2):

                    @pl.when(buf == bb)
                    def _():
                        for copy in down_stores(m - 2, bb):
                            copy.wait()

            right_c = cb[:, cols]
            for j in range(2):
                dds[buf, j] = dot_tn(hwe[j], right_c)
            dss[2, :, cols] = dot_tn(hws[...], right_c).astype(BF)
            for bb in range(2):

                @pl.when(buf == bb)
                def _():
                    for copy in down_stores(m, bb):
                        copy.start()

            return carry

        lax.fori_loop(0, n_m, down_grad, 0)
        ds_copy = pltpu.make_async_copy(dss, ds_out, store.at[21])
        ds_copy.start()
        for m in (n_m - 2, n_m - 1):
            for copy in down_stores(m, m % 2):
                copy.wait()

        for wire in z_w:
            wire.landed()
        for r in range(piece // step):
            total = last[row_at(me.t * piece, r), :].astype(F32)
            for k in range(n_tp - 1):
                total = total + got[k, r * step : (r + 1) * step, :].astype(F32)
            two_out[r * step : (r + 1) * step, :] = total
        for copy in n2_copies:
            copy.wait()
        y_copy.wait()
        ds_copy.wait()
        for wire in net.all:
            wire.sent()

    ins = (two_own, cot_all, gate, up, down, sg_t, su_t, sd, w_router)
    outs = [
        ((piece, part_w), F32),
        ((tokens, width), BF),
        (gate.shape, F32),
        (up.shape, F32),
        (down.shape, F32),
        ((3, hid_s, width), BF),
        ((8, rows, shard_w), BF),
    ]
    scratch = [
        VMEM((tokens, width), BF),
        VMEM((tokens, pack), BF),
        VMEM(gate.shape, BF),
        VMEM(up.shape, BF),
        VMEM(down.shape, BF),
        VMEM((3, hid_s, width), BF),
        VMEM(w_router.shape, BF),
        *[VMEM((2, tokens, hid), BF)] * 3,
        *[VMEM((tokens, hid_s), BF)] * 3,
        VMEM((tokens, part_w), BF),
        VMEM((tokens, width), BF),
        VMEM((4, rows, part_w), BF),
        VMEM((2, rows, edge), BF),
        VMEM((2, rows, part_w - edge), BF),
        VMEM((rows, edge), BF),
        VMEM((rows, part_w - edge), BF),
        VMEM((rows, edge), BF),
        VMEM((rows, part_w - edge), BF),
        VMEM((rows, part_w), BF),
        VMEM((n_tp - 1, piece, part_w), BF),
        VMEM((2, 4, 256, hid), F32),
        VMEM((2, 2, hid, 256), F32),
        VMEM((3, hid_s, width), BF),
    ]
    return pl.pallas_call(
        body,
        out_shape=tuple(jax.ShapeDtypeStruct(*o) for o in outs),
        in_specs=[pl.BlockSpec(memory_space=VMEM)] + [pl.BlockSpec(memory_space=ANY)] * 8,
        out_specs=(pl.BlockSpec(memory_space=VMEM), *[pl.BlockSpec(memory_space=ANY)] * 6),
        scratch_shapes=[
            *scratch,
            pltpu.SemaphoreType.DMA((n_wires,)),
            pltpu.SemaphoreType.DMA((n_wires,)),
            pltpu.SemaphoreType.DMA((15,)),
            pltpu.SemaphoreType.DMA((22,)),
        ],
        compiler_params=pltpu.CompilerParams(
            collective_id=4, has_side_effects=True, vmem_limit_bytes=66 * 10**6
        ),
        name="feed_forward",
    )(*ins)


def per_device(
    block_input,
    norm1_gain,
    q_weight,
    kva_weight,
    kv_norm_gain,
    kvb_weight,
    out_weight,
    norm2_gain,
    router_weight,
    shared_gate,
    shared_up,
    shared_down,
    expert_gate,
    expert_up,
    expert_down,
    routes,
    cotangent,
):
    n_tp = lax.axis_size(TP)
    rows, width = block_input.shape
    topk = routes.shape[1]
    experts = router_weight.shape[1]
    heads = q_weight.shape[1] // (DN + DR)
    scale = (DN + DR) ** (-0.5)
    piece = rows // n_tp
    s_id, c_id, t_id = lax.axis_index(SHARD), lax.axis_index(CTX), lax.axis_index(TP)
    shard_w = width // 4
    kv_w = KVR // 4

    small = jnp.concatenate(
        [
            norm1_gain.reshape(-1, LANES),
            norm2_gain.reshape(-1, LANES),
            kv_norm_gain.reshape(-1, LANES),
            jnp.zeros((7, LANES), BF),
            jnp.pad(router_weight, ((0, 0), (0, LANES - experts))),
        ]
    )
    w_query, w_latent, w_expand, w_output, small_all, x_pair = start_gather(
        (q_weight, kva_weight, kvb_weight, out_weight), small, block_input, n_tp
    )
    w_query = w_query.reshape(width, -1)
    w_latent = w_latent.reshape(width, -1)
    w_expand = w_expand.reshape(KVR, -1)
    w_output = w_output.transpose(1, 0, 2).reshape(-1, width)
    gain_one = small_all[:, 0:4].reshape(-1)
    gain_two = small_all[:, 4:8].reshape(-1)
    gain_kv = small_all[:, 8:9].reshape(-1)
    w_router = small_all[:, 16:, :experts].reshape(width, experts)

    cot_b = cotangent.astype(BF)
    cot_pack = jnp.concatenate(
        [cot_b, jnp.pad(routes.astype(BF), ((0, 0), (0, LANES - topk)))], axis=1
    )
    cot_all, sg_t, su_t, sd = plane_exchange(
        (cot_pack,), (), (shared_gate.T, shared_up.T, shared_down), n_tp, 1, "early_exchange"
    )

    x_float = block_input.astype(F32)
    cosine, sine = rope_tables(rows, (c_id * rows).astype(F32))
    cos_all, sin_all = rope_tables(2 * rows, jnp.float32(0))
    normed_pair = norm_rows(x_pair.reshape(2 * rows, width).astype(F32), gain_one).astype(BF)
    normed_one = norm_rows(x_float, gain_one).astype(BF)
    query = mdot(normed_one, w_query).reshape(rows, heads, DN + DR)
    query_nope = query[..., :DN].astype(BF)
    query_rope = rotate(query[..., DN:], cosine[:, None, :], sine[:, None, :]).astype(BF)
    latent = mdot(normed_pair, w_latent)
    latent_pair = norm_rows(latent[:, :KVR], gain_kv).astype(BF)
    rope_pair = rotate(latent[:, KVR:], cos_all, sin_all).astype(BF)
    kv_pair = mdot(latent_pair, w_expand).astype(BF).reshape(2 * rows, heads, DN + DV)
    key_pair, value_pair = kv_pair[..., :DN], kv_pair[..., DN:]
    score = jnp.einsum("qhd,khd->hqk", query_nope, key_pair, preferred_element_type=F32)
    score = score + jnp.einsum("qhd,kd->hqk", query_rope, rope_pair, preferred_element_type=F32)
    q_pos = c_id * rows + jnp.arange(rows, dtype=jnp.int32)
    k_pos = jnp.arange(2 * rows, dtype=jnp.int32)
    score = jnp.where(k_pos[None, None, :] <= q_pos[None, :, None], score * scale, NEG)
    top = jnp.max(score, axis=-1, keepdims=True)
    expo = jnp.exp(score - top)
    total = jnp.sum(expo, axis=-1, keepdims=True)
    attn = jnp.einsum("hqk,khd->hqd", expo.astype(BF), value_pair, preferred_element_type=F32)
    attn_rows = (attn / total).astype(BF).transpose(1, 0, 2)
    lse = top + jnp.log(total)
    attn_flat = attn_rows.reshape(rows, heads * DV)

    def own(a):
        return lax.dynamic_slice_in_dim(a, t_id * piece, piece, 0)

    attn_full = tp_reduce_scatter(mdot(attn_flat, w_output).astype(BF), n_tp, 2, "attn_scatter")
    mid = own(x_float) + attn_full
    two_own = norm_rows(mid, gain_two).astype(BF)
    summed, y_part, grad_expert_gate, grad_expert_up, grad_expert_down, shared_grads, two_cols = feed_forward(
        two_own,
        cot_all,
        expert_gate,
        expert_up,
        expert_down,
        sg_t,
        su_t,
        sd,
        jnp.pad(w_router, ((0, 0), (0, LANES - experts))),
        experts,
        topk,
        n_tp,
    )
    two_grad = summed[:, :width]
    prob_grad = summed[:, width : width + experts]
    prob_grad = prob_grad + summed[:, width + LANES // 2 : width + LANES // 2 + experts]
    y_part = y_part.reshape(2, 2, 2, rows, width).transpose(0, 2, 1, 3, 4).reshape(8, rows, width)
    out_own = mid + reduce_everywhere(y_part, n_tp, 3, "y_scatter")
    shared_grads = [shared_grads[i] for i in range(3)]

    probs_own = jax.nn.softmax(mdot(two_own, w_router), axis=-1)
    logit_grad = (
        probs_own * (prob_grad - jnp.sum(probs_own * prob_grad, axis=-1, keepdims=True))
    ).astype(BF)
    two_grad = two_grad + dot_nt(logit_grad, w_router)
    mid_norm_grad, gain_two_terms = norm_back(mid, gain_two, two_grad)
    mid_grad = own(cotangent) + mid_norm_grad
    mid_pack = jnp.concatenate(
        [mid_grad.astype(BF), jnp.pad(logit_grad, ((0, 0), (0, LANES - experts)))], axis=1
    )
    (mid_pack,) = tp_all_gather((mid_pack,), n_tp, 5, "mid_grad_gather")
    mid_b = mid_pack[:, :width]

    out_grad = dot_nt(mid_b, w_output).reshape(rows, heads, DV)
    out_grad_b = out_grad.astype(BF)
    delta = jnp.sum(out_grad * attn_rows.astype(F32), axis=-1).T[..., None]
    prob = jnp.exp(score - lse)
    dprob = jnp.einsum("qhd,khd->hqk", out_grad_b, value_pair, preferred_element_type=F32)
    dscore = (prob * (dprob - delta)).astype(BF)
    nope_grad = jnp.einsum("hqk,khd->qhd", dscore, key_pair, preferred_element_type=F32) * scale
    rope_qgrad = jnp.einsum("hqk,kd->qhd", dscore, rope_pair, preferred_element_type=F32) * scale
    key_grad = jnp.einsum("hqk,qhd->khd", dscore, query_nope, preferred_element_type=F32) * scale
    value_grad = jnp.einsum(
        "hqk,qhd->khd", prob.astype(BF), out_grad_b, preferred_element_type=F32
    )
    rope_kgrad = jnp.einsum("hqk,qhd->kd", dscore, query_rope, preferred_element_type=F32) * scale
    kv_terms = jnp.concatenate(
        [
            jnp.concatenate([key_grad, value_grad], axis=-1).reshape(2 * rows, -1),
            jnp.pad(rope_kgrad, ((0, 0), (0, LANES - DR))),
        ],
        axis=1,
    )
    mine = lax.dynamic_slice_in_dim(kv_terms, c_id * rows, rows, 0)
    other = lax.dynamic_slice_in_dim(kv_terms, (1 - c_id) * rows, rows, 0).astype(BF)
    kv_sum = mine + ctx_swap(other, 6, "kv_grad_swap").astype(F32)
    kv_grad = kv_sum[:, : heads * (DN + DV)].astype(BF)
    rope_part = rotate_back(kv_sum[:, heads * (DN + DV) :][:, :DR], cosine, sine)
    rope_qback = rotate_back(rope_qgrad, cosine[:, None, :], sine[:, None, :])
    query_grad = jnp.concatenate([nope_grad, rope_qback], axis=-1).astype(BF).reshape(rows, -1)
    latent_part = dot_nt(kv_grad, w_expand)
    one_part = dot_nt(query_grad, w_query)
    back_part = jnp.concatenate(
        [one_part, latent_part, jnp.pad(rope_part, ((0, 0), (0, LANES - DR)))], axis=1
    ).astype(BF)
    back = tp_reduce_scatter(back_part, n_tp, 7, "attn_back_scatter")

    compressed = own(lax.dynamic_slice_in_dim(latent, c_id * rows, rows, 0))[:, :KVR]
    compressed_grad, gain_kv_terms = norm_back(compressed, gain_kv, back[:, width : width + KVR])
    latent_grad = jnp.concatenate(
        [compressed_grad, back[:, width + KVR : width + KVR + DR]], axis=1
    ).astype(BF)
    one_grad = back[:, :width] + dot_nt(latent_grad, w_latent)
    input_norm_grad, gain_one_terms = norm_back(own(x_float), gain_one, one_grad)
    input_own = mid_grad + input_norm_grad

    block_output, input_grad = tp_all_gather((out_own, input_own), n_tp, 8, "output_gather")
    lat_pack = jnp.pad(latent_grad, ((0, 0), (0, 5 * LANES - KVR - DR)))
    (latent_rows,) = tp_all_gather((lat_pack,), n_tp, 9, "latent_gather")
    latent_own = lax.dynamic_slice_in_dim(latent_pair, c_id * rows, rows, 0)
    head_pack = jnp.concatenate(
        [query_grad, kv_grad, attn_flat, latent_rows, mid_pack[:, width:]], axis=1
    )
    head_all, one_cols, lat_cols, mid_cols, sg_cols, su_cols, sd_cols = plane_exchange(
        (head_pack,), (normed_one, latent_own, mid_b, *shared_grads), (), n_tp, 10, "late_exchange"
    )
    head_all = head_all.reshape(8 * rows, -1)
    edges = [0, heads * (DN + DR), heads * (DN + DV), heads * DV, 5 * LANES, LANES]
    edges = [sum(edges[: i + 1]) for i in range(len(edges))]
    dq_all, dkv_all, attn_all, lat_all, logit_all = (
        head_all[:, a:b] for a, b in zip(edges[:-1], edges[1:])
    )
    one_cols = one_cols.reshape(8 * rows, -1)
    lat_cols = lat_cols.reshape(8 * rows, -1)
    mid_cols = mid_cols.reshape(8 * rows, -1)
    grad_query = dot_tn(one_cols, dq_all)
    grad_latent = dot_tn(one_cols, lat_all[:, : KVR + DR])
    grad_expand = dot_tn(lat_cols, dkv_all)
    grad_out_w = dot_tn(attn_all, mid_cols)
    grad_router = dot_tn(two_cols.reshape(8 * rows, -1), logit_all[:, :experts])
    grad_sgate = sg_cols.reshape(-1, shard_w).T.astype(F32)
    grad_sup = su_cols.reshape(-1, shard_w).T.astype(F32)
    grad_sdown = sd_cols.reshape(-1, shard_w).astype(F32)

    gains = jnp.concatenate(
        [
            jnp.sum(gain_one_terms, axis=0),
            jnp.sum(gain_two_terms, axis=0),
            jnp.sum(gain_kv_terms, axis=0),
            jnp.zeros((512,), F32),
        ]
    ).reshape(8, -1)
    gains = sum_everywhere(gains, n_tp, 11, "gain_sum").reshape(-1)
    grad_one = lax.dynamic_slice_in_dim(gains, s_id * shard_w, shard_w, 0)
    grad_two = lax.dynamic_slice_in_dim(gains, width + s_id * shard_w, shard_w, 0)
    grad_kv = lax.dynamic_slice_in_dim(gains, 2 * width + s_id * kv_w, kv_w, 0)
    return (
        block_output,
        input_grad,
        grad_one,
        grad_query,
        grad_latent,
        grad_kv,
        grad_expand,
        grad_out_w,
        grad_two,
        grad_router,
        grad_sgate,
        grad_sup,
        grad_sdown,
        grad_expert_gate,
        grad_expert_up,
        grad_expert_down,
    )


def send_rows(buffer):
    return lax.all_to_all(buffer, (SHARD, CTX), split_axis=0, concat_axis=0, tiled=True)


def return_rows(partial_value, slots):
    back_rows = lax.all_to_all(
        partial_value, (SHARD, CTX), split_axis=0, concat_axis=0, tiled=True
    )
    flat_back = back_rows.reshape(-1, back_rows.shape[-1])
    return flat_back[slots]


def per_device_general(
    block_input,
    norm1_gain,
    q_weight,
    kva_weight,
    kv_norm_gain,
    kvb_weight,
    out_weight,
    norm2_gain,
    router_weight,
    shared_gate,
    shared_up,
    shared_down,
    expert_gate,
    expert_up,
    expert_down,
    routes,
    cotangent,
):
    tok_rows = block_input.shape[0]
    head_count = q_weight.shape[1] // (DN + DR)
    score_scale = (DN + DR) ** (-0.5)
    (
        gain_one,
        w_query,
        w_latent,
        gain_kv,
        w_expand,
        w_output,
        gain_two,
        w_router,
        w_sgate,
        w_sup,
        w_sdown,
    ) = (
        lax.all_gather(norm1_gain, SHARD, axis=0, tiled=True),
        lax.all_gather(q_weight, SHARD, axis=0, tiled=True),
        lax.all_gather(kva_weight, SHARD, axis=0, tiled=True),
        lax.all_gather(kv_norm_gain, SHARD, axis=0, tiled=True),
        lax.all_gather(kvb_weight, SHARD, axis=0, tiled=True),
        lax.all_gather(out_weight, SHARD, axis=1, tiled=True),
        lax.all_gather(norm2_gain, SHARD, axis=0, tiled=True),
        lax.all_gather(router_weight, SHARD, axis=0, tiled=True),
        lax.all_gather(shared_gate, SHARD, axis=0, tiled=True),
        lax.all_gather(shared_up, SHARD, axis=0, tiled=True),
        lax.all_gather(shared_down, SHARD, axis=1, tiled=True),
    )
    block_index = lax.axis_index(CTX)
    cosine, sine_table = rope_tables(tok_rows, (block_index * tok_rows).astype(jnp.float32))
    x_float = block_input.astype(jnp.float32)
    normed_one = norm_rows(x_float, gain_one).astype(jnp.bfloat16)
    query = mdot(normed_one, w_query).reshape(tok_rows, head_count, DN + DR)
    query_rot = rotate(query[..., DN:], cosine[:, None, :], sine_table[:, None, :])
    query = jnp.concatenate([query[..., :DN], query_rot], axis=-1).astype(jnp.bfloat16)
    query_nope = query[..., :DN]
    query_rope = query[..., DN:]
    latent = mdot(normed_one, w_latent)
    compressed = latent[:, :KVR]
    latent_n = norm_rows(compressed, gain_kv).astype(jnp.bfloat16)
    rope_key = rotate(latent[:, KVR:], cosine, sine_table).astype(jnp.bfloat16)
    first_piece = mdot(latent_n, w_expand).astype(jnp.bfloat16)
    gathered, rope_all = (
        lax.all_gather(first_piece, CTX, axis=0, tiled=True),
        lax.all_gather(rope_key, CTX, axis=0, tiled=True),
    )
    query_pos = block_index * tok_rows + jnp.arange(tok_rows, dtype=jnp.int32)

    def scores_at(block_id):
        blk_start = block_id * tok_rows
        kv_block = lax.dynamic_slice_in_dim(gathered, blk_start, tok_rows, 0).reshape(
            tok_rows, head_count, DN + DV
        )
        rope_block = lax.dynamic_slice_in_dim(rope_all, blk_start, tok_rows, 0)
        score = jnp.einsum(
            "qhd,khd->hqk", query_nope, kv_block[..., :DN], preferred_element_type=jnp.float32
        )
        score = score + jnp.einsum(
            "qhd,kd->hqk", query_rope, rope_block, preferred_element_type=jnp.float32
        )
        score = score * score_scale
        key_pos = blk_start + jnp.arange(tok_rows, dtype=jnp.int32)
        score = jnp.where(key_pos[None, None, :] <= query_pos[None, :, None], score, NEG)
        return (score, kv_block, rope_block)

    def forward_block(block_id, carry):
        run_max, run_sum, weighted = carry
        score, kv_block, rope_block = scores_at(block_id)
        new_max = jnp.maximum(run_max, jnp.max(score, axis=-1))
        factor = jnp.exp(run_max - new_max)
        expo = jnp.exp(score - new_max[..., None])
        run_sum = factor * run_sum + jnp.sum(expo, axis=-1)
        weighted = factor[..., None] * weighted + jnp.einsum(
            "hqk,khd->hqd",
            expo.astype(jnp.bfloat16),
            kv_block[..., DN:],
            preferred_element_type=jnp.float32,
        )
        return (new_max, run_sum, weighted)

    start_state = (
        jnp.full((head_count, tok_rows), NEG, jnp.float32),
        jnp.zeros((head_count, tok_rows), jnp.float32),
        jnp.zeros((head_count, tok_rows, DV), jnp.float32),
    )
    run_max, run_sum, weighted = lax.fori_loop(0, block_index + 1, forward_block, start_state)
    lse = run_max + jnp.log(run_sum)
    attn_rows = (weighted / run_sum[..., None]).astype(jnp.bfloat16).transpose(1, 0, 2)
    attn_flat = attn_rows.reshape(tok_rows, head_count * DV)
    attn_full = lax.psum(mdot(attn_flat, w_output), TP)
    mid = x_float + attn_full
    normed_two = norm_rows(mid, gain_two).astype(jnp.bfloat16)
    probs = jax.nn.softmax(mdot(normed_two, w_router), axis=-1)
    experts = probs.shape[1]
    topk = routes.shape[1]
    picks = (routes[:, :, None] == jnp.arange(experts, dtype=jnp.int32)[None, None, :]).astype(
        jnp.float32
    )
    route_w = jnp.sum(picks * probs[:, None, :], axis=-1)
    shared_a = mdot(normed_two, w_sgate)
    shared_b = mdot(normed_two, w_sup)
    shared_h = (jax.nn.silu(shared_a) * shared_b).astype(jnp.bfloat16)
    shared_y = mdot(shared_h, w_sdown)
    capacity = 2 * tok_rows * topk // experts
    owners = lax.axis_size((SHARD, CTX))
    local_experts = expert_gate.shape[0]
    width = normed_two.shape[1]
    flat_routes = routes.reshape(-1)
    onehot = (flat_routes[:, None] == jnp.arange(experts, dtype=jnp.int32)[None, :]).astype(
        jnp.int32
    )
    rank = jnp.sum((jnp.cumsum(onehot, axis=0) - 1) * onehot, axis=1)
    slots = flat_routes * capacity + rank
    source_row = jnp.arange(tok_rows * topk, dtype=jnp.int32) // topk
    send_buffer = (
        jnp.zeros((experts * capacity, width), jnp.bfloat16).at[slots].set(normed_two[source_row])
    )
    received = send_rows(send_buffer.reshape(owners, local_experts * capacity, width)).reshape(
        owners, local_experts, capacity, width
    )
    gate_act = jnp.einsum(
        "gecd,edf->gecf", received, expert_gate, preferred_element_type=jnp.float32
    )
    up_act = jnp.einsum("gecd,edf->gecf", received, expert_up, preferred_element_type=jnp.float32)
    hidden = (jax.nn.silu(gate_act) * up_act).astype(jnp.bfloat16)
    expert_y = jnp.einsum("gecf,efd->gecd", hidden, expert_down, preferred_element_type=jnp.float32)
    routed_out = return_rows(
        expert_y.reshape(owners, local_experts * capacity, width), slots
    ).reshape(tok_rows, topk, width)
    routed_part = jnp.sum(route_w[:, :, None] * routed_out, axis=1) + shared_y
    weight_part = jnp.sum(routed_out * cotangent[:, None, :], axis=-1)
    moe_out, route_grad = lax.psum((routed_part, weight_part), TP)
    block_output = mid + moe_out
    cot_b = cotangent.astype(jnp.bfloat16)
    routed_grad = (
        (route_w[:, :, None] * cotangent[:, None, :])
        .astype(jnp.bfloat16)
        .reshape(tok_rows * topk, width)
    )
    grad_buffer = jnp.zeros((experts * capacity, width), jnp.bfloat16).at[slots].set(routed_grad)
    grad_recv = send_rows(grad_buffer.reshape(owners, local_experts * capacity, width)).reshape(
        owners, local_experts, capacity, width
    )
    hidden_grad = jnp.einsum(
        "gecd,efd->gecf", grad_recv, expert_down, preferred_element_type=jnp.float32
    )
    gate_grad = (hidden_grad * up_act * silu_slope(gate_act)).astype(jnp.bfloat16)
    up_grad = (hidden_grad * jax.nn.silu(gate_act)).astype(jnp.bfloat16)
    grad_expert_down = jnp.einsum(
        "gecf,gecd->efd", hidden, grad_recv, preferred_element_type=jnp.float32
    )
    grad_expert_gate = jnp.einsum(
        "gecd,gecf->edf", received, gate_grad, preferred_element_type=jnp.float32
    )
    grad_expert_up = jnp.einsum(
        "gecd,gecf->edf", received, up_grad, preferred_element_type=jnp.float32
    )
    row_grad = jnp.einsum(
        "gecf,edf->gecd", gate_grad, expert_gate, preferred_element_type=jnp.float32
    )
    row_grad = row_grad + jnp.einsum(
        "gecf,edf->gecd", up_grad, expert_up, preferred_element_type=jnp.float32
    )
    routed_back = return_rows(
        row_grad.reshape(owners, local_experts * capacity, width), slots
    ).reshape(tok_rows, topk, width)
    shared_grad = jnp.einsum("td,fd->tf", cot_b, w_sdown, preferred_element_type=jnp.float32)
    sgate_grad = (shared_grad * shared_b * silu_slope(shared_a)).astype(jnp.bfloat16)
    sup_grad = (shared_grad * jax.nn.silu(shared_a)).astype(jnp.bfloat16)
    grad_sdown = jnp.einsum("tf,td->fd", shared_h, cot_b, preferred_element_type=jnp.float32)
    grad_sgate = jnp.einsum("td,tf->df", normed_two, sgate_grad, preferred_element_type=jnp.float32)
    grad_sup = jnp.einsum("td,tf->df", normed_two, sup_grad, preferred_element_type=jnp.float32)
    two_part = jnp.sum(routed_back, axis=1)
    two_part = two_part + jnp.einsum(
        "tf,df->td", sgate_grad, w_sgate, preferred_element_type=jnp.float32
    )
    two_part = two_part + jnp.einsum(
        "tf,df->td", sup_grad, w_sup, preferred_element_type=jnp.float32
    )
    two_grad = lax.psum(two_part, TP)
    prob_grad = jnp.sum(picks * route_grad[:, :, None], axis=1)
    logit_grad = (probs * (prob_grad - jnp.sum(probs * prob_grad, axis=-1, keepdims=True))).astype(
        jnp.bfloat16
    )
    grad_router = jnp.einsum(
        "td,te->de", normed_two, logit_grad, preferred_element_type=jnp.float32
    )
    two_grad = two_grad + jnp.einsum(
        "te,de->td", logit_grad, w_router, preferred_element_type=jnp.float32
    )
    _, norm_two_back = jax.vjp(norm_rows, mid, gain_two.astype(jnp.float32))
    mid_norm_grad, grad_gain_two = norm_two_back(two_grad)
    mid_grad = cotangent + mid_norm_grad
    mid_b = mid_grad.astype(jnp.bfloat16)
    grad_out_w = jnp.einsum("tj,td->jd", attn_flat, mid_b, preferred_element_type=jnp.float32)
    out_grad = jnp.einsum("td,jd->tj", mid_b, w_output, preferred_element_type=jnp.float32).reshape(
        tok_rows, head_count, DV
    )
    out_grad_b = out_grad.astype(jnp.bfloat16)
    delta = jnp.sum(out_grad * attn_rows.astype(jnp.float32), axis=-1).T
    key_count = gathered.shape[0]
    term_width = head_count * (DN + DV + DR)

    def back_block(block_id, carry):
        nope_grad, rope_qgrad, terms = carry
        score, kv_block, rope_block = scores_at(block_id)
        probs_blk = jnp.exp(score - lse[..., None])
        prob_b = probs_blk.astype(jnp.bfloat16)
        dprob = jnp.einsum(
            "qhd,khd->hqk", out_grad_b, kv_block[..., DN:], preferred_element_type=jnp.float32
        )
        dscore = (probs_blk * (dprob - delta[..., None])).astype(jnp.bfloat16)
        nope_grad = (
            nope_grad
            + jnp.einsum(
                "hqk,khd->qhd", dscore, kv_block[..., :DN], preferred_element_type=jnp.float32
            )
            * score_scale
        )
        rope_qgrad = (
            rope_qgrad
            + jnp.einsum("hqk,kd->qhd", dscore, rope_block, preferred_element_type=jnp.float32)
            * score_scale
        )
        key_nope_grad = (
            jnp.einsum("hqk,qhd->khd", dscore, query_nope, preferred_element_type=jnp.float32)
            * score_scale
        )
        key_rope_grad = (
            jnp.einsum("hqk,qhd->khd", dscore, query_rope, preferred_element_type=jnp.float32)
            * score_scale
        )
        value_grad = jnp.einsum(
            "hqk,qhd->khd", prob_b, out_grad_b, preferred_element_type=jnp.float32
        )
        block_terms = jnp.concatenate([key_nope_grad, value_grad, key_rope_grad], axis=-1).reshape(
            tok_rows, term_width
        )
        terms = lax.dynamic_update_slice_in_dim(terms, block_terms, block_id * tok_rows, 0)
        return (nope_grad, rope_qgrad, terms)

    back_init = (
        jnp.zeros((tok_rows, head_count, DN), jnp.float32),
        jnp.zeros((tok_rows, head_count, DR), jnp.float32),
        jnp.zeros((key_count, term_width), jnp.float32),
    )
    nope_grad, rope_qgrad, terms = lax.fori_loop(0, block_index + 1, back_block, back_init)
    key_terms = lax.psum_scatter(terms, CTX, scatter_dimension=0, tiled=True).reshape(
        tok_rows, head_count, DN + DV + DR
    )
    kv_grad = (
        key_terms[..., : DN + DV].reshape(tok_rows, head_count * (DN + DV)).astype(jnp.bfloat16)
    )
    rope_grad = rotate_back(jnp.sum(key_terms[..., DN + DV :], axis=1), cosine, sine_table)
    grad_expand = jnp.einsum("ti,tj->ij", latent_n, kv_grad, preferred_element_type=jnp.float32)
    latent_part = jnp.einsum("tj,ij->ti", kv_grad, w_expand, preferred_element_type=jnp.float32)
    rope_qback = rotate_back(rope_qgrad, cosine[:, None, :], sine_table[:, None, :])
    query_grad = (
        jnp.concatenate([nope_grad, rope_qback], axis=-1)
        .astype(jnp.bfloat16)
        .reshape(tok_rows, head_count * (DN + DR))
    )
    grad_query = jnp.einsum("td,tj->dj", normed_one, query_grad, preferred_element_type=jnp.float32)
    normed_part = jnp.einsum("tj,dj->td", query_grad, w_query, preferred_element_type=jnp.float32)
    latent_sum, normed_sum = lax.psum(
        (jnp.concatenate([latent_part, rope_grad], axis=-1), normed_part), TP
    )
    _, kv_back = jax.vjp(norm_rows, compressed, gain_kv.astype(jnp.float32))
    compressed_grad, grad_gain_kv = kv_back(latent_sum[:, :KVR])
    latent_grad = jnp.concatenate([compressed_grad, latent_sum[:, KVR:]], axis=-1).astype(
        jnp.bfloat16
    )
    grad_latent = jnp.einsum(
        "td,tl->dl", normed_one, latent_grad, preferred_element_type=jnp.float32
    )
    one_grad = normed_sum + jnp.einsum(
        "tl,dl->td", latent_grad, w_latent, preferred_element_type=jnp.float32
    )
    _, one_back = jax.vjp(norm_rows, x_float, gain_one.astype(jnp.float32))
    input_norm_grad, grad_gain_one = one_back(one_grad)
    input_grad = mid_grad + input_norm_grad
    (
        red_one,
        red_query,
        red_latent,
        red_kv,
        red_expand,
        red_output,
        red_two,
        red_router,
        red_sgate,
        red_sup,
        red_sdown,
    ) = (
        lax.psum_scatter(grad_gain_one, SHARD, scatter_dimension=0, tiled=True),
        lax.psum_scatter(grad_query, SHARD, scatter_dimension=0, tiled=True),
        lax.psum_scatter(grad_latent, SHARD, scatter_dimension=0, tiled=True),
        lax.psum_scatter(grad_gain_kv, SHARD, scatter_dimension=0, tiled=True),
        lax.psum_scatter(grad_expand, SHARD, scatter_dimension=0, tiled=True),
        lax.psum_scatter(grad_out_w, SHARD, scatter_dimension=1, tiled=True),
        lax.psum_scatter(grad_gain_two, SHARD, scatter_dimension=0, tiled=True),
        lax.psum_scatter(grad_router, SHARD, scatter_dimension=0, tiled=True),
        lax.psum_scatter(grad_sgate, SHARD, scatter_dimension=0, tiled=True),
        lax.psum_scatter(grad_sup, SHARD, scatter_dimension=0, tiled=True),
        lax.psum_scatter(grad_sdown, SHARD, scatter_dimension=1, tiled=True),
    )
    (
        sum_one,
        sum_query,
        sum_latent,
        sum_kv,
        sum_expand,
        sum_output,
        sum_two,
        sum_router,
        sum_sgate,
        sum_sup,
        sum_sdown,
    ) = lax.psum(
        (
            red_one,
            red_query,
            red_latent,
            red_kv,
            red_expand,
            red_output,
            red_two,
            red_router,
            red_sgate,
            red_sup,
            red_sdown,
        ),
        CTX,
    )
    return (
        block_output,
        input_grad,
        sum_one,
        sum_query,
        sum_latent,
        sum_kv,
        sum_expand,
        sum_output,
        sum_two,
        sum_router,
        sum_sgate,
        sum_sup,
        sum_sdown,
        grad_expert_gate,
        grad_expert_up,
        grad_expert_down,
    )


def solution(mesh):
    in_specs = (
        P((SHARD, CTX), None),
        P(SHARD),
        P(SHARD, TP),
        P(SHARD, None),
        P(SHARD),
        P(SHARD, TP),
        P(TP, SHARD),
        P(SHARD),
        P(SHARD, None),
        P(SHARD, TP),
        P(SHARD, TP),
        P(TP, SHARD),
        P((SHARD, CTX), None, TP),
        P((SHARD, CTX), None, TP),
        P((SHARD, CTX), TP, None),
        P((SHARD, CTX), None),
        P((SHARD, CTX), None),
    )
    out_specs = (
        P((SHARD, CTX), None),
        P((SHARD, CTX), None),
        P(SHARD),
        P(SHARD, TP),
        P(SHARD, None),
        P(SHARD),
        P(SHARD, TP),
        P(TP, SHARD),
        P(SHARD),
        P(SHARD, None),
        P(SHARD, TP),
        P(SHARD, TP),
        P(TP, SHARD),
        P((SHARD, CTX), None, TP),
        P((SHARD, CTX), None, TP),
        P((SHARD, CTX), TP, None),
    )
    routed = mesh.shape[SHARD] == 4 and mesh.shape[CTX] == 2 and mesh.shape[TP] == 4
    return jax.shard_map(
        per_device if routed else per_device_general, mesh=mesh, in_specs=in_specs, out_specs=out_specs, check_vma=False
    )
```

```python
import functools

import jax
import jax.numpy as jnp
from jax import lax
from jax.experimental import pallas as pl
from jax.experimental.pallas import tpu as pltpu
from jax.sharding import PartitionSpec as P

DN = 128
DR = 64
DV = 128
KVR = 512
LANES = 128
SHARD, CTX, TP = "shard", "ctx", "tp"

EPS = 1e-06
NEG = -1e30

BF = jnp.bfloat16
F32 = jnp.float32
MESH = pl.DeviceIdType.MESH
ANY = pl.ANY
VMEM = pltpu.VMEM


def norm_rows(value, gain):
    factor = lax.rsqrt(jnp.mean(value * value, axis=-1, keepdims=True) + EPS)
    return value * factor * gain.astype(F32)


def norm_back(value, gain, grad):
    factor = lax.rsqrt(jnp.mean(value * value, axis=-1, keepdims=True) + EPS)
    scaled = grad * gain.astype(F32)
    inner = jnp.mean(scaled * value, axis=-1, keepdims=True)
    return factor * (scaled - value * (factor * factor * inner)), grad * value * factor


def rope_tables(count, offset):
    half_size = DR // 2
    position = jnp.arange(count, dtype=F32) + offset
    freqs = 10000.0 ** (-(jnp.arange(half_size, dtype=F32) * 2.0 / DR))
    angle = position[:, None] * freqs[None, :]
    return (jnp.cos(angle), jnp.sin(angle))


def rotate(value, cosine, sine_table):
    half_size = DR // 2
    first = value[..., :half_size]
    second = value[..., half_size:]
    return jnp.concatenate(
        [first * cosine - second * sine_table, first * sine_table + second * cosine], axis=-1
    )


def rotate_back(grad, cosine, sine_table):
    half_size = DR // 2
    first = grad[..., :half_size]
    second = grad[..., half_size:]
    return jnp.concatenate(
        [first * cosine + second * sine_table, second * cosine - first * sine_table], axis=-1
    )


def silu_slope(value):
    sigmoid = jax.nn.sigmoid(value)
    return sigmoid * (1.0 + value * (1.0 - sigmoid))


def mdot(left, right):
    return jnp.dot(left, right, preferred_element_type=F32)


def dot_nt(left, right):
    return lax.dot_general(left, right, (((1,), (1,)), ((), ())), preferred_element_type=F32)


def dot_tn(left, right):
    return lax.dot_general(left, right, (((0,), (0,)), ((), ())), preferred_element_type=F32)


class Place:
    def __init__(self, n_tp):
        self.s = lax.axis_index(SHARD)
        self.c = lax.axis_index(CTX)
        self.t = lax.axis_index(TP)
        self.core = lax.rem(self.s, 2)
        self.y = self.s // 2
        self.n_tp = n_tp
        self.over_x = self.flip(0, 0, 1)
        self.over_y = self.flip(1, 0, 0)
        self.over_core = self.flip(0, 1, 0)

    def along(self, step):
        t = lax.rem(self.t + step + self.n_tp, self.n_tp)
        return {SHARD: self.s, CTX: self.c, TP: t}

    def flip(self, dy, dcore, dx):
        y = self.y + dy * (1 - 2 * self.y)
        core = self.core + dcore * (1 - 2 * self.core)
        x = self.c + dx * (1 - 2 * self.c)
        return {SHARD: 2 * y + core, CTX: x, TP: self.t}

    def peers(self, kinds):
        flips = []
        if "p" in kinds:
            flips = FLIPS
        else:
            flips = [f for kind, f in (("x", FLIPS[0]), ("k", FLIPS[1]), ("y", FLIPS[3])) if kind in kinds]
        out = [self.flip(*f) for f in flips]
        if "z" in kinds:
            out += [self.along(k) for k in range(1, self.n_tp)]
        return out


FLIPS = [(dy, dk, dx) for dy in (0, 1) for dk in (0, 1) for dx in (0, 1)][1:]


def slot(s, c):
    return 2 * s + c


class Net:
    def __init__(self, send, recv, local):
        self.send, self.recv, self.local = send, recv, local
        self.puts = []
        self.n_local = 0

    def put(self, src, dst, to):
        i = len(self.puts)
        copy = pltpu.make_async_remote_copy(
            src_ref=src,
            dst_ref=dst,
            send_sem=self.send.at[i],
            recv_sem=self.recv.at[i],
            device_id=to,
            device_id_type=MESH,
        )
        copy.start()
        self.puts.append(copy)
        return copy

    def move(self, src, dst):
        copy = pltpu.make_async_copy(src, dst, self.local.at[self.n_local])
        self.n_local += 1
        copy.start()
        return copy

    def finish(self):
        for copy in self.puts:
            copy.wait_send()


def greet(peers):
    barrier = pltpu.get_barrier_semaphore()
    for peer in peers:
        pl.semaphore_signal(barrier, inc=1, device_id=peer, device_id_type=MESH)
    pl.semaphore_wait(barrier, len(peers))


class Job:
    def __init__(self, run, ins, outs, scratch, n_put, n_local, peers):
        self.run, self.ins, self.outs, self.scratch = run, ins, outs, scratch
        self.n_put, self.n_local, self.peers = n_put, n_local, peers


def comm_kernel(jobs, n_tp, collective_id, name):
    ins = [i for job in jobs for i in job.ins]
    outs = [o for job in jobs for o in job.outs]
    scratch = [s for job in jobs for s in job.scratch]
    n_put = sum(job.n_put for job in jobs)
    n_local = max(sum(job.n_local for job in jobs), 1)
    kinds = "".join(sorted(set("".join(job.peers for job in jobs))))

    def body(*refs):
        in_refs, out_refs = refs[: len(ins)], refs[len(ins) : len(ins) + len(outs)]
        rest = refs[len(ins) + len(outs) :]
        me = Place(n_tp)
        net = Net(*rest[len(scratch) :])
        greet(me.peers(kinds))
        running = []
        i = o = s = 0
        for job in jobs:
            ni, no, ns = len(job.ins), len(job.outs), len(job.scratch)
            running.append(
                job.run(net, me, in_refs[i : i + ni], out_refs[o : o + no], rest[s : s + ns])
            )
            i, o, s = i + ni, o + no, s + ns
        while running:
            running = [r for r in running if next(r, None) is not None]
        net.finish()

    got = pl.pallas_call(
        body,
        out_shape=tuple(jax.ShapeDtypeStruct(shape, dtype) for shape, dtype, _ in outs),
        in_specs=[pl.BlockSpec(memory_space=space) for _, space in ins],
        out_specs=tuple(pl.BlockSpec(memory_space=space) for _, _, space in outs),
        scratch_shapes=[
            *scratch,
            pltpu.SemaphoreType.DMA((n_put,)),
            pltpu.SemaphoreType.DMA((n_put,)),
            pltpu.SemaphoreType.DMA((n_local,)),
        ],
        compiler_params=pltpu.CompilerParams(
            collective_id=collective_id, has_side_effects=True, vmem_limit_bytes=60 * 2**20
        ),
        name=name,
    )(*[a for a, _ in ins])
    split, o = [], 0
    for job in jobs:
        split.append(got[o : o + len(job.outs)])
        o += len(job.outs)
    return split


def shard_gather(weights, block):
    shapes = [w.shape for w, _ in weights]
    side = [by for _, by in weights]

    def run(net, me, ins, outs, bounce):
        n = len(shapes)
        x_in, x_out = ins[n], outs[n]
        other = lax.rem(me.s + 2, 4)

        def place(i, s, which=None):
            rows, cols = shapes[i]
            at = pl.ds(0, rows)
            if which is not None:
                at = pl.ds(pl.multiple_of(which * (rows // 2), rows // 2), rows // 2)
            if side[i]:
                return outs[i].at[at, pl.ds(pl.multiple_of(s * cols, LANES), cols)]
            return outs[i].at[s, at]

        loads = [net.move(src, b) for src, b in zip(ins, bounce)]
        from_y, own = [], []
        for i in range(n):
            rows = shapes[i][0]
            at = pl.ds(pl.multiple_of(me.c * (rows // 2), rows // 2), rows // 2)
            from_y.append(net.put(ins[i].at[at], place(i, me.s, me.c), me.over_y))
            if i == 0:
                wait_x = net.put(x_in, x_out.at[me.c], me.over_x)
        for i in range(n):
            own.append(net.put(ins[i], place(i, me.s), me.over_core))
        yield 1
        stores = []
        for i, (load, b) in enumerate(zip(loads, bounce)):
            load.wait()
            stores.append(net.move(b, place(i, me.s) if i < n else x_out.at[me.c]))
        from_x, relays = [], []
        for i in range(n):
            from_y[i].wait_recv()
            piece = place(i, other, me.c)
            from_x.append(net.put(piece, piece, me.over_x))
            relays.append(net.put(piece, piece, me.over_core))
            yield 1
        for i in range(n):
            from_x[i].wait_recv()
            piece = place(i, other, 1 - me.c)
            relays.append(net.put(piece, piece, me.over_core))
            yield 1
        wait_x.wait_recv()
        for got in own + relays:
            got.wait_recv()
        for store in stores:
            store.wait()

    n = len(weights)
    outs = []
    for (rows, cols), by in zip(shapes, side):
        outs.append(((rows, 4 * cols) if by else (4, rows, cols), BF, ANY))
    outs.append(((2, *block.shape), BF, ANY))
    return Job(
        run,
        [(w, ANY) for w, _ in weights] + [(block, ANY)],
        outs,
        [VMEM(w.shape, w.dtype) for w, _ in weights] + [VMEM(block.shape, BF)],
        5 * n + 1,
        2 * n + 2,
        "xyk",
    )


def tp_reduce_scatter(part, n_tp):
    rows, width = part.shape
    piece = rows // n_tp

    def run(net, me, ins, outs, scratch):
        (src,), (out,), (got,) = ins, outs, scratch
        waits = []
        for k in range(1, n_tp):
            to = pl.multiple_of(lax.rem(me.t + k, n_tp) * piece, piece)
            waits.append(net.put(src.at[pl.ds(to, piece)], got.at[k - 1], me.along(k)))
        yield 1
        for wait in waits:
            wait.wait_recv()
        total = src[pl.ds(pl.multiple_of(me.t * piece, piece), piece), :].astype(F32)
        for k in range(1, n_tp):
            total = total + got[k - 1].astype(F32)
        out[...] = total

    return Job(
        run,
        [(part, VMEM)],
        [((piece, width), F32, VMEM)],
        [VMEM((n_tp - 1, piece, width), BF)],
        n_tp - 1,
        0,
        "z",
    )


def tp_all_gather(own, n_tp):
    size, width = own.shape
    half = size // 2

    def run(net, me, ins, outs, scratch):
        (src,), (out,) = ins, outs

        def rows(p, which=None):
            if which is None:
                return out.at[pl.ds(pl.multiple_of(p * size, size), size)]
            return out.at[pl.ds(pl.multiple_of(p * size + which * half, half), half)]

        right, left = me.along(1), me.along(-1)
        p_left, p_right = lax.rem(me.t + 3, 4), lax.rem(me.t + 1, 4)
        to_right = net.put(src, rows(me.t), right)
        to_left = net.put(src, rows(me.t), left)
        out[pl.ds(pl.multiple_of(me.t * size, size), size), :] = src[...]
        yield 1
        to_right.wait_recv()
        hop_right = net.put(rows(p_left, 0), rows(p_left, 0), right)
        to_left.wait_recv()
        hop_left = net.put(rows(p_right, 1), rows(p_right, 1), left)
        yield 1
        yield 1
        hop_right.wait_recv()
        hop_left.wait_recv()

    return Job(
        run, [(own, VMEM)], [((n_tp * size, width), own.dtype, VMEM)], [], 4, 0, "z"
    )


def relay_chunks(net, me, out, chunks):
    g_x, g_y = slot(me.s, 1 - me.c), slot(lax.rem(me.s + 2, 4), me.c)
    g_d = slot(lax.rem(me.s + 2, 4), 1 - me.c)
    first = 1 - me.core
    relay_slot = first * g_x + me.core * g_y
    relay_to = me.flip(first, 0, me.core)
    diags, waits = [], []
    for from_x, from_y, start, size in chunks:
        from_x.wait_recv()
        from_y.wait_recv()
        src = out.at[relay_slot, pl.ds(start, size)]
        diags.append(net.put(src, src, relay_to))
        for g in (g_x, g_y):
            piece = out.at[g, pl.ds(start, size)]
            waits.append(net.put(piece, piece, me.over_core))
        yield 1
    for diag, (_, _, start, size) in zip(diags, chunks):
        diag.wait_recv()
        piece = out.at[g_d, pl.ds(start, size)]
        waits.append(net.put(piece, piece, me.over_core))
        yield 1
    for wait in waits:
        wait.wait_recv()


def plane_gather(own, n_chunk=4):
    rows, width = own.shape
    size = rows // n_chunk

    def run(net, me, ins, outs, scratch):
        (src,), (out,), (bounce,) = ins, outs, scratch
        g_me = slot(me.s, me.c)
        load = net.move(src, bounce)
        chunks, cores = [], []
        for j in range(n_chunk):
            part = src.at[pl.ds(j * size, size)]
            to = out.at[g_me, pl.ds(j * size, size)]
            chunks.append(
                (net.put(part, to, me.over_x), net.put(part, to, me.over_y), j * size, size)
            )
            cores.append(net.put(part, to, me.over_core))
        yield 1
        load.wait()
        store = net.move(bounce, out.at[g_me])
        yield from relay_chunks(net, me, out, chunks)
        for core in cores:
            core.wait_recv()
        store.wait()

    return Job(
        run,
        [(own, ANY)],
        [((8, rows, width), own.dtype, ANY)],
        [VMEM(own.shape, own.dtype)],
        7 * n_chunk,
        2,
        "xyk",
    )


def plane_columns(array):
    rows, width = array.shape
    w = width // 4

    def run(net, me, ins, outs, scratch):
        (src,), (out,), (bounce,) = ins, outs, scratch
        g_me = slot(me.s, me.c)

        def cols(s):
            return src.at[:, pl.ds(pl.multiple_of(s * w, LANES), w)]

        load = net.move(cols(me.s), bounce)
        waits = []
        for f in FLIPS:
            peer = me.flip(*f)
            waits.append(net.put(cols(peer[SHARD]), out.at[g_me], peer))
        yield 1
        load.wait()
        store = net.move(bounce, out.at[g_me])
        for wait in waits:
            yield 1
            wait.wait_recv()
        store.wait()

    return Job(
        run,
        [(array, ANY)],
        [((8, rows, w), array.dtype, ANY)],
        [VMEM((rows, w), array.dtype)],
        7,
        2,
        "p",
    )


def shard_rows(array):
    h, w = array.shape[0] // 8, array.shape[1]

    def run(net, me, ins, outs, scratch):
        (src,), (out,), (bounce,) = ins, outs, scratch

        def rows(s):
            return src.at[pl.ds(pl.multiple_of(slot(s, me.c) * h, 8), h)]

        to = out.at[:, pl.ds(pl.multiple_of(me.s * w, LANES), w)]
        load = net.move(rows(me.s), bounce)
        waits = []
        for f in FLIPS:
            if f[2] == 0:
                peer = me.flip(*f)
                waits.append(net.put(rows(peer[SHARD]), to, peer))
        yield 1
        load.wait()
        store = net.move(bounce, to)
        yield 1
        for wait in waits:
            wait.wait_recv()
        store.wait()

    return Job(
        run,
        [(array, ANY)],
        [((h, 4 * w), array.dtype, ANY)],
        [VMEM((h, w), array.dtype)],
        3,
        2,
        "p",
    )


def ctx_swap(block):
    def run(net, me, ins, outs, scratch):
        (src,), (out,) = ins, outs
        got = net.put(src, out, me.over_x)
        yield 1
        yield 1
        got.wait_recv()

    return Job(run, [(block, ANY)], [(block.shape, block.dtype, ANY)], [], 1, 0, "x")


def reduce_everywhere(part, n_tp):
    tokens, width = part.shape
    rows = tokens // 8
    half = width // 2
    piece = rows // n_tp
    step = 16

    def run(net, me, ins, outs, scratch):
        (src,), (out,) = ins, outs
        mine, rc, rx, ry, q0, q1, r0, r1, last, got = scratch
        a, b = pl.ds(0, half), pl.ds(half, half)
        order = [(1, 1), (0, 1), (1, 0), (0, 0)]
        chips, loads, cores = [], [], []
        for dy, dx in order:
            ch = 2 * (me.y + dy * (1 - 2 * me.y)) + me.c + dx * (1 - 2 * me.c)
            chips.append(ch)
            base = ch * 2 * rows
            theirs = src.at[pl.ds(pl.multiple_of(base + (1 - me.core) * rows, rows), rows)]
            ours = src.at[pl.ds(pl.multiple_of(base + me.core * rows, rows), rows)]
            cores.append(net.put(theirs, rc.at[ch], me.over_core))
            loads.append(net.move(ours, mine.at[ch]))
        yield 1

        def add(target, cols, left, right):
            def one(r, carry):
                at = pl.ds(pl.multiple_of(r * step, step), step)
                target[at, cols] = (left(at).astype(F32) + right(at).astype(F32)).astype(BF)
                return carry

            lax.fori_loop(0, rows // step, one, 0)

        def sum_cores(k):
            ch = chips[k]
            loads[k].wait()
            cores[k].wait_recv()
            add(mine.at[ch], pl.ds(0, width), lambda at: mine[ch, at, :], lambda at: rc[ch, at, :])
            return ch

        c_d = sum_cores(0)
        ax0 = net.put(mine.at[c_d, :, a], rx.at[0], me.over_x)
        by0 = net.put(mine.at[c_d, :, b], ry.at[0], me.over_y)
        c_x = sum_cores(1)
        ax1 = net.put(mine.at[c_x, :, a], rx.at[1], me.over_x)
        c_y = sum_cores(2)
        by1 = net.put(mine.at[c_y, :, b], ry.at[1], me.over_y)
        c_me = sum_cores(3)
        yield 1
        every = pl.ds(0, half)
        ax0.wait_recv()
        add(q0, every, lambda at: mine[c_y, at, a], lambda at: rx[0, at, :])
        y0 = net.put(q0, r0, me.over_y)
        by0.wait_recv()
        add(q1, every, lambda at: mine[c_x, at, b], lambda at: ry[0, at, :])
        x1 = net.put(q1, r1, me.over_x)
        yield 1
        ax1.wait_recv()
        by1.wait_recv()
        y0.wait_recv()
        x1.wait_recv()

        def final(r, carry):
            at = pl.ds(pl.multiple_of(r * step, step), step)
            left = mine[c_me, at, a].astype(F32) + rx[1, at, :].astype(F32) + r0[at, :].astype(F32)
            right = mine[c_me, at, b].astype(F32) + ry[1, at, :].astype(F32) + r1[at, :].astype(F32)
            last[at, a] = left.astype(BF)
            last[at, b] = right.astype(BF)
            return carry

        lax.fori_loop(0, rows // step, final, 0)
        waits = []
        for k in range(1, n_tp):
            to = pl.multiple_of(lax.rem(me.t + k, n_tp) * piece, piece)
            waits.append(net.put(last.at[pl.ds(to, piece)], got.at[k - 1], me.along(k)))
        yield 1
        for wait in waits:
            wait.wait_recv()
        for r in range(piece // step):
            at = pl.ds(pl.multiple_of(me.t * piece + r * step, step), step)
            total = last[at, :].astype(F32)
            for k in range(n_tp - 1):
                total = total + got[k, r * step : (r + 1) * step, :].astype(F32)
            out[r * step : (r + 1) * step, :] = total

    block = (rows, width)
    return Job(
        run,
        [(part, ANY)],
        [((piece, width), F32, VMEM)],
        [
            VMEM((4, *block), BF),
            VMEM((4, *block), BF),
            VMEM((2, rows, half), BF),
            VMEM((2, rows, half), BF),
            VMEM((rows, half), BF),
            VMEM((rows, half), BF),
            VMEM((rows, half), BF),
            VMEM((rows, half), BF),
            VMEM(block, BF),
            VMEM((n_tp - 1, piece, width), BF),
        ],
        10 + n_tp - 1,
        4,
        "xykz",
    )


def sum_everywhere(part, n_tp):
    def run(net, me, ins, outs, scratch):
        (src,), (out,) = ins, outs
        from_tp, mid, from_plane = scratch
        waits = [net.put(src, from_tp.at[k - 1], me.along(k)) for k in range(1, n_tp)]
        yield 1
        for wait in waits:
            wait.wait_recv()
        total = src[...]
        for k in range(n_tp - 1):
            total = total + from_tp[k]
        mid[...] = total
        waits = [net.put(mid, from_plane.at[i], me.flip(*f)) for i, f in enumerate(FLIPS)]
        yield 1
        yield 1
        for wait in waits:
            wait.wait_recv()
        total = mid[...]
        for i in range(7):
            total = total + from_plane[i]
        out[...] = total

    return Job(
        run,
        [(part, VMEM)],
        [(part.shape, F32, VMEM)],
        [VMEM((n_tp - 1, *part.shape), F32), VMEM(part.shape, F32), VMEM((7, *part.shape), F32)],
        n_tp - 1 + 7,
        0,
        "zp",
    )


def gather_rows(own, n_tp):
    piece, width = own.shape
    half = piece // 2

    def run(net, me, ins, outs, scratch):
        (src,), (out,), (bounce,) = ins, outs, scratch
        load = net.move(src, bounce)
        g_me = slot(me.s, me.c)
        chunks, cores = [], []

        def rows(p, which=None):
            if which is None:
                return out.at[g_me, pl.ds(pl.multiple_of(p * piece, piece), piece)]
            return out.at[g_me, pl.ds(pl.multiple_of(p * piece + which * half, half), half)]

        def spread(ref, p):
            dst = rows(p)
            chunks.append(
                (net.put(ref, dst, me.over_x), net.put(ref, dst, me.over_y), pl.multiple_of(p * piece, piece), piece)
            )
            cores.append(net.put(ref, dst, me.over_core))

        right, left = me.along(1), me.along(-1)
        p_left, p_right = lax.rem(me.t + 3, 4), lax.rem(me.t + 1, 4)
        far = lax.rem(me.t + 2, 4)
        to_right = net.put(src, rows(me.t), right)
        to_left = net.put(src, rows(me.t), left)
        spread(src, me.t)
        load.wait()
        store = net.move(bounce, rows(me.t))
        yield 1
        to_right.wait_recv()
        hop_right = net.put(rows(p_left, 0), rows(p_left, 0), right)
        spread(rows(p_left), p_left)
        to_left.wait_recv()
        hop_left = net.put(rows(p_right, 1), rows(p_right, 1), left)
        spread(rows(p_right), p_right)
        yield 1
        hop_right.wait_recv()
        hop_left.wait_recv()
        spread(rows(far), far)
        yield from relay_chunks(net, me, out, chunks)
        for core in cores:
            core.wait_recv()
        store.wait()

    return Job(
        run,
        [(own, ANY)],
        [((8, n_tp * piece, width), own.dtype, ANY)],
        [VMEM(own.shape, own.dtype)],
        4 * 7 + 4,
        2,
        "xykz",
    )


class Wire:
    def __init__(self, net, build):
        self.net, self.build, self.i = net, build, len(net.all)
        net.all.append(self)

    def copy(self):
        src, dst, to = self.build()
        return pltpu.make_async_remote_copy(
            src_ref=src,
            dst_ref=dst,
            send_sem=self.net.send.at[self.i],
            recv_sem=self.net.recv.at[self.i],
            device_id=to,
            device_id_type=MESH,
        )

    def start(self):
        self.copy().start()

    def landed(self):
        self.copy().wait_recv()

    def sent(self):
        self.copy().wait_send()


class Wires:
    def __init__(self, send, recv):
        self.send, self.recv, self.all = send, recv, []

    def wire(self, build):
        return Wire(self, build)


def padded(count, to=LANES):
    return -(-count // to) * to


def feed_forward(
    two_own, mid_own, cot_own, gain_two, cot_all, gate, up, down, sg_t, su_t, sd, router_t, attn, normed, latent, topk, n_tp
):
    piece, width = two_own.shape
    rows = piece * n_tp
    tokens = 8 * rows
    pack = cot_all.shape[-1]
    hid, hid_s = gate.shape[1], sg_t.shape[0]
    experts = router_t.shape[0]
    used = 2 * hid + hid_s
    H = padded(used)
    tile = H - LANES
    off = used - tile
    edge = width // 2
    part_w = width + LANES
    group = 2 * rows
    shard_w = width // 4
    lat_w = latent.shape[1] // 4
    attn_w = attn.shape[1]
    n_wires = 4 + 12 + 16 + 4 + 6 + (n_tp - 1) + 7 + 14 + 4
    n_col = 4
    col_w = width // n_col
    m_w = 256
    n_m = width // m_w

    def body(*refs):
        (two_ref, mid_ref, cot_own_ref, gain_ref) = refs[:4]
        (cot_ref, gate_ref, up_ref, down_ref, sg_ref, su_ref, sd_ref, wr_ref, attn_ref, one_ref, lat_ref) = refs[4:15]
        (mid_out, gain_out, mid_pack, ya_out, yb_out, dg_out, du_out, dd_out, ds_out, n2_out) = refs[15:25]
        (attn_out, one_out, lat_out) = refs[25:28]
        (nb, cb, wgu, wd, gu, gut, hw, hwt, dnb, yb) = refs[28:38]
        (rc, rxa, ryb, q0, q1, r0, r1, last, got, gus, dds, dss) = refs[38:50]
        send, recv, load, store = refs[50:]
        me = Place(n_tp)
        net = Wires(send, recv)

        def chip(dy, dx):
            return 2 * (me.y + dy * (1 - 2 * me.y)) + me.c + dx * (1 - 2 * me.c)

        def block(ch, core, p=None):
            start = ch * group + core * rows
            if p is None:
                return pl.ds(pl.multiple_of(start, rows), rows)
            return pl.ds(pl.multiple_of(start + p * piece, piece), piece)

        here = chip(0, 0)
        g_me = slot(me.s, me.c)
        pieces = [me.t, lax.rem(me.t + 3, 4), lax.rem(me.t + 1, 4), lax.rem(me.t + 2, 4)]
        half = piece // 2
        right, left = me.along(1), me.along(-1)

        def halves(p, which):
            start = here * group + me.core * rows + p * piece + which * half
            return nb.at[pl.ds(pl.multiple_of(start, half), half)]

        def mine(p):
            return nb.at[block(here, me.core, p)]

        z_r = net.wire(lambda: (two_ref, mine(me.t), right))
        z_l = net.wire(lambda: (two_ref, mine(me.t), left))
        hop_r = net.wire(lambda: (halves(pieces[1], 0), halves(pieces[1], 0), right))
        hop_l = net.wire(lambda: (halves(pieces[2], 1), halves(pieces[2], 1), left))
        to_x, to_y, to_c = [], [], []
        for j in range(4):
            src = (lambda: two_ref) if j == 0 else (lambda j=j: mine(pieces[j]))
            to_x.append(net.wire(lambda j=j, src=src: (src(), mine(pieces[j]), me.over_x)))
            to_y.append(net.wire(lambda j=j, src=src: (src(), mine(pieces[j]), me.over_y)))
            to_c.append(net.wire(lambda j=j, src=src: (src(), mine(pieces[j]), me.over_core)))
        chip_x, chip_y, chip_d = chip(0, 1), chip(1, 0), chip(1, 1)
        first = 1 - me.core
        relay_chip = first * chip_x + me.core * chip_y
        relay_to = me.flip(first, 0, me.core)
        relay, fwd_x, fwd_y, fwd_d = [], [], [], []
        for j in range(4):
            same = lambda ch, j=j: nb.at[block(ch, me.core, pieces[j])]
            relay.append(net.wire(lambda same=same: (same(relay_chip), same(relay_chip), relay_to)))
            fwd_x.append(net.wire(lambda same=same: (same(chip_x), same(chip_x), me.over_core)))
            fwd_y.append(net.wire(lambda same=same: (same(chip_y), same(chip_y), me.over_core)))
            fwd_d.append(net.wire(lambda same=same: (same(chip_d), same(chip_d), me.over_core)))

        g_x, g_y = slot(me.s, 1 - me.c), slot(lax.rem(me.s + 2, 4), me.c)
        g_d = slot(lax.rem(me.s + 2, 4), 1 - me.c)
        g_relay = first * g_x + me.core * g_y
        at_direct = [
            net.wire(lambda to=to: (attn_ref, attn_out.at[g_me], to))
            for to in (me.over_x, me.over_y, me.over_core)
        ]
        at_relay = net.wire(lambda: (attn_out.at[g_relay], attn_out.at[g_relay], relay_to))
        at_fwd = [
            net.wire(lambda g=g: (attn_out.at[g], attn_out.at[g], me.over_core)) for g in (g_x, g_y, g_d)
        ]
        cols_w = []
        for f in FLIPS:
            peer = me.flip(*f)
            for src, dst, w in ((one_ref, one_out, shard_w), (lat_ref, lat_out, lat_w)):
                cols_w.append(
                    net.wire(
                        lambda src=src, dst=dst, w=w, peer=peer: (
                            src.at[:, pl.ds(pl.multiple_of(peer[SHARD] * w, LANES), w)],
                            dst.at[g_me],
                            peer,
                        )
                    )
                )

        a, b = pl.ds(0, edge), pl.ds(edge, part_w - edge)
        flips = [(0, 0), (0, 1), (1, 0), (1, 1)]
        core_w = [
            net.wire(
                lambda k=k: (dnb.at[block(chip(*flips[k]), 1 - me.core)], rc.at[k], me.over_core)
            )
            for k in range(4)
        ]
        ax0 = net.wire(lambda: (dnb.at[block(chip_d, me.core), a], rxa.at[0], me.over_x))
        by0 = net.wire(lambda: (dnb.at[block(chip_d, me.core), b], ryb.at[0], me.over_y))
        ax1 = net.wire(lambda: (dnb.at[block(chip_x, me.core), a], rxa.at[1], me.over_x))
        by1 = net.wire(lambda: (dnb.at[block(chip_y, me.core), b], ryb.at[1], me.over_y))
        y0 = net.wire(lambda: (q0, r0, me.over_y))
        x1 = net.wire(lambda: (q1, r1, me.over_x))
        z_w = []
        for k in range(1, n_tp):
            to = lax.rem(me.t + k, n_tp)
            z_w.append(
                net.wire(
                    lambda k=k, to=to: (
                        last.at[pl.ds(pl.multiple_of(to * piece, piece), piece)],
                        got.at[k - 1],
                        me.along(k),
                    )
                )
            )

        def packed(p, which=None):
            if which is None:
                return mid_pack.at[pl.ds(pl.multiple_of(p * piece, piece), piece)]
            return mid_pack.at[pl.ds(pl.multiple_of(p * piece + which * half, half), half)]

        m_r = net.wire(lambda: (packed(me.t), packed(me.t), right))
        m_l = net.wire(lambda: (packed(me.t), packed(me.t), left))
        m_hr = net.wire(lambda: (packed(pieces[1], 0), packed(pieces[1], 0), right))
        m_hl = net.wire(lambda: (packed(pieces[2], 1), packed(pieces[2], 1), left))

        moves = [
            (down_ref.at[0], wd.at[pl.ds(0, hid)]),
            (down_ref.at[1], wd.at[pl.ds(hid, hid)]),
            (sd_ref, wd.at[pl.ds(2 * hid, hid_s)]),
            (gate_ref.at[0], wgu.at[pl.ds(0, hid)]),
            (gate_ref.at[1], wgu.at[pl.ds(hid, hid)]),
            (sg_ref, wgu.at[pl.ds(2 * hid, hid_s)]),
            (wr_ref, wgu.at[pl.ds(used, experts)]),
            (up_ref.at[0], wgu.at[pl.ds(H, hid)]),
            (up_ref.at[1], wgu.at[pl.ds(H + hid, hid)]),
            (su_ref, wgu.at[pl.ds(H + 2 * hid, hid_s)]),
        ]
        for g in range(8):
            row = (2 * (g // 4) + g % 2) * group + (g % 4) // 2 * rows
            moves.append((cot_ref.at[g], cb.at[pl.ds(row, rows)]))
        loads = [pltpu.make_async_copy(src, dst, load.at[i]) for i, (src, dst) in enumerate(moves)]
        for copy in loads:
            copy.start()
        greet(me.peers("xykzp"))
        for wire in (z_r, z_l, to_x[0], to_y[0], to_c[0]):
            wire.start()
        nb[block(here, me.core, me.t), :] = two_ref[...]
        wgu[used + experts : H, :] = jnp.zeros((H - used - experts, width), BF)
        wgu[H + used :, :] = jnp.zeros((H - used, width), BF)
        wd[used:, :] = jnp.zeros((H - used, width), BF)
        z_r.landed()
        hop_r.start()
        for wires in (to_x, to_y, to_c):
            wires[1].start()
        z_l.landed()
        hop_l.start()
        for wires in (to_x, to_y, to_c):
            wires[2].start()
        for copy in loads:
            copy.wait()
        hop_r.landed()
        hop_l.landed()
        for wires in (to_x, to_y, to_c):
            wires[3].start()
        for wire in to_c:
            wire.landed()

        lane = lax.broadcasted_iota(jnp.int32, (group, LANES), 1)
        unit = lax.broadcasted_iota(jnp.int32, (group, H), 1)
        e_first = g_me * 2

        def softmax_tile(logits, lanes):
            logits = jnp.where((lanes >= off) & (lanes < off + experts), logits, NEG)
            e = jnp.exp(logits - jnp.max(logits, axis=1, keepdims=True))
            return e / jnp.sum(e, axis=1, keepdims=True)

        def flip_chip(k):
            return chip(k // 2, lax.rem(k, 2))

        def hidden(k, carry):
            at = pl.ds(pl.multiple_of(flip_chip(k) * group, group), group)

            @pl.when(k == 1)
            def _():
                for j in range(4):
                    to_x[j].landed()
                    to_y[j].landed()
                    relay[j].start()
                    fwd_x[j].start()
                    fwd_y[j].start()
                for j in range(4):
                    fwd_x[j].landed()

            @pl.when(k == 2)
            def _():
                for j in range(4):
                    fwd_y[j].landed()

            @pl.when(k == 3)
            def _():
                for j in range(4):
                    relay[j].landed()
                    fwd_d[j].start()
                for wire in at_direct + cols_w:
                    wire.start()
                for j in range(4):
                    fwd_d[j].landed()

            acts = dot_nt(nb[at, :], wgu[...])
            back = dot_nt(cb[at, 0:width], wd[...])
            probs = softmax_tile(acts[:, tile:H], lane)
            routed = cb[at, width : width + LANES].astype(F32)
            chosen, weight = [], []
            for j in range(2):
                expert = e_first + j
                hit = jnp.where((lane < topk) & (routed == expert.astype(F32)), 1.0, 0.0)
                chosen.append(jnp.max(hit, axis=1, keepdims=True))
                weight.append(
                    chosen[j]
                    * jnp.sum(jnp.where(lane == off + expert, probs, 0.0), axis=1, keepdims=True)
                )
            scale = jnp.where(unit < hid, weight[0], jnp.where(unit < 2 * hid, weight[1], 1.0))
            g, u = acts[:, :H], acts[:, H:]
            sig = 1.0 / (1.0 + jnp.exp(-g))
            silu = g * sig
            h = silu * u
            terms = h * back
            pg = jnp.zeros((group, LANES), F32)
            for j in range(2):
                own = (unit >= j * hid) & (unit < (j + 1) * hid)
                grad = chosen[j] * jnp.sum(jnp.where(own, terms, 0.0), axis=1, keepdims=True)
                high = grad.astype(BF).astype(F32)
                pg = jnp.where(lane == off + e_first + j, high, pg)
                pg = jnp.where(lane == off + e_first + j + LANES // 2, grad - high, pg)
            dnb[at, width:part_w] = pg.astype(BF)
            h = (h * scale).astype(BF)
            back = back * scale
            gate_grad = (back * u * (sig * (1.0 + g * (1.0 - sig)))).astype(BF)
            up_grad = (back * silu).astype(BF)
            hw[at, :] = h
            gu[at, 0:H] = gate_grad
            gu[at, H:] = up_grad
            hwt[:, at] = h.T
            gut[0:H, at] = gate_grad.T
            gut[H:, at] = up_grad.T
            return carry

        lax.fori_loop(0, 4, hidden, 0)

        cols_s = pl.ds(pl.multiple_of(me.s * shard_w, shard_w), shard_w)
        locals_ = []
        for g in range(8):
            row = (2 * (g // 4) + g % 2) * group + (g % 4) // 2 * rows
            locals_.append((nb.at[pl.ds(row, rows), cols_s], n2_out.at[g]))
        locals_.append((attn_ref, attn_out.at[g_me]))
        locals_.append((one_ref.at[:, cols_s], one_out.at[g_me]))
        locals_.append((lat_ref.at[:, pl.ds(pl.multiple_of(me.s * lat_w, LANES), lat_w)], lat_out.at[g_me]))
        local_copies = [pltpu.make_async_copy(src, dst, store.at[i]) for i, (src, dst) in enumerate(locals_)]
        for copy in local_copies:
            copy.start()

        step = 16

        def row_at(base, r):
            return pl.ds(pl.multiple_of(base + r * step, step), step)

        def add(target, t_at, cols, left, right, count):
            def one(r, carry):
                total = left(r).astype(F32) + right(r).astype(F32)
                target[row_at(t_at, r), cols] = total.astype(BF)
                return carry

            lax.fori_loop(0, count // step, one, 0)

        every = pl.ds(0, part_w)

        def sum_cores(k):
            base = chip(*flips[k]) * group + me.core * rows
            core_w[k].landed()
            add(
                dnb,
                base,
                every,
                lambda r: dnb[row_at(base, r), every],
                lambda r: rc[k, row_at(0, r), :],
                rows,
            )

        def normed_grad(i, carry):
            k = 3 - i
            at = pl.ds(pl.multiple_of(flip_chip(k) * group, group), group)

            def columns(n, carry):
                cols = pl.ds(pl.multiple_of(n * col_w, col_w), col_w)
                dnb[at, cols] = mdot(gu[at, :], wgu[:, cols]).astype(BF)
                return carry

            lax.fori_loop(0, n_col, columns, 0)
            for kk in range(4):

                @pl.when(k == kk)
                def _():
                    core_w[kk].start()
                    if kk < 3:
                        sum_cores(kk + 1)
                    if kk == 2:
                        ax0.start()
                        by0.start()
                    if kk == 1:
                        by1.start()
                        at_direct[0].landed()
                        at_direct[1].landed()
                        at_relay.start()
                        at_fwd[0].start()
                        at_fwd[1].start()
                    if kk == 0:
                        ax1.start()

            return carry

        lax.fori_loop(0, 4, normed_grad, 0)

        def stage_two():
            base_y, base_x = chip_y * group + me.core * rows, chip_x * group + me.core * rows
            ax0.landed()
            add(q0, 0, pl.ds(0, edge), lambda r: dnb[row_at(base_y, r), a], lambda r: rxa[0, row_at(0, r), :], rows)
            y0.start()
            by0.landed()
            add(
                q1,
                0,
                pl.ds(0, part_w - edge),
                lambda r: dnb[row_at(base_x, r), b],
                lambda r: ryb[0, row_at(0, r), :],
                rows,
            )
            x1.start()

        def output(k, carry):
            at = pl.ds(pl.multiple_of(k * group, group), group)

            @pl.when(k == 1)
            def _():
                sum_cores(0)

            @pl.when(k == 3)
            def _():
                stage_two()
                at_relay.landed()
                at_fwd[2].start()

            def columns(n, carry):
                cols = pl.ds(pl.multiple_of(n * col_w, col_w), col_w)
                yb[at, cols] = mdot(hw[at, :], wd[:, cols]).astype(BF)
                return carry

            lax.fori_loop(0, n_col, columns, 0)
            return carry

        lax.fori_loop(0, 4, output, 0)
        y_copies = [
            pltpu.make_async_copy(yb.at[:, pl.ds(i * edge, edge)], out, store.at[11 + i])
            for i, out in enumerate((ya_out, yb_out))
        ]
        for copy in y_copies:
            copy.start()

        def finish_plane():
            base = here * group + me.core * rows
            for wire in (ax1, by1, y0, x1):
                wire.landed()

            def final(r, carry):
                at, big = row_at(0, r), row_at(base, r)
                one = dnb[big, a].astype(F32) + rxa[1, at, :].astype(F32) + r0[at, :].astype(F32)
                two = dnb[big, b].astype(F32) + ryb[1, at, :].astype(F32) + r1[at, :].astype(F32)
                last[at, a] = one.astype(BF)
                last[at, b] = two.astype(BF)
                return carry

            lax.fori_loop(0, rows // step, final, 0)
            for wire in z_w:
                wire.start()

        def router_and_norm():
            for wire in z_w:
                wire.landed()
            total = last[pl.ds(pl.multiple_of(me.t * piece, piece), piece), :].astype(F32)
            for k in range(n_tp - 1):
                total = total + got[k].astype(F32)
            small = lax.broadcasted_iota(jnp.int32, (piece, LANES), 1)
            probs = softmax_tile(dot_nt(two_ref[...], wgu[tile:H, :]), small)
            pg = total[:, width:]
            pg = pg + pltpu.roll(pg, LANES // 2, 1)
            pg = jnp.where((small >= off) & (small < off + experts), pg, 0.0)
            logit_grad = (probs * (pg - jnp.sum(probs * pg, axis=1, keepdims=True))).astype(BF)
            grad = total[:, :width] + mdot(logit_grad, wgu[tile:H, :])
            value = mid_ref[...]
            back, terms = norm_back(value, gain_ref[...], grad)
            mid_grad = cot_own_ref[...] + back
            mid_out[...] = mid_grad
            gain_out[...] = jnp.sum(terms, axis=0, keepdims=True)
            at = pl.ds(pl.multiple_of(me.t * piece, piece), piece)
            mid_pack[at, 0:width] = mid_grad.astype(BF)
            mid_pack[at, width:] = logit_grad
            m_r.start()
            m_l.start()

        def stores(m, buf):
            cols = pl.ds(pl.multiple_of(m * m_w, m_w), m_w)
            made = []
            for j in range(2):
                at = pl.ds(j * hid, hid)
                made.append((gus.at[buf, at], dg_out.at[j, :, cols]))
                made.append((gus.at[buf, pl.ds(H + j * hid, hid)], du_out.at[j, :, cols]))
                made.append((dds.at[buf, at], dd_out.at[j, :, cols]))
            return [
                pltpu.make_async_copy(src, dst, store.at[14 + 6 * buf + i])
                for i, (src, dst) in enumerate(made)
            ]

        def weight_grad(m, carry):
            buf = lax.rem(m, 2)
            cols = pl.ds(pl.multiple_of(m * m_w, m_w), m_w)

            @pl.when(m >= 2)
            def _():
                for bb in range(2):

                    @pl.when(buf == bb)
                    def _():
                        for copy in stores(m - 2, bb):
                            copy.wait()

            @pl.when(m == 2)
            def _():
                finish_plane()

            @pl.when(m == 6)
            def _():
                router_and_norm()

            both = mdot(gut[...], nb[:, cols])
            gus[buf] = both
            dss[0, :, cols] = both[2 * hid : used].astype(BF)
            dss[1, :, cols] = both[H + 2 * hid : H + used].astype(BF)
            third = mdot(hwt[...], cb[:, cols])
            dds[buf] = third
            dss[2, :, cols] = third[2 * hid : used].astype(BF)
            for bb in range(2):

                @pl.when(buf == bb)
                def _():
                    for copy in stores(m, bb):
                        copy.start()

            return carry

        lax.fori_loop(0, n_m, weight_grad, 0)
        m_r.landed()
        m_hr.start()
        m_l.landed()
        m_hl.start()
        ds_copy = pltpu.make_async_copy(dss, ds_out, store.at[13])
        ds_copy.start()
        for m in (n_m - 2, n_m - 1):
            for copy in stores(m, m % 2):
                copy.wait()
        for wire in [at_direct[2], *at_fwd, *cols_w, m_hr, m_hl]:
            wire.landed()
        for copy in local_copies + y_copies:
            copy.wait()
        ds_copy.wait()
        for wire in net.all:
            wire.sent()

    ins = (
        two_own, mid_own, cot_own, gain_two,
        cot_all, gate, up, down, sg_t, su_t, sd, router_t, attn, normed, latent,
    )
    outs = [
        ((piece, width), F32),
        ((1, width), F32),
        ((rows, part_w), BF),
        ((tokens, edge), BF),
        ((tokens, edge), BF),
        (gate.shape, F32),
        (up.shape, F32),
        (down.shape, F32),
        ((3, hid_s, width), BF),
        ((8, rows, shard_w), BF),
        ((8, rows, attn_w), BF),
        ((8, rows, shard_w), BF),
        ((8, rows, lat_w), BF),
    ]
    scratch = [
        VMEM((tokens, width), BF),
        VMEM((tokens, pack), BF),
        VMEM((2 * H, width), BF),
        VMEM((H, width), BF),
        VMEM((tokens, 2 * H), BF),
        VMEM((2 * H, tokens), BF),
        VMEM((tokens, H), BF),
        VMEM((H, tokens), BF),
        VMEM((tokens, part_w), BF),
        VMEM((tokens, width), BF),
        VMEM((4, rows, part_w), BF),
        VMEM((2, rows, edge), BF),
        VMEM((2, rows, part_w - edge), BF),
        VMEM((rows, edge), BF),
        VMEM((rows, part_w - edge), BF),
        VMEM((rows, edge), BF),
        VMEM((rows, part_w - edge), BF),
        VMEM((rows, part_w), BF),
        VMEM((n_tp - 1, piece, part_w), BF),
        VMEM((2, 2 * H, m_w), F32),
        VMEM((2, H, m_w), F32),
        VMEM((3, hid_s, width), BF),
    ]
    return pl.pallas_call(
        body,
        out_shape=tuple(jax.ShapeDtypeStruct(*o) for o in outs),
        in_specs=[pl.BlockSpec(memory_space=VMEM)] * 4 + [pl.BlockSpec(memory_space=ANY)] * 11,
        out_specs=(*[pl.BlockSpec(memory_space=VMEM)] * 3, *[pl.BlockSpec(memory_space=ANY)] * 10),
        scratch_shapes=[
            *scratch,
            pltpu.SemaphoreType.DMA((n_wires,)),
            pltpu.SemaphoreType.DMA((n_wires,)),
            pltpu.SemaphoreType.DMA((18,)),
            pltpu.SemaphoreType.DMA((26,)),
        ],
        compiler_params=pltpu.CompilerParams(
            collective_id=4, has_side_effects=True, vmem_limit_bytes=67 * 10**6
        ),
        name="feed_forward",
    )(*ins)


def per_device(
    block_input,
    norm1_gain,
    q_weight,
    kva_weight,
    kv_norm_gain,
    kvb_weight,
    out_weight,
    norm2_gain,
    router_weight,
    shared_gate,
    shared_up,
    shared_down,
    expert_gate,
    expert_up,
    expert_down,
    routes,
    cotangent,
):
    n_tp = lax.axis_size(TP)
    rows, width = block_input.shape
    topk = routes.shape[1]
    experts = router_weight.shape[1]
    heads = q_weight.shape[1] // (DN + DR)
    scale = (DN + DR) ** (-0.5)
    piece = rows // n_tp
    s_id, c_id, t_id = lax.axis_index(SHARD), lax.axis_index(CTX), lax.axis_index(TP)
    shard_w = width // 4
    kv_w = KVR // 4
    pad = LANES - experts

    small = jnp.concatenate(
        [
            norm1_gain.reshape(-1, LANES),
            norm2_gain.reshape(-1, LANES),
            kv_norm_gain.reshape(-1, LANES),
            jnp.zeros((7, LANES), BF),
        ]
    )
    (gathered,) = comm_kernel(
        [
            shard_gather(
                [
                    (q_weight, False),
                    (kva_weight.T, True),
                    (kvb_weight, False),
                    (small, False),
                    (out_weight, True),
                    (router_weight.T, True),
                ],
                block_input,
            )
        ],
        n_tp,
        0,
        "start",
    )
    w_query, w_latent_t, w_expand, small_all, w_output, router_t, x_pair = gathered
    w_query = w_query.reshape(width, -1)
    w_expand = w_expand.reshape(KVR, -1)
    gain_one = small_all[:, 0:4].reshape(-1)
    gain_two = small_all[:, 4:8].reshape(-1)
    gain_kv = small_all[:, 8:9].reshape(-1)

    x_float = block_input.astype(F32)
    cosine, sine = rope_tables(rows, (c_id * rows).astype(F32))
    cos_all, sin_all = rope_tables(2 * rows, jnp.float32(0))
    normed_pair = norm_rows(x_pair.reshape(2 * rows, width).astype(F32), gain_one).astype(BF)
    normed_one = norm_rows(x_float, gain_one).astype(BF)
    query = mdot(normed_one, w_query).reshape(rows, heads, DN + DR)
    query_nope = query[..., :DN].astype(BF)
    query_rope = rotate(query[..., DN:], cosine[:, None, :], sine[:, None, :]).astype(BF)
    latent = dot_nt(normed_pair, w_latent_t)
    latent_pair = norm_rows(latent[:, :KVR], gain_kv).astype(BF)
    rope_pair = rotate(latent[:, KVR:], cos_all, sin_all).astype(BF)
    kv_pair = mdot(latent_pair, w_expand).astype(BF).reshape(2 * rows, heads, DN + DV)
    key_pair, value_pair = kv_pair[..., :DN], kv_pair[..., DN:]
    score = jnp.einsum("qhd,khd->hqk", query_nope, key_pair, preferred_element_type=F32)
    score = score + jnp.einsum("qhd,kd->hqk", query_rope, rope_pair, preferred_element_type=F32)
    q_pos = c_id * rows + jnp.arange(rows, dtype=jnp.int32)
    k_pos = jnp.arange(2 * rows, dtype=jnp.int32)
    score = jnp.where(k_pos[None, None, :] <= q_pos[None, :, None], score * scale, NEG)
    top = jnp.max(score, axis=-1, keepdims=True)
    expo = jnp.exp(score - top)
    total = jnp.sum(expo, axis=-1, keepdims=True)
    attn = jnp.einsum("hqk,khd->hqd", expo.astype(BF), value_pair, preferred_element_type=F32)
    attn_rows = (attn / total).astype(BF).transpose(1, 0, 2)
    lse = top + jnp.log(total)
    attn_flat = attn_rows.reshape(rows, heads * DV)

    def own(a):
        return lax.dynamic_slice_in_dim(a, t_id * piece, piece, 0)

    cot_pack = jnp.concatenate(
        [cotangent.astype(BF), jnp.pad(routes.astype(BF), ((0, 0), (0, LANES - topk)))], axis=1
    )
    (attn_full,), (cot_all,), (sg_t,), (su_t,), (sd,) = comm_kernel(
        [
            tp_reduce_scatter(mdot(attn_flat, w_output).astype(BF), n_tp),
            plane_gather(cot_pack),
            shard_rows(shared_gate.T),
            shard_rows(shared_up.T),
            shard_rows(shared_down),
        ],
        n_tp,
        1,
        "middle",
    )
    mid = own(x_float) + attn_full
    two_own = norm_rows(mid, gain_two).astype(BF)
    latent_own = lax.dynamic_slice_in_dim(latent_pair, c_id * rows, rows, 0)

    (
        mid_grad, gain_two_sum, mid_pack, y_left, y_right, grad_gate, grad_up, grad_expert_down, shared_grads,
        two_cols, attn_all, one_cols, lat_cols,
    ) = feed_forward(
        two_own,
        mid,
        own(cotangent),
        gain_two.astype(F32)[None, :],
        cot_all,
        expert_gate.transpose(0, 2, 1),
        expert_up.transpose(0, 2, 1),
        expert_down,
        sg_t,
        su_t,
        sd,
        router_t,
        attn_flat,
        normed_one,
        latent_own,
        topk,
        n_tp,
    )
    mid_b = mid_pack[:, :width]

    out_grad = dot_nt(mid_b, w_output).reshape(rows, heads, DV)
    out_grad_b = out_grad.astype(BF)
    delta = jnp.sum(out_grad * attn_rows.astype(F32), axis=-1).T[..., None]
    prob = jnp.exp(score - lse)
    dprob = jnp.einsum("qhd,khd->hqk", out_grad_b, value_pair, preferred_element_type=F32)
    dscore = (prob * (dprob - delta)).astype(BF)
    nope_grad = jnp.einsum("hqk,khd->qhd", dscore, key_pair, preferred_element_type=F32) * scale
    rope_qgrad = jnp.einsum("hqk,kd->qhd", dscore, rope_pair, preferred_element_type=F32) * scale
    key_grad = jnp.einsum("hqk,qhd->khd", dscore, query_nope, preferred_element_type=F32) * scale
    value_grad = jnp.einsum(
        "hqk,qhd->khd", prob.astype(BF), out_grad_b, preferred_element_type=F32
    )
    rope_kgrad = jnp.einsum("hqk,qhd->kd", dscore, query_rope, preferred_element_type=F32) * scale
    kv_terms = jnp.concatenate(
        [
            jnp.concatenate([key_grad, value_grad], axis=-1).reshape(2 * rows, -1),
            jnp.pad(rope_kgrad, ((0, 0), (0, LANES - DR))),
        ],
        axis=1,
    )
    mine = lax.dynamic_slice_in_dim(kv_terms, c_id * rows, rows, 0)
    other = lax.dynamic_slice_in_dim(kv_terms, (1 - c_id) * rows, rows, 0).astype(BF)
    (swapped,), (y_left,), (mid_cols,), (logit_all,) = comm_kernel(
        [
            ctx_swap(other),
            reduce_everywhere(y_left, n_tp),
            plane_columns(mid_b),
            plane_gather(mid_pack[:, width:], 1),
        ],
        n_tp,
        2,
        "swap",
    )
    kv_sum = mine + swapped.astype(F32)
    kv_grad = kv_sum[:, : heads * (DN + DV)].astype(BF)
    rope_part = rotate_back(kv_sum[:, heads * (DN + DV) :][:, :DR], cosine, sine)
    rope_qback = rotate_back(rope_qgrad, cosine[:, None, :], sine[:, None, :])
    query_grad = jnp.concatenate([nope_grad, rope_qback], axis=-1).astype(BF).reshape(rows, -1)
    latent_part = dot_nt(kv_grad, w_expand)
    one_part = dot_nt(query_grad, w_query)
    back_part = jnp.concatenate(
        [one_part, latent_part, jnp.pad(rope_part, ((0, 0), (0, LANES - DR)))], axis=1
    ).astype(BF)
    (back,), (y_right,), (shared_cols,) = comm_kernel(
        [
            tp_reduce_scatter(back_part, n_tp),
            reduce_everywhere(y_right, n_tp),
            plane_columns(shared_grads.reshape(-1, width)),
        ],
        n_tp,
        3,
        "back",
    )
    out_own = mid + jnp.concatenate([y_left, y_right], axis=1)

    compressed = own(lax.dynamic_slice_in_dim(latent, c_id * rows, rows, 0))[:, :KVR]
    compressed_grad, gain_kv_terms = norm_back(compressed, gain_kv, back[:, width : width + KVR])
    latent_grad = jnp.concatenate(
        [compressed_grad, back[:, width + KVR : width + KVR + DR]], axis=1
    ).astype(BF)
    one_grad = back[:, :width] + mdot(latent_grad, w_latent_t)
    input_norm_grad, gain_one_terms = norm_back(own(x_float), gain_one, one_grad)
    input_own = mid_grad + input_norm_grad

    lat_pack = jnp.pad(latent_grad, ((0, 0), (0, 5 * LANES - KVR - DR)))
    gains = jnp.concatenate(
        [
            jnp.sum(gain_one_terms, axis=0),
            gain_two_sum[0],
            jnp.sum(gain_kv_terms, axis=0),
            jnp.zeros((512,), F32),
        ]
    ).reshape(8, -1)
    (lat_all,), (head_all,), (block_output,), (input_grad,), (gains,) = comm_kernel(
        [
            gather_rows(lat_pack, n_tp),
            plane_gather(jnp.concatenate([query_grad, kv_grad], axis=1)),
            tp_all_gather(out_own.astype(BF), n_tp),
            tp_all_gather(input_own.astype(BF), n_tp),
            sum_everywhere(gains, n_tp),
        ],
        n_tp,
        5,
        "finish",
    )
    head_all = head_all.reshape(8 * rows, -1)
    split = heads * (DN + DR)
    lat_all = lat_all.reshape(8 * rows, -1)[:, : KVR + DR]
    one_cols = one_cols.reshape(8 * rows, -1)
    grad_query = dot_tn(one_cols, head_all[:, :split])
    grad_latent = dot_tn(lat_all, one_cols).T
    grad_expand = dot_tn(lat_cols.reshape(8 * rows, -1), head_all[:, split:])
    grad_out_w = dot_tn(attn_all.reshape(8 * rows, -1), mid_cols.reshape(8 * rows, -1))
    off = (2 * expert_gate.shape[2] + sg_t.shape[0]) % LANES
    logit_all = logit_all.reshape(8 * rows, -1)[:, off : off + experts]
    grad_router = dot_tn(logit_all, two_cols.reshape(8 * rows, -1)).T
    shared_cols = shared_cols.reshape(8, 3, -1, shard_w)
    grad_sgate, grad_sup, grad_sdown = (
        shared_cols[:, i].reshape(-1, shard_w).astype(F32) for i in range(3)
    )
    gains = gains.reshape(-1)
    grad_one = lax.dynamic_slice_in_dim(gains, s_id * shard_w, shard_w, 0)
    grad_two = lax.dynamic_slice_in_dim(gains, width + s_id * shard_w, shard_w, 0)
    grad_kv = lax.dynamic_slice_in_dim(gains, 2 * width + s_id * kv_w, kv_w, 0)
    return (
        block_output.astype(F32),
        input_grad.astype(F32),
        grad_one,
        grad_query,
        grad_latent,
        grad_kv,
        grad_expand,
        grad_out_w,
        grad_two,
        grad_router,
        grad_sgate.T,
        grad_sup.T,
        grad_sdown,
        grad_gate.transpose(0, 2, 1),
        grad_up.transpose(0, 2, 1),
        grad_expert_down,
    )


def send_rows(buffer):
    return lax.all_to_all(buffer, (SHARD, CTX), split_axis=0, concat_axis=0, tiled=True)


def return_rows(partial_value, slots):
    back_rows = lax.all_to_all(
        partial_value, (SHARD, CTX), split_axis=0, concat_axis=0, tiled=True
    )
    flat_back = back_rows.reshape(-1, back_rows.shape[-1])
    return flat_back[slots]


def per_device_general(
    block_input,
    norm1_gain,
    q_weight,
    kva_weight,
    kv_norm_gain,
    kvb_weight,
    out_weight,
    norm2_gain,
    router_weight,
    shared_gate,
    shared_up,
    shared_down,
    expert_gate,
    expert_up,
    expert_down,
    routes,
    cotangent,
):
    tok_rows = block_input.shape[0]
    head_count = q_weight.shape[1] // (DN + DR)
    score_scale = (DN + DR) ** (-0.5)
    (
        gain_one,
        w_query,
        w_latent,
        gain_kv,
        w_expand,
        w_output,
        gain_two,
        w_router,
        w_sgate,
        w_sup,
        w_sdown,
    ) = (
        lax.all_gather(norm1_gain, SHARD, axis=0, tiled=True),
        lax.all_gather(q_weight, SHARD, axis=0, tiled=True),
        lax.all_gather(kva_weight, SHARD, axis=0, tiled=True),
        lax.all_gather(kv_norm_gain, SHARD, axis=0, tiled=True),
        lax.all_gather(kvb_weight, SHARD, axis=0, tiled=True),
        lax.all_gather(out_weight, SHARD, axis=1, tiled=True),
        lax.all_gather(norm2_gain, SHARD, axis=0, tiled=True),
        lax.all_gather(router_weight, SHARD, axis=0, tiled=True),
        lax.all_gather(shared_gate, SHARD, axis=0, tiled=True),
        lax.all_gather(shared_up, SHARD, axis=0, tiled=True),
        lax.all_gather(shared_down, SHARD, axis=1, tiled=True),
    )
    block_index = lax.axis_index(CTX)
    cosine, sine_table = rope_tables(tok_rows, (block_index * tok_rows).astype(jnp.float32))
    x_float = block_input.astype(jnp.float32)
    normed_one = norm_rows(x_float, gain_one).astype(jnp.bfloat16)
    query = mdot(normed_one, w_query).reshape(tok_rows, head_count, DN + DR)
    query_rot = rotate(query[..., DN:], cosine[:, None, :], sine_table[:, None, :])
    query = jnp.concatenate([query[..., :DN], query_rot], axis=-1).astype(jnp.bfloat16)
    query_nope = query[..., :DN]
    query_rope = query[..., DN:]
    latent = mdot(normed_one, w_latent)
    compressed = latent[:, :KVR]
    latent_n = norm_rows(compressed, gain_kv).astype(jnp.bfloat16)
    rope_key = rotate(latent[:, KVR:], cosine, sine_table).astype(jnp.bfloat16)
    first_piece = mdot(latent_n, w_expand).astype(jnp.bfloat16)
    gathered, rope_all = (
        lax.all_gather(first_piece, CTX, axis=0, tiled=True),
        lax.all_gather(rope_key, CTX, axis=0, tiled=True),
    )
    query_pos = block_index * tok_rows + jnp.arange(tok_rows, dtype=jnp.int32)

    def scores_at(block_id):
        blk_start = block_id * tok_rows
        kv_block = lax.dynamic_slice_in_dim(gathered, blk_start, tok_rows, 0).reshape(
            tok_rows, head_count, DN + DV
        )
        rope_block = lax.dynamic_slice_in_dim(rope_all, blk_start, tok_rows, 0)
        score = jnp.einsum(
            "qhd,khd->hqk", query_nope, kv_block[..., :DN], preferred_element_type=jnp.float32
        )
        score = score + jnp.einsum(
            "qhd,kd->hqk", query_rope, rope_block, preferred_element_type=jnp.float32
        )
        score = score * score_scale
        key_pos = blk_start + jnp.arange(tok_rows, dtype=jnp.int32)
        score = jnp.where(key_pos[None, None, :] <= query_pos[None, :, None], score, NEG)
        return (score, kv_block, rope_block)

    def forward_block(block_id, carry):
        run_max, run_sum, weighted = carry
        score, kv_block, rope_block = scores_at(block_id)
        new_max = jnp.maximum(run_max, jnp.max(score, axis=-1))
        factor = jnp.exp(run_max - new_max)
        expo = jnp.exp(score - new_max[..., None])
        run_sum = factor * run_sum + jnp.sum(expo, axis=-1)
        weighted = factor[..., None] * weighted + jnp.einsum(
            "hqk,khd->hqd",
            expo.astype(jnp.bfloat16),
            kv_block[..., DN:],
            preferred_element_type=jnp.float32,
        )
        return (new_max, run_sum, weighted)

    start_state = (
        jnp.full((head_count, tok_rows), NEG, jnp.float32),
        jnp.zeros((head_count, tok_rows), jnp.float32),
        jnp.zeros((head_count, tok_rows, DV), jnp.float32),
    )
    run_max, run_sum, weighted = lax.fori_loop(0, block_index + 1, forward_block, start_state)
    lse = run_max + jnp.log(run_sum)
    attn_rows = (weighted / run_sum[..., None]).astype(jnp.bfloat16).transpose(1, 0, 2)
    attn_flat = attn_rows.reshape(tok_rows, head_count * DV)
    attn_full = lax.psum(mdot(attn_flat, w_output), TP)
    mid = x_float + attn_full
    normed_two = norm_rows(mid, gain_two).astype(jnp.bfloat16)
    probs = jax.nn.softmax(mdot(normed_two, w_router), axis=-1)
    experts = probs.shape[1]
    topk = routes.shape[1]
    picks = (routes[:, :, None] == jnp.arange(experts, dtype=jnp.int32)[None, None, :]).astype(
        jnp.float32
    )
    route_w = jnp.sum(picks * probs[:, None, :], axis=-1)
    shared_a = mdot(normed_two, w_sgate)
    shared_b = mdot(normed_two, w_sup)
    shared_h = (jax.nn.silu(shared_a) * shared_b).astype(jnp.bfloat16)
    shared_y = mdot(shared_h, w_sdown)
    capacity = 2 * tok_rows * topk // experts
    owners = lax.axis_size((SHARD, CTX))
    local_experts = expert_gate.shape[0]
    width = normed_two.shape[1]
    flat_routes = routes.reshape(-1)
    onehot = (flat_routes[:, None] == jnp.arange(experts, dtype=jnp.int32)[None, :]).astype(
        jnp.int32
    )
    rank = jnp.sum((jnp.cumsum(onehot, axis=0) - 1) * onehot, axis=1)
    slots = flat_routes * capacity + rank
    source_row = jnp.arange(tok_rows * topk, dtype=jnp.int32) // topk
    send_buffer = (
        jnp.zeros((experts * capacity, width), jnp.bfloat16).at[slots].set(normed_two[source_row])
    )
    received = send_rows(send_buffer.reshape(owners, local_experts * capacity, width)).reshape(
        owners, local_experts, capacity, width
    )
    gate_act = jnp.einsum(
        "gecd,edf->gecf", received, expert_gate, preferred_element_type=jnp.float32
    )
    up_act = jnp.einsum("gecd,edf->gecf", received, expert_up, preferred_element_type=jnp.float32)
    hidden = (jax.nn.silu(gate_act) * up_act).astype(jnp.bfloat16)
    expert_y = jnp.einsum("gecf,efd->gecd", hidden, expert_down, preferred_element_type=jnp.float32)
    routed_out = return_rows(
        expert_y.reshape(owners, local_experts * capacity, width), slots
    ).reshape(tok_rows, topk, width)
    routed_part = jnp.sum(route_w[:, :, None] * routed_out, axis=1) + shared_y
    weight_part = jnp.sum(routed_out * cotangent[:, None, :], axis=-1)
    moe_out, route_grad = lax.psum((routed_part, weight_part), TP)
    block_output = mid + moe_out
    cot_b = cotangent.astype(jnp.bfloat16)
    routed_grad = (
        (route_w[:, :, None] * cotangent[:, None, :])
        .astype(jnp.bfloat16)
        .reshape(tok_rows * topk, width)
    )
    grad_buffer = jnp.zeros((experts * capacity, width), jnp.bfloat16).at[slots].set(routed_grad)
    grad_recv = send_rows(grad_buffer.reshape(owners, local_experts * capacity, width)).reshape(
        owners, local_experts, capacity, width
    )
    hidden_grad = jnp.einsum(
        "gecd,efd->gecf", grad_recv, expert_down, preferred_element_type=jnp.float32
    )
    gate_grad = (hidden_grad * up_act * silu_slope(gate_act)).astype(jnp.bfloat16)
    up_grad = (hidden_grad * jax.nn.silu(gate_act)).astype(jnp.bfloat16)
    grad_expert_down = jnp.einsum(
        "gecf,gecd->efd", hidden, grad_recv, preferred_element_type=jnp.float32
    )
    grad_expert_gate = jnp.einsum(
        "gecd,gecf->edf", received, gate_grad, preferred_element_type=jnp.float32
    )
    grad_expert_up = jnp.einsum(
        "gecd,gecf->edf", received, up_grad, preferred_element_type=jnp.float32
    )
    row_grad = jnp.einsum(
        "gecf,edf->gecd", gate_grad, expert_gate, preferred_element_type=jnp.float32
    )
    row_grad = row_grad + jnp.einsum(
        "gecf,edf->gecd", up_grad, expert_up, preferred_element_type=jnp.float32
    )
    routed_back = return_rows(
        row_grad.reshape(owners, local_experts * capacity, width), slots
    ).reshape(tok_rows, topk, width)
    shared_grad = jnp.einsum("td,fd->tf", cot_b, w_sdown, preferred_element_type=jnp.float32)
    sgate_grad = (shared_grad * shared_b * silu_slope(shared_a)).astype(jnp.bfloat16)
    sup_grad = (shared_grad * jax.nn.silu(shared_a)).astype(jnp.bfloat16)
    grad_sdown = jnp.einsum("tf,td->fd", shared_h, cot_b, preferred_element_type=jnp.float32)
    grad_sgate = jnp.einsum("td,tf->df", normed_two, sgate_grad, preferred_element_type=jnp.float32)
    grad_sup = jnp.einsum("td,tf->df", normed_two, sup_grad, preferred_element_type=jnp.float32)
    two_part = jnp.sum(routed_back, axis=1)
    two_part = two_part + jnp.einsum(
        "tf,df->td", sgate_grad, w_sgate, preferred_element_type=jnp.float32
    )
    two_part = two_part + jnp.einsum(
        "tf,df->td", sup_grad, w_sup, preferred_element_type=jnp.float32
    )
    two_grad = lax.psum(two_part, TP)
    prob_grad = jnp.sum(picks * route_grad[:, :, None], axis=1)
    logit_grad = (probs * (prob_grad - jnp.sum(probs * prob_grad, axis=-1, keepdims=True))).astype(
        jnp.bfloat16
    )
    grad_router = jnp.einsum(
        "td,te->de", normed_two, logit_grad, preferred_element_type=jnp.float32
    )
    two_grad = two_grad + jnp.einsum(
        "te,de->td", logit_grad, w_router, preferred_element_type=jnp.float32
    )
    _, norm_two_back = jax.vjp(norm_rows, mid, gain_two.astype(jnp.float32))
    mid_norm_grad, grad_gain_two = norm_two_back(two_grad)
    mid_grad = cotangent + mid_norm_grad
    mid_b = mid_grad.astype(jnp.bfloat16)
    grad_out_w = jnp.einsum("tj,td->jd", attn_flat, mid_b, preferred_element_type=jnp.float32)
    out_grad = jnp.einsum("td,jd->tj", mid_b, w_output, preferred_element_type=jnp.float32).reshape(
        tok_rows, head_count, DV
    )
    out_grad_b = out_grad.astype(jnp.bfloat16)
    delta = jnp.sum(out_grad * attn_rows.astype(jnp.float32), axis=-1).T
    key_count = gathered.shape[0]
    term_width = head_count * (DN + DV + DR)

    def back_block(block_id, carry):
        nope_grad, rope_qgrad, terms = carry
        score, kv_block, rope_block = scores_at(block_id)
        probs_blk = jnp.exp(score - lse[..., None])
        prob_b = probs_blk.astype(jnp.bfloat16)
        dprob = jnp.einsum(
            "qhd,khd->hqk", out_grad_b, kv_block[..., DN:], preferred_element_type=jnp.float32
        )
        dscore = (probs_blk * (dprob - delta[..., None])).astype(jnp.bfloat16)
        nope_grad = (
            nope_grad
            + jnp.einsum(
                "hqk,khd->qhd", dscore, kv_block[..., :DN], preferred_element_type=jnp.float32
            )
            * score_scale
        )
        rope_qgrad = (
            rope_qgrad
            + jnp.einsum("hqk,kd->qhd", dscore, rope_block, preferred_element_type=jnp.float32)
            * score_scale
        )
        key_nope_grad = (
            jnp.einsum("hqk,qhd->khd", dscore, query_nope, preferred_element_type=jnp.float32)
            * score_scale
        )
        key_rope_grad = (
            jnp.einsum("hqk,qhd->khd", dscore, query_rope, preferred_element_type=jnp.float32)
            * score_scale
        )
        value_grad = jnp.einsum(
            "hqk,qhd->khd", prob_b, out_grad_b, preferred_element_type=jnp.float32
        )
        block_terms = jnp.concatenate([key_nope_grad, value_grad, key_rope_grad], axis=-1).reshape(
            tok_rows, term_width
        )
        terms = lax.dynamic_update_slice_in_dim(terms, block_terms, block_id * tok_rows, 0)
        return (nope_grad, rope_qgrad, terms)

    back_init = (
        jnp.zeros((tok_rows, head_count, DN), jnp.float32),
        jnp.zeros((tok_rows, head_count, DR), jnp.float32),
        jnp.zeros((key_count, term_width), jnp.float32),
    )
    nope_grad, rope_qgrad, terms = lax.fori_loop(0, block_index + 1, back_block, back_init)
    key_terms = lax.psum_scatter(terms, CTX, scatter_dimension=0, tiled=True).reshape(
        tok_rows, head_count, DN + DV + DR
    )
    kv_grad = (
        key_terms[..., : DN + DV].reshape(tok_rows, head_count * (DN + DV)).astype(jnp.bfloat16)
    )
    rope_grad = rotate_back(jnp.sum(key_terms[..., DN + DV :], axis=1), cosine, sine_table)
    grad_expand = jnp.einsum("ti,tj->ij", latent_n, kv_grad, preferred_element_type=jnp.float32)
    latent_part = jnp.einsum("tj,ij->ti", kv_grad, w_expand, preferred_element_type=jnp.float32)
    rope_qback = rotate_back(rope_qgrad, cosine[:, None, :], sine_table[:, None, :])
    query_grad = (
        jnp.concatenate([nope_grad, rope_qback], axis=-1)
        .astype(jnp.bfloat16)
        .reshape(tok_rows, head_count * (DN + DR))
    )
    grad_query = jnp.einsum("td,tj->dj", normed_one, query_grad, preferred_element_type=jnp.float32)
    normed_part = jnp.einsum("tj,dj->td", query_grad, w_query, preferred_element_type=jnp.float32)
    latent_sum, normed_sum = lax.psum(
        (jnp.concatenate([latent_part, rope_grad], axis=-1), normed_part), TP
    )
    _, kv_back = jax.vjp(norm_rows, compressed, gain_kv.astype(jnp.float32))
    compressed_grad, grad_gain_kv = kv_back(latent_sum[:, :KVR])
    latent_grad = jnp.concatenate([compressed_grad, latent_sum[:, KVR:]], axis=-1).astype(
        jnp.bfloat16
    )
    grad_latent = jnp.einsum(
        "td,tl->dl", normed_one, latent_grad, preferred_element_type=jnp.float32
    )
    one_grad = normed_sum + jnp.einsum(
        "tl,dl->td", latent_grad, w_latent, preferred_element_type=jnp.float32
    )
    _, one_back = jax.vjp(norm_rows, x_float, gain_one.astype(jnp.float32))
    input_norm_grad, grad_gain_one = one_back(one_grad)
    input_grad = mid_grad + input_norm_grad
    (
        red_one,
        red_query,
        red_latent,
        red_kv,
        red_expand,
        red_output,
        red_two,
        red_router,
        red_sgate,
        red_sup,
        red_sdown,
    ) = (
        lax.psum_scatter(grad_gain_one, SHARD, scatter_dimension=0, tiled=True),
        lax.psum_scatter(grad_query, SHARD, scatter_dimension=0, tiled=True),
        lax.psum_scatter(grad_latent, SHARD, scatter_dimension=0, tiled=True),
        lax.psum_scatter(grad_gain_kv, SHARD, scatter_dimension=0, tiled=True),
        lax.psum_scatter(grad_expand, SHARD, scatter_dimension=0, tiled=True),
        lax.psum_scatter(grad_out_w, SHARD, scatter_dimension=1, tiled=True),
        lax.psum_scatter(grad_gain_two, SHARD, scatter_dimension=0, tiled=True),
        lax.psum_scatter(grad_router, SHARD, scatter_dimension=0, tiled=True),
        lax.psum_scatter(grad_sgate, SHARD, scatter_dimension=0, tiled=True),
        lax.psum_scatter(grad_sup, SHARD, scatter_dimension=0, tiled=True),
        lax.psum_scatter(grad_sdown, SHARD, scatter_dimension=1, tiled=True),
    )
    (
        sum_one,
        sum_query,
        sum_latent,
        sum_kv,
        sum_expand,
        sum_output,
        sum_two,
        sum_router,
        sum_sgate,
        sum_sup,
        sum_sdown,
    ) = lax.psum(
        (
            red_one,
            red_query,
            red_latent,
            red_kv,
            red_expand,
            red_output,
            red_two,
            red_router,
            red_sgate,
            red_sup,
            red_sdown,
        ),
        CTX,
    )
    return (
        block_output,
        input_grad,
        sum_one,
        sum_query,
        sum_latent,
        sum_kv,
        sum_expand,
        sum_output,
        sum_two,
        sum_router,
        sum_sgate,
        sum_sup,
        sum_sdown,
        grad_expert_gate,
        grad_expert_up,
        grad_expert_down,
    )


def solution(mesh):
    in_specs = (
        P((SHARD, CTX), None),
        P(SHARD),
        P(SHARD, TP),
        P(SHARD, None),
        P(SHARD),
        P(SHARD, TP),
        P(TP, SHARD),
        P(SHARD),
        P(SHARD, None),
        P(SHARD, TP),
        P(SHARD, TP),
        P(TP, SHARD),
        P((SHARD, CTX), None, TP),
        P((SHARD, CTX), None, TP),
        P((SHARD, CTX), TP, None),
        P((SHARD, CTX), None),
        P((SHARD, CTX), None),
    )
    out_specs = (
        P((SHARD, CTX), None),
        P((SHARD, CTX), None),
        P(SHARD),
        P(SHARD, TP),
        P(SHARD, None),
        P(SHARD),
        P(SHARD, TP),
        P(TP, SHARD),
        P(SHARD),
        P(SHARD, None),
        P(SHARD, TP),
        P(SHARD, TP),
        P(TP, SHARD),
        P((SHARD, CTX), None, TP),
        P((SHARD, CTX), None, TP),
        P((SHARD, CTX), TP, None),
    )
    routed = mesh.shape[SHARD] == 4 and mesh.shape[CTX] == 2 and mesh.shape[TP] == 4
    return jax.shard_map(
        per_device if routed else per_device_general, mesh=mesh, in_specs=in_specs, out_specs=out_specs, check_vma=False
    )
```

```python
import functools

import jax
import jax.numpy as jnp
from jax import lax
from jax.experimental import pallas as pl
from jax.experimental.pallas import tpu as pltpu
from jax.sharding import PartitionSpec as P

DN = 128
DR = 64
DV = 128
KVR = 512
LANES = 128
SHARD, CTX, TP = "shard", "ctx", "tp"

EPS = 1e-06
NEG = -1e30

BF = jnp.bfloat16
F32 = jnp.float32
MESH = pl.DeviceIdType.MESH
ANY = pl.ANY
VMEM = pltpu.VMEM


def norm_rows(value, gain):
    factor = lax.rsqrt(jnp.mean(value * value, axis=-1, keepdims=True) + EPS)
    return value * factor * gain.astype(F32)


def norm_back(value, gain, grad):
    factor = lax.rsqrt(jnp.mean(value * value, axis=-1, keepdims=True) + EPS)
    scaled = grad * gain.astype(F32)
    inner = jnp.mean(scaled * value, axis=-1, keepdims=True)
    return factor * (scaled - value * (factor * factor * inner)), grad * value * factor


def rope_tables(count, offset):
    half_size = DR // 2
    position = jnp.arange(count, dtype=F32) + offset
    freqs = 10000.0 ** (-(jnp.arange(half_size, dtype=F32) * 2.0 / DR))
    angle = position[:, None] * freqs[None, :]
    return (jnp.cos(angle), jnp.sin(angle))


def rotate(value, cosine, sine_table):
    half_size = DR // 2
    first = value[..., :half_size]
    second = value[..., half_size:]
    return jnp.concatenate(
        [first * cosine - second * sine_table, first * sine_table + second * cosine], axis=-1
    )


def rotate_back(grad, cosine, sine_table):
    half_size = DR // 2
    first = grad[..., :half_size]
    second = grad[..., half_size:]
    return jnp.concatenate(
        [first * cosine + second * sine_table, second * cosine - first * sine_table], axis=-1
    )


def silu_slope(value):
    sigmoid = jax.nn.sigmoid(value)
    return sigmoid * (1.0 + value * (1.0 - sigmoid))


def mdot(left, right):
    return jnp.dot(left, right, preferred_element_type=F32)


def dot_nt(left, right):
    return lax.dot_general(left, right, (((1,), (1,)), ((), ())), preferred_element_type=F32)


def dot_tn(left, right):
    return lax.dot_general(left, right, (((0,), (0,)), ((), ())), preferred_element_type=F32)


class Place:
    def __init__(self, n_tp):
        self.s = lax.axis_index(SHARD)
        self.c = lax.axis_index(CTX)
        self.t = lax.axis_index(TP)
        self.core = lax.rem(self.s, 2)
        self.y = self.s // 2
        self.n_tp = n_tp
        self.over_x = self.flip(0, 0, 1)
        self.over_y = self.flip(1, 0, 0)
        self.over_core = self.flip(0, 1, 0)

    def along(self, step):
        t = lax.rem(self.t + step + self.n_tp, self.n_tp)
        return {SHARD: self.s, CTX: self.c, TP: t}

    def flip(self, dy, dcore, dx):
        y = self.y + dy * (1 - 2 * self.y)
        core = self.core + dcore * (1 - 2 * self.core)
        x = self.c + dx * (1 - 2 * self.c)
        return {SHARD: 2 * y + core, CTX: x, TP: self.t}

    def peers(self, kinds):
        flips = []
        if "p" in kinds:
            flips = FLIPS
        else:
            flips = [f for kind, f in (("x", FLIPS[0]), ("k", FLIPS[1]), ("y", FLIPS[3])) if kind in kinds]
        out = [self.flip(*f) for f in flips]
        if "z" in kinds:
            out += [self.along(k) for k in range(1, self.n_tp)]
        return out


FLIPS = [(dy, dk, dx) for dy in (0, 1) for dk in (0, 1) for dx in (0, 1)][1:]


def slot(s, c):
    return 2 * s + c


class Net:
    def __init__(self, send, recv, local):
        self.send, self.recv, self.local = send, recv, local
        self.puts = []
        self.n_local = 0

    def put(self, src, dst, to):
        i = len(self.puts)
        copy = pltpu.make_async_remote_copy(
            src_ref=src,
            dst_ref=dst,
            send_sem=self.send.at[i],
            recv_sem=self.recv.at[i],
            device_id=to,
            device_id_type=MESH,
        )
        copy.start()
        self.puts.append(copy)
        return copy

    def move(self, src, dst):
        copy = pltpu.make_async_copy(src, dst, self.local.at[self.n_local])
        self.n_local += 1
        copy.start()
        return copy

    def finish(self):
        for copy in self.puts:
            copy.wait_send()


def greet(peers):
    barrier = pltpu.get_barrier_semaphore()
    for peer in peers:
        pl.semaphore_signal(barrier, inc=1, device_id=peer, device_id_type=MESH)
    pl.semaphore_wait(barrier, len(peers))


class Job:
    def __init__(self, run, ins, outs, scratch, n_put, n_local, peers):
        self.run, self.ins, self.outs, self.scratch = run, ins, outs, scratch
        self.n_put, self.n_local, self.peers = n_put, n_local, peers


def comm_kernel(jobs, n_tp, collective_id, name):
    ins = [i for job in jobs for i in job.ins]
    outs = [o for job in jobs for o in job.outs]
    scratch = [s for job in jobs for s in job.scratch]
    n_put = sum(job.n_put for job in jobs)
    n_local = max(sum(job.n_local for job in jobs), 1)
    kinds = "".join(sorted(set("".join(job.peers for job in jobs))))

    def body(*refs):
        in_refs, out_refs = refs[: len(ins)], refs[len(ins) : len(ins) + len(outs)]
        rest = refs[len(ins) + len(outs) :]
        me = Place(n_tp)
        net = Net(*rest[len(scratch) :])
        greet(me.peers(kinds))
        running = []
        i = o = s = 0
        for job in jobs:
            ni, no, ns = len(job.ins), len(job.outs), len(job.scratch)
            running.append(
                job.run(net, me, in_refs[i : i + ni], out_refs[o : o + no], rest[s : s + ns])
            )
            i, o, s = i + ni, o + no, s + ns
        while running:
            running = [r for r in running if next(r, None) is not None]
        net.finish()

    got = pl.pallas_call(
        body,
        out_shape=tuple(jax.ShapeDtypeStruct(shape, dtype) for shape, dtype, _ in outs),
        in_specs=[pl.BlockSpec(memory_space=space) for _, space in ins],
        out_specs=tuple(pl.BlockSpec(memory_space=space) for _, _, space in outs),
        scratch_shapes=[
            *scratch,
            pltpu.SemaphoreType.DMA((n_put,)),
            pltpu.SemaphoreType.DMA((n_put,)),
            pltpu.SemaphoreType.DMA((n_local,)),
        ],
        compiler_params=pltpu.CompilerParams(
            collective_id=collective_id, has_side_effects=True, vmem_limit_bytes=60 * 2**20
        ),
        name=name,
    )(*[a for a, _ in ins])
    split, o = [], 0
    for job in jobs:
        split.append(got[o : o + len(job.outs)])
        o += len(job.outs)
    return split


def shard_gather(weights, block):
    shapes = [w.shape for w, _ in weights]
    side = [by for _, by in weights]

    def run(net, me, ins, outs, bounce):
        n = len(shapes)
        x_in, x_out = ins[n], outs[n]
        other = lax.rem(me.s + 2, 4)

        def place(i, s, which=None):
            rows, cols = shapes[i]
            at = pl.ds(0, rows)
            if which is not None:
                at = pl.ds(pl.multiple_of(which * (rows // 2), rows // 2), rows // 2)
            if side[i]:
                return outs[i].at[at, pl.ds(pl.multiple_of(s * cols, LANES), cols)]
            return outs[i].at[s, at]

        loads = [net.move(src, b) for src, b in zip(ins, bounce)]
        from_y, own = [], []
        for i in range(n):
            rows = shapes[i][0]
            at = pl.ds(pl.multiple_of(me.c * (rows // 2), rows // 2), rows // 2)
            from_y.append(net.put(ins[i].at[at], place(i, me.s, me.c), me.over_y))
            if i == 0:
                wait_x = net.put(x_in, x_out.at[me.c], me.over_x)
        for i in range(n):
            own.append(net.put(ins[i], place(i, me.s), me.over_core))
        yield 1
        stores = []
        for i, (load, b) in enumerate(zip(loads, bounce)):
            load.wait()
            stores.append(net.move(b, place(i, me.s) if i < n else x_out.at[me.c]))
        from_x, relays = [], []
        for i in range(n):
            from_y[i].wait_recv()
            piece = place(i, other, me.c)
            from_x.append(net.put(piece, piece, me.over_x))
            relays.append(net.put(piece, piece, me.over_core))
            yield 1
        for i in range(n):
            from_x[i].wait_recv()
            piece = place(i, other, 1 - me.c)
            relays.append(net.put(piece, piece, me.over_core))
            yield 1
        wait_x.wait_recv()
        for got in own + relays:
            got.wait_recv()
        for store in stores:
            store.wait()

    n = len(weights)
    outs = []
    for (rows, cols), by in zip(shapes, side):
        outs.append(((rows, 4 * cols) if by else (4, rows, cols), BF, ANY))
    outs.append(((2, *block.shape), BF, ANY))
    return Job(
        run,
        [(w, ANY) for w, _ in weights] + [(block, ANY)],
        outs,
        [VMEM(w.shape, w.dtype) for w, _ in weights] + [VMEM(block.shape, BF)],
        5 * n + 1,
        2 * n + 2,
        "xyk",
    )


def tp_reduce_scatter(part, n_tp):
    rows, width = part.shape
    piece = rows // n_tp

    def run(net, me, ins, outs, scratch):
        (src,), (out,), (got,) = ins, outs, scratch
        waits = []
        for k in range(1, n_tp):
            to = pl.multiple_of(lax.rem(me.t + k, n_tp) * piece, piece)
            waits.append(net.put(src.at[pl.ds(to, piece)], got.at[k - 1], me.along(k)))
        yield 1
        for wait in waits:
            wait.wait_recv()
        total = src[pl.ds(pl.multiple_of(me.t * piece, piece), piece), :].astype(F32)
        for k in range(1, n_tp):
            total = total + got[k - 1].astype(F32)
        out[...] = total

    return Job(
        run,
        [(part, VMEM)],
        [((piece, width), F32, VMEM)],
        [VMEM((n_tp - 1, piece, width), BF)],
        n_tp - 1,
        0,
        "z",
    )


def tp_all_gather(own, n_tp):
    size, width = own.shape
    half = size // 2

    def run(net, me, ins, outs, scratch):
        (src,), (out,) = ins, outs

        def rows(p, which=None):
            if which is None:
                return out.at[pl.ds(pl.multiple_of(p * size, size), size)]
            return out.at[pl.ds(pl.multiple_of(p * size + which * half, half), half)]

        right, left = me.along(1), me.along(-1)
        p_left, p_right = lax.rem(me.t + 3, 4), lax.rem(me.t + 1, 4)
        to_right = net.put(src, rows(me.t), right)
        to_left = net.put(src, rows(me.t), left)
        out[pl.ds(pl.multiple_of(me.t * size, size), size), :] = src[...]
        yield 1
        to_right.wait_recv()
        hop_right = net.put(rows(p_left, 0), rows(p_left, 0), right)
        to_left.wait_recv()
        hop_left = net.put(rows(p_right, 1), rows(p_right, 1), left)
        yield 1
        yield 1
        hop_right.wait_recv()
        hop_left.wait_recv()

    return Job(
        run, [(own, VMEM)], [((n_tp * size, width), own.dtype, VMEM)], [], 4, 0, "z"
    )


def relay_chunks(net, me, out, chunks):
    g_x, g_y = slot(me.s, 1 - me.c), slot(lax.rem(me.s + 2, 4), me.c)
    g_d = slot(lax.rem(me.s + 2, 4), 1 - me.c)
    first = 1 - me.core
    relay_slot = first * g_x + me.core * g_y
    relay_to = me.flip(first, 0, me.core)
    diags, waits = [], []
    for from_x, from_y, start, size in chunks:
        from_x.wait_recv()
        from_y.wait_recv()
        src = out.at[relay_slot, pl.ds(start, size)]
        diags.append(net.put(src, src, relay_to))
        for g in (g_x, g_y):
            piece = out.at[g, pl.ds(start, size)]
            waits.append(net.put(piece, piece, me.over_core))
        yield 1
    for diag, (_, _, start, size) in zip(diags, chunks):
        diag.wait_recv()
        piece = out.at[g_d, pl.ds(start, size)]
        waits.append(net.put(piece, piece, me.over_core))
        yield 1
    for wait in waits:
        wait.wait_recv()


def plane_gather(own, n_chunk=4):
    rows, width = own.shape
    size = rows // n_chunk

    def run(net, me, ins, outs, scratch):
        (src,), (out,), (bounce,) = ins, outs, scratch
        g_me = slot(me.s, me.c)
        load = net.move(src, bounce)
        chunks, cores = [], []
        for j in range(n_chunk):
            part = src.at[pl.ds(j * size, size)]
            to = out.at[g_me, pl.ds(j * size, size)]
            chunks.append(
                (net.put(part, to, me.over_x), net.put(part, to, me.over_y), j * size, size)
            )
            cores.append(net.put(part, to, me.over_core))
        yield 1
        load.wait()
        store = net.move(bounce, out.at[g_me])
        yield from relay_chunks(net, me, out, chunks)
        for core in cores:
            core.wait_recv()
        store.wait()

    return Job(
        run,
        [(own, ANY)],
        [((8, rows, width), own.dtype, ANY)],
        [VMEM(own.shape, own.dtype)],
        7 * n_chunk,
        2,
        "xyk",
    )


def plane_columns(array):
    rows, width = array.shape
    w = width // 4

    def run(net, me, ins, outs, scratch):
        (src,), (out,), (bounce,) = ins, outs, scratch
        g_me = slot(me.s, me.c)

        def cols(s):
            return src.at[:, pl.ds(pl.multiple_of(s * w, LANES), w)]

        load = net.move(cols(me.s), bounce)
        waits = []
        for f in FLIPS:
            peer = me.flip(*f)
            waits.append(net.put(cols(peer[SHARD]), out.at[g_me], peer))
        yield 1
        load.wait()
        store = net.move(bounce, out.at[g_me])
        for wait in waits:
            yield 1
            wait.wait_recv()
        store.wait()

    return Job(
        run,
        [(array, ANY)],
        [((8, rows, w), array.dtype, ANY)],
        [VMEM((rows, w), array.dtype)],
        7,
        2,
        "p",
    )


def shard_rows(array):
    h, w = array.shape[0] // 8, array.shape[1]

    def run(net, me, ins, outs, scratch):
        (src,), (out,), (bounce,) = ins, outs, scratch

        def rows(s):
            return src.at[pl.ds(pl.multiple_of(slot(s, me.c) * h, 8), h)]

        to = out.at[:, pl.ds(pl.multiple_of(me.s * w, LANES), w)]
        load = net.move(rows(me.s), bounce)
        waits = []
        for f in FLIPS:
            if f[2] == 0:
                peer = me.flip(*f)
                waits.append(net.put(rows(peer[SHARD]), to, peer))
        yield 1
        load.wait()
        store = net.move(bounce, to)
        yield 1
        for wait in waits:
            wait.wait_recv()
        store.wait()

    return Job(
        run,
        [(array, ANY)],
        [((h, 4 * w), array.dtype, ANY)],
        [VMEM((h, w), array.dtype)],
        3,
        2,
        "p",
    )


def ctx_swap(block):
    def run(net, me, ins, outs, scratch):
        (src,), (out,) = ins, outs
        got = net.put(src, out, me.over_x)
        yield 1
        yield 1
        got.wait_recv()

    return Job(run, [(block, ANY)], [(block.shape, block.dtype, ANY)], [], 1, 0, "x")


def reduce_everywhere(part, n_tp):
    tokens, width = part.shape
    rows = tokens // 8
    half = width // 2
    piece = rows // n_tp
    step = 16

    def run(net, me, ins, outs, scratch):
        (src,), (out,) = ins, outs
        mine, rc, rx, ry, q0, q1, r0, r1, last, got = scratch
        a, b = pl.ds(0, half), pl.ds(half, half)
        order = [(1, 1), (0, 1), (1, 0), (0, 0)]
        chips, loads, cores = [], [], []
        for dy, dx in order:
            ch = 2 * (me.y + dy * (1 - 2 * me.y)) + me.c + dx * (1 - 2 * me.c)
            chips.append(ch)
            base = ch * 2 * rows
            theirs = src.at[pl.ds(pl.multiple_of(base + (1 - me.core) * rows, rows), rows)]
            ours = src.at[pl.ds(pl.multiple_of(base + me.core * rows, rows), rows)]
            cores.append(net.put(theirs, rc.at[ch], me.over_core))
            loads.append(net.move(ours, mine.at[ch]))
        yield 1

        def add(target, cols, left, right):
            def one(r, carry):
                at = pl.ds(pl.multiple_of(r * step, step), step)
                target[at, cols] = (left(at).astype(F32) + right(at).astype(F32)).astype(BF)
                return carry

            lax.fori_loop(0, rows // step, one, 0)

        def sum_cores(k):
            ch = chips[k]
            loads[k].wait()
            cores[k].wait_recv()
            add(mine.at[ch], pl.ds(0, width), lambda at: mine[ch, at, :], lambda at: rc[ch, at, :])
            return ch

        c_d = sum_cores(0)
        ax0 = net.put(mine.at[c_d, :, a], rx.at[0], me.over_x)
        by0 = net.put(mine.at[c_d, :, b], ry.at[0], me.over_y)
        c_x = sum_cores(1)
        ax1 = net.put(mine.at[c_x, :, a], rx.at[1], me.over_x)
        c_y = sum_cores(2)
        by1 = net.put(mine.at[c_y, :, b], ry.at[1], me.over_y)
        c_me = sum_cores(3)
        yield 1
        every = pl.ds(0, half)
        ax0.wait_recv()
        add(q0, every, lambda at: mine[c_y, at, a], lambda at: rx[0, at, :])
        y0 = net.put(q0, r0, me.over_y)
        by0.wait_recv()
        add(q1, every, lambda at: mine[c_x, at, b], lambda at: ry[0, at, :])
        x1 = net.put(q1, r1, me.over_x)
        yield 1
        ax1.wait_recv()
        by1.wait_recv()
        y0.wait_recv()
        x1.wait_recv()

        def final(r, carry):
            at = pl.ds(pl.multiple_of(r * step, step), step)
            left = mine[c_me, at, a].astype(F32) + rx[1, at, :].astype(F32) + r0[at, :].astype(F32)
            right = mine[c_me, at, b].astype(F32) + ry[1, at, :].astype(F32) + r1[at, :].astype(F32)
            last[at, a] = left.astype(BF)
            last[at, b] = right.astype(BF)
            return carry

        lax.fori_loop(0, rows // step, final, 0)
        waits = []
        for k in range(1, n_tp):
            to = pl.multiple_of(lax.rem(me.t + k, n_tp) * piece, piece)
            waits.append(net.put(last.at[pl.ds(to, piece)], got.at[k - 1], me.along(k)))
        yield 1
        for wait in waits:
            wait.wait_recv()
        for r in range(piece // step):
            at = pl.ds(pl.multiple_of(me.t * piece + r * step, step), step)
            total = last[at, :].astype(F32)
            for k in range(n_tp - 1):
                total = total + got[k, r * step : (r + 1) * step, :].astype(F32)
            out[r * step : (r + 1) * step, :] = total

    block = (rows, width)
    return Job(
        run,
        [(part, ANY)],
        [((piece, width), F32, VMEM)],
        [
            VMEM((4, *block), BF),
            VMEM((4, *block), BF),
            VMEM((2, rows, half), BF),
            VMEM((2, rows, half), BF),
            VMEM((rows, half), BF),
            VMEM((rows, half), BF),
            VMEM((rows, half), BF),
            VMEM((rows, half), BF),
            VMEM(block, BF),
            VMEM((n_tp - 1, piece, width), BF),
        ],
        10 + n_tp - 1,
        4,
        "xykz",
    )


def sum_everywhere(part, n_tp):
    def run(net, me, ins, outs, scratch):
        (src,), (out,) = ins, outs
        from_tp, mid, from_plane = scratch
        waits = [net.put(src, from_tp.at[k - 1], me.along(k)) for k in range(1, n_tp)]
        yield 1
        for wait in waits:
            wait.wait_recv()
        total = src[...]
        for k in range(n_tp - 1):
            total = total + from_tp[k]
        mid[...] = total
        waits = [net.put(mid, from_plane.at[i], me.flip(*f)) for i, f in enumerate(FLIPS)]
        yield 1
        yield 1
        for wait in waits:
            wait.wait_recv()
        total = mid[...]
        for i in range(7):
            total = total + from_plane[i]
        out[...] = total

    return Job(
        run,
        [(part, VMEM)],
        [(part.shape, F32, VMEM)],
        [VMEM((n_tp - 1, *part.shape), F32), VMEM(part.shape, F32), VMEM((7, *part.shape), F32)],
        n_tp - 1 + 7,
        0,
        "zp",
    )


def gather_rows(own, n_tp):
    piece, width = own.shape
    half = piece // 2

    def run(net, me, ins, outs, scratch):
        (src,), (out,), (bounce,) = ins, outs, scratch
        load = net.move(src, bounce)
        g_me = slot(me.s, me.c)
        chunks, cores = [], []

        def rows(p, which=None):
            if which is None:
                return out.at[g_me, pl.ds(pl.multiple_of(p * piece, piece), piece)]
            return out.at[g_me, pl.ds(pl.multiple_of(p * piece + which * half, half), half)]

        def spread(ref, p):
            dst = rows(p)
            chunks.append(
                (net.put(ref, dst, me.over_x), net.put(ref, dst, me.over_y), pl.multiple_of(p * piece, piece), piece)
            )
            cores.append(net.put(ref, dst, me.over_core))

        right, left = me.along(1), me.along(-1)
        p_left, p_right = lax.rem(me.t + 3, 4), lax.rem(me.t + 1, 4)
        far = lax.rem(me.t + 2, 4)
        to_right = net.put(src, rows(me.t), right)
        to_left = net.put(src, rows(me.t), left)
        spread(src, me.t)
        load.wait()
        store = net.move(bounce, rows(me.t))
        yield 1
        to_right.wait_recv()
        hop_right = net.put(rows(p_left, 0), rows(p_left, 0), right)
        spread(rows(p_left), p_left)
        to_left.wait_recv()
        hop_left = net.put(rows(p_right, 1), rows(p_right, 1), left)
        spread(rows(p_right), p_right)
        yield 1
        hop_right.wait_recv()
        hop_left.wait_recv()
        spread(rows(far), far)
        yield from relay_chunks(net, me, out, chunks)
        for core in cores:
            core.wait_recv()
        store.wait()

    return Job(
        run,
        [(own, ANY)],
        [((8, n_tp * piece, width), own.dtype, ANY)],
        [VMEM(own.shape, own.dtype)],
        4 * 7 + 4,
        2,
        "xykz",
    )


class Wire:
    def __init__(self, net, build):
        self.net, self.build, self.i = net, build, len(net.all)
        net.all.append(self)

    def copy(self):
        src, dst, to = self.build()
        return pltpu.make_async_remote_copy(
            src_ref=src,
            dst_ref=dst,
            send_sem=self.net.send.at[self.i],
            recv_sem=self.net.recv.at[self.i],
            device_id=to,
            device_id_type=MESH,
        )

    def start(self):
        self.copy().start()

    def landed(self):
        self.copy().wait_recv()

    def sent(self):
        self.copy().wait_send()


class Wires:
    def __init__(self, send, recv):
        self.send, self.recv, self.all = send, recv, []

    def wire(self, build):
        return Wire(self, build)


class PlaneSum:
    def __init__(self, net, me, data, buffers, edge, chip, block, rows):
        self.data, self.rows, self.block, self.me, self.chip = data, rows, block, me, chip
        self.rc, self.rxa, self.ryb, self.q0, self.q1, self.r0, self.r1 = buffers
        self.width = data.shape[1]
        self.edge = edge
        self.a, self.b = pl.ds(0, edge), pl.ds(edge, self.width - edge)
        part = lambda ch, cols: data.at[block(ch, me.core), cols]
        self.cores = [
            net.wire(
                lambda k=k: (data.at[block(chip[k], 1 - me.core)], self.rc.at[k], me.over_core)
            )
            for k in range(4)
        ]
        self.ax0 = net.wire(lambda: (part(chip[3], self.a), self.rxa.at[0], me.over_x))
        self.by0 = net.wire(lambda: (part(chip[3], self.b), self.ryb.at[0], me.over_y))
        self.ax1 = net.wire(lambda: (part(chip[1], self.a), self.rxa.at[1], me.over_x))
        self.by1 = net.wire(lambda: (part(chip[2], self.b), self.ryb.at[1], me.over_y))
        self.y0 = net.wire(lambda: (self.q0, self.r0, me.over_y))
        self.x1 = net.wire(lambda: (self.q1, self.r1, me.over_x))

    def base(self, k):
        return (self.chip[k] * 2 + self.me.core) * self.rows

    def add(self, target, t_at, cols, left, right):
        def one(r, carry):
            total = left(r).astype(F32) + right(r).astype(F32)
            target[row_at(t_at, r), cols] = total.astype(BF)
            return carry

        lax.fori_loop(0, self.rows // STEP, one, 0)

    def sum_cores(self, k):
        base, every = self.base(k), pl.ds(0, self.width)
        self.cores[k].landed()
        self.add(
            self.data,
            base,
            every,
            lambda r: self.data[row_at(base, r), every],
            lambda r: self.rc[k, row_at(0, r), :],
        )

    def stage_two(self):
        over_y, over_x = self.base(2), self.base(1)
        self.ax0.landed()
        self.add(
            self.q0,
            0,
            pl.ds(0, self.edge),
            lambda r: self.data[row_at(over_y, r), self.a],
            lambda r: self.rxa[0, row_at(0, r), :],
        )
        self.y0.start()
        self.by0.landed()
        self.add(
            self.q1,
            0,
            pl.ds(0, self.width - self.edge),
            lambda r: self.data[row_at(over_x, r), self.b],
            lambda r: self.ryb[0, row_at(0, r), :],
        )
        self.x1.start()

    def finish(self, last):
        base = self.base(0)
        for wire in (self.ax1, self.by1, self.y0, self.x1):
            wire.landed()

        def final(r, carry):
            at, big = row_at(0, r), row_at(base, r)
            one = self.data[big, self.a].astype(F32) + self.rxa[1, at, :].astype(F32)
            last[at, self.a] = (one + self.r0[at, :].astype(F32)).astype(BF)
            two = self.data[big, self.b].astype(F32) + self.ryb[1, at, :].astype(F32)
            last[at, self.b] = (two + self.r1[at, :].astype(F32)).astype(BF)
            return carry

        lax.fori_loop(0, self.rows // STEP, final, 0)


def plane_sum_scratch(rows, width, edge):
    return [
        VMEM((4, rows, width), BF),
        VMEM((2, rows, edge), BF),
        VMEM((2, rows, width - edge), BF),
        VMEM((rows, edge), BF),
        VMEM((rows, width - edge), BF),
        VMEM((rows, edge), BF),
        VMEM((rows, width - edge), BF),
    ]


STEP = 16


def row_at(base, r):
    return pl.ds(pl.multiple_of(base + r * STEP, STEP), STEP)


def padded(count, to=LANES):
    return -(-count // to) * to


def feed_forward(
    two_own, mid_own, cot_own, gain_two, cot_all, gate, up, down, sg_t, su_t, sd, router_t, attn, normed, latent, topk, n_tp
):
    piece, width = two_own.shape
    rows = piece * n_tp
    tokens = 8 * rows
    pack = cot_all.shape[-1]
    hid, hid_s = gate.shape[1], sg_t.shape[0]
    experts = router_t.shape[0]
    used = 2 * hid + hid_s
    H = padded(used)
    tile = H - LANES
    off = used - tile
    edge = width // 2
    part_w = width + LANES
    group = 2 * rows
    shard_w = width // 4
    lat_w = latent.shape[1] // 4
    attn_w = attn.shape[1]
    n_wires = 4 + 12 + 16 + 10 + 10 + (n_tp - 1) + 7 + 14 + 4
    n_col = 4
    col_w = width // n_col
    m_w = 256
    n_m = width // m_w

    def body(*refs):
        (two_ref, mid_ref, cot_own_ref, gain_ref) = refs[:4]
        (cot_ref, gate_ref, up_ref, down_ref, sg_ref, su_ref, sd_ref, wr_ref, attn_ref, one_ref, lat_ref) = refs[4:15]
        (mid_out, gain_out, mid_pack, y_out, dg_out, du_out, dd_out, ds_out, n2_out) = refs[15:24]
        (attn_out, one_out, lat_out) = refs[24:27]
        (nb, cb, wgu, wd, gu, gut, hw, hwt, dnb, yb) = refs[27:37]
        two_buf, y_buf, (last, got, gus, dds, dss) = refs[37:44], refs[44:51], refs[51:56]
        send, recv, load, store = refs[56:]
        me = Place(n_tp)
        net = Wires(send, recv)

        def chip(dy, dx):
            return 2 * (me.y + dy * (1 - 2 * me.y)) + me.c + dx * (1 - 2 * me.c)

        def block(ch, core, p=None):
            start = ch * group + core * rows
            if p is None:
                return pl.ds(pl.multiple_of(start, rows), rows)
            return pl.ds(pl.multiple_of(start + p * piece, piece), piece)

        here = chip(0, 0)
        g_me = slot(me.s, me.c)
        pieces = [me.t, lax.rem(me.t + 3, 4), lax.rem(me.t + 1, 4), lax.rem(me.t + 2, 4)]
        half = piece // 2
        right, left = me.along(1), me.along(-1)

        def halves(p, which):
            start = here * group + me.core * rows + p * piece + which * half
            return nb.at[pl.ds(pl.multiple_of(start, half), half)]

        def mine(p):
            return nb.at[block(here, me.core, p)]

        z_r = net.wire(lambda: (two_ref, mine(me.t), right))
        z_l = net.wire(lambda: (two_ref, mine(me.t), left))
        hop_r = net.wire(lambda: (halves(pieces[1], 0), halves(pieces[1], 0), right))
        hop_l = net.wire(lambda: (halves(pieces[2], 1), halves(pieces[2], 1), left))
        to_x, to_y, to_c = [], [], []
        for j in range(4):
            src = (lambda: two_ref) if j == 0 else (lambda j=j: mine(pieces[j]))
            to_x.append(net.wire(lambda j=j, src=src: (src(), mine(pieces[j]), me.over_x)))
            to_y.append(net.wire(lambda j=j, src=src: (src(), mine(pieces[j]), me.over_y)))
            to_c.append(net.wire(lambda j=j, src=src: (src(), mine(pieces[j]), me.over_core)))
        chip_x, chip_y, chip_d = chip(0, 1), chip(1, 0), chip(1, 1)
        first = 1 - me.core
        relay_chip = first * chip_x + me.core * chip_y
        relay_to = me.flip(first, 0, me.core)
        relay, fwd_x, fwd_y, fwd_d = [], [], [], []
        for j in range(4):
            same = lambda ch, j=j: nb.at[block(ch, me.core, pieces[j])]
            relay.append(net.wire(lambda same=same: (same(relay_chip), same(relay_chip), relay_to)))
            fwd_x.append(net.wire(lambda same=same: (same(chip_x), same(chip_x), me.over_core)))
            fwd_y.append(net.wire(lambda same=same: (same(chip_y), same(chip_y), me.over_core)))
            fwd_d.append(net.wire(lambda same=same: (same(chip_d), same(chip_d), me.over_core)))

        g_x, g_y = slot(me.s, 1 - me.c), slot(lax.rem(me.s + 2, 4), me.c)
        g_d = slot(lax.rem(me.s + 2, 4), 1 - me.c)
        g_relay = first * g_x + me.core * g_y
        at_direct = [
            net.wire(lambda to=to: (attn_ref, attn_out.at[g_me], to))
            for to in (me.over_x, me.over_y, me.over_core)
        ]
        at_relay = net.wire(lambda: (attn_out.at[g_relay], attn_out.at[g_relay], relay_to))
        at_fwd = [
            net.wire(lambda g=g: (attn_out.at[g], attn_out.at[g], me.over_core)) for g in (g_x, g_y, g_d)
        ]
        cols_w = []
        for f in FLIPS:
            peer = me.flip(*f)
            for src, dst, w in ((one_ref, one_out, shard_w), (lat_ref, lat_out, lat_w)):
                cols_w.append(
                    net.wire(
                        lambda src=src, dst=dst, w=w, peer=peer: (
                            src.at[:, pl.ds(pl.multiple_of(peer[SHARD] * w, LANES), w)],
                            dst.at[g_me],
                            peer,
                        )
                    )
                )

        chips = [here, chip_x, chip_y, chip_d]
        two_sum = PlaneSum(net, me, dnb, two_buf, edge, chips, block, rows)
        y_sum = PlaneSum(net, me, yb, y_buf, edge, chips, block, rows)
        z_w = []
        for k in range(1, n_tp):
            to = lax.rem(me.t + k, n_tp)
            z_w.append(
                net.wire(
                    lambda k=k, to=to: (
                        last.at[pl.ds(pl.multiple_of(to * piece, piece), piece)],
                        got.at[k - 1],
                        me.along(k),
                    )
                )
            )

        def packed(p, which=None):
            if which is None:
                return mid_pack.at[pl.ds(pl.multiple_of(p * piece, piece), piece)]
            return mid_pack.at[pl.ds(pl.multiple_of(p * piece + which * half, half), half)]

        m_r = net.wire(lambda: (packed(me.t), packed(me.t), right))
        m_l = net.wire(lambda: (packed(me.t), packed(me.t), left))
        m_hr = net.wire(lambda: (packed(pieces[1], 0), packed(pieces[1], 0), right))
        m_hl = net.wire(lambda: (packed(pieces[2], 1), packed(pieces[2], 1), left))

        moves = [
            (down_ref.at[0], wd.at[pl.ds(0, hid)]),
            (down_ref.at[1], wd.at[pl.ds(hid, hid)]),
            (sd_ref, wd.at[pl.ds(2 * hid, hid_s)]),
            (gate_ref.at[0], wgu.at[pl.ds(0, hid)]),
            (gate_ref.at[1], wgu.at[pl.ds(hid, hid)]),
            (sg_ref, wgu.at[pl.ds(2 * hid, hid_s)]),
            (wr_ref, wgu.at[pl.ds(used, experts)]),
            (up_ref.at[0], wgu.at[pl.ds(H, hid)]),
            (up_ref.at[1], wgu.at[pl.ds(H + hid, hid)]),
            (su_ref, wgu.at[pl.ds(H + 2 * hid, hid_s)]),
        ]
        for g in range(8):
            row = (2 * (g // 4) + g % 2) * group + (g % 4) // 2 * rows
            moves.append((cot_ref.at[g], cb.at[pl.ds(row, rows)]))
        loads = [pltpu.make_async_copy(src, dst, load.at[i]) for i, (src, dst) in enumerate(moves)]
        for copy in loads:
            copy.start()
        greet(me.peers("xykzp"))
        for wire in (z_r, z_l, to_x[0], to_y[0], to_c[0]):
            wire.start()
        nb[block(here, me.core, me.t), :] = two_ref[...]
        wgu[used + experts : H, :] = jnp.zeros((H - used - experts, width), BF)
        wgu[H + used :, :] = jnp.zeros((H - used, width), BF)
        wd[used:, :] = jnp.zeros((H - used, width), BF)
        z_r.landed()
        hop_r.start()
        for wires in (to_x, to_y, to_c):
            wires[1].start()
        z_l.landed()
        hop_l.start()
        for wires in (to_x, to_y, to_c):
            wires[2].start()
        for copy in loads:
            copy.wait()
        hop_r.landed()
        hop_l.landed()
        for wires in (to_x, to_y, to_c):
            wires[3].start()
        for wire in to_c:
            wire.landed()

        lane = lax.broadcasted_iota(jnp.int32, (group, LANES), 1)
        unit = lax.broadcasted_iota(jnp.int32, (group, H), 1)
        e_first = g_me * 2

        def softmax_tile(logits, lanes):
            logits = jnp.where((lanes >= off) & (lanes < off + experts), logits, NEG)
            e = jnp.exp(logits - jnp.max(logits, axis=1, keepdims=True))
            return e / jnp.sum(e, axis=1, keepdims=True)

        def flip_chip(k):
            return chip(k // 2, lax.rem(k, 2))

        def hidden(k, carry):
            at = pl.ds(pl.multiple_of(flip_chip(k) * group, group), group)

            @pl.when(k == 1)
            def _():
                for j in range(4):
                    to_x[j].landed()
                    to_y[j].landed()
                    relay[j].start()
                    fwd_x[j].start()
                    fwd_y[j].start()
                for j in range(4):
                    fwd_x[j].landed()

            @pl.when(k == 2)
            def _():
                for j in range(4):
                    fwd_y[j].landed()

            @pl.when(k == 3)
            def _():
                for j in range(4):
                    relay[j].landed()
                    fwd_d[j].start()
                for wire in at_direct + cols_w:
                    wire.start()
                for j in range(4):
                    fwd_d[j].landed()

            acts = dot_nt(nb[at, :], wgu[...])
            back = dot_nt(cb[at, 0:width], wd[...])
            probs = softmax_tile(acts[:, tile:H], lane)
            routed = cb[at, width : width + LANES].astype(F32)
            chosen, weight = [], []
            for j in range(2):
                expert = e_first + j
                hit = jnp.where((lane < topk) & (routed == expert.astype(F32)), 1.0, 0.0)
                chosen.append(jnp.max(hit, axis=1, keepdims=True))
                weight.append(
                    chosen[j]
                    * jnp.sum(jnp.where(lane == off + expert, probs, 0.0), axis=1, keepdims=True)
                )
            scale = jnp.where(unit < hid, weight[0], jnp.where(unit < 2 * hid, weight[1], 1.0))
            g, u = acts[:, :H], acts[:, H:]
            sig = 1.0 / (1.0 + jnp.exp(-g))
            silu = g * sig
            h = silu * u
            terms = h * back
            pg = jnp.zeros((group, LANES), F32)
            for j in range(2):
                own = (unit >= j * hid) & (unit < (j + 1) * hid)
                grad = chosen[j] * jnp.sum(jnp.where(own, terms, 0.0), axis=1, keepdims=True)
                high = grad.astype(BF).astype(F32)
                pg = jnp.where(lane == off + e_first + j, high, pg)
                pg = jnp.where(lane == off + e_first + j + LANES // 2, grad - high, pg)
            dnb[at, width:part_w] = pg.astype(BF)
            h = (h * scale).astype(BF)
            back = back * scale
            gate_grad = (back * u * (sig * (1.0 + g * (1.0 - sig)))).astype(BF)
            up_grad = (back * silu).astype(BF)
            hw[at, :] = h
            gu[at, 0:H] = gate_grad
            gu[at, H:] = up_grad
            hwt[:, at] = h.T
            gut[0:H, at] = gate_grad.T
            gut[H:, at] = up_grad.T
            return carry

        lax.fori_loop(0, 4, hidden, 0)

        cols_s = pl.ds(pl.multiple_of(me.s * shard_w, shard_w), shard_w)
        locals_ = []
        for g in range(8):
            row = (2 * (g // 4) + g % 2) * group + (g % 4) // 2 * rows
            locals_.append((nb.at[pl.ds(row, rows), cols_s], n2_out.at[g]))
        locals_.append((attn_ref, attn_out.at[g_me]))
        locals_.append((one_ref.at[:, cols_s], one_out.at[g_me]))
        locals_.append((lat_ref.at[:, pl.ds(pl.multiple_of(me.s * lat_w, LANES), lat_w)], lat_out.at[g_me]))
        local_copies = [pltpu.make_async_copy(src, dst, store.at[i]) for i, (src, dst) in enumerate(locals_)]
        for copy in local_copies:
            copy.start()

        def normed_grad(i, carry):
            k = 3 - i
            at = pl.ds(pl.multiple_of(flip_chip(k) * group, group), group)

            def columns(n, carry):
                cols = pl.ds(pl.multiple_of(n * col_w, col_w), col_w)
                dnb[at, cols] = mdot(gu[at, :], wgu[:, cols]).astype(BF)
                return carry

            lax.fori_loop(0, n_col, columns, 0)
            for kk in range(4):

                @pl.when(k == kk)
                def _():
                    two_sum.cores[kk].start()
                    if kk < 3:
                        two_sum.sum_cores(kk + 1)
                    if kk == 2:
                        two_sum.ax0.start()
                        two_sum.by0.start()
                    if kk == 1:
                        two_sum.by1.start()
                    if kk == 0:
                        two_sum.ax1.start()

            return carry

        lax.fori_loop(0, 4, normed_grad, 0)

        def output(k, carry):
            at = pl.ds(pl.multiple_of(k * group, group), group)

            @pl.when(k == 1)
            def _():
                two_sum.sum_cores(0)
                two_sum.stage_two()

            def columns(n, carry):
                cols = pl.ds(pl.multiple_of(n * col_w, col_w), col_w)
                yb[at, cols] = mdot(hw[at, :], wd[:, cols]).astype(BF)
                return carry

            lax.fori_loop(0, n_col, columns, 0)
            return carry

        lax.fori_loop(0, 4, output, 0)
        two_sum.finish(last)
        for wire in z_w:
            wire.start()
        for wire in y_sum.cores:
            wire.start()

        def router_and_norm():
            for wire in z_w:
                wire.landed()
            total = last[pl.ds(pl.multiple_of(me.t * piece, piece), piece), :].astype(F32)
            for k in range(n_tp - 1):
                total = total + got[k].astype(F32)
            small = lax.broadcasted_iota(jnp.int32, (piece, LANES), 1)
            probs = softmax_tile(dot_nt(two_ref[...], wgu[tile:H, :]), small)
            pg = total[:, width:]
            pg = pg + pltpu.roll(pg, LANES // 2, 1)
            pg = jnp.where((small >= off) & (small < off + experts), pg, 0.0)
            logit_grad = (probs * (pg - jnp.sum(probs * pg, axis=1, keepdims=True))).astype(BF)
            grad = total[:, :width] + mdot(logit_grad, wgu[tile:H, :])
            value = mid_ref[...]
            back, terms = norm_back(value, gain_ref[...], grad)
            mid_grad = cot_own_ref[...] + back
            mid_out[...] = mid_grad
            gain_out[...] = jnp.sum(terms, axis=0, keepdims=True)
            at = pl.ds(pl.multiple_of(me.t * piece, piece), piece)
            mid_pack[at, 0:width] = mid_grad.astype(BF)
            mid_pack[at, width:] = logit_grad
            m_r.start()
            m_l.start()

        def stores(m, buf):
            cols = pl.ds(pl.multiple_of(m * m_w, m_w), m_w)
            made = []
            for j in range(2):
                at = pl.ds(j * hid, hid)
                made.append((gus.at[buf, at], dg_out.at[j, :, cols]))
                made.append((gus.at[buf, pl.ds(H + j * hid, hid)], du_out.at[j, :, cols]))
                made.append((dds.at[buf, at], dd_out.at[j, :, cols]))
            return [
                pltpu.make_async_copy(src, dst, store.at[14 + 6 * buf + i])
                for i, (src, dst) in enumerate(made)
            ]

        def weight_grad(m, carry):
            buf = lax.rem(m, 2)
            cols = pl.ds(pl.multiple_of(m * m_w, m_w), m_w)

            @pl.when(m >= 2)
            def _():
                for bb in range(2):

                    @pl.when(buf == bb)
                    def _():
                        for copy in stores(m - 2, bb):
                            copy.wait()

            @pl.when(m == 1)
            def _():
                for k in range(4):
                    y_sum.sum_cores(k)
                for wire in (y_sum.ax0, y_sum.by0, y_sum.ax1, y_sum.by1):
                    wire.start()
                at_direct[0].landed()
                at_direct[1].landed()
                for wire in (at_relay, at_fwd[0], at_fwd[1]):
                    wire.start()

            @pl.when(m == 5)
            def _():
                router_and_norm()

            @pl.when(m == 6)
            def _():
                y_sum.stage_two()
                at_relay.landed()
                at_fwd[2].start()

            both = mdot(gut[...], nb[:, cols])
            gus[buf] = both
            dss[0, :, cols] = both[2 * hid : used].astype(BF)
            dss[1, :, cols] = both[H + 2 * hid : H + used].astype(BF)
            third = mdot(hwt[...], cb[:, cols])
            dds[buf] = third
            dss[2, :, cols] = third[2 * hid : used].astype(BF)
            for bb in range(2):

                @pl.when(buf == bb)
                def _():
                    for copy in stores(m, bb):
                        copy.start()

            return carry

        lax.fori_loop(0, n_m, weight_grad, 0)
        m_r.landed()
        m_hr.start()
        m_l.landed()
        m_hl.start()
        y_sum.finish(y_out)
        ds_copy = pltpu.make_async_copy(dss, ds_out, store.at[13])
        ds_copy.start()
        for m in (n_m - 2, n_m - 1):
            for copy in stores(m, m % 2):
                copy.wait()
        for wire in [at_direct[2], *at_fwd, *cols_w, m_hr, m_hl]:
            wire.landed()
        for copy in local_copies:
            copy.wait()
        ds_copy.wait()
        for wire in net.all:
            wire.sent()

    ins = (
        two_own, mid_own, cot_own, gain_two,
        cot_all, gate, up, down, sg_t, su_t, sd, router_t, attn, normed, latent,
    )
    outs = [
        ((piece, width), F32),
        ((1, width), F32),
        ((rows, part_w), BF),
        ((rows, width), BF),
        (gate.shape, F32),
        (up.shape, F32),
        (down.shape, F32),
        ((3, hid_s, width), BF),
        ((8, rows, shard_w), BF),
        ((8, rows, attn_w), BF),
        ((8, rows, shard_w), BF),
        ((8, rows, lat_w), BF),
    ]
    scratch = [
        VMEM((tokens, width), BF),
        VMEM((tokens, pack), BF),
        VMEM((2 * H, width), BF),
        VMEM((H, width), BF),
        VMEM((tokens, 2 * H), BF),
        VMEM((2 * H, tokens), BF),
        VMEM((tokens, H), BF),
        VMEM((H, tokens), BF),
        VMEM((tokens, part_w), BF),
        VMEM((tokens, width), BF),
        *plane_sum_scratch(rows, part_w, edge),
        *plane_sum_scratch(rows, width, edge),
        VMEM((rows, part_w), BF),
        VMEM((n_tp - 1, piece, part_w), BF),
        VMEM((2, 2 * H, m_w), F32),
        VMEM((2, H, m_w), F32),
        VMEM((3, hid_s, width), BF),
    ]
    return pl.pallas_call(
        body,
        out_shape=tuple(jax.ShapeDtypeStruct(*o) for o in outs),
        in_specs=[pl.BlockSpec(memory_space=VMEM)] * 4 + [pl.BlockSpec(memory_space=ANY)] * 11,
        out_specs=(*[pl.BlockSpec(memory_space=VMEM)] * 4, *[pl.BlockSpec(memory_space=ANY)] * 8),
        scratch_shapes=[
            *scratch,
            pltpu.SemaphoreType.DMA((n_wires,)),
            pltpu.SemaphoreType.DMA((n_wires,)),
            pltpu.SemaphoreType.DMA((18,)),
            pltpu.SemaphoreType.DMA((26,)),
        ],
        compiler_params=pltpu.CompilerParams(
            collective_id=4, has_side_effects=True, vmem_limit_bytes=67 * 10**6
        ),
        name="feed_forward",
    )(*ins)


class Background:
    def __init__(self):
        self.runs = []

    def add(self, run):
        next(run)
        self.runs.append(run)

    def step(self):
        self.runs = [r for r in self.runs if next(r, None) is not None]

    def drain(self):
        while self.runs:
            self.step()


def fold_heads(a, b, lane):
    def fold(v):
        v = v + pltpu.roll(v, 64, 1)
        return v + pltpu.roll(v, 32, 1)

    return jnp.where(lane < DR // 2, fold(a), jnp.where(lane < DR, fold(b), 0.0))


def attention_back(
    mid_pack, attn, prob, kv, keys_rope, q_nope, q_rope, tables, compressed, gains_in, rows_in, y_part, shared_grads,
    w_output, w_expand, w_query, w_latent_t, gain_two_sum, n_tp,
):
    rows, part_w = mid_pack.shape
    width = w_output.shape[1]
    piece = rows // n_tp
    n_head = prob.shape[0]
    nope_w = n_head * DN
    q_w = nope_w + 2 * LANES
    kv_w = kv.shape[1]
    lat_w = 5 * LANES
    back_w = width + KVR + LANES
    scale = (DN + DR) ** (-0.5)
    f32 = lambda *shape: jax.ShapeDtypeStruct(shape, F32)
    bf = lambda *shape: jax.ShapeDtypeStruct(shape, BF)
    subs = dict(
        y=tp_reduce_scatter(bf(rows, width), n_tp),
        mid=plane_columns(bf(rows, width)),
        logit=plane_gather(bf(rows, part_w - width), 1),
        shared=plane_columns(shared_grads),
        head=plane_gather(bf(rows, q_w + kv_w)),
        back=tp_reduce_scatter(bf(rows, back_w), n_tp),
        out=tp_all_gather(bf(piece, width), n_tp),
        inp=tp_all_gather(bf(piece, width), n_tp),
        lat=gather_rows(bf(piece, lat_w), n_tp),
        gain=sum_everywhere(f32(16, 512), n_tp),
    )
    own_scratch = [
        VMEM(w_output.shape, BF),
        VMEM(w_expand.shape, BF),
        VMEM(w_query.shape, BF),
        VMEM((lat_w, width), BF),
        VMEM((rows, nope_w), BF),
        VMEM((2 * rows, kv_w + LANES), F32),
        VMEM((rows, kv_w + LANES), BF),
        VMEM((rows, kv_w + LANES), BF),
        VMEM((rows, q_w + kv_w), BF),
        VMEM((rows, back_w), BF),
        VMEM((piece, width), F32),
        VMEM((piece, back_w), F32),
        VMEM((piece, width), BF),
        VMEM((piece, width), BF),
        VMEM((piece, lat_w), BF),
        VMEM((16, 512), F32),
    ]
    at, sub_at = len(own_scratch), {}
    for key, job in subs.items():
        sub_at[key] = (at, at + len(job.scratch))
        at += len(job.scratch)

    def run(net, me, ins, outs, scratch):
        (mid_ref, attn_ref, prob_ref, kv_ref, ka_ref, kb_ref, qn_ref, qa_ref, qb_ref, cos_ref, sin_ref) = ins[:11]
        (comp_ref, gk_ref, g1_ref, x_ref, mg_ref, m_ref, y_ref, gt_ref) = ins[11:19]
        (ds_ref, wo_ref, we_ref, wq_ref, wl_ref) = ins[19:]
        (block_out, input_out, gain_out, mid_out, logit_out, shared_out, head_out, lat_out) = outs
        (wo, we, wq, wl, ogb, terms, swap_src, swap_got, head, part) = scratch[:10]
        (y32, back32, ob, ib, lat, gains) = scratch[10:16]

        def sub(key, src, dst):
            a, b = sub_at[key]
            return subs[key].run(net, me, (src,), (dst,), scratch[a:b])

        loads = [
            net.move(wo_ref, wo),
            net.move(we_ref, we),
            net.move(wq_ref, wq),
            net.move(wl_ref, wl.at[pl.ds(0, KVR + DR)]),
        ]
        bg = Background()
        y_run = sub("y", y_ref, y32)
        next(y_run)
        bg.add(sub("mid", mid_ref.at[:, pl.ds(0, width)], mid_out))
        bg.add(sub("logit", mid_ref.at[:, pl.ds(width, part_w - width)], logit_out))
        wl[KVR + DR :, :] = jnp.zeros((lat_w - KVR - DR, width), BF)
        lane = lax.broadcasted_iota(jnp.int32, (rows, LANES), 1)
        lane2 = lax.broadcasted_iota(jnp.int32, (2 * rows, LANES), 1)

        loads[0].wait()
        out_grad = dot_nt(mid_ref[:, 0:width], wo[...])
        ogb[...] = out_grad.astype(BF)
        weighted = out_grad * attn_ref[...].astype(F32)
        dqa = jnp.zeros((rows, LANES), F32)
        dqb, dka, dkb = dqa, jnp.zeros((2 * rows, LANES), F32), jnp.zeros((2 * rows, LANES), F32)
        for h in range(n_head):
            mine = (lane >= h * (DR // 2)) & (lane < (h + 1) * (DR // 2))
            k_at, v_at = pl.ds(h * (DN + DV), DN), pl.ds(h * (DN + DV) + DN, DV)
            og_h = ogb[:, h * DV : (h + 1) * DV]
            p = prob_ref[h]
            delta = jnp.sum(weighted[:, h * DV : (h + 1) * DV], axis=1, keepdims=True)
            ds = (p * (dot_nt(og_h, kv_ref[:, v_at]) - delta)).astype(BF)
            head[:, h * DN : (h + 1) * DN] = (mdot(ds, kv_ref[:, k_at]) * scale).astype(BF)
            dqa = dqa + jnp.where(mine, mdot(ds, ka_ref[...]), 0.0)
            dqb = dqb + jnp.where(mine, mdot(ds, kb_ref[...]), 0.0)
            terms[:, k_at] = dot_tn(ds, qn_ref[:, h * DN : (h + 1) * DN]) * scale
            terms[:, v_at] = dot_tn(p.astype(BF), og_h)
            zero = jnp.zeros((), BF)
            dka = dka + dot_tn(ds, jnp.where(mine, qa_ref[...], zero))
            dkb = dkb + dot_tn(ds, jnp.where(mine, qb_ref[...], zero))
        terms[:, kv_w:] = fold_heads(dka * scale, dkb * scale, lane2)
        theirs = pl.ds(pl.multiple_of((1 - me.c) * rows, rows), rows)
        swap_src[...] = terms[theirs, :].astype(BF)
        swap = net.put(swap_src, swap_got, me.over_x)
        dqa, dqb = dqa * scale, dqb * scale
        cos, sin = cos_ref[...], sin_ref[...]
        head[:, nope_w : nope_w + LANES] = (dqa * cos + dqb * sin).astype(BF)
        head[:, nope_w + LANES : q_w] = (dqb * cos - dqa * sin).astype(BF)
        next(y_run, None)
        ob[...] = (m_ref[...] + y32[...]).astype(BF)
        out_run = sub("out", ob, block_out)
        next(out_run)
        yield 1
        for load in loads[1:]:
            load.wait()
        n_col = 4
        col_w = width // n_col

        def columns(n, carry):
            cols = pl.ds(pl.multiple_of(n * col_w, col_w), col_w)
            part[:, cols] = dot_nt(head[:, 0:q_w], wq[cols, :]).astype(BF)
            return carry

        lax.fori_loop(0, n_col, columns, 0)
        swap.wait_recv()
        ours = pl.ds(pl.multiple_of(me.c * rows, rows), rows)
        head[:, q_w:] = (terms[ours, 0:kv_w] + swap_got[:, 0:kv_w].astype(F32)).astype(BF)
        rope = terms[ours, kv_w:] + swap_got[:, kv_w:].astype(F32)
        part[:, width : width + KVR] = dot_nt(head[:, q_w:], we[...]).astype(BF)
        turned = jnp.where(
            lane < DR // 2,
            rope * cos + pltpu.roll(rope, LANES - DR // 2, 1) * sin,
            jnp.where(lane < DR, rope * cos - pltpu.roll(rope, DR // 2, 1) * sin, 0.0),
        )
        part[:, width + KVR :] = turned.astype(BF)
        back_run = sub("back", part, back32)
        next(back_run)
        bg.add(sub("head", head, head_out))
        bg.add(out_run)
        next(back_run, None)
        comp_grad, gk = norm_back(comp_ref[...], gk_ref[...], back32[:, width : width + KVR])
        lat[:, 0:KVR] = comp_grad.astype(BF)
        lat[:, KVR:] = back32[:, width + KVR :].astype(BF)
        one_grad = back32[:, 0:width] + mdot(lat[...], wl[...])
        lat_run = sub("lat", lat, lat_out)
        next(lat_run)
        norm_grad, g1 = norm_back(x_ref[...], g1_ref[...], one_grad)
        ib[...] = (mg_ref[...] + norm_grad).astype(BF)
        bg.add(sub("inp", ib, input_out))
        gains[...] = jnp.zeros_like(gains)
        g1 = jnp.sum(g1, axis=0, keepdims=True)
        for i in range(4):
            gains[i : i + 1, :] = g1[:, i * 512 : (i + 1) * 512]
            gains[4 + i : 5 + i, :] = gt_ref[:, i * 512 : (i + 1) * 512]
        gains[8:9, :] = jnp.sum(gk, axis=0, keepdims=True)
        bg.add(sub("gain", gains, gain_out))
        bg.add(sub("shared", ds_ref, shared_out))
        bg.add(lat_run)
        bg.drain()

    spaces = [VMEM] * 19 + [ANY] * 5
    ins = (
        mid_pack, attn, prob, kv, *keys_rope, q_nope, *q_rope, *tables,
        compressed, *gains_in, *rows_in, y_part, gain_two_sum,
        shared_grads, w_output, w_expand, w_query, w_latent_t,
    )
    outs = [
        ((rows, width), BF, VMEM),
        ((rows, width), BF, VMEM),
        ((16, 512), F32, VMEM),
        *subs["mid"].outs,
        *subs["logit"].outs,
        *subs["shared"].outs,
        *subs["head"].outs,
        *subs["lat"].outs,
    ]
    return Job(
        run,
        list(zip(ins, spaces)),
        outs,
        own_scratch + [s for job in subs.values() for s in job.scratch],
        1 + sum(job.n_put for job in subs.values()),
        4 + sum(job.n_local for job in subs.values()),
        "xykzp",
    )


def attention_forward(
    block, tables, w_query, w_latent_t, w_expand, w_output, router_t, small, cot_pack, shared, n_tp
):
    rows, width = block.shape
    piece = rows // n_tp
    q_w = w_query.shape[1]
    nope_w = q_w - 2 * LANES
    n_head = nope_w // DN
    kv_w = w_expand.shape[1]
    lat_rows = w_latent_t.shape[0]
    lat_pad = padded(lat_rows)
    scale = (DN + DR) ** (-0.5)
    k_w, e_w = w_query.shape[0], w_expand.shape[0]
    shard_w = w_output.shape[1]
    f32 = lambda *shape: jax.ShapeDtypeStruct(shape, F32)
    bf = lambda *shape: jax.ShapeDtypeStruct(shape, BF)
    subs = dict(
        cot=plane_gather(cot_pack),
        sg=shard_rows(shared[0]),
        su=shard_rows(shared[1]),
        sd=shard_rows(shared[2]),
        rs=tp_reduce_scatter(bf(rows, width), n_tp),
    )
    own_scratch = [
        VMEM((4 * k_w, q_w), BF),
        VMEM((lat_pad, width), BF),
        VMEM((4 * e_w, kv_w), BF),
        VMEM((w_output.shape[0], width), BF),
        VMEM((router_t.shape[0], width), BF),
        VMEM((4, *small.shape), F32),
        VMEM((rows, width), BF),
        VMEM((2 * rows, width), BF),
        VMEM((2 * rows, KVR), F32),
        VMEM((2 * rows, KVR), BF),
        VMEM((rows, width), BF),
        VMEM((piece, width), F32),
    ]
    at, sub_at = len(own_scratch), {}
    for key, job in subs.items():
        sub_at[key] = (at, at + len(job.scratch))
        at += len(job.scratch)

    def run(net, me, ins, outs, scratch):
        x_ref, cos_ref, sin_ref = ins[:3]
        wq_in, wl_in, we_in, wo_in, rt_in, small_in, cot_in = ins[3:10]
        shared_in = ins[10:13]
        (mid_out, two_out, attn_out, prob_out, kv_out, ka_out, kb_out, qn_out, qa_out, qb_out) = outs[:10]
        (comp_out, one_out, latn_out, gain_out) = outs[10:14]
        weights_out, cot_out, shared_out = outs[14:19], outs[19], outs[20:23]
        (wq, wl, we, wo, rt, small_all, xo, n1, lat32, ln, part, res) = scratch[:12]

        def sub(key, src, dst):
            a, b = sub_at[key]
            return subs[key].run(net, me, (src,), (dst,), scratch[a:b])

        other = lax.rem(me.s + 2, 4)

        def stacked(ref, size):
            def place(s, which=None):
                if which is None:
                    return ref.at[pl.ds(pl.multiple_of(s * size, size), size)]
                half = size // 2
                return ref.at[pl.ds(pl.multiple_of(s * size + which * half, half), half)]

            return place

        def beside(ref, count):
            def place(s, which=None):
                cols = pl.ds(pl.multiple_of(s * shard_w, shard_w), shard_w)
                if which is None:
                    return ref.at[pl.ds(0, count), cols]
                half = count // 2
                return ref.at[pl.ds(pl.multiple_of(which * half, half), half), cols]

            return place

        halved = [
            (wq_in, k_w, stacked(wq, k_w)),
            (wl_in, lat_rows, beside(wl, lat_rows)),
            (we_in, e_w, stacked(we, e_w)),
        ]
        whole = [
            (small_in, lambda s: small_all.at[s]),
            (wo_in, beside(wo, w_output.shape[0])),
            (rt_in, beside(rt, router_t.shape[0])),
        ]
        local = [net.move(ref, place(me.s)) for ref, _, place in halved]
        local += [net.move(ref, place(me.s)) for ref, place in whole]
        whole_y = [net.put(small_in, small_all.at[me.s], me.over_y)]
        whole_c = [net.put(small_in, small_all.at[me.s], me.over_core)]
        half_y, half_c = [], []
        for i, (ref, count, place) in enumerate(halved):
            rows_c = pl.ds(pl.multiple_of(me.c * (count // 2), count // 2), count // 2)
            half_y.append(net.put(ref.at[rows_c], place(me.s, me.c), me.over_y))
            if i == 0:
                x_wire = net.put(x_ref, xo, me.over_x)
            half_c.append(net.put(ref, place(me.s), me.over_core))
        for ref, place in whole[1:]:
            whole_y.append(net.put(ref, place(me.s), me.over_y))
            whole_c.append(net.put(ref, place(me.s), me.over_core))
        wl[lat_rows:, :] = jnp.zeros((lat_pad - lat_rows, width), BF)

        whole_y[0].wait_recv()
        fwd = [net.put(small_all.at[other], small_all.at[other], me.over_core)]
        whole_c[0].wait_recv()
        fwd[0].wait_recv()
        local[3].wait()
        gain_out[...] = jnp.zeros_like(gain_out)
        for s in range(4):
            for i in range(4):
                cols = pl.ds((4 * s + i) * LANES, LANES)
                gain_out[0:1, cols] = small_all[s, i : i + 1, :]
                gain_out[1:2, cols] = small_all[s, 4 + i : 5 + i, :]
            gain_out[2:3, s * LANES : (s + 1) * LANES] = small_all[s, 8:9, :]

        def norm_rows_into(src, base):
            def one(r, carry):
                v = src[row_at(0, r), :].astype(F32)
                n1[row_at(base, r), :] = norm_rows(v, gain_out[0:1, :]).astype(BF)
                return carry

            lax.fori_loop(0, rows // STEP, one, 0)

        ours, theirs = me.c * rows, (1 - me.c) * rows
        norm_rows_into(x_ref, ours)
        at_us = pl.ds(pl.multiple_of(ours, rows), rows)
        one_out[...] = n1[at_us, :]
        half_x, relays = [], []
        for got, (_, _, place) in zip(half_y, halved):
            got.wait_recv()
            piece_ref = place(other, me.c)
            half_x.append(net.put(piece_ref, piece_ref, me.over_x))
            relays.append(net.put(piece_ref, piece_ref, me.over_core))
        x_wire.wait_recv()
        norm_rows_into(xo, theirs)
        for got, (_, place) in zip(whole_y[1:], whole[1:]):
            got.wait_recv()
            relays.append(net.put(place(other), place(other), me.over_core))
        for got, (_, _, place) in zip(half_x, halved):
            got.wait_recv()
            piece_ref = place(other, 1 - me.c)
            relays.append(net.put(piece_ref, piece_ref, me.over_core))
        bg = Background()
        bg.add(sub("cot", cot_in, cot_out))
        for key, src, dst in zip(("sg", "su", "sd"), shared_in, shared_out):
            bg.add(sub(key, src, dst))
        for got in half_c + whole_c[1:] + relays:
            got.wait_recv()
        for copy in local[:3] + local[4:]:
            copy.wait()
        stores = [
            net.move(src, dst)
            for src, dst in zip((wq, wl.at[pl.ds(0, lat_rows)], we, wo, rt), weights_out)
        ]

        lane = lax.broadcasted_iota(jnp.int32, (rows, LANES), 1)
        lane2 = lax.broadcasted_iota(jnp.int32, (2 * rows, LANES), 1)
        query = mdot(n1[at_us, :], wq[...])
        cos, sin = cos_ref[at_us, :], sin_ref[at_us, :]
        a, b = query[:, nope_w : nope_w + LANES], query[:, nope_w + LANES :]
        qn_out[...] = query[:, :nope_w].astype(BF)
        qa_out[...] = (a * cos - b * sin).astype(BF)
        qb_out[...] = (a * sin + b * cos).astype(BF)
        latent = dot_nt(n1[...], wl[...])
        lat32[...] = latent[:, :KVR]
        ln[...] = norm_rows(latent[:, :KVR], gain_out[2:3, 0:KVR]).astype(BF)
        latn_out[...] = ln[at_us, :]
        comp_out[...] = lat32[pl.ds(pl.multiple_of(ours + me.t * piece, piece), piece), :]

        def spread_heads(v):
            v = jnp.where(lane2 < DR // 2, v, 0.0)
            v = v + pltpu.roll(v, DR // 2, 1)
            return v + pltpu.roll(v, DR, 1)

        tile = latent[:, KVR:]
        a, b = spread_heads(tile), spread_heads(pltpu.roll(tile, LANES - DR // 2, 1))
        ka_out[...] = (a * cos_ref[...] - b * sin_ref[...]).astype(BF)
        kb_out[...] = (a * sin_ref[...] + b * cos_ref[...]).astype(BF)
        kv_out[...] = mdot(ln[...], we[...]).astype(BF)
        q_pos = ours + lax.broadcasted_iota(jnp.int32, (rows, 2 * rows), 0)
        k_pos = lax.broadcasted_iota(jnp.int32, (rows, 2 * rows), 1)
        zero = jnp.zeros((), BF)
        for h in range(n_head):
            mine = (lane >= h * (DR // 2)) & (lane < (h + 1) * (DR // 2))
            k_at, v_at = pl.ds(h * (DN + DV), DN), pl.ds(h * (DN + DV) + DN, DV)
            score = dot_nt(qn_out[:, h * DN : (h + 1) * DN], kv_out[:, k_at])
            score = score + dot_nt(jnp.where(mine, qa_out[...], zero), ka_out[...])
            score = score + dot_nt(jnp.where(mine, qb_out[...], zero), kb_out[...])
            score = jnp.where(k_pos <= q_pos, score * scale, NEG)
            top = jnp.max(score, axis=1, keepdims=True)
            expo = jnp.exp(score - top)
            total = jnp.sum(expo, axis=1, keepdims=True)
            value = mdot(expo.astype(BF), kv_out[:, v_at])
            attn_out[:, h * DV : (h + 1) * DV] = (value / total).astype(BF)
            prob_out[h] = jnp.exp(score - (top + jnp.log(total)))
        n_col = 4
        col_w = width // n_col

        def columns(n, carry):
            cols = pl.ds(pl.multiple_of(n * col_w, col_w), col_w)
            part[:, cols] = mdot(attn_out[...], wo[:, cols]).astype(BF)
            return carry

        lax.fori_loop(0, n_col, columns, 0)
        rs = sub("rs", part, res)
        next(rs)
        yield 1
        for _ in range(3):
            bg.step()
        next(rs, None)
        quarter = pl.ds(pl.multiple_of(me.t * piece, piece), piece)
        mid = x_ref[quarter, :].astype(F32) + res[...]
        mid_out[...] = mid
        two_out[...] = norm_rows(mid, gain_out[1:2, :]).astype(BF)
        bg.drain()
        for store in stores:
            store.wait()

    ins = (
        block, *tables,
        w_query, w_latent_t, w_expand, w_output, router_t, small, cot_pack, *shared,
    )
    outs = [
        ((piece, width), F32, VMEM),
        ((piece, width), BF, VMEM),
        ((rows, n_head * DV), BF, VMEM),
        ((n_head, rows, 2 * rows), F32, VMEM),
        ((2 * rows, kv_w), BF, VMEM),
        ((2 * rows, LANES), BF, VMEM),
        ((2 * rows, LANES), BF, VMEM),
        ((rows, nope_w), BF, VMEM),
        ((rows, LANES), BF, VMEM),
        ((rows, LANES), BF, VMEM),
        ((piece, KVR), F32, VMEM),
        ((rows, width), BF, VMEM),
        ((rows, KVR), BF, VMEM),
        ((8, width), F32, VMEM),
        ((4 * k_w, q_w), BF, ANY),
        ((lat_rows, width), BF, ANY),
        ((4 * e_w, kv_w), BF, ANY),
        ((w_output.shape[0], width), BF, ANY),
        ((router_t.shape[0], width), BF, ANY),
        *subs["cot"].outs,
        *subs["sg"].outs,
        *subs["su"].outs,
        *subs["sd"].outs,
    ]
    return Job(
        run,
        list(zip(ins, [VMEM] * 3 + [ANY] * 10)),
        outs,
        own_scratch + [s for job in subs.values() for s in job.scratch],
        25 + sum(job.n_put for job in subs.values()),
        11 + sum(job.n_local for job in subs.values()),
        "xykzp",
    )


def per_device(
    block_input,
    norm1_gain,
    q_weight,
    kva_weight,
    kv_norm_gain,
    kvb_weight,
    out_weight,
    norm2_gain,
    router_weight,
    shared_gate,
    shared_up,
    shared_down,
    expert_gate,
    expert_up,
    expert_down,
    routes,
    cotangent,
):
    n_tp = lax.axis_size(TP)
    rows, width = block_input.shape
    topk = routes.shape[1]
    experts = router_weight.shape[1]
    heads = q_weight.shape[1] // (DN + DR)
    piece = rows // n_tp
    s_id, c_id, t_id = lax.axis_index(SHARD), lax.axis_index(CTX), lax.axis_index(TP)
    shard_w = width // 4
    kv_w = KVR // 4

    by_head = q_weight.reshape(-1, heads, DN + DR)
    q_weight = jnp.concatenate(
        [
            by_head[:, :, :DN].reshape(-1, heads * DN),
            by_head[:, :, DN : DN + DR // 2].reshape(-1, LANES),
            by_head[:, :, DN + DR // 2 :].reshape(-1, LANES),
        ],
        axis=1,
    )

    def own(a):
        return lax.dynamic_slice_in_dim(a, t_id * piece, piece, 0)

    small = jnp.concatenate(
        [
            norm1_gain.reshape(-1, LANES),
            norm2_gain.reshape(-1, LANES),
            kv_norm_gain.reshape(-1, LANES),
            jnp.zeros((7, LANES), BF),
        ]
    ).astype(F32)
    cot_pack = jnp.concatenate(
        [cotangent.astype(BF), jnp.pad(routes.astype(BF), ((0, 0), (0, LANES - topk)))], axis=1
    )
    tables = [jnp.tile(v, (1, heads)) for v in rope_tables(2 * rows, jnp.float32(0))]
    (
        (
            mid, two_own, attn_flat, prob, kv_flat, keys_first, keys_second, q_nope, q_first, q_second,
            compressed, normed_one, latent_own, gains_all, w_query, w_latent_t, w_expand, w_output, router_t,
            cot_all, sg_t, su_t, sd,
        ),
    ) = comm_kernel(
        [
            attention_forward(
                block_input,
                tables,
                q_weight,
                kva_weight.T,
                kvb_weight,
                out_weight,
                router_weight.T,
                small,
                cot_pack,
                (shared_gate.T, shared_up.T, shared_down),
                n_tp,
            )
        ],
        n_tp,
        0,
        "attention",
    )
    x_own = own(block_input).astype(F32)

    (
        mid_grad, gain_two_sum, mid_pack, y_part, grad_gate, grad_up, grad_expert_down, shared_grads,
        two_cols, attn_all, one_cols, lat_cols,
    ) = feed_forward(
        two_own,
        mid,
        own(cotangent),
        gains_all[1:2],
        cot_all,
        expert_gate.transpose(0, 2, 1),
        expert_up.transpose(0, 2, 1),
        expert_down,
        sg_t,
        su_t,
        sd,
        router_t,
        attn_flat,
        normed_one,
        latent_own,
        topk,
        n_tp,
    )
    ((block_output, input_grad, gains, mid_cols, logit_all, shared_cols, head_all, lat_all),) = comm_kernel(
        [
            attention_back(
                mid_pack,
                attn_flat,
                prob,
                kv_flat,
                [keys_first, keys_second],
                q_nope,
                [q_first, q_second],
                [lax.dynamic_slice_in_dim(v, c_id * rows, rows, 0) for v in tables],
                compressed,
                [gains_all[2:3, :KVR], gains_all[0:1]],
                [x_own, mid_grad, mid],
                y_part,
                shared_grads.reshape(-1, width),
                w_output,
                w_expand,
                w_query,
                w_latent_t,
                gain_two_sum,
                n_tp,
            )
        ],
        n_tp,
        2,
        "back",
    )
    head_all = head_all.reshape(8 * rows, -1)
    split = heads * (DN + DR)
    lat_all = lat_all.reshape(8 * rows, -1)[:, : KVR + DR]
    one_cols = one_cols.reshape(8 * rows, -1)
    grad_query = dot_tn(one_cols, head_all[:, :split])
    grad_query = jnp.concatenate(
        [
            grad_query[:, : heads * DN].reshape(shard_w, heads, DN),
            grad_query[:, heads * DN : heads * DN + LANES].reshape(shard_w, heads, DR // 2),
            grad_query[:, heads * DN + LANES :].reshape(shard_w, heads, DR // 2),
        ],
        axis=2,
    ).reshape(shard_w, -1)
    grad_latent = dot_tn(lat_all, one_cols).T
    grad_expand = dot_tn(lat_cols.reshape(8 * rows, -1), head_all[:, split:])
    grad_out_w = dot_tn(attn_all.reshape(8 * rows, -1), mid_cols.reshape(8 * rows, -1))
    off = (2 * expert_gate.shape[2] + sg_t.shape[0]) % LANES
    logit_all = logit_all.reshape(8 * rows, -1)[:, off : off + experts]
    grad_router = dot_tn(logit_all, two_cols.reshape(8 * rows, -1)).T
    shared_cols = shared_cols.reshape(8, 3, -1, shard_w)
    grad_sgate, grad_sup, grad_sdown = (
        shared_cols[:, i].reshape(-1, shard_w).astype(F32) for i in range(3)
    )
    gains = gains.reshape(-1)
    grad_one = lax.dynamic_slice_in_dim(gains, s_id * shard_w, shard_w, 0)
    grad_two = lax.dynamic_slice_in_dim(gains, width + s_id * shard_w, shard_w, 0)
    grad_kv = lax.dynamic_slice_in_dim(gains, 2 * width + s_id * kv_w, kv_w, 0)
    return (
        block_output.astype(F32),
        input_grad.astype(F32),
        grad_one,
        grad_query,
        grad_latent,
        grad_kv,
        grad_expand,
        grad_out_w,
        grad_two,
        grad_router,
        grad_sgate.T,
        grad_sup.T,
        grad_sdown,
        grad_gate.transpose(0, 2, 1),
        grad_up.transpose(0, 2, 1),
        grad_expert_down,
    )


def send_rows(buffer):
    return lax.all_to_all(buffer, (SHARD, CTX), split_axis=0, concat_axis=0, tiled=True)


def return_rows(partial_value, slots):
    back_rows = lax.all_to_all(
        partial_value, (SHARD, CTX), split_axis=0, concat_axis=0, tiled=True
    )
    flat_back = back_rows.reshape(-1, back_rows.shape[-1])
    return flat_back[slots]


def per_device_general(
    block_input,
    norm1_gain,
    q_weight,
    kva_weight,
    kv_norm_gain,
    kvb_weight,
    out_weight,
    norm2_gain,
    router_weight,
    shared_gate,
    shared_up,
    shared_down,
    expert_gate,
    expert_up,
    expert_down,
    routes,
    cotangent,
):
    tok_rows = block_input.shape[0]
    head_count = q_weight.shape[1] // (DN + DR)
    score_scale = (DN + DR) ** (-0.5)
    (
        gain_one,
        w_query,
        w_latent,
        gain_kv,
        w_expand,
        w_output,
        gain_two,
        w_router,
        w_sgate,
        w_sup,
        w_sdown,
    ) = (
        lax.all_gather(norm1_gain, SHARD, axis=0, tiled=True),
        lax.all_gather(q_weight, SHARD, axis=0, tiled=True),
        lax.all_gather(kva_weight, SHARD, axis=0, tiled=True),
        lax.all_gather(kv_norm_gain, SHARD, axis=0, tiled=True),
        lax.all_gather(kvb_weight, SHARD, axis=0, tiled=True),
        lax.all_gather(out_weight, SHARD, axis=1, tiled=True),
        lax.all_gather(norm2_gain, SHARD, axis=0, tiled=True),
        lax.all_gather(router_weight, SHARD, axis=0, tiled=True),
        lax.all_gather(shared_gate, SHARD, axis=0, tiled=True),
        lax.all_gather(shared_up, SHARD, axis=0, tiled=True),
        lax.all_gather(shared_down, SHARD, axis=1, tiled=True),
    )
    block_index = lax.axis_index(CTX)
    cosine, sine_table = rope_tables(tok_rows, (block_index * tok_rows).astype(jnp.float32))
    x_float = block_input.astype(jnp.float32)
    normed_one = norm_rows(x_float, gain_one).astype(jnp.bfloat16)
    query = mdot(normed_one, w_query).reshape(tok_rows, head_count, DN + DR)
    query_rot = rotate(query[..., DN:], cosine[:, None, :], sine_table[:, None, :])
    query = jnp.concatenate([query[..., :DN], query_rot], axis=-1).astype(jnp.bfloat16)
    query_nope = query[..., :DN]
    query_rope = query[..., DN:]
    latent = mdot(normed_one, w_latent)
    compressed = latent[:, :KVR]
    latent_n = norm_rows(compressed, gain_kv).astype(jnp.bfloat16)
    rope_key = rotate(latent[:, KVR:], cosine, sine_table).astype(jnp.bfloat16)
    first_piece = mdot(latent_n, w_expand).astype(jnp.bfloat16)
    gathered, rope_all = (
        lax.all_gather(first_piece, CTX, axis=0, tiled=True),
        lax.all_gather(rope_key, CTX, axis=0, tiled=True),
    )
    query_pos = block_index * tok_rows + jnp.arange(tok_rows, dtype=jnp.int32)

    def scores_at(block_id):
        blk_start = block_id * tok_rows
        kv_block = lax.dynamic_slice_in_dim(gathered, blk_start, tok_rows, 0).reshape(
            tok_rows, head_count, DN + DV
        )
        rope_block = lax.dynamic_slice_in_dim(rope_all, blk_start, tok_rows, 0)
        score = jnp.einsum(
            "qhd,khd->hqk", query_nope, kv_block[..., :DN], preferred_element_type=jnp.float32
        )
        score = score + jnp.einsum(
            "qhd,kd->hqk", query_rope, rope_block, preferred_element_type=jnp.float32
        )
        score = score * score_scale
        key_pos = blk_start + jnp.arange(tok_rows, dtype=jnp.int32)
        score = jnp.where(key_pos[None, None, :] <= query_pos[None, :, None], score, NEG)
        return (score, kv_block, rope_block)

    def forward_block(block_id, carry):
        run_max, run_sum, weighted = carry
        score, kv_block, rope_block = scores_at(block_id)
        new_max = jnp.maximum(run_max, jnp.max(score, axis=-1))
        factor = jnp.exp(run_max - new_max)
        expo = jnp.exp(score - new_max[..., None])
        run_sum = factor * run_sum + jnp.sum(expo, axis=-1)
        weighted = factor[..., None] * weighted + jnp.einsum(
            "hqk,khd->hqd",
            expo.astype(jnp.bfloat16),
            kv_block[..., DN:],
            preferred_element_type=jnp.float32,
        )
        return (new_max, run_sum, weighted)

    start_state = (
        jnp.full((head_count, tok_rows), NEG, jnp.float32),
        jnp.zeros((head_count, tok_rows), jnp.float32),
        jnp.zeros((head_count, tok_rows, DV), jnp.float32),
    )
    run_max, run_sum, weighted = lax.fori_loop(0, block_index + 1, forward_block, start_state)
    lse = run_max + jnp.log(run_sum)
    attn_rows = (weighted / run_sum[..., None]).astype(jnp.bfloat16).transpose(1, 0, 2)
    attn_flat = attn_rows.reshape(tok_rows, head_count * DV)
    attn_full = lax.psum(mdot(attn_flat, w_output), TP)
    mid = x_float + attn_full
    normed_two = norm_rows(mid, gain_two).astype(jnp.bfloat16)
    probs = jax.nn.softmax(mdot(normed_two, w_router), axis=-1)
    experts = probs.shape[1]
    topk = routes.shape[1]
    picks = (routes[:, :, None] == jnp.arange(experts, dtype=jnp.int32)[None, None, :]).astype(
        jnp.float32
    )
    route_w = jnp.sum(picks * probs[:, None, :], axis=-1)
    shared_a = mdot(normed_two, w_sgate)
    shared_b = mdot(normed_two, w_sup)
    shared_h = (jax.nn.silu(shared_a) * shared_b).astype(jnp.bfloat16)
    shared_y = mdot(shared_h, w_sdown)
    capacity = 2 * tok_rows * topk // experts
    owners = lax.axis_size((SHARD, CTX))
    local_experts = expert_gate.shape[0]
    width = normed_two.shape[1]
    flat_routes = routes.reshape(-1)
    onehot = (flat_routes[:, None] == jnp.arange(experts, dtype=jnp.int32)[None, :]).astype(
        jnp.int32
    )
    rank = jnp.sum((jnp.cumsum(onehot, axis=0) - 1) * onehot, axis=1)
    slots = flat_routes * capacity + rank
    source_row = jnp.arange(tok_rows * topk, dtype=jnp.int32) // topk
    send_buffer = (
        jnp.zeros((experts * capacity, width), jnp.bfloat16).at[slots].set(normed_two[source_row])
    )
    received = send_rows(send_buffer.reshape(owners, local_experts * capacity, width)).reshape(
        owners, local_experts, capacity, width
    )
    gate_act = jnp.einsum(
        "gecd,edf->gecf", received, expert_gate, preferred_element_type=jnp.float32
    )
    up_act = jnp.einsum("gecd,edf->gecf", received, expert_up, preferred_element_type=jnp.float32)
    hidden = (jax.nn.silu(gate_act) * up_act).astype(jnp.bfloat16)
    expert_y = jnp.einsum("gecf,efd->gecd", hidden, expert_down, preferred_element_type=jnp.float32)
    routed_out = return_rows(
        expert_y.reshape(owners, local_experts * capacity, width), slots
    ).reshape(tok_rows, topk, width)
    routed_part = jnp.sum(route_w[:, :, None] * routed_out, axis=1) + shared_y
    weight_part = jnp.sum(routed_out * cotangent[:, None, :], axis=-1)
    moe_out, route_grad = lax.psum((routed_part, weight_part), TP)
    block_output = mid + moe_out
    cot_b = cotangent.astype(jnp.bfloat16)
    routed_grad = (
        (route_w[:, :, None] * cotangent[:, None, :])
        .astype(jnp.bfloat16)
        .reshape(tok_rows * topk, width)
    )
    grad_buffer = jnp.zeros((experts * capacity, width), jnp.bfloat16).at[slots].set(routed_grad)
    grad_recv = send_rows(grad_buffer.reshape(owners, local_experts * capacity, width)).reshape(
        owners, local_experts, capacity, width
    )
    hidden_grad = jnp.einsum(
        "gecd,efd->gecf", grad_recv, expert_down, preferred_element_type=jnp.float32
    )
    gate_grad = (hidden_grad * up_act * silu_slope(gate_act)).astype(jnp.bfloat16)
    up_grad = (hidden_grad * jax.nn.silu(gate_act)).astype(jnp.bfloat16)
    grad_expert_down = jnp.einsum(
        "gecf,gecd->efd", hidden, grad_recv, preferred_element_type=jnp.float32
    )
    grad_expert_gate = jnp.einsum(
        "gecd,gecf->edf", received, gate_grad, preferred_element_type=jnp.float32
    )
    grad_expert_up = jnp.einsum(
        "gecd,gecf->edf", received, up_grad, preferred_element_type=jnp.float32
    )
    row_grad = jnp.einsum(
        "gecf,edf->gecd", gate_grad, expert_gate, preferred_element_type=jnp.float32
    )
    row_grad = row_grad + jnp.einsum(
        "gecf,edf->gecd", up_grad, expert_up, preferred_element_type=jnp.float32
    )
    routed_back = return_rows(
        row_grad.reshape(owners, local_experts * capacity, width), slots
    ).reshape(tok_rows, topk, width)
    shared_grad = jnp.einsum("td,fd->tf", cot_b, w_sdown, preferred_element_type=jnp.float32)
    sgate_grad = (shared_grad * shared_b * silu_slope(shared_a)).astype(jnp.bfloat16)
    sup_grad = (shared_grad * jax.nn.silu(shared_a)).astype(jnp.bfloat16)
    grad_sdown = jnp.einsum("tf,td->fd", shared_h, cot_b, preferred_element_type=jnp.float32)
    grad_sgate = jnp.einsum("td,tf->df", normed_two, sgate_grad, preferred_element_type=jnp.float32)
    grad_sup = jnp.einsum("td,tf->df", normed_two, sup_grad, preferred_element_type=jnp.float32)
    two_part = jnp.sum(routed_back, axis=1)
    two_part = two_part + jnp.einsum(
        "tf,df->td", sgate_grad, w_sgate, preferred_element_type=jnp.float32
    )
    two_part = two_part + jnp.einsum(
        "tf,df->td", sup_grad, w_sup, preferred_element_type=jnp.float32
    )
    two_grad = lax.psum(two_part, TP)
    prob_grad = jnp.sum(picks * route_grad[:, :, None], axis=1)
    logit_grad = (probs * (prob_grad - jnp.sum(probs * prob_grad, axis=-1, keepdims=True))).astype(
        jnp.bfloat16
    )
    grad_router = jnp.einsum(
        "td,te->de", normed_two, logit_grad, preferred_element_type=jnp.float32
    )
    two_grad = two_grad + jnp.einsum(
        "te,de->td", logit_grad, w_router, preferred_element_type=jnp.float32
    )
    _, norm_two_back = jax.vjp(norm_rows, mid, gain_two.astype(jnp.float32))
    mid_norm_grad, grad_gain_two = norm_two_back(two_grad)
    mid_grad = cotangent + mid_norm_grad
    mid_b = mid_grad.astype(jnp.bfloat16)
    grad_out_w = jnp.einsum("tj,td->jd", attn_flat, mid_b, preferred_element_type=jnp.float32)
    out_grad = jnp.einsum("td,jd->tj", mid_b, w_output, preferred_element_type=jnp.float32).reshape(
        tok_rows, head_count, DV
    )
    out_grad_b = out_grad.astype(jnp.bfloat16)
    delta = jnp.sum(out_grad * attn_rows.astype(jnp.float32), axis=-1).T
    key_count = gathered.shape[0]
    term_width = head_count * (DN + DV + DR)

    def back_block(block_id, carry):
        nope_grad, rope_qgrad, terms = carry
        score, kv_block, rope_block = scores_at(block_id)
        probs_blk = jnp.exp(score - lse[..., None])
        prob_b = probs_blk.astype(jnp.bfloat16)
        dprob = jnp.einsum(
            "qhd,khd->hqk", out_grad_b, kv_block[..., DN:], preferred_element_type=jnp.float32
        )
        dscore = (probs_blk * (dprob - delta[..., None])).astype(jnp.bfloat16)
        nope_grad = (
            nope_grad
            + jnp.einsum(
                "hqk,khd->qhd", dscore, kv_block[..., :DN], preferred_element_type=jnp.float32
            )
            * score_scale
        )
        rope_qgrad = (
            rope_qgrad
            + jnp.einsum("hqk,kd->qhd", dscore, rope_block, preferred_element_type=jnp.float32)
            * score_scale
        )
        key_nope_grad = (
            jnp.einsum("hqk,qhd->khd", dscore, query_nope, preferred_element_type=jnp.float32)
            * score_scale
        )
        key_rope_grad = (
            jnp.einsum("hqk,qhd->khd", dscore, query_rope, preferred_element_type=jnp.float32)
            * score_scale
        )
        value_grad = jnp.einsum(
            "hqk,qhd->khd", prob_b, out_grad_b, preferred_element_type=jnp.float32
        )
        block_terms = jnp.concatenate([key_nope_grad, value_grad, key_rope_grad], axis=-1).reshape(
            tok_rows, term_width
        )
        terms = lax.dynamic_update_slice_in_dim(terms, block_terms, block_id * tok_rows, 0)
        return (nope_grad, rope_qgrad, terms)

    back_init = (
        jnp.zeros((tok_rows, head_count, DN), jnp.float32),
        jnp.zeros((tok_rows, head_count, DR), jnp.float32),
        jnp.zeros((key_count, term_width), jnp.float32),
    )
    nope_grad, rope_qgrad, terms = lax.fori_loop(0, block_index + 1, back_block, back_init)
    key_terms = lax.psum_scatter(terms, CTX, scatter_dimension=0, tiled=True).reshape(
        tok_rows, head_count, DN + DV + DR
    )
    kv_grad = (
        key_terms[..., : DN + DV].reshape(tok_rows, head_count * (DN + DV)).astype(jnp.bfloat16)
    )
    rope_grad = rotate_back(jnp.sum(key_terms[..., DN + DV :], axis=1), cosine, sine_table)
    grad_expand = jnp.einsum("ti,tj->ij", latent_n, kv_grad, preferred_element_type=jnp.float32)
    latent_part = jnp.einsum("tj,ij->ti", kv_grad, w_expand, preferred_element_type=jnp.float32)
    rope_qback = rotate_back(rope_qgrad, cosine[:, None, :], sine_table[:, None, :])
    query_grad = (
        jnp.concatenate([nope_grad, rope_qback], axis=-1)
        .astype(jnp.bfloat16)
        .reshape(tok_rows, head_count * (DN + DR))
    )
    grad_query = jnp.einsum("td,tj->dj", normed_one, query_grad, preferred_element_type=jnp.float32)
    normed_part = jnp.einsum("tj,dj->td", query_grad, w_query, preferred_element_type=jnp.float32)
    latent_sum, normed_sum = lax.psum(
        (jnp.concatenate([latent_part, rope_grad], axis=-1), normed_part), TP
    )
    _, kv_back = jax.vjp(norm_rows, compressed, gain_kv.astype(jnp.float32))
    compressed_grad, grad_gain_kv = kv_back(latent_sum[:, :KVR])
    latent_grad = jnp.concatenate([compressed_grad, latent_sum[:, KVR:]], axis=-1).astype(
        jnp.bfloat16
    )
    grad_latent = jnp.einsum(
        "td,tl->dl", normed_one, latent_grad, preferred_element_type=jnp.float32
    )
    one_grad = normed_sum + jnp.einsum(
        "tl,dl->td", latent_grad, w_latent, preferred_element_type=jnp.float32
    )
    _, one_back = jax.vjp(norm_rows, x_float, gain_one.astype(jnp.float32))
    input_norm_grad, grad_gain_one = one_back(one_grad)
    input_grad = mid_grad + input_norm_grad
    (
        red_one,
        red_query,
        red_latent,
        red_kv,
        red_expand,
        red_output,
        red_two,
        red_router,
        red_sgate,
        red_sup,
        red_sdown,
    ) = (
        lax.psum_scatter(grad_gain_one, SHARD, scatter_dimension=0, tiled=True),
        lax.psum_scatter(grad_query, SHARD, scatter_dimension=0, tiled=True),
        lax.psum_scatter(grad_latent, SHARD, scatter_dimension=0, tiled=True),
        lax.psum_scatter(grad_gain_kv, SHARD, scatter_dimension=0, tiled=True),
        lax.psum_scatter(grad_expand, SHARD, scatter_dimension=0, tiled=True),
        lax.psum_scatter(grad_out_w, SHARD, scatter_dimension=1, tiled=True),
        lax.psum_scatter(grad_gain_two, SHARD, scatter_dimension=0, tiled=True),
        lax.psum_scatter(grad_router, SHARD, scatter_dimension=0, tiled=True),
        lax.psum_scatter(grad_sgate, SHARD, scatter_dimension=0, tiled=True),
        lax.psum_scatter(grad_sup, SHARD, scatter_dimension=0, tiled=True),
        lax.psum_scatter(grad_sdown, SHARD, scatter_dimension=1, tiled=True),
    )
    (
        sum_one,
        sum_query,
        sum_latent,
        sum_kv,
        sum_expand,
        sum_output,
        sum_two,
        sum_router,
        sum_sgate,
        sum_sup,
        sum_sdown,
    ) = lax.psum(
        (
            red_one,
            red_query,
            red_latent,
            red_kv,
            red_expand,
            red_output,
            red_two,
            red_router,
            red_sgate,
            red_sup,
            red_sdown,
        ),
        CTX,
    )
    return (
        block_output,
        input_grad,
        sum_one,
        sum_query,
        sum_latent,
        sum_kv,
        sum_expand,
        sum_output,
        sum_two,
        sum_router,
        sum_sgate,
        sum_sup,
        sum_sdown,
        grad_expert_gate,
        grad_expert_up,
        grad_expert_down,
    )


def solution(mesh):
    in_specs = (
        P((SHARD, CTX), None),
        P(SHARD),
        P(SHARD, TP),
        P(SHARD, None),
        P(SHARD),
        P(SHARD, TP),
        P(TP, SHARD),
        P(SHARD),
        P(SHARD, None),
        P(SHARD, TP),
        P(SHARD, TP),
        P(TP, SHARD),
        P((SHARD, CTX), None, TP),
        P((SHARD, CTX), None, TP),
        P((SHARD, CTX), TP, None),
        P((SHARD, CTX), None),
        P((SHARD, CTX), None),
    )
    out_specs = (
        P((SHARD, CTX), None),
        P((SHARD, CTX), None),
        P(SHARD),
        P(SHARD, TP),
        P(SHARD, None),
        P(SHARD),
        P(SHARD, TP),
        P(TP, SHARD),
        P(SHARD),
        P(SHARD, None),
        P(SHARD, TP),
        P(SHARD, TP),
        P(TP, SHARD),
        P((SHARD, CTX), None, TP),
        P((SHARD, CTX), None, TP),
        P((SHARD, CTX), TP, None),
    )
    routed = mesh.shape[SHARD] == 4 and mesh.shape[CTX] == 2 and mesh.shape[TP] == 4
    return jax.shard_map(
        per_device if routed else per_device_general, mesh=mesh, in_specs=in_specs, out_specs=out_specs, check_vma=False
    )
```

```python
import functools

import jax
import jax.numpy as jnp
from jax import lax
from jax.experimental import pallas as pl
from jax.experimental.pallas import tpu as pltpu
from jax.sharding import PartitionSpec as P

DN = 128
DR = 64
DV = 128
KVR = 512
LANES = 128
SHARD, CTX, TP = "shard", "ctx", "tp"

EPS = 1e-06
NEG = -1e30

BF = jnp.bfloat16
F32 = jnp.float32
MESH = pl.DeviceIdType.MESH
ANY = pl.ANY
VMEM = pltpu.VMEM


def norm_rows(value, gain):
    factor = lax.rsqrt(jnp.mean(value * value, axis=-1, keepdims=True) + EPS)
    return value * factor * gain.astype(F32)


def norm_back(value, gain, grad):
    factor = lax.rsqrt(jnp.mean(value * value, axis=-1, keepdims=True) + EPS)
    scaled = grad * gain.astype(F32)
    inner = jnp.mean(scaled * value, axis=-1, keepdims=True)
    return factor * (scaled - value * (factor * factor * inner)), grad * value * factor


def rope_tables(count, offset):
    half_size = DR // 2
    position = jnp.arange(count, dtype=F32) + offset
    freqs = 10000.0 ** (-(jnp.arange(half_size, dtype=F32) * 2.0 / DR))
    angle = position[:, None] * freqs[None, :]
    return (jnp.cos(angle), jnp.sin(angle))


def rotate(value, cosine, sine_table):
    half_size = DR // 2
    first = value[..., :half_size]
    second = value[..., half_size:]
    return jnp.concatenate(
        [first * cosine - second * sine_table, first * sine_table + second * cosine], axis=-1
    )


def rotate_back(grad, cosine, sine_table):
    half_size = DR // 2
    first = grad[..., :half_size]
    second = grad[..., half_size:]
    return jnp.concatenate(
        [first * cosine + second * sine_table, second * cosine - first * sine_table], axis=-1
    )


def silu_slope(value):
    sigmoid = jax.nn.sigmoid(value)
    return sigmoid * (1.0 + value * (1.0 - sigmoid))


def mdot(left, right):
    return jnp.dot(left, right, preferred_element_type=F32)


def dot_nt(left, right):
    return lax.dot_general(left, right, (((1,), (1,)), ((), ())), preferred_element_type=F32)


def dot_tn(left, right):
    return lax.dot_general(left, right, (((0,), (0,)), ((), ())), preferred_element_type=F32)


class Place:
    def __init__(self, n_tp):
        self.s = lax.axis_index(SHARD)
        self.c = lax.axis_index(CTX)
        self.t = lax.axis_index(TP)
        self.core = lax.rem(self.s, 2)
        self.y = self.s // 2
        self.n_tp = n_tp
        self.over_x = self.flip(0, 0, 1)
        self.over_y = self.flip(1, 0, 0)
        self.over_core = self.flip(0, 1, 0)

    def along(self, step):
        t = lax.rem(self.t + step + self.n_tp, self.n_tp)
        return {SHARD: self.s, CTX: self.c, TP: t}

    def flip(self, dy, dcore, dx):
        y = self.y + dy * (1 - 2 * self.y)
        core = self.core + dcore * (1 - 2 * self.core)
        x = self.c + dx * (1 - 2 * self.c)
        return {SHARD: 2 * y + core, CTX: x, TP: self.t}

    def peers(self, kinds):
        flips = []
        if "p" in kinds:
            flips = FLIPS
        else:
            flips = [f for kind, f in (("x", FLIPS[0]), ("k", FLIPS[1]), ("y", FLIPS[3])) if kind in kinds]
        out = [self.flip(*f) for f in flips]
        if "z" in kinds:
            out += [self.along(k) for k in range(1, self.n_tp)]
        return out


FLIPS = [(dy, dk, dx) for dy in (0, 1) for dk in (0, 1) for dx in (0, 1)][1:]


def slot(s, c):
    return 2 * s + c


class Net:
    def __init__(self, send, recv, local):
        self.send, self.recv, self.local = send, recv, local
        self.puts = []
        self.n_local = 0

    def put(self, src, dst, to):
        i = len(self.puts)
        copy = pltpu.make_async_remote_copy(
            src_ref=src,
            dst_ref=dst,
            send_sem=self.send.at[i],
            recv_sem=self.recv.at[i],
            device_id=to,
            device_id_type=MESH,
        )
        copy.start()
        self.puts.append(copy)
        return copy

    def move(self, src, dst):
        copy = pltpu.make_async_copy(src, dst, self.local.at[self.n_local])
        self.n_local += 1
        copy.start()
        return copy

    def finish(self):
        for copy in self.puts:
            copy.wait_send()


def greet(peers):
    barrier = pltpu.get_barrier_semaphore()
    for peer in peers:
        pl.semaphore_signal(barrier, inc=1, device_id=peer, device_id_type=MESH)
    pl.semaphore_wait(barrier, len(peers))


class Job:
    def __init__(self, run, ins, outs, scratch, n_put, n_local, peers):
        self.run, self.ins, self.outs, self.scratch = run, ins, outs, scratch
        self.n_put, self.n_local, self.peers = n_put, n_local, peers


def comm_kernel(jobs, n_tp, collective_id, name):
    ins = [i for job in jobs for i in job.ins]
    outs = [o for job in jobs for o in job.outs]
    scratch = [s for job in jobs for s in job.scratch]
    n_put = sum(job.n_put for job in jobs)
    n_local = max(sum(job.n_local for job in jobs), 1)
    kinds = "".join(sorted(set("".join(job.peers for job in jobs))))

    def body(*refs):
        in_refs, out_refs = refs[: len(ins)], refs[len(ins) : len(ins) + len(outs)]
        rest = refs[len(ins) + len(outs) :]
        me = Place(n_tp)
        net = Net(*rest[len(scratch) :])
        greet(me.peers(kinds))
        running = []
        i = o = s = 0
        for job in jobs:
            ni, no, ns = len(job.ins), len(job.outs), len(job.scratch)
            running.append(
                job.run(net, me, in_refs[i : i + ni], out_refs[o : o + no], rest[s : s + ns])
            )
            i, o, s = i + ni, o + no, s + ns
        while running:
            running = [r for r in running if next(r, None) is not None]
        net.finish()

    got = pl.pallas_call(
        body,
        out_shape=tuple(jax.ShapeDtypeStruct(shape, dtype) for shape, dtype, _ in outs),
        in_specs=[pl.BlockSpec(memory_space=space) for _, space in ins],
        out_specs=tuple(pl.BlockSpec(memory_space=space) for _, _, space in outs),
        scratch_shapes=[
            *scratch,
            pltpu.SemaphoreType.DMA((n_put,)),
            pltpu.SemaphoreType.DMA((n_put,)),
            pltpu.SemaphoreType.DMA((n_local,)),
        ],
        compiler_params=pltpu.CompilerParams(
            collective_id=collective_id, has_side_effects=True, vmem_limit_bytes=60 * 2**20
        ),
        name=name,
    )(*[a for a, _ in ins])
    split, o = [], 0
    for job in jobs:
        split.append(got[o : o + len(job.outs)])
        o += len(job.outs)
    return split


def shard_gather(weights, block):
    shapes = [w.shape for w, _ in weights]
    side = [by for _, by in weights]

    def run(net, me, ins, outs, bounce):
        n = len(shapes)
        x_in, x_out = ins[n], outs[n]
        other = lax.rem(me.s + 2, 4)

        def place(i, s, which=None):
            rows, cols = shapes[i]
            at = pl.ds(0, rows)
            if which is not None:
                at = pl.ds(pl.multiple_of(which * (rows // 2), rows // 2), rows // 2)
            if side[i]:
                return outs[i].at[at, pl.ds(pl.multiple_of(s * cols, LANES), cols)]
            return outs[i].at[s, at]

        loads = [net.move(src, b) for src, b in zip(ins, bounce)]
        from_y, own = [], []
        for i in range(n):
            rows = shapes[i][0]
            at = pl.ds(pl.multiple_of(me.c * (rows // 2), rows // 2), rows // 2)
            from_y.append(net.put(ins[i].at[at], place(i, me.s, me.c), me.over_y))
            if i == 0:
                wait_x = net.put(x_in, x_out.at[me.c], me.over_x)
        for i in range(n):
            own.append(net.put(ins[i], place(i, me.s), me.over_core))
        yield 1
        stores = []
        for i, (load, b) in enumerate(zip(loads, bounce)):
            load.wait()
            stores.append(net.move(b, place(i, me.s) if i < n else x_out.at[me.c]))
        from_x, relays = [], []
        for i in range(n):
            from_y[i].wait_recv()
            piece = place(i, other, me.c)
            from_x.append(net.put(piece, piece, me.over_x))
            relays.append(net.put(piece, piece, me.over_core))
            yield 1
        for i in range(n):
            from_x[i].wait_recv()
            piece = place(i, other, 1 - me.c)
            relays.append(net.put(piece, piece, me.over_core))
            yield 1
        wait_x.wait_recv()
        for got in own + relays:
            got.wait_recv()
        for store in stores:
            store.wait()

    n = len(weights)
    outs = []
    for (rows, cols), by in zip(shapes, side):
        outs.append(((rows, 4 * cols) if by else (4, rows, cols), BF, ANY))
    outs.append(((2, *block.shape), BF, ANY))
    return Job(
        run,
        [(w, ANY) for w, _ in weights] + [(block, ANY)],
        outs,
        [VMEM(w.shape, w.dtype) for w, _ in weights] + [VMEM(block.shape, BF)],
        5 * n + 1,
        2 * n + 2,
        "xyk",
    )


def tp_reduce_scatter(part, n_tp):
    rows, width = part.shape
    piece = rows // n_tp

    def run(net, me, ins, outs, scratch):
        (src,), (out,), (got,) = ins, outs, scratch
        waits = []
        for k in range(1, n_tp):
            to = pl.multiple_of(lax.rem(me.t + k, n_tp) * piece, piece)
            waits.append(net.put(src.at[pl.ds(to, piece)], got.at[k - 1], me.along(k)))
        yield 1
        for wait in waits:
            wait.wait_recv()
        total = src[pl.ds(pl.multiple_of(me.t * piece, piece), piece), :].astype(F32)
        for k in range(1, n_tp):
            total = total + got[k - 1].astype(F32)
        out[...] = total

    return Job(
        run,
        [(part, VMEM)],
        [((piece, width), F32, VMEM)],
        [VMEM((n_tp - 1, piece, width), BF)],
        n_tp - 1,
        0,
        "z",
    )


def tp_all_gather(own, n_tp):
    size, width = own.shape
    half = size // 2

    def run(net, me, ins, outs, scratch):
        (src,), (out,) = ins, outs

        def rows(p, which=None):
            if which is None:
                return out.at[pl.ds(pl.multiple_of(p * size, size), size)]
            return out.at[pl.ds(pl.multiple_of(p * size + which * half, half), half)]

        right, left = me.along(1), me.along(-1)
        p_left, p_right = lax.rem(me.t + 3, 4), lax.rem(me.t + 1, 4)
        to_right = net.put(src, rows(me.t), right)
        to_left = net.put(src, rows(me.t), left)
        out[pl.ds(pl.multiple_of(me.t * size, size), size), :] = src[...]
        yield 1
        to_right.wait_recv()
        hop_right = net.put(rows(p_left, 0), rows(p_left, 0), right)
        to_left.wait_recv()
        hop_left = net.put(rows(p_right, 1), rows(p_right, 1), left)
        yield 1
        yield 1
        hop_right.wait_recv()
        hop_left.wait_recv()

    return Job(
        run, [(own, VMEM)], [((n_tp * size, width), own.dtype, VMEM)], [], 4, 0, "z"
    )


def relay_chunks(net, me, out, chunks):
    g_x, g_y = slot(me.s, 1 - me.c), slot(lax.rem(me.s + 2, 4), me.c)
    g_d = slot(lax.rem(me.s + 2, 4), 1 - me.c)
    first = 1 - me.core
    relay_slot = first * g_x + me.core * g_y
    relay_to = me.flip(first, 0, me.core)
    diags, waits = [], []
    for from_x, from_y, start, size in chunks:
        from_x.wait_recv()
        from_y.wait_recv()
        src = out.at[relay_slot, pl.ds(start, size)]
        diags.append(net.put(src, src, relay_to))
        for g in (g_x, g_y):
            piece = out.at[g, pl.ds(start, size)]
            waits.append(net.put(piece, piece, me.over_core))
        yield 1
    for diag, (_, _, start, size) in zip(diags, chunks):
        diag.wait_recv()
        piece = out.at[g_d, pl.ds(start, size)]
        waits.append(net.put(piece, piece, me.over_core))
        yield 1
    for wait in waits:
        wait.wait_recv()


def plane_gather(own, n_chunk=4):
    rows, width = own.shape
    size = rows // n_chunk

    def run(net, me, ins, outs, scratch):
        (src,), (out,), (bounce,) = ins, outs, scratch
        g_me = slot(me.s, me.c)
        load = net.move(src, bounce)
        chunks, cores = [], []
        for j in range(n_chunk):
            part = src.at[pl.ds(j * size, size)]
            to = out.at[g_me, pl.ds(j * size, size)]
            chunks.append(
                (net.put(part, to, me.over_x), net.put(part, to, me.over_y), j * size, size)
            )
            cores.append(net.put(part, to, me.over_core))
        yield 1
        load.wait()
        store = net.move(bounce, out.at[g_me])
        yield from relay_chunks(net, me, out, chunks)
        for core in cores:
            core.wait_recv()
        store.wait()

    return Job(
        run,
        [(own, ANY)],
        [((8, rows, width), own.dtype, ANY)],
        [VMEM(own.shape, own.dtype)],
        7 * n_chunk,
        2,
        "xyk",
    )


def plane_columns(array):
    rows, width = array.shape
    w = width // 4

    def run(net, me, ins, outs, scratch):
        (src,), (out,), (bounce,) = ins, outs, scratch
        g_me = slot(me.s, me.c)

        def cols(s):
            return src.at[:, pl.ds(pl.multiple_of(s * w, LANES), w)]

        load = net.move(cols(me.s), bounce)
        waits = []
        for f in FLIPS:
            peer = me.flip(*f)
            waits.append(net.put(cols(peer[SHARD]), out.at[g_me], peer))
        yield 1
        load.wait()
        store = net.move(bounce, out.at[g_me])
        for wait in waits:
            yield 1
            wait.wait_recv()
        store.wait()

    return Job(
        run,
        [(array, ANY)],
        [((8, rows, w), array.dtype, ANY)],
        [VMEM((rows, w), array.dtype)],
        7,
        2,
        "p",
    )


def shard_rows(array):
    h, w = array.shape[0] // 8, array.shape[1]

    def run(net, me, ins, outs, scratch):
        (src,), (out,), (bounce,) = ins, outs, scratch

        def rows(s):
            return src.at[pl.ds(pl.multiple_of(slot(s, me.c) * h, 8), h)]

        to = out.at[:, pl.ds(pl.multiple_of(me.s * w, LANES), w)]
        load = net.move(rows(me.s), bounce)
        waits = []
        for f in FLIPS:
            if f[2] == 0:
                peer = me.flip(*f)
                waits.append(net.put(rows(peer[SHARD]), to, peer))
        yield 1
        load.wait()
        store = net.move(bounce, to)
        yield 1
        for wait in waits:
            wait.wait_recv()
        store.wait()

    return Job(
        run,
        [(array, ANY)],
        [((h, 4 * w), array.dtype, ANY)],
        [VMEM((h, w), array.dtype)],
        3,
        2,
        "p",
    )


def ctx_swap(block):
    def run(net, me, ins, outs, scratch):
        (src,), (out,) = ins, outs
        got = net.put(src, out, me.over_x)
        yield 1
        yield 1
        got.wait_recv()

    return Job(run, [(block, ANY)], [(block.shape, block.dtype, ANY)], [], 1, 0, "x")


def reduce_everywhere(part, n_tp):
    tokens, width = part.shape
    rows = tokens // 8
    half = width // 2
    piece = rows // n_tp
    step = 16

    def run(net, me, ins, outs, scratch):
        (src,), (out,) = ins, outs
        mine, rc, rx, ry, q0, q1, r0, r1, last, got = scratch
        a, b = pl.ds(0, half), pl.ds(half, half)
        order = [(1, 1), (0, 1), (1, 0), (0, 0)]
        chips, loads, cores = [], [], []
        for dy, dx in order:
            ch = 2 * (me.y + dy * (1 - 2 * me.y)) + me.c + dx * (1 - 2 * me.c)
            chips.append(ch)
            base = ch * 2 * rows
            theirs = src.at[pl.ds(pl.multiple_of(base + (1 - me.core) * rows, rows), rows)]
            ours = src.at[pl.ds(pl.multiple_of(base + me.core * rows, rows), rows)]
            cores.append(net.put(theirs, rc.at[ch], me.over_core))
            loads.append(net.move(ours, mine.at[ch]))
        yield 1

        def add(target, cols, left, right):
            def one(r, carry):
                at = pl.ds(pl.multiple_of(r * step, step), step)
                target[at, cols] = (left(at).astype(F32) + right(at).astype(F32)).astype(BF)
                return carry

            lax.fori_loop(0, rows // step, one, 0)

        def sum_cores(k):
            ch = chips[k]
            loads[k].wait()
            cores[k].wait_recv()
            add(mine.at[ch], pl.ds(0, width), lambda at: mine[ch, at, :], lambda at: rc[ch, at, :])
            return ch

        c_d = sum_cores(0)
        ax0 = net.put(mine.at[c_d, :, a], rx.at[0], me.over_x)
        by0 = net.put(mine.at[c_d, :, b], ry.at[0], me.over_y)
        c_x = sum_cores(1)
        ax1 = net.put(mine.at[c_x, :, a], rx.at[1], me.over_x)
        c_y = sum_cores(2)
        by1 = net.put(mine.at[c_y, :, b], ry.at[1], me.over_y)
        c_me = sum_cores(3)
        yield 1
        every = pl.ds(0, half)
        ax0.wait_recv()
        add(q0, every, lambda at: mine[c_y, at, a], lambda at: rx[0, at, :])
        y0 = net.put(q0, r0, me.over_y)
        by0.wait_recv()
        add(q1, every, lambda at: mine[c_x, at, b], lambda at: ry[0, at, :])
        x1 = net.put(q1, r1, me.over_x)
        yield 1
        ax1.wait_recv()
        by1.wait_recv()
        y0.wait_recv()
        x1.wait_recv()

        def final(r, carry):
            at = pl.ds(pl.multiple_of(r * step, step), step)
            left = mine[c_me, at, a].astype(F32) + rx[1, at, :].astype(F32) + r0[at, :].astype(F32)
            right = mine[c_me, at, b].astype(F32) + ry[1, at, :].astype(F32) + r1[at, :].astype(F32)
            last[at, a] = left.astype(BF)
            last[at, b] = right.astype(BF)
            return carry

        lax.fori_loop(0, rows // step, final, 0)
        waits = []
        for k in range(1, n_tp):
            to = pl.multiple_of(lax.rem(me.t + k, n_tp) * piece, piece)
            waits.append(net.put(last.at[pl.ds(to, piece)], got.at[k - 1], me.along(k)))
        yield 1
        for wait in waits:
            wait.wait_recv()
        for r in range(piece // step):
            at = pl.ds(pl.multiple_of(me.t * piece + r * step, step), step)
            total = last[at, :].astype(F32)
            for k in range(n_tp - 1):
                total = total + got[k, r * step : (r + 1) * step, :].astype(F32)
            out[r * step : (r + 1) * step, :] = total

    block = (rows, width)
    return Job(
        run,
        [(part, ANY)],
        [((piece, width), F32, VMEM)],
        [
            VMEM((4, *block), BF),
            VMEM((4, *block), BF),
            VMEM((2, rows, half), BF),
            VMEM((2, rows, half), BF),
            VMEM((rows, half), BF),
            VMEM((rows, half), BF),
            VMEM((rows, half), BF),
            VMEM((rows, half), BF),
            VMEM(block, BF),
            VMEM((n_tp - 1, piece, width), BF),
        ],
        10 + n_tp - 1,
        4,
        "xykz",
    )


def sum_everywhere(part, n_tp):
    def run(net, me, ins, outs, scratch):
        (src,), (out,) = ins, outs
        from_tp, mid, from_plane = scratch
        waits = [net.put(src, from_tp.at[k - 1], me.along(k)) for k in range(1, n_tp)]
        yield 1
        for wait in waits:
            wait.wait_recv()
        total = src[...]
        for k in range(n_tp - 1):
            total = total + from_tp[k]
        mid[...] = total
        waits = [net.put(mid, from_plane.at[i], me.flip(*f)) for i, f in enumerate(FLIPS)]
        yield 1
        yield 1
        for wait in waits:
            wait.wait_recv()
        total = mid[...]
        for i in range(7):
            total = total + from_plane[i]
        out[...] = total

    return Job(
        run,
        [(part, VMEM)],
        [(part.shape, F32, VMEM)],
        [VMEM((n_tp - 1, *part.shape), F32), VMEM(part.shape, F32), VMEM((7, *part.shape), F32)],
        n_tp - 1 + 7,
        0,
        "zp",
    )


def gather_rows(own, n_tp):
    piece, width = own.shape
    half = piece // 2

    def run(net, me, ins, outs, scratch):
        (src,), (out,), (bounce,) = ins, outs, scratch
        load = net.move(src, bounce)
        g_me = slot(me.s, me.c)
        chunks, cores = [], []

        def rows(p, which=None):
            if which is None:
                return out.at[g_me, pl.ds(pl.multiple_of(p * piece, piece), piece)]
            return out.at[g_me, pl.ds(pl.multiple_of(p * piece + which * half, half), half)]

        def spread(ref, p):
            dst = rows(p)
            chunks.append(
                (net.put(ref, dst, me.over_x), net.put(ref, dst, me.over_y), pl.multiple_of(p * piece, piece), piece)
            )
            cores.append(net.put(ref, dst, me.over_core))

        right, left = me.along(1), me.along(-1)
        p_left, p_right = lax.rem(me.t + 3, 4), lax.rem(me.t + 1, 4)
        far = lax.rem(me.t + 2, 4)
        to_right = net.put(src, rows(me.t), right)
        to_left = net.put(src, rows(me.t), left)
        spread(src, me.t)
        load.wait()
        store = net.move(bounce, rows(me.t))
        yield 1
        to_right.wait_recv()
        hop_right = net.put(rows(p_left, 0), rows(p_left, 0), right)
        spread(rows(p_left), p_left)
        to_left.wait_recv()
        hop_left = net.put(rows(p_right, 1), rows(p_right, 1), left)
        spread(rows(p_right), p_right)
        yield 1
        hop_right.wait_recv()
        hop_left.wait_recv()
        spread(rows(far), far)
        yield from relay_chunks(net, me, out, chunks)
        for core in cores:
            core.wait_recv()
        store.wait()

    return Job(
        run,
        [(own, ANY)],
        [((8, n_tp * piece, width), own.dtype, ANY)],
        [VMEM(own.shape, own.dtype)],
        4 * 7 + 4,
        2,
        "xykz",
    )


def wide_gather(own, n_tp):
    rows, width = own.shape
    qw = width // n_tp
    half = rows // 2

    def run(net, me, ins, outs, scratch):
        (src,), (out,), (bounce,) = ins, outs, scratch
        g_me = slot(me.s, me.c)
        g_x, g_y = slot(me.s, 1 - me.c), slot(lax.rem(me.s + 2, 4), me.c)
        g_d = slot(lax.rem(me.s + 2, 4), 1 - me.c)
        first = 1 - me.core
        relay_slot = first * g_x + me.core * g_y
        relay_to = me.flip(first, 0, me.core)

        def cols(p):
            return pl.ds(pl.multiple_of(p * qw, LANES), qw)

        def quarter(g, p):
            return out.at[g, :, cols(p)]

        def part(g, p, which):
            return out.at[g, pl.ds(which * half, half), cols(p)]

        load = net.move(src, bounce)
        from_x = net.put(src.at[:, cols(me.t)], quarter(g_me, me.t), me.over_x)
        from_y = net.put(src.at[:, cols(me.t)], quarter(g_me, me.t), me.over_y)
        cores = [net.put(src, out.at[g_me], me.over_core)]
        right, left = me.along(1), me.along(-1)
        p_left, p_right = lax.rem(me.t + 3, 4), lax.rem(me.t + 1, 4)
        yield 1
        load.wait()
        store = net.move(bounce, out.at[g_me])
        from_x.wait_recv()
        from_y.wait_recv()
        diag = net.put(quarter(relay_slot, me.t), quarter(relay_slot, me.t), relay_to)
        ring = []

        def along(g):
            piece = quarter(g, me.t)
            ring.append((g, net.put(piece, piece, right), net.put(piece, piece, left)))

        along(g_x)
        along(g_y)
        yield 1
        diag.wait_recv()
        along(g_d)
        yield 1
        hops = []
        for g, to_right, to_left in ring:
            to_right.wait_recv()
            hop_right = net.put(part(g, p_left, 0), part(g, p_left, 0), right)
            to_left.wait_recv()
            hops.append((g, hop_right, net.put(part(g, p_right, 1), part(g, p_right, 1), left)))
        yield 1
        for g, hop_right, hop_left in hops:
            hop_right.wait_recv()
            hop_left.wait_recv()
            cores.append(net.put(out.at[g], out.at[g], me.over_core))
        yield 1
        for core in cores:
            core.wait_recv()
        store.wait()

    return Job(
        run,
        [(own, ANY)],
        [((8, rows, width), own.dtype, ANY)],
        [VMEM(own.shape, own.dtype)],
        19,
        2,
        "xykz",
    )


class Wire:
    def __init__(self, net, build):
        self.net, self.build, self.i = net, build, len(net.all)
        net.all.append(self)

    def copy(self):
        src, dst, to = self.build()
        return pltpu.make_async_remote_copy(
            src_ref=src,
            dst_ref=dst,
            send_sem=self.net.send.at[self.i],
            recv_sem=self.net.recv.at[self.i],
            device_id=to,
            device_id_type=MESH,
        )

    def start(self):
        self.copy().start()

    def landed(self):
        self.copy().wait_recv()

    def sent(self):
        self.copy().wait_send()


class Wires:
    def __init__(self, send, recv):
        self.send, self.recv, self.all = send, recv, []

    def wire(self, build):
        return Wire(self, build)


class PlaneSum:
    def __init__(self, net, me, data, buffers, edge, chip, block, rows):
        self.data, self.rows, self.block, self.me, self.chip = data, rows, block, me, chip
        self.rc, self.rxa, self.ryb, self.q0, self.q1, self.r0, self.r1 = buffers
        self.width = data.shape[1]
        self.edge = edge
        self.a, self.b = pl.ds(0, edge), pl.ds(edge, self.width - edge)
        part = lambda ch, cols: data.at[block(ch, me.core), cols]
        self.cores = [
            net.wire(
                lambda k=k: (data.at[block(chip[k], 1 - me.core)], self.rc.at[k], me.over_core)
            )
            for k in range(4)
        ]
        self.ax0 = net.wire(lambda: (part(chip[3], self.a), self.rxa.at[0], me.over_x))
        self.by0 = net.wire(lambda: (part(chip[3], self.b), self.ryb.at[0], me.over_y))
        self.ax1 = net.wire(lambda: (part(chip[1], self.a), self.rxa.at[1], me.over_x))
        self.by1 = net.wire(lambda: (part(chip[2], self.b), self.ryb.at[1], me.over_y))
        self.y0 = net.wire(lambda: (self.q0, self.r0, me.over_y))
        self.x1 = net.wire(lambda: (self.q1, self.r1, me.over_x))

    def base(self, k):
        return (self.chip[k] * 2 + self.me.core) * self.rows

    def add(self, target, t_at, cols, left, right):
        def one(r, carry):
            total = left(r).astype(F32) + right(r).astype(F32)
            target[row_at(t_at, r), cols] = total.astype(BF)
            return carry

        lax.fori_loop(0, self.rows // STEP, one, 0)

    def sum_cores(self, k):
        base, every = self.base(k), pl.ds(0, self.width)
        self.cores[k].landed()
        self.add(
            self.data,
            base,
            every,
            lambda r: self.data[row_at(base, r), every],
            lambda r: self.rc[k, row_at(0, r), :],
        )

    def stage_two(self):
        over_y, over_x = self.base(2), self.base(1)
        self.ax0.landed()
        self.add(
            self.q0,
            0,
            pl.ds(0, self.edge),
            lambda r: self.data[row_at(over_y, r), self.a],
            lambda r: self.rxa[0, row_at(0, r), :],
        )
        self.y0.start()
        self.by0.landed()
        self.add(
            self.q1,
            0,
            pl.ds(0, self.width - self.edge),
            lambda r: self.data[row_at(over_x, r), self.b],
            lambda r: self.ryb[0, row_at(0, r), :],
        )
        self.x1.start()

    def finish(self, last):
        base = self.base(0)
        for wire in (self.ax1, self.by1, self.y0, self.x1):
            wire.landed()

        def final(r, carry):
            at, big = row_at(0, r), row_at(base, r)
            one = self.data[big, self.a].astype(F32) + self.rxa[1, at, :].astype(F32)
            last[at, self.a] = (one + self.r0[at, :].astype(F32)).astype(BF)
            two = self.data[big, self.b].astype(F32) + self.ryb[1, at, :].astype(F32)
            last[at, self.b] = (two + self.r1[at, :].astype(F32)).astype(BF)
            return carry

        lax.fori_loop(0, self.rows // STEP, final, 0)


def plane_sum_scratch(rows, width, edge):
    return [
        VMEM((4, rows, width), BF),
        VMEM((2, rows, edge), BF),
        VMEM((2, rows, width - edge), BF),
        VMEM((rows, edge), BF),
        VMEM((rows, width - edge), BF),
        VMEM((rows, edge), BF),
        VMEM((rows, width - edge), BF),
    ]


STEP = 16


def row_at(base, r):
    return pl.ds(pl.multiple_of(base + r * STEP, STEP), STEP)


def padded(count, to=LANES):
    return -(-count // to) * to


def feed_forward(
    two_own, mid_own, cot_block, gains, cot_all, routes_all, gate, up, down, sg_t, su_t, sd, router_t, attn, topk, n_tp
):
    piece, width = two_own.shape
    rows = piece * n_tp
    tokens = 8 * rows
    pack = width + LANES
    hid, hid_s = gate.shape[1], sg_t.shape[0]
    experts = router_t.shape[0]
    used = 2 * hid + hid_s
    H = padded(used)
    tile = H - LANES
    off = used - tile
    edge = width // 2
    part_w = width + LANES
    group = 2 * rows
    shard_w = width // 4
    attn_w = attn.shape[1]
    n_wires = 4 + 12 + 16 + 10 + 10 + (n_tp - 1) + 7 + 4
    n_col = 4
    col_w = width // n_col
    m_w = 256
    n_m = width // m_w

    def body(*refs):
        (two_ref, mid_ref, cot_own_ref, gain_ref) = refs[:4]
        (cot_ref, routes_ref, gate_ref, up_ref, down_ref, sg_ref, su_ref, sd_ref, wr_ref, attn_ref) = refs[4:14]
        (mid_out, gain_out, mid_pack, y_out, dg_out, du_out, dd_out, ds_out, n2_out, attn_out) = refs[14:24]
        (nb, cb, wgu, wd, gu, gut, hw, hwt, dnb, yb) = refs[24:34]
        two_buf, y_buf, (last, got, gus, dds, dss) = refs[34:41], refs[41:48], refs[48:53]
        send, recv, load, store = refs[53:]
        me = Place(n_tp)
        net = Wires(send, recv)

        def chip(dy, dx):
            return 2 * (me.y + dy * (1 - 2 * me.y)) + me.c + dx * (1 - 2 * me.c)

        def block(ch, core, p=None):
            start = ch * group + core * rows
            if p is None:
                return pl.ds(pl.multiple_of(start, rows), rows)
            return pl.ds(pl.multiple_of(start + p * piece, piece), piece)

        here = chip(0, 0)
        g_me = slot(me.s, me.c)
        pieces = [me.t, lax.rem(me.t + 3, 4), lax.rem(me.t + 1, 4), lax.rem(me.t + 2, 4)]
        half = piece // 2
        right, left = me.along(1), me.along(-1)

        def halves(p, which):
            start = here * group + me.core * rows + p * piece + which * half
            return nb.at[pl.ds(pl.multiple_of(start, half), half)]

        def mine(p):
            return nb.at[block(here, me.core, p)]

        z_r = net.wire(lambda: (two_ref, mine(me.t), right))
        z_l = net.wire(lambda: (two_ref, mine(me.t), left))
        hop_r = net.wire(lambda: (halves(pieces[1], 0), halves(pieces[1], 0), right))
        hop_l = net.wire(lambda: (halves(pieces[2], 1), halves(pieces[2], 1), left))
        to_x, to_y, to_c = [], [], []
        for j in range(4):
            src = (lambda: two_ref) if j == 0 else (lambda j=j: mine(pieces[j]))
            to_x.append(net.wire(lambda j=j, src=src: (src(), mine(pieces[j]), me.over_x)))
            to_y.append(net.wire(lambda j=j, src=src: (src(), mine(pieces[j]), me.over_y)))
            to_c.append(net.wire(lambda j=j, src=src: (src(), mine(pieces[j]), me.over_core)))
        chip_x, chip_y, chip_d = chip(0, 1), chip(1, 0), chip(1, 1)
        first = 1 - me.core
        relay_chip = first * chip_x + me.core * chip_y
        relay_to = me.flip(first, 0, me.core)
        relay, fwd_x, fwd_y, fwd_d = [], [], [], []
        for j in range(4):
            same = lambda ch, j=j: nb.at[block(ch, me.core, pieces[j])]
            relay.append(net.wire(lambda same=same: (same(relay_chip), same(relay_chip), relay_to)))
            fwd_x.append(net.wire(lambda same=same: (same(chip_x), same(chip_x), me.over_core)))
            fwd_y.append(net.wire(lambda same=same: (same(chip_y), same(chip_y), me.over_core)))
            fwd_d.append(net.wire(lambda same=same: (same(chip_d), same(chip_d), me.over_core)))

        g_x, g_y = slot(me.s, 1 - me.c), slot(lax.rem(me.s + 2, 4), me.c)
        g_d = slot(lax.rem(me.s + 2, 4), 1 - me.c)
        g_relay = first * g_x + me.core * g_y
        at_direct = [
            net.wire(lambda to=to: (attn_ref, attn_out.at[g_me], to))
            for to in (me.over_x, me.over_y, me.over_core)
        ]
        at_relay = net.wire(lambda: (attn_out.at[g_relay], attn_out.at[g_relay], relay_to))
        at_fwd = [
            net.wire(lambda g=g: (attn_out.at[g], attn_out.at[g], me.over_core)) for g in (g_x, g_y, g_d)
        ]

        chips = [here, chip_x, chip_y, chip_d]
        two_sum = PlaneSum(net, me, dnb, two_buf, edge, chips, block, rows)
        y_sum = PlaneSum(net, me, yb, y_buf, edge, chips, block, rows)
        z_w = []
        for k in range(1, n_tp):
            to = lax.rem(me.t + k, n_tp)
            z_w.append(
                net.wire(
                    lambda k=k, to=to: (
                        last.at[pl.ds(pl.multiple_of(to * piece, piece), piece)],
                        got.at[k - 1],
                        me.along(k),
                    )
                )
            )

        def packed(p, which=None):
            if which is None:
                return mid_pack.at[pl.ds(pl.multiple_of(p * piece, piece), piece)]
            return mid_pack.at[pl.ds(pl.multiple_of(p * piece + which * half, half), half)]

        m_r = net.wire(lambda: (packed(me.t), packed(me.t), right))
        m_l = net.wire(lambda: (packed(me.t), packed(me.t), left))
        m_hr = net.wire(lambda: (packed(pieces[1], 0), packed(pieces[1], 0), right))
        m_hl = net.wire(lambda: (packed(pieces[2], 1), packed(pieces[2], 1), left))

        moves = [
            (down_ref.at[0], wd.at[pl.ds(0, hid)]),
            (down_ref.at[1], wd.at[pl.ds(hid, hid)]),
            (sd_ref, wd.at[pl.ds(2 * hid, hid_s)]),
            (gate_ref.at[0], wgu.at[pl.ds(0, hid)]),
            (gate_ref.at[1], wgu.at[pl.ds(hid, hid)]),
            (sg_ref, wgu.at[pl.ds(2 * hid, hid_s)]),
            (wr_ref, wgu.at[pl.ds(used, experts)]),
            (up_ref.at[0], wgu.at[pl.ds(H, hid)]),
            (up_ref.at[1], wgu.at[pl.ds(H + hid, hid)]),
            (su_ref, wgu.at[pl.ds(H + 2 * hid, hid_s)]),
        ]
        for g in range(8):
            row = (2 * (g // 4) + g % 2) * group + (g % 4) // 2 * rows
            moves.append((cot_ref.at[g], cb.at[pl.ds(row, rows), pl.ds(0, width)]))
            moves.append((routes_ref.at[g], cb.at[pl.ds(row, rows), pl.ds(width, LANES)]))
        loads = [pltpu.make_async_copy(src, dst, load.at[i]) for i, (src, dst) in enumerate(moves)]
        for copy in loads:
            copy.start()
        greet(me.peers("xykzp"))
        for wire in (z_r, z_l, to_x[0], to_y[0], to_c[0]):
            wire.start()
        nb[block(here, me.core, me.t), :] = two_ref[...]
        wgu[used + experts : H, :] = jnp.zeros((H - used - experts, width), BF)
        wgu[H + used :, :] = jnp.zeros((H - used, width), BF)
        wd[used:, :] = jnp.zeros((H - used, width), BF)
        z_r.landed()
        hop_r.start()
        for wires in (to_x, to_y, to_c):
            wires[1].start()
        z_l.landed()
        hop_l.start()
        for wires in (to_x, to_y, to_c):
            wires[2].start()
        for copy in loads:
            copy.wait()
        hop_r.landed()
        hop_l.landed()
        for wires in (to_x, to_y, to_c):
            wires[3].start()
        for wire in to_c:
            wire.landed()

        lane = lax.broadcasted_iota(jnp.int32, (group, LANES), 1)
        unit = lax.broadcasted_iota(jnp.int32, (group, H), 1)
        e_first = g_me * 2

        def softmax_tile(logits, lanes):
            logits = jnp.where((lanes >= off) & (lanes < off + experts), logits, NEG)
            e = jnp.exp(logits - jnp.max(logits, axis=1, keepdims=True))
            return e / jnp.sum(e, axis=1, keepdims=True)

        def flip_chip(k):
            return chip(k // 2, lax.rem(k, 2))

        def hidden(k, carry):
            at = pl.ds(pl.multiple_of(flip_chip(k) * group, group), group)

            @pl.when(k == 1)
            def _():
                for j in range(4):
                    to_x[j].landed()
                    to_y[j].landed()
                    relay[j].start()
                    fwd_x[j].start()
                    fwd_y[j].start()
                for j in range(4):
                    fwd_x[j].landed()

            @pl.when(k == 2)
            def _():
                for j in range(4):
                    fwd_y[j].landed()

            @pl.when(k == 3)
            def _():
                for j in range(4):
                    relay[j].landed()
                    fwd_d[j].start()
                for wire in at_direct:
                    wire.start()
                for j in range(4):
                    fwd_d[j].landed()

            acts = dot_nt(nb[at, :], wgu[...])
            back = dot_nt(cb[at, 0:width], wd[...])
            probs = softmax_tile(acts[:, tile:H], lane)
            routed = cb[at, width : width + LANES].astype(F32)
            chosen, weight = [], []
            for j in range(2):
                expert = e_first + j
                hit = jnp.where((lane < topk) & (routed == expert.astype(F32)), 1.0, 0.0)
                chosen.append(jnp.max(hit, axis=1, keepdims=True))
                weight.append(
                    chosen[j]
                    * jnp.sum(jnp.where(lane == off + expert, probs, 0.0), axis=1, keepdims=True)
                )
            scale = jnp.where(unit < hid, weight[0], jnp.where(unit < 2 * hid, weight[1], 1.0))
            g, u = acts[:, :H], acts[:, H:]
            sig = 1.0 / (1.0 + jnp.exp(-g))
            silu = g * sig
            h = silu * u
            terms = h * back
            pg = jnp.zeros((group, LANES), F32)
            for j in range(2):
                own = (unit >= j * hid) & (unit < (j + 1) * hid)
                grad = chosen[j] * jnp.sum(jnp.where(own, terms, 0.0), axis=1, keepdims=True)
                high = grad.astype(BF).astype(F32)
                pg = jnp.where(lane == off + e_first + j, high, pg)
                pg = jnp.where(lane == off + e_first + j + LANES // 2, grad - high, pg)
            dnb[at, width:part_w] = pg.astype(BF)
            h = (h * scale).astype(BF)
            back = back * scale
            gate_grad = (back * u * (sig * (1.0 + g * (1.0 - sig)))).astype(BF)
            up_grad = (back * silu).astype(BF)
            hw[at, :] = h
            gu[at, 0:H] = gate_grad
            gu[at, H:] = up_grad
            hwt[:, at] = h.T
            gut[0:H, at] = gate_grad.T
            gut[H:, at] = up_grad.T
            return carry

        lax.fori_loop(0, 4, hidden, 0)

        cols_s = pl.ds(pl.multiple_of(me.s * shard_w, shard_w), shard_w)
        locals_ = []
        for g in range(8):
            row = (2 * (g // 4) + g % 2) * group + (g % 4) // 2 * rows
            locals_.append((nb.at[pl.ds(row, rows), cols_s], n2_out.at[g]))
        locals_.append((attn_ref, attn_out.at[g_me]))
        local_copies = [pltpu.make_async_copy(src, dst, store.at[i]) for i, (src, dst) in enumerate(locals_)]
        for copy in local_copies:
            copy.start()

        def normed_grad(i, carry):
            k = 3 - i
            at = pl.ds(pl.multiple_of(flip_chip(k) * group, group), group)

            def columns(n, carry):
                cols = pl.ds(pl.multiple_of(n * col_w, col_w), col_w)
                dnb[at, cols] = mdot(gu[at, :], wgu[:, cols]).astype(BF)
                return carry

            lax.fori_loop(0, n_col, columns, 0)
            for kk in range(4):

                @pl.when(k == kk)
                def _():
                    two_sum.cores[kk].start()
                    if kk < 3:
                        two_sum.sum_cores(kk + 1)
                    if kk == 2:
                        two_sum.ax0.start()
                        two_sum.by0.start()
                    if kk == 1:
                        two_sum.by1.start()
                    if kk == 0:
                        two_sum.ax1.start()

            return carry

        lax.fori_loop(0, 4, normed_grad, 0)

        def output(k, carry):
            at = pl.ds(pl.multiple_of(k * group, group), group)

            @pl.when(k == 1)
            def _():
                two_sum.sum_cores(0)
                two_sum.stage_two()

            def columns(n, carry):
                cols = pl.ds(pl.multiple_of(n * col_w, col_w), col_w)
                yb[at, cols] = mdot(hw[at, :], wd[:, cols]).astype(BF)
                return carry

            lax.fori_loop(0, n_col, columns, 0)
            return carry

        lax.fori_loop(0, 4, output, 0)
        two_sum.finish(last)
        for wire in z_w:
            wire.start()
        for wire in y_sum.cores:
            wire.start()

        def router_and_norm():
            for wire in z_w:
                wire.landed()
            total = last[pl.ds(pl.multiple_of(me.t * piece, piece), piece), :].astype(F32)
            for k in range(n_tp - 1):
                total = total + got[k].astype(F32)
            small = lax.broadcasted_iota(jnp.int32, (piece, LANES), 1)
            probs = softmax_tile(dot_nt(two_ref[...], wgu[tile:H, :]), small)
            pg = total[:, width:]
            pg = pg + pltpu.roll(pg, LANES // 2, 1)
            pg = jnp.where((small >= off) & (small < off + experts), pg, 0.0)
            logit_grad = (probs * (pg - jnp.sum(probs * pg, axis=1, keepdims=True))).astype(BF)
            grad = total[:, :width] + mdot(logit_grad, wgu[tile:H, :])
            value = mid_ref[...]
            back, terms = norm_back(value, gain_ref[1:2, :], grad)
            quarter = pl.ds(pl.multiple_of(me.t * piece, piece), piece)
            mid_grad = cot_own_ref[quarter, :] + back
            mid_out[...] = mid_grad
            gain_out[...] = jnp.sum(terms, axis=0, keepdims=True)
            at = pl.ds(pl.multiple_of(me.t * piece, piece), piece)
            mid_pack[at, 0:width] = mid_grad.astype(BF)
            mid_pack[at, width:] = logit_grad
            m_r.start()
            m_l.start()

        def stores(m, buf):
            cols = pl.ds(pl.multiple_of(m * m_w, m_w), m_w)
            made = []
            for j in range(2):
                at = pl.ds(j * hid, hid)
                made.append((gus.at[buf, at], dg_out.at[j, :, cols]))
                made.append((gus.at[buf, pl.ds(H + j * hid, hid)], du_out.at[j, :, cols]))
                made.append((dds.at[buf, at], dd_out.at[j, :, cols]))
            return [
                pltpu.make_async_copy(src, dst, store.at[14 + 6 * buf + i])
                for i, (src, dst) in enumerate(made)
            ]

        def weight_grad(m, carry):
            buf = lax.rem(m, 2)
            cols = pl.ds(pl.multiple_of(m * m_w, m_w), m_w)

            @pl.when(m >= 2)
            def _():
                for bb in range(2):

                    @pl.when(buf == bb)
                    def _():
                        for copy in stores(m - 2, bb):
                            copy.wait()

            @pl.when(m == 1)
            def _():
                for k in range(4):
                    y_sum.sum_cores(k)
                for wire in (y_sum.ax0, y_sum.by0, y_sum.ax1, y_sum.by1):
                    wire.start()
                at_direct[0].landed()
                at_direct[1].landed()
                for wire in (at_relay, at_fwd[0], at_fwd[1]):
                    wire.start()

            @pl.when(m == 5)
            def _():
                router_and_norm()

            @pl.when(m == 6)
            def _():
                y_sum.stage_two()
                at_relay.landed()
                at_fwd[2].start()

            both = mdot(gut[...], nb[:, cols])
            gus[buf] = both.astype(BF)
            dss[0, :, cols] = both[2 * hid : used].astype(BF)
            dss[1, :, cols] = both[H + 2 * hid : H + used].astype(BF)
            third = mdot(hwt[...], cb[:, cols])
            dds[buf] = third.astype(BF)
            dss[2, :, cols] = third[2 * hid : used].astype(BF)
            for bb in range(2):

                @pl.when(buf == bb)
                def _():
                    for copy in stores(m, bb):
                        copy.start()

            return carry

        lax.fori_loop(0, n_m, weight_grad, 0)
        m_r.landed()
        m_hr.start()
        m_l.landed()
        m_hl.start()
        y_sum.finish(y_out)
        ds_copy = pltpu.make_async_copy(dss, ds_out, store.at[13])
        ds_copy.start()
        for m in (n_m - 2, n_m - 1):
            for copy in stores(m, m % 2):
                copy.wait()
        for wire in [at_direct[2], *at_fwd, m_hr, m_hl]:
            wire.landed()
        for copy in local_copies:
            copy.wait()
        ds_copy.wait()
        for wire in net.all:
            wire.sent()

    ins = (
        two_own, mid_own, cot_block, gains,
        cot_all, routes_all, gate, up, down, sg_t, su_t, sd, router_t, attn,
    )
    outs = [
        ((piece, width), F32),
        ((1, width), F32),
        ((rows, part_w), BF),
        ((rows, width), BF),
        (gate.shape, BF),
        (up.shape, BF),
        (down.shape, BF),
        ((3, hid_s, width), BF),
        ((8, rows, shard_w), BF),
        ((8, rows, attn_w), BF),
    ]
    scratch = [
        VMEM((tokens, width), BF),
        VMEM((tokens, pack), BF),
        VMEM((2 * H, width), BF),
        VMEM((H, width), BF),
        VMEM((tokens, 2 * H), BF),
        VMEM((2 * H, tokens), BF),
        VMEM((tokens, H), BF),
        VMEM((H, tokens), BF),
        VMEM((tokens, part_w), BF),
        VMEM((tokens, width), BF),
        *plane_sum_scratch(rows, part_w, edge),
        *plane_sum_scratch(rows, width, edge),
        VMEM((rows, part_w), BF),
        VMEM((n_tp - 1, piece, part_w), BF),
        VMEM((2, 2 * H, m_w), BF),
        VMEM((2, H, m_w), BF),
        VMEM((3, hid_s, width), BF),
    ]
    return pl.pallas_call(
        body,
        out_shape=tuple(jax.ShapeDtypeStruct(*o) for o in outs),
        in_specs=[pl.BlockSpec(memory_space=VMEM)] * 4 + [pl.BlockSpec(memory_space=ANY)] * 10,
        out_specs=(*[pl.BlockSpec(memory_space=VMEM)] * 4, *[pl.BlockSpec(memory_space=ANY)] * 6),
        scratch_shapes=[
            *scratch,
            pltpu.SemaphoreType.DMA((n_wires,)),
            pltpu.SemaphoreType.DMA((n_wires,)),
            pltpu.SemaphoreType.DMA((26,)),
            pltpu.SemaphoreType.DMA((26,)),
        ],
        compiler_params=pltpu.CompilerParams(
            collective_id=4, has_side_effects=True, vmem_limit_bytes=67 * 10**6
        ),
        name="feed_forward",
    )(*ins)


class Background:
    def __init__(self):
        self.runs = []

    def add(self, run):
        next(run)
        self.runs.append(run)

    def step(self):
        self.runs = [r for r in self.runs if next(r, None) is not None]

    def drain(self):
        while self.runs:
            self.step()


def fold_heads(a, b, lane):
    def fold(v):
        v = v + pltpu.roll(v, 64, 1)
        return v + pltpu.roll(v, 32, 1)

    return jnp.where(lane < DR // 2, fold(a), jnp.where(lane < DR, fold(b), 0.0))


def attention_back(
    mid_pack, attn, prob, kv, keys_rope, q_nope, q_rope, tables, compressed, gains_in, rows_in, y_part, shared_grads,
    w_output, w_expand, w_query, w_latent_t, gain_two_sum, n_tp,
):
    rows, part_w = mid_pack.shape
    width = w_output.shape[1]
    piece = rows // n_tp
    n_head = prob.shape[0]
    nope_w = n_head * DN
    q_w = nope_w + 2 * LANES
    kv_w = kv.shape[1]
    lat_w = 5 * LANES
    back_w = width + KVR + LANES
    scale = (DN + DR) ** (-0.5)
    f32 = lambda *shape: jax.ShapeDtypeStruct(shape, F32)
    bf = lambda *shape: jax.ShapeDtypeStruct(shape, BF)
    subs = dict(
        y=tp_reduce_scatter(bf(rows, width), n_tp),
        mid=plane_columns(bf(rows, width)),
        logit=plane_gather(bf(rows, part_w - width), 1),
        shared0=plane_columns(bf(*shared_grads.shape[1:])),
        shared1=plane_columns(bf(*shared_grads.shape[1:])),
        shared2=plane_columns(bf(*shared_grads.shape[1:])),
        head=plane_gather(bf(rows, q_w + kv_w)),
        back=tp_reduce_scatter(bf(rows, width), n_tp),
        back2=tp_reduce_scatter(bf(rows, back_w - width), n_tp),
        out=tp_all_gather(bf(piece, width), n_tp),
        inp=tp_all_gather(bf(piece, width), n_tp),
        lat=gather_rows(bf(piece, lat_w), n_tp),
        gain=sum_everywhere(f32(16, 512), n_tp),
    )
    own_scratch = [
        VMEM(w_output.shape, BF),
        VMEM(w_expand.shape, BF),
        VMEM(w_query.shape, BF),
        VMEM((lat_w, width), BF),
        VMEM((rows, nope_w), BF),
        VMEM((2 * rows, kv_w + LANES), F32),
        VMEM((rows, kv_w + LANES), BF),
        VMEM((rows, kv_w + LANES), BF),
        VMEM((rows, q_w + kv_w), BF),
        VMEM((rows, width), BF),
        VMEM((rows, back_w - width), BF),
        VMEM((piece, width), F32),
        VMEM((piece, width), F32),
        VMEM((piece, back_w - width), F32),
        VMEM((piece, width), BF),
        VMEM((piece, width), BF),
        VMEM((piece, lat_w), BF),
        VMEM((16, 512), F32),
    ]
    at, sub_at = len(own_scratch), {}
    for key, job in subs.items():
        sub_at[key] = (at, at + len(job.scratch))
        at += len(job.scratch)

    def run(net, me, ins, outs, scratch):
        (mid_ref, attn_ref, prob_ref, kv_ref, ka_ref, kb_ref, qn_ref, qa_ref, qb_ref, cos_ref, sin_ref) = ins[:11]
        (comp_ref, gains_ref, x_ref, mg_ref, m_ref, y_ref, gt_ref) = ins[11:18]
        (ds_ref, wo_ref, we_ref, wq_ref, wl_ref) = ins[18:]
        quarter = pl.ds(pl.multiple_of(me.t * piece, piece), piece)
        (block_out, input_out, gain_out, mid_out, logit_out, sg_out, su_out, sd_out, head_out, lat_out) = outs
        (wo, we, wq, wl, ogb, terms, swap_src, swap_got, head, part, part2) = scratch[:11]
        (y32, back32, back2, ob, ib, lat, gains) = scratch[11:18]

        def sub(key, src, dst):
            a, b = sub_at[key]
            return subs[key].run(net, me, (src,), (dst,), scratch[a:b])

        loads = [
            net.move(wo_ref, wo),
            net.move(we_ref, we),
            net.move(wq_ref, wq),
            net.move(wl_ref, wl.at[pl.ds(0, KVR + DR)]),
        ]
        bg = Background()
        y_run = sub("y", y_ref, y32)
        next(y_run)
        bg.add(sub("shared0", ds_ref.at[0], sg_out))
        wl[KVR + DR :, :] = jnp.zeros((lat_w - KVR - DR, width), BF)
        lane = lax.broadcasted_iota(jnp.int32, (rows, LANES), 1)
        lane2 = lax.broadcasted_iota(jnp.int32, (2 * rows, LANES), 1)

        loads[0].wait()
        out_grad = dot_nt(mid_ref[:, 0:width], wo[...])
        ogb[...] = out_grad.astype(BF)
        weighted = out_grad * attn_ref[...].astype(F32)
        dqa = jnp.zeros((rows, LANES), F32)
        dqb, dka, dkb = dqa, jnp.zeros((2 * rows, LANES), F32), jnp.zeros((2 * rows, LANES), F32)
        for h in range(n_head):
            mine = (lane >= h * (DR // 2)) & (lane < (h + 1) * (DR // 2))
            k_at, v_at = pl.ds(h * (DN + DV), DN), pl.ds(h * (DN + DV) + DN, DV)
            og_h = ogb[:, h * DV : (h + 1) * DV]
            p = prob_ref[h]
            delta = jnp.sum(weighted[:, h * DV : (h + 1) * DV], axis=1, keepdims=True)
            ds = (p * (dot_nt(og_h, kv_ref[:, v_at]) - delta)).astype(BF)
            head[:, h * DN : (h + 1) * DN] = (mdot(ds, kv_ref[:, k_at]) * scale).astype(BF)
            dqa = dqa + jnp.where(mine, mdot(ds, ka_ref[...]), 0.0)
            dqb = dqb + jnp.where(mine, mdot(ds, kb_ref[...]), 0.0)
            terms[:, k_at] = dot_tn(ds, qn_ref[:, h * DN : (h + 1) * DN]) * scale
            terms[:, v_at] = dot_tn(p.astype(BF), og_h)
            zero = jnp.zeros((), BF)
            dka = dka + dot_tn(ds, jnp.where(mine, qa_ref[...], zero))
            dkb = dkb + dot_tn(ds, jnp.where(mine, qb_ref[...], zero))
        terms[:, kv_w:] = fold_heads(dka * scale, dkb * scale, lane2)
        theirs = pl.ds(pl.multiple_of((1 - me.c) * rows, rows), rows)
        swap_src[...] = terms[theirs, :].astype(BF)
        swap = net.put(swap_src, swap_got, me.over_x)
        bg.add(sub("shared1", ds_ref.at[1], su_out))
        dqa, dqb = dqa * scale, dqb * scale
        ours = pl.ds(pl.multiple_of(me.c * rows, rows), rows)
        cos, sin = cos_ref[ours, :], sin_ref[ours, :]
        head[:, nope_w : nope_w + LANES] = (dqa * cos + dqb * sin).astype(BF)
        head[:, nope_w + LANES : q_w] = (dqb * cos - dqa * sin).astype(BF)
        next(y_run, None)
        ob[...] = (m_ref[...] + y32[...]).astype(BF)
        yield 1
        for load in loads[1:]:
            load.wait()
        n_col = 4
        col_w = width // n_col

        def columns(n, carry):
            cols = pl.ds(pl.multiple_of(n * col_w, col_w), col_w)
            part[:, cols] = dot_nt(head[:, 0:q_w], wq[cols, :]).astype(BF)
            return carry

        lax.fori_loop(0, n_col, columns, 0)
        back_run = sub("back", part, back32)
        next(back_run)
        swap.wait_recv()
        head[:, q_w:] = (terms[ours, 0:kv_w] + swap_got[:, 0:kv_w].astype(F32)).astype(BF)
        rope = terms[ours, kv_w:] + swap_got[:, kv_w:].astype(F32)
        part2[:, 0:KVR] = dot_nt(head[:, q_w:], we[...]).astype(BF)
        turned = jnp.where(
            lane < DR // 2,
            rope * cos + pltpu.roll(rope, LANES - DR // 2, 1) * sin,
            jnp.where(lane < DR, rope * cos - pltpu.roll(rope, DR // 2, 1) * sin, 0.0),
        )
        part2[:, KVR:] = turned.astype(BF)
        back_run2 = sub("back2", part2, back2)
        next(back_run2)
        bg.add(sub("head", head, head_out))
        bg.add(sub("shared2", ds_ref.at[2], sd_out))
        bg.add(sub("out", ob, block_out))
        next(back_run, None)
        next(back_run2, None)
        comp_grad, gk = norm_back(comp_ref[...], gains_ref[2:3, 0:KVR], back2[:, 0:KVR])
        lat[:, 0:KVR] = comp_grad.astype(BF)
        lat[:, KVR:] = back2[:, KVR:].astype(BF)
        one_grad = back32[...] + mdot(lat[...], wl[...])
        lat_run = sub("lat", lat, lat_out)
        next(lat_run)
        norm_grad, g1 = norm_back(x_ref[quarter, :].astype(F32), gains_ref[0:1, :], one_grad)
        ib[...] = (mg_ref[...] + norm_grad).astype(BF)
        bg.add(sub("inp", ib, input_out))
        gains[...] = jnp.zeros_like(gains)
        g1 = jnp.sum(g1, axis=0, keepdims=True)
        for i in range(4):
            gains[i : i + 1, :] = g1[:, i * 512 : (i + 1) * 512]
            gains[4 + i : 5 + i, :] = gt_ref[:, i * 512 : (i + 1) * 512]
        gains[8:9, :] = jnp.sum(gk, axis=0, keepdims=True)
        bg.add(sub("gain", gains, gain_out))
        bg.add(sub("mid", mid_ref.at[:, pl.ds(0, width)], mid_out))
        bg.add(sub("logit", mid_ref.at[:, pl.ds(width, part_w - width)], logit_out))
        bg.add(lat_run)
        bg.drain()

    spaces = [VMEM] * 18 + [ANY] * 5
    ins = (
        mid_pack, attn, prob, kv, *keys_rope, q_nope, *q_rope, *tables,
        compressed, gains_in, *rows_in, y_part, gain_two_sum,
        shared_grads, w_output, w_expand, w_query, w_latent_t,
    )
    outs = [
        ((rows, width), BF, VMEM),
        ((rows, width), BF, VMEM),
        ((16, 512), F32, VMEM),
        *subs["mid"].outs,
        *subs["logit"].outs,
        *subs["shared0"].outs,
        *subs["shared1"].outs,
        *subs["shared2"].outs,
        *subs["head"].outs,
        *subs["lat"].outs,
    ]
    return Job(
        run,
        list(zip(ins, spaces)),
        outs,
        own_scratch + [s for job in subs.values() for s in job.scratch],
        1 + sum(job.n_put for job in subs.values()),
        4 + sum(job.n_local for job in subs.values()),
        "xykzp",
    )


def attention_forward(
    block, tables, w_query, w_latent_t, w_expand, w_output, router_t, small, cot, routes, shared, n_tp
):
    rows, width = block.shape
    piece = rows // n_tp
    q_w = w_query.shape[1]
    nope_w = q_w - 2 * LANES
    n_head = nope_w // DN
    kv_w = w_expand.shape[1]
    lat_rows = w_latent_t.shape[0]
    lat_pad = padded(lat_rows)
    scale = (DN + DR) ** (-0.5)
    k_w, e_w = w_query.shape[0], w_expand.shape[0]
    shard_w = w_output.shape[1]
    f32 = lambda *shape: jax.ShapeDtypeStruct(shape, F32)
    bf = lambda *shape: jax.ShapeDtypeStruct(shape, BF)
    subs = dict(
        cot=wide_gather(cot, n_tp),
        routes=plane_gather(routes, 1),
        one=plane_columns(bf(rows, width)),
        lat=plane_columns(bf(rows, KVR)),
        sg=shard_rows(shared[0]),
        su=shard_rows(shared[1]),
        sd=shard_rows(shared[2]),
        rs=tp_reduce_scatter(bf(rows, width), n_tp),
    )
    own_scratch = [
        VMEM((4 * k_w, q_w), BF),
        VMEM((lat_pad, width), BF),
        VMEM((4 * e_w, kv_w), BF),
        VMEM((w_output.shape[0], width), BF),
        VMEM((router_t.shape[0], width), BF),
        VMEM((4, *small.shape), F32),
        VMEM((rows, width), BF),
        VMEM((2 * rows, width), BF),
        VMEM((2 * rows, KVR), F32),
        VMEM((2 * rows, KVR), BF),
        VMEM((rows, width), BF),
        VMEM((piece, width), F32),
    ]
    at, sub_at = len(own_scratch), {}
    for key, job in subs.items():
        sub_at[key] = (at, at + len(job.scratch))
        at += len(job.scratch)

    def run(net, me, ins, outs, scratch):
        x_ref, cos_ref, sin_ref = ins[:3]
        wq_in, wl_in, we_in, wo_in, rt_in, small_in, cot_in, routes_in = ins[3:11]
        shared_in = ins[11:14]
        (mid_out, two_out, attn_out, prob_out, kv_out, ka_out, kb_out, qn_out, qa_out, qb_out) = outs[:10]
        comp_out, gain_out = outs[10:12]
        weights_out, (cot_out, routes_out, one_out, latn_out), shared_out = outs[12:17], outs[17:21], outs[21:24]
        (wq, wl, we, wo, rt, small_all, xo, n1, lat32, ln, part, res) = scratch[:12]

        def sub(key, src, dst):
            a, b = sub_at[key]
            return subs[key].run(net, me, (src,), (dst,), scratch[a:b])

        other = lax.rem(me.s + 2, 4)

        def stacked(ref, size):
            def place(s, which=None):
                if which is None:
                    return ref.at[pl.ds(pl.multiple_of(s * size, size), size)]
                half = size // 2
                return ref.at[pl.ds(pl.multiple_of(s * size + which * half, half), half)]

            return place

        def beside(ref, count):
            def place(s, which=None):
                cols = pl.ds(pl.multiple_of(s * shard_w, shard_w), shard_w)
                if which is None:
                    return ref.at[pl.ds(0, count), cols]
                half = count // 2
                return ref.at[pl.ds(pl.multiple_of(which * half, half), half), cols]

            return place

        halved = [
            (wq_in, k_w, stacked(wq, k_w)),
            (wl_in, lat_rows, beside(wl, lat_rows)),
            (we_in, e_w, stacked(we, e_w)),
        ]
        whole = [
            (small_in, lambda s: small_all.at[s]),
            (wo_in, beside(wo, w_output.shape[0])),
            (rt_in, beside(rt, router_t.shape[0])),
        ]
        local = [net.move(ref, place(me.s)) for ref, _, place in halved]
        local += [net.move(ref, place(me.s)) for ref, place in whole]
        whole_y = [net.put(small_in, small_all.at[me.s], me.over_y)]
        whole_c = [net.put(small_in, small_all.at[me.s], me.over_core)]
        half_y, half_c = [], []
        bg = Background()
        for i, (ref, count, place) in enumerate(halved):
            rows_c = pl.ds(pl.multiple_of(me.c * (count // 2), count // 2), count // 2)
            half_y.append(net.put(ref.at[rows_c], place(me.s, me.c), me.over_y))
            if i == 0:
                x_wire = net.put(x_ref, xo, me.over_x)
            half_c.append(net.put(ref, place(me.s), me.over_core))
            if i == 0:
                cot_run = sub("cot", cot_in, cot_out)
                next(cot_run)
        for ref, place in whole[1:]:
            whole_y.append(net.put(ref, place(me.s), me.over_y))
            whole_c.append(net.put(ref, place(me.s), me.over_core))
        wl[lat_rows:, :] = jnp.zeros((lat_pad - lat_rows, width), BF)

        whole_y[0].wait_recv()
        fwd = [net.put(small_all.at[other], small_all.at[other], me.over_core)]
        whole_c[0].wait_recv()
        fwd[0].wait_recv()
        local[3].wait()
        gain_out[...] = jnp.zeros_like(gain_out)
        for s in range(4):
            for i in range(4):
                cols = pl.ds((4 * s + i) * LANES, LANES)
                gain_out[0:1, cols] = small_all[s, i : i + 1, :]
                gain_out[1:2, cols] = small_all[s, 4 + i : 5 + i, :]
            gain_out[2:3, s * LANES : (s + 1) * LANES] = small_all[s, 8:9, :]

        def norm_rows_into(src, base):
            def one(r, carry):
                v = src[row_at(0, r), :].astype(F32)
                n1[row_at(base, r), :] = norm_rows(v, gain_out[0:1, :]).astype(BF)
                return carry

            lax.fori_loop(0, rows // STEP, one, 0)

        ours, theirs = me.c * rows, (1 - me.c) * rows
        norm_rows_into(x_ref, ours)
        at_us = pl.ds(pl.multiple_of(ours, rows), rows)
        half_x, relays = [], []
        for i, (got, (_, _, place)) in enumerate(zip(half_y, halved)):
            got.wait_recv()
            if i == 2:
                next(cot_run)
            piece_ref = place(other, me.c)
            half_x.append(net.put(piece_ref, piece_ref, me.over_x))
            relays.append(net.put(piece_ref, piece_ref, me.over_core))
        x_wire.wait_recv()
        norm_rows_into(xo, theirs)
        next(cot_run)
        for got, (_, place) in zip(whole_y[1:], whole[1:]):
            got.wait_recv()
            relays.append(net.put(place(other), place(other), me.over_core))
        for got, (_, _, place) in zip(half_x, halved):
            got.wait_recv()
            piece_ref = place(other, 1 - me.c)
            relays.append(net.put(piece_ref, piece_ref, me.over_core))
        bg.add(sub("routes", routes_in, routes_out))
        bg.add(sub("one", n1.at[at_us], one_out))
        for key, src, dst in zip(("sg", "su", "sd"), shared_in, shared_out):
            bg.add(sub(key, src, dst))
        for got in half_c + whole_c[1:] + relays:
            got.wait_recv()
        for copy in local[:3] + local[4:]:
            copy.wait()
        stores = [
            net.move(src, dst)
            for src, dst in zip((wq, wl.at[pl.ds(0, lat_rows)], we, wo, rt), weights_out)
        ]

        lane = lax.broadcasted_iota(jnp.int32, (rows, LANES), 1)
        lane2 = lax.broadcasted_iota(jnp.int32, (2 * rows, LANES), 1)
        query = mdot(n1[at_us, :], wq[...])
        cos, sin = cos_ref[at_us, :], sin_ref[at_us, :]
        a, b = query[:, nope_w : nope_w + LANES], query[:, nope_w + LANES :]
        qn_out[...] = query[:, :nope_w].astype(BF)
        qa_out[...] = (a * cos - b * sin).astype(BF)
        qb_out[...] = (a * sin + b * cos).astype(BF)
        latent = dot_nt(n1[...], wl[...])
        lat32[...] = latent[:, :KVR]
        ln[...] = norm_rows(latent[:, :KVR], gain_out[2:3, 0:KVR]).astype(BF)
        bg.add(sub("lat", ln.at[at_us], latn_out))
        comp_out[...] = lat32[pl.ds(pl.multiple_of(ours + me.t * piece, piece), piece), :]

        def spread_heads(v):
            v = jnp.where(lane2 < DR // 2, v, 0.0)
            v = v + pltpu.roll(v, DR // 2, 1)
            return v + pltpu.roll(v, DR, 1)

        tile = latent[:, KVR:]
        a, b = spread_heads(tile), spread_heads(pltpu.roll(tile, LANES - DR // 2, 1))
        ka_out[...] = (a * cos_ref[...] - b * sin_ref[...]).astype(BF)
        kb_out[...] = (a * sin_ref[...] + b * cos_ref[...]).astype(BF)
        kv_out[...] = mdot(ln[...], we[...]).astype(BF)
        next(cot_run)
        q_pos = ours + lax.broadcasted_iota(jnp.int32, (rows, 2 * rows), 0)
        k_pos = lax.broadcasted_iota(jnp.int32, (rows, 2 * rows), 1)
        zero = jnp.zeros((), BF)
        for h in range(n_head):
            mine = (lane >= h * (DR // 2)) & (lane < (h + 1) * (DR // 2))
            k_at, v_at = pl.ds(h * (DN + DV), DN), pl.ds(h * (DN + DV) + DN, DV)
            score = dot_nt(qn_out[:, h * DN : (h + 1) * DN], kv_out[:, k_at])
            score = score + dot_nt(jnp.where(mine, qa_out[...], zero), ka_out[...])
            score = score + dot_nt(jnp.where(mine, qb_out[...], zero), kb_out[...])
            score = jnp.where(k_pos <= q_pos, score * scale, NEG)
            top = jnp.max(score, axis=1, keepdims=True)
            expo = jnp.exp(score - top)
            total = jnp.sum(expo, axis=1, keepdims=True)
            value = mdot(expo.astype(BF), kv_out[:, v_at])
            attn_out[:, h * DV : (h + 1) * DV] = (value / total).astype(BF)
            prob_out[h] = jnp.exp(score - (top + jnp.log(total)))
        n_col = 4
        col_w = width // n_col

        def columns(n, carry):
            cols = pl.ds(pl.multiple_of(n * col_w, col_w), col_w)
            part[:, cols] = mdot(attn_out[...], wo[:, cols]).astype(BF)
            return carry

        lax.fori_loop(0, n_col, columns, 0)
        rs = sub("rs", part, res)
        next(rs)
        yield 1
        next(cot_run)
        bg.runs.append(cot_run)
        next(rs, None)
        quarter = pl.ds(pl.multiple_of(me.t * piece, piece), piece)
        mid = x_ref[quarter, :].astype(F32) + res[...]
        mid_out[...] = mid
        two_out[...] = norm_rows(mid, gain_out[1:2, :]).astype(BF)
        bg.drain()
        for store in stores:
            store.wait()

    ins = (
        block, *tables,
        w_query, w_latent_t, w_expand, w_output, router_t, small, cot, routes, *shared,
    )
    outs = [
        ((piece, width), F32, VMEM),
        ((piece, width), BF, VMEM),
        ((rows, n_head * DV), BF, VMEM),
        ((n_head, rows, 2 * rows), F32, VMEM),
        ((2 * rows, kv_w), BF, VMEM),
        ((2 * rows, LANES), BF, VMEM),
        ((2 * rows, LANES), BF, VMEM),
        ((rows, nope_w), BF, VMEM),
        ((rows, LANES), BF, VMEM),
        ((rows, LANES), BF, VMEM),
        ((piece, KVR), F32, VMEM),
        ((8, width), F32, VMEM),
        ((4 * k_w, q_w), BF, ANY),
        ((lat_rows, width), BF, ANY),
        ((4 * e_w, kv_w), BF, ANY),
        ((w_output.shape[0], width), BF, ANY),
        ((router_t.shape[0], width), BF, ANY),
        *subs["cot"].outs,
        *subs["routes"].outs,
        *subs["one"].outs,
        *subs["lat"].outs,
        *subs["sg"].outs,
        *subs["su"].outs,
        *subs["sd"].outs,
    ]
    return Job(
        run,
        list(zip(ins, [VMEM] * 3 + [ANY] * 11)),
        outs,
        own_scratch + [s for job in subs.values() for s in job.scratch],
        25 + sum(job.n_put for job in subs.values()),
        11 + sum(job.n_local for job in subs.values()),
        "xykzp",
    )


def weight_grads(one, head, lat, lat_cols, attn, mid, logit, two, plain, heads, lat_rows, first_logit, experts):
    tokens, shard_w = one.shape
    q_w = heads * (DN + DR)
    kv_w = head.shape[1] - q_w
    mats = (one, head, lat, lat_cols, attn, mid, logit, two)
    n_in, n_plain = len(mats) + len(plain), len(plain)
    outs = [
        (shard_w, q_w),
        (lat_rows, shard_w),
        (lat_cols.shape[1], kv_w),
        (attn.shape[1], shard_w),
        (experts, shard_w),
        *[p.shape for p in plain],
    ]

    def body(*refs):
        srcs, dsts = refs[:n_in], refs[n_in : n_in + len(outs)]
        held = refs[n_in + len(outs) : 2 * n_in + len(outs)]
        made = refs[2 * n_in + len(outs) : 2 * n_in + 2 * len(outs)]
        load, store = refs[2 * n_in + 2 * len(outs) :]
        loads = [pltpu.make_async_copy(s, h, load.at[i]) for i, (s, h) in enumerate(zip(srcs, held))]
        stores = [pltpu.make_async_copy(m, d, store.at[i]) for i, (m, d) in enumerate(zip(made, dsts))]
        order = list(range(len(mats), n_in)) + list(range(len(mats)))
        for i in order:
            loads[i].start()

        def widen(src, dst, count, step):
            def one_step(r, carry):
                at = pl.ds(pl.multiple_of(r * step, step), step)
                dst[at, :] = src[at, :].astype(F32)
                return carry

            lax.fori_loop(0, count // step, one_step, 0)

        for i in range(n_plain):
            src, dst = held[len(mats) + i], made[5 + i]
            loads[len(mats) + i].wait()
            if len(src.shape) == 2:
                widen(src, dst, src.shape[0], STEP)
            else:
                for j in range(src.shape[0]):
                    count = src.shape[1]
                    widen(src.at[j], dst.at[j], count, 32 if count % 32 == 0 else 8)
            stores[5 + i].start()
        (one_v, head_v, lat_v, lc_v, attn_v, mid_v, logit_v, two_v) = held[: len(mats)]
        for i in range(len(mats)):
            loads[i].wait()
        col = lax.broadcasted_iota(jnp.int32, (q_w, q_w), 1)
        row = lax.broadcasted_iota(jnp.int32, (q_w, q_w), 0)
        source = col
        for h in range(heads):
            r = col - h * (DN + DR)
            mine = jnp.where(
                r < DN,
                h * DN + r,
                jnp.where(
                    r < DN + DR // 2,
                    heads * DN + h * (DR // 2) + r - DN,
                    heads * DN + LANES + h * (DR // 2) + r - DN - DR // 2,
                ),
            )
            source = jnp.where((r >= 0) & (r < DN + DR), mine, source)
        turn = jnp.where(row == source, 1.0, 0.0).astype(BF)
        dq = mdot(head_v[:, 0:q_w], turn).astype(BF)
        made[0][...] = dot_tn(one_v[...], dq)
        stores[0].start()
        made[1][...] = dot_tn(lat_v[...], one_v[...])[0:lat_rows]
        stores[1].start()
        made[2][...] = dot_tn(lc_v[...], head_v[:, q_w:])
        stores[2].start()
        made[3][...] = dot_tn(attn_v[...], mid_v[...])
        stores[3].start()
        made[4][...] = dot_tn(logit_v[...], two_v[...])[first_logit : first_logit + experts]
        for copy in [stores[4]]:
            copy.start()
        for copy in stores:
            copy.wait()

    return pl.pallas_call(
        body,
        out_shape=tuple(jax.ShapeDtypeStruct(o, F32) for o in outs),
        in_specs=[pl.BlockSpec(memory_space=ANY)] * n_in,
        out_specs=tuple(pl.BlockSpec(memory_space=ANY) for _ in outs),
        scratch_shapes=[
            *[VMEM(a.shape, a.dtype) for a in (*mats, *plain)],
            *[VMEM(o, F32) for o in outs],
            pltpu.SemaphoreType.DMA((n_in,)),
            pltpu.SemaphoreType.DMA((len(outs),)),
        ],
        compiler_params=pltpu.CompilerParams(vmem_limit_bytes=67 * 10**6),
        name="weight_grads",
    )(*mats, *plain)


def per_device(
    block_input,
    norm1_gain,
    q_weight,
    kva_weight,
    kv_norm_gain,
    kvb_weight,
    out_weight,
    norm2_gain,
    router_weight,
    shared_gate,
    shared_up,
    shared_down,
    expert_gate,
    expert_up,
    expert_down,
    routes,
    cotangent,
):
    n_tp = lax.axis_size(TP)
    rows, width = block_input.shape
    topk = routes.shape[1]
    experts = router_weight.shape[1]
    heads = q_weight.shape[1] // (DN + DR)
    s_id = lax.axis_index(SHARD)
    shard_w = width // 4
    kv_w = KVR // 4

    by_head = q_weight.reshape(-1, heads, DN + DR)
    q_weight = jnp.concatenate(
        [
            by_head[:, :, :DN].reshape(-1, heads * DN),
            by_head[:, :, DN : DN + DR // 2].reshape(-1, LANES),
            by_head[:, :, DN + DR // 2 :].reshape(-1, LANES),
        ],
        axis=1,
    )

    small = jnp.concatenate(
        [
            norm1_gain.reshape(-1, LANES),
            norm2_gain.reshape(-1, LANES),
            kv_norm_gain.reshape(-1, LANES),
            jnp.zeros((7, LANES), BF),
        ]
    ).astype(F32)
    tables = [jnp.tile(v, (1, heads)) for v in rope_tables(2 * rows, jnp.float32(0))]
    (
        (
            mid, two_own, attn_flat, prob, kv_flat, keys_first, keys_second, q_nope, q_first, q_second,
            compressed, gains_all, w_query, w_latent_t, w_expand, w_output, router_t,
            cot_all, routes_all, one_cols, lat_cols, sg_t, su_t, sd,
        ),
    ) = comm_kernel(
        [
            attention_forward(
                block_input,
                tables,
                q_weight,
                kva_weight.T,
                kvb_weight,
                out_weight,
                router_weight.T,
                small,
                cotangent.astype(BF),
                jnp.pad(routes.astype(BF), ((0, 0), (0, LANES - topk))),
                (shared_gate.T, shared_up.T, shared_down),
                n_tp,
            )
        ],
        n_tp,
        0,
        "attention",
    )
    (
        mid_grad, gain_two_sum, mid_pack, y_part, grad_gate, grad_up, grad_expert_down, shared_grads,
        two_cols, attn_all,
    ) = feed_forward(
        two_own,
        mid,
        cotangent,
        gains_all,
        cot_all,
        routes_all,
        expert_gate.transpose(0, 2, 1),
        expert_up.transpose(0, 2, 1),
        expert_down,
        sg_t,
        su_t,
        sd,
        router_t,
        attn_flat,
        topk,
        n_tp,
    )
    ((block_output, input_grad, gains, mid_cols, logit_all, *shared_cols, head_all, lat_all),) = comm_kernel(
        [
            attention_back(
                mid_pack,
                attn_flat,
                prob,
                kv_flat,
                [keys_first, keys_second],
                q_nope,
                [q_first, q_second],
                tables,
                compressed,
                gains_all,
                [block_input, mid_grad, mid],
                y_part,
                shared_grads,
                w_output,
                w_expand,
                w_query,
                w_latent_t,
                gain_two_sum,
                n_tp,
            )
        ],
        n_tp,
        2,
        "back",
    )
    off = (2 * expert_gate.shape[2] + sg_t.shape[0]) % LANES
    (
        grad_query, grad_latent, grad_expand, grad_out_w, grad_router,
        grad_gate, grad_up, grad_expert_down, grad_sgate, grad_sup, grad_sdown, block_output, input_grad,
    ) = weight_grads(
        *(v.reshape(8 * rows, -1) for v in (one_cols, head_all, lat_all, lat_cols, attn_all, mid_cols, logit_all, two_cols)),
        (grad_gate, grad_up, grad_expert_down, *shared_cols, block_output, input_grad),
        heads,
        KVR + DR,
        off,
        experts,
    )
    grad_sgate, grad_sup, grad_sdown = (
        v.reshape(-1, shard_w) for v in (grad_sgate, grad_sup, grad_sdown)
    )
    gains = gains.reshape(-1)
    grad_one = lax.dynamic_slice_in_dim(gains, s_id * shard_w, shard_w, 0)
    grad_two = lax.dynamic_slice_in_dim(gains, width + s_id * shard_w, shard_w, 0)
    grad_kv = lax.dynamic_slice_in_dim(gains, 2 * width + s_id * kv_w, kv_w, 0)
    return (
        block_output,
        input_grad,
        grad_one,
        grad_query,
        grad_latent.T,
        grad_kv,
        grad_expand,
        grad_out_w,
        grad_two,
        grad_router.T,
        grad_sgate.T,
        grad_sup.T,
        grad_sdown,
        grad_gate.transpose(0, 2, 1),
        grad_up.transpose(0, 2, 1),
        grad_expert_down,
    )


def send_rows(buffer):
    return lax.all_to_all(buffer, (SHARD, CTX), split_axis=0, concat_axis=0, tiled=True)


def return_rows(partial_value, slots):
    back_rows = lax.all_to_all(
        partial_value, (SHARD, CTX), split_axis=0, concat_axis=0, tiled=True
    )
    flat_back = back_rows.reshape(-1, back_rows.shape[-1])
    return flat_back[slots]


def per_device_general(
    block_input,
    norm1_gain,
    q_weight,
    kva_weight,
    kv_norm_gain,
    kvb_weight,
    out_weight,
    norm2_gain,
    router_weight,
    shared_gate,
    shared_up,
    shared_down,
    expert_gate,
    expert_up,
    expert_down,
    routes,
    cotangent,
):
    tok_rows = block_input.shape[0]
    head_count = q_weight.shape[1] // (DN + DR)
    score_scale = (DN + DR) ** (-0.5)
    (
        gain_one,
        w_query,
        w_latent,
        gain_kv,
        w_expand,
        w_output,
        gain_two,
        w_router,
        w_sgate,
        w_sup,
        w_sdown,
    ) = (
        lax.all_gather(norm1_gain, SHARD, axis=0, tiled=True),
        lax.all_gather(q_weight, SHARD, axis=0, tiled=True),
        lax.all_gather(kva_weight, SHARD, axis=0, tiled=True),
        lax.all_gather(kv_norm_gain, SHARD, axis=0, tiled=True),
        lax.all_gather(kvb_weight, SHARD, axis=0, tiled=True),
        lax.all_gather(out_weight, SHARD, axis=1, tiled=True),
        lax.all_gather(norm2_gain, SHARD, axis=0, tiled=True),
        lax.all_gather(router_weight, SHARD, axis=0, tiled=True),
        lax.all_gather(shared_gate, SHARD, axis=0, tiled=True),
        lax.all_gather(shared_up, SHARD, axis=0, tiled=True),
        lax.all_gather(shared_down, SHARD, axis=1, tiled=True),
    )
    block_index = lax.axis_index(CTX)
    cosine, sine_table = rope_tables(tok_rows, (block_index * tok_rows).astype(jnp.float32))
    x_float = block_input.astype(jnp.float32)
    normed_one = norm_rows(x_float, gain_one).astype(jnp.bfloat16)
    query = mdot(normed_one, w_query).reshape(tok_rows, head_count, DN + DR)
    query_rot = rotate(query[..., DN:], cosine[:, None, :], sine_table[:, None, :])
    query = jnp.concatenate([query[..., :DN], query_rot], axis=-1).astype(jnp.bfloat16)
    query_nope = query[..., :DN]
    query_rope = query[..., DN:]
    latent = mdot(normed_one, w_latent)
    compressed = latent[:, :KVR]
    latent_n = norm_rows(compressed, gain_kv).astype(jnp.bfloat16)
    rope_key = rotate(latent[:, KVR:], cosine, sine_table).astype(jnp.bfloat16)
    first_piece = mdot(latent_n, w_expand).astype(jnp.bfloat16)
    gathered, rope_all = (
        lax.all_gather(first_piece, CTX, axis=0, tiled=True),
        lax.all_gather(rope_key, CTX, axis=0, tiled=True),
    )
    query_pos = block_index * tok_rows + jnp.arange(tok_rows, dtype=jnp.int32)

    def scores_at(block_id):
        blk_start = block_id * tok_rows
        kv_block = lax.dynamic_slice_in_dim(gathered, blk_start, tok_rows, 0).reshape(
            tok_rows, head_count, DN + DV
        )
        rope_block = lax.dynamic_slice_in_dim(rope_all, blk_start, tok_rows, 0)
        score = jnp.einsum(
            "qhd,khd->hqk", query_nope, kv_block[..., :DN], preferred_element_type=jnp.float32
        )
        score = score + jnp.einsum(
            "qhd,kd->hqk", query_rope, rope_block, preferred_element_type=jnp.float32
        )
        score = score * score_scale
        key_pos = blk_start + jnp.arange(tok_rows, dtype=jnp.int32)
        score = jnp.where(key_pos[None, None, :] <= query_pos[None, :, None], score, NEG)
        return (score, kv_block, rope_block)

    def forward_block(block_id, carry):
        run_max, run_sum, weighted = carry
        score, kv_block, rope_block = scores_at(block_id)
        new_max = jnp.maximum(run_max, jnp.max(score, axis=-1))
        factor = jnp.exp(run_max - new_max)
        expo = jnp.exp(score - new_max[..., None])
        run_sum = factor * run_sum + jnp.sum(expo, axis=-1)
        weighted = factor[..., None] * weighted + jnp.einsum(
            "hqk,khd->hqd",
            expo.astype(jnp.bfloat16),
            kv_block[..., DN:],
            preferred_element_type=jnp.float32,
        )
        return (new_max, run_sum, weighted)

    start_state = (
        jnp.full((head_count, tok_rows), NEG, jnp.float32),
        jnp.zeros((head_count, tok_rows), jnp.float32),
        jnp.zeros((head_count, tok_rows, DV), jnp.float32),
    )
    run_max, run_sum, weighted = lax.fori_loop(0, block_index + 1, forward_block, start_state)
    lse = run_max + jnp.log(run_sum)
    attn_rows = (weighted / run_sum[..., None]).astype(jnp.bfloat16).transpose(1, 0, 2)
    attn_flat = attn_rows.reshape(tok_rows, head_count * DV)
    attn_full = lax.psum(mdot(attn_flat, w_output), TP)
    mid = x_float + attn_full
    normed_two = norm_rows(mid, gain_two).astype(jnp.bfloat16)
    probs = jax.nn.softmax(mdot(normed_two, w_router), axis=-1)
    experts = probs.shape[1]
    topk = routes.shape[1]
    picks = (routes[:, :, None] == jnp.arange(experts, dtype=jnp.int32)[None, None, :]).astype(
        jnp.float32
    )
    route_w = jnp.sum(picks * probs[:, None, :], axis=-1)
    shared_a = mdot(normed_two, w_sgate)
    shared_b = mdot(normed_two, w_sup)
    shared_h = (jax.nn.silu(shared_a) * shared_b).astype(jnp.bfloat16)
    shared_y = mdot(shared_h, w_sdown)
    capacity = 2 * tok_rows * topk // experts
    owners = lax.axis_size((SHARD, CTX))
    local_experts = expert_gate.shape[0]
    width = normed_two.shape[1]
    flat_routes = routes.reshape(-1)
    onehot = (flat_routes[:, None] == jnp.arange(experts, dtype=jnp.int32)[None, :]).astype(
        jnp.int32
    )
    rank = jnp.sum((jnp.cumsum(onehot, axis=0) - 1) * onehot, axis=1)
    slots = flat_routes * capacity + rank
    source_row = jnp.arange(tok_rows * topk, dtype=jnp.int32) // topk
    send_buffer = (
        jnp.zeros((experts * capacity, width), jnp.bfloat16).at[slots].set(normed_two[source_row])
    )
    received = send_rows(send_buffer.reshape(owners, local_experts * capacity, width)).reshape(
        owners, local_experts, capacity, width
    )
    gate_act = jnp.einsum(
        "gecd,edf->gecf", received, expert_gate, preferred_element_type=jnp.float32
    )
    up_act = jnp.einsum("gecd,edf->gecf", received, expert_up, preferred_element_type=jnp.float32)
    hidden = (jax.nn.silu(gate_act) * up_act).astype(jnp.bfloat16)
    expert_y = jnp.einsum("gecf,efd->gecd", hidden, expert_down, preferred_element_type=jnp.float32)
    routed_out = return_rows(
        expert_y.reshape(owners, local_experts * capacity, width), slots
    ).reshape(tok_rows, topk, width)
    routed_part = jnp.sum(route_w[:, :, None] * routed_out, axis=1) + shared_y
    weight_part = jnp.sum(routed_out * cotangent[:, None, :], axis=-1)
    moe_out, route_grad = lax.psum((routed_part, weight_part), TP)
    block_output = mid + moe_out
    cot_b = cotangent.astype(jnp.bfloat16)
    routed_grad = (
        (route_w[:, :, None] * cotangent[:, None, :])
        .astype(jnp.bfloat16)
        .reshape(tok_rows * topk, width)
    )
    grad_buffer = jnp.zeros((experts * capacity, width), jnp.bfloat16).at[slots].set(routed_grad)
    grad_recv = send_rows(grad_buffer.reshape(owners, local_experts * capacity, width)).reshape(
        owners, local_experts, capacity, width
    )
    hidden_grad = jnp.einsum(
        "gecd,efd->gecf", grad_recv, expert_down, preferred_element_type=jnp.float32
    )
    gate_grad = (hidden_grad * up_act * silu_slope(gate_act)).astype(jnp.bfloat16)
    up_grad = (hidden_grad * jax.nn.silu(gate_act)).astype(jnp.bfloat16)
    grad_expert_down = jnp.einsum(
        "gecf,gecd->efd", hidden, grad_recv, preferred_element_type=jnp.float32
    )
    grad_expert_gate = jnp.einsum(
        "gecd,gecf->edf", received, gate_grad, preferred_element_type=jnp.float32
    )
    grad_expert_up = jnp.einsum(
        "gecd,gecf->edf", received, up_grad, preferred_element_type=jnp.float32
    )
    row_grad = jnp.einsum(
        "gecf,edf->gecd", gate_grad, expert_gate, preferred_element_type=jnp.float32
    )
    row_grad = row_grad + jnp.einsum(
        "gecf,edf->gecd", up_grad, expert_up, preferred_element_type=jnp.float32
    )
    routed_back = return_rows(
        row_grad.reshape(owners, local_experts * capacity, width), slots
    ).reshape(tok_rows, topk, width)
    shared_grad = jnp.einsum("td,fd->tf", cot_b, w_sdown, preferred_element_type=jnp.float32)
    sgate_grad = (shared_grad * shared_b * silu_slope(shared_a)).astype(jnp.bfloat16)
    sup_grad = (shared_grad * jax.nn.silu(shared_a)).astype(jnp.bfloat16)
    grad_sdown = jnp.einsum("tf,td->fd", shared_h, cot_b, preferred_element_type=jnp.float32)
    grad_sgate = jnp.einsum("td,tf->df", normed_two, sgate_grad, preferred_element_type=jnp.float32)
    grad_sup = jnp.einsum("td,tf->df", normed_two, sup_grad, preferred_element_type=jnp.float32)
    two_part = jnp.sum(routed_back, axis=1)
    two_part = two_part + jnp.einsum(
        "tf,df->td", sgate_grad, w_sgate, preferred_element_type=jnp.float32
    )
    two_part = two_part + jnp.einsum(
        "tf,df->td", sup_grad, w_sup, preferred_element_type=jnp.float32
    )
    two_grad = lax.psum(two_part, TP)
    prob_grad = jnp.sum(picks * route_grad[:, :, None], axis=1)
    logit_grad = (probs * (prob_grad - jnp.sum(probs * prob_grad, axis=-1, keepdims=True))).astype(
        jnp.bfloat16
    )
    grad_router = jnp.einsum(
        "td,te->de", normed_two, logit_grad, preferred_element_type=jnp.float32
    )
    two_grad = two_grad + jnp.einsum(
        "te,de->td", logit_grad, w_router, preferred_element_type=jnp.float32
    )
    _, norm_two_back = jax.vjp(norm_rows, mid, gain_two.astype(jnp.float32))
    mid_norm_grad, grad_gain_two = norm_two_back(two_grad)
    mid_grad = cotangent + mid_norm_grad
    mid_b = mid_grad.astype(jnp.bfloat16)
    grad_out_w = jnp.einsum("tj,td->jd", attn_flat, mid_b, preferred_element_type=jnp.float32)
    out_grad = jnp.einsum("td,jd->tj", mid_b, w_output, preferred_element_type=jnp.float32).reshape(
        tok_rows, head_count, DV
    )
    out_grad_b = out_grad.astype(jnp.bfloat16)
    delta = jnp.sum(out_grad * attn_rows.astype(jnp.float32), axis=-1).T
    key_count = gathered.shape[0]
    term_width = head_count * (DN + DV + DR)

    def back_block(block_id, carry):
        nope_grad, rope_qgrad, terms = carry
        score, kv_block, rope_block = scores_at(block_id)
        probs_blk = jnp.exp(score - lse[..., None])
        prob_b = probs_blk.astype(jnp.bfloat16)
        dprob = jnp.einsum(
            "qhd,khd->hqk", out_grad_b, kv_block[..., DN:], preferred_element_type=jnp.float32
        )
        dscore = (probs_blk * (dprob - delta[..., None])).astype(jnp.bfloat16)
        nope_grad = (
            nope_grad
            + jnp.einsum(
                "hqk,khd->qhd", dscore, kv_block[..., :DN], preferred_element_type=jnp.float32
            )
            * score_scale
        )
        rope_qgrad = (
            rope_qgrad
            + jnp.einsum("hqk,kd->qhd", dscore, rope_block, preferred_element_type=jnp.float32)
            * score_scale
        )
        key_nope_grad = (
            jnp.einsum("hqk,qhd->khd", dscore, query_nope, preferred_element_type=jnp.float32)
            * score_scale
        )
        key_rope_grad = (
            jnp.einsum("hqk,qhd->khd", dscore, query_rope, preferred_element_type=jnp.float32)
            * score_scale
        )
        value_grad = jnp.einsum(
            "hqk,qhd->khd", prob_b, out_grad_b, preferred_element_type=jnp.float32
        )
        block_terms = jnp.concatenate([key_nope_grad, value_grad, key_rope_grad], axis=-1).reshape(
            tok_rows, term_width
        )
        terms = lax.dynamic_update_slice_in_dim(terms, block_terms, block_id * tok_rows, 0)
        return (nope_grad, rope_qgrad, terms)

    back_init = (
        jnp.zeros((tok_rows, head_count, DN), jnp.float32),
        jnp.zeros((tok_rows, head_count, DR), jnp.float32),
        jnp.zeros((key_count, term_width), jnp.float32),
    )
    nope_grad, rope_qgrad, terms = lax.fori_loop(0, block_index + 1, back_block, back_init)
    key_terms = lax.psum_scatter(terms, CTX, scatter_dimension=0, tiled=True).reshape(
        tok_rows, head_count, DN + DV + DR
    )
    kv_grad = (
        key_terms[..., : DN + DV].reshape(tok_rows, head_count * (DN + DV)).astype(jnp.bfloat16)
    )
    rope_grad = rotate_back(jnp.sum(key_terms[..., DN + DV :], axis=1), cosine, sine_table)
    grad_expand = jnp.einsum("ti,tj->ij", latent_n, kv_grad, preferred_element_type=jnp.float32)
    latent_part = jnp.einsum("tj,ij->ti", kv_grad, w_expand, preferred_element_type=jnp.float32)
    rope_qback = rotate_back(rope_qgrad, cosine[:, None, :], sine_table[:, None, :])
    query_grad = (
        jnp.concatenate([nope_grad, rope_qback], axis=-1)
        .astype(jnp.bfloat16)
        .reshape(tok_rows, head_count * (DN + DR))
    )
    grad_query = jnp.einsum("td,tj->dj", normed_one, query_grad, preferred_element_type=jnp.float32)
    normed_part = jnp.einsum("tj,dj->td", query_grad, w_query, preferred_element_type=jnp.float32)
    latent_sum, normed_sum = lax.psum(
        (jnp.concatenate([latent_part, rope_grad], axis=-1), normed_part), TP
    )
    _, kv_back = jax.vjp(norm_rows, compressed, gain_kv.astype(jnp.float32))
    compressed_grad, grad_gain_kv = kv_back(latent_sum[:, :KVR])
    latent_grad = jnp.concatenate([compressed_grad, latent_sum[:, KVR:]], axis=-1).astype(
        jnp.bfloat16
    )
    grad_latent = jnp.einsum(
        "td,tl->dl", normed_one, latent_grad, preferred_element_type=jnp.float32
    )
    one_grad = normed_sum + jnp.einsum(
        "tl,dl->td", latent_grad, w_latent, preferred_element_type=jnp.float32
    )
    _, one_back = jax.vjp(norm_rows, x_float, gain_one.astype(jnp.float32))
    input_norm_grad, grad_gain_one = one_back(one_grad)
    input_grad = mid_grad + input_norm_grad
    (
        red_one,
        red_query,
        red_latent,
        red_kv,
        red_expand,
        red_output,
        red_two,
        red_router,
        red_sgate,
        red_sup,
        red_sdown,
    ) = (
        lax.psum_scatter(grad_gain_one, SHARD, scatter_dimension=0, tiled=True),
        lax.psum_scatter(grad_query, SHARD, scatter_dimension=0, tiled=True),
        lax.psum_scatter(grad_latent, SHARD, scatter_dimension=0, tiled=True),
        lax.psum_scatter(grad_gain_kv, SHARD, scatter_dimension=0, tiled=True),
        lax.psum_scatter(grad_expand, SHARD, scatter_dimension=0, tiled=True),
        lax.psum_scatter(grad_out_w, SHARD, scatter_dimension=1, tiled=True),
        lax.psum_scatter(grad_gain_two, SHARD, scatter_dimension=0, tiled=True),
        lax.psum_scatter(grad_router, SHARD, scatter_dimension=0, tiled=True),
        lax.psum_scatter(grad_sgate, SHARD, scatter_dimension=0, tiled=True),
        lax.psum_scatter(grad_sup, SHARD, scatter_dimension=0, tiled=True),
        lax.psum_scatter(grad_sdown, SHARD, scatter_dimension=1, tiled=True),
    )
    (
        sum_one,
        sum_query,
        sum_latent,
        sum_kv,
        sum_expand,
        sum_output,
        sum_two,
        sum_router,
        sum_sgate,
        sum_sup,
        sum_sdown,
    ) = lax.psum(
        (
            red_one,
            red_query,
            red_latent,
            red_kv,
            red_expand,
            red_output,
            red_two,
            red_router,
            red_sgate,
            red_sup,
            red_sdown,
        ),
        CTX,
    )
    return (
        block_output,
        input_grad,
        sum_one,
        sum_query,
        sum_latent,
        sum_kv,
        sum_expand,
        sum_output,
        sum_two,
        sum_router,
        sum_sgate,
        sum_sup,
        sum_sdown,
        grad_expert_gate,
        grad_expert_up,
        grad_expert_down,
    )


def solution(mesh):
    in_specs = (
        P((SHARD, CTX), None),
        P(SHARD),
        P(SHARD, TP),
        P(SHARD, None),
        P(SHARD),
        P(SHARD, TP),
        P(TP, SHARD),
        P(SHARD),
        P(SHARD, None),
        P(SHARD, TP),
        P(SHARD, TP),
        P(TP, SHARD),
        P((SHARD, CTX), None, TP),
        P((SHARD, CTX), None, TP),
        P((SHARD, CTX), TP, None),
        P((SHARD, CTX), None),
        P((SHARD, CTX), None),
    )
    out_specs = (
        P((SHARD, CTX), None),
        P((SHARD, CTX), None),
        P(SHARD),
        P(SHARD, TP),
        P(SHARD, None),
        P(SHARD),
        P(SHARD, TP),
        P(TP, SHARD),
        P(SHARD),
        P(SHARD, None),
        P(SHARD, TP),
        P(SHARD, TP),
        P(TP, SHARD),
        P((SHARD, CTX), None, TP),
        P((SHARD, CTX), None, TP),
        P((SHARD, CTX), TP, None),
    )
    routed = mesh.shape[SHARD] == 4 and mesh.shape[CTX] == 2 and mesh.shape[TP] == 4
    return jax.shard_map(
        per_device if routed else per_device_general, mesh=mesh, in_specs=in_specs, out_specs=out_specs, check_vma=False
    )
```
